32 devices in a mesh: fsdp: 32 (over z, y, x, core).
Axes of the slice: x: 2, y: 2, z: 4, core: 2. Of those that a mesh axis runs over, the one named last changes fastest.
Arguments:
- tokens: bfloat16 [2, 12288, 1024], P(None, 'fsdp'), may hold values from -6 to 6
- valid_slots: int32 [2, 12288], P(None, 'fsdp'), may hold values from 0 to 1, as said below
- cotangent: bfloat16 [2, 12288, 1024], P(None, 'fsdp'), may hold values from -6 to 6
- first_gain: bfloat16 [1024], P('fsdp'), may hold values from 0.5 to 1.5
- first_shift: bfloat16 [1024], P('fsdp'), may hold values from -3 to 3
- qkv_weight: bfloat16 [1024, 3072], P('fsdp'), may hold values from -0.1875 to 0.1875
- query_bias: bfloat16 [1024], P('fsdp'), may hold values from -3 to 3
- value_bias: bfloat16 [1024], P('fsdp'), may hold values from -3 to 3
- proj_weight: bfloat16 [1024, 1024], P('fsdp'), may hold values from -3 to 3
- proj_bias: bfloat16 [1024], P('fsdp'), may hold values from -3 to 3
- second_gain: bfloat16 [1024], P('fsdp'), may hold values from 0.5 to 1.5
- second_shift: bfloat16 [1024], P('fsdp'), may hold values from -3 to 3
- up_weight: bfloat16 [1024, 4096], P('fsdp'), may hold values from -0.1875 to 0.1875
- up_bias: bfloat16 [4096], P('fsdp'), may hold values from -3 to 3
- down_weight: bfloat16 [4096, 1024], P('fsdp'), may hold values from -0.09375 to 0.09375
- down_bias: bfloat16 [1024], P('fsdp'), may hold values from -3 to 3
Outputs:
- block_output: bfloat16 [2, 12288, 1024], P(None, 'fsdp')
- tokens_grad: float32 [2, 12288, 1024], P(None, 'fsdp')
- first_gain_grad: float32 [1024], P('fsdp')
- first_shift_grad: float32 [1024], P('fsdp')
- qkv_weight_grad: float32 [1024, 3072], P('fsdp')
- query_bias_grad: float32 [1024], P('fsdp')
- value_bias_grad: float32 [1024], P('fsdp')
- proj_weight_grad: float32 [1024, 1024], P('fsdp')
- proj_bias_grad: float32 [1024], P('fsdp')
- second_gain_grad: float32 [1024], P('fsdp')
- second_shift_grad: float32 [1024], P('fsdp')
- up_weight_grad: float32 [1024, 4096], P('fsdp')
- up_bias_grad: float32 [4096], P('fsdp')
- down_weight_grad: float32 [4096, 1024], P('fsdp')
- down_bias_grad: float32 [1024], P('fsdp')
The draws below stay inside these ranges and needn't reach their ends.
Inputs may be any that keep to these rules, and one draw needn't show every extreme that they name: `valid_slots`: in each clip of 768 consecutive slots of a micro-batch, the slots with 1 are a prefix of 384 to 768 slots; the first clip of each micro-batch has 1 in all its slots.
All inputs are finite; a program needn't handle non-finite values.
Results may differ from the reference program's by a relative error of at most 0.0098.
Values may be sent and summed in bfloat16 or wider, within the bound.
A program may use at most 256 MiB of HBM per device.

```python
import jax
import jax.numpy as jnp
from jax import lax

D = 1024
HEADS = 16
HEAD = 64
FF = 4096
MICRO = 2
CLIP_SLOTS = 768
CLIPS = 16
TOKENS = 12288


def draw_valid_slots(key, part):
    lengths = jax.random.randint(key, (MICRO, CLIPS), CLIP_SLOTS // 2, CLIP_SLOTS + 1)
    lengths = lengths.at[:, 0].set(CLIP_SLOTS)
    offsets = jnp.arange(CLIP_SLOTS, dtype=jnp.int32)
    slot_mask = (offsets[None, None, :] < lengths[:, :, None]).astype(jnp.int32)
    return slot_mask.reshape(MICRO, TOKENS)


def block_levels(own_key, shape, pieces, smallest, largest):
    def one(dim, shards_of):
        steps = jax.random.uniform(jax.random.fold_in(jax.random.fold_in(own_key, 6), dim), (shards_of,), jnp.float32, smallest / len(pieces), largest / len(pieces))
        return jnp.repeat(jnp.exp(steps), shape[dim] // shards_of).reshape((-1,) + (1,) * (len(shape) - dim - 1))

    loudness = one(*pieces[0])
    for cut in pieces[1:]:
        loudness = loudness * one(*cut)
    return loudness


def scatter_about(key, extent, scale, most, cuts=(), kind=jnp.bfloat16):
    values = jax.random.normal(key, extent, jnp.float32) * scale
    if len(cuts) > 0:
        values = block_levels(key, extent, cuts, -0.22, 0.18) * values
    return jnp.clip(values, min=-most, max=most).astype(kind)


def setup_inputs(seed: int = 0) -> dict:
    splits = jax.random.split(jax.random.key(seed), 17)
    return {
        "tokens": scatter_about(splits[0], (MICRO, TOKENS, D), 1.0, 6.0, ((1, 32),)),
        "valid_slots": draw_valid_slots(jax.random.fold_in(splits[16], 71), 0),
        "cotangent": scatter_about(splits[2], (MICRO, TOKENS, D), 1.0, 6.0, ((1, 32),)),
        "first_gain": jnp.clip(1.0 + 0.1 * jax.random.normal(splits[3], (D,), jnp.float32), 0.5, 1.5).astype(jnp.bfloat16),
        "first_shift": scatter_about(splits[4], (D,), 0.3, 3.0, ((0, 32),)),
        "qkv_weight": scatter_about(splits[5], (D, 3 * D), D ** -0.5, 0.1875, ((0, 32),)),
        "query_bias": scatter_about(splits[6], (D,), 0.3, 3.0, ((0, 32),)),
        "value_bias": scatter_about(splits[7], (D,), 0.3, 3.0, ((0, 32),)),
        "proj_weight": scatter_about(splits[8], (D, D), (D // 256) ** -0.5, 3.0, ((0, 32),)),
        "proj_bias": scatter_about(splits[9], (D,), 0.3, 3.0, ((0, 32),)),
        "second_gain": jnp.clip(1.0 + 0.1 * jax.random.normal(splits[10], (D,), jnp.float32), 0.5, 1.5).astype(jnp.bfloat16),
        "second_shift": scatter_about(splits[11], (D,), 0.3, 3.0, ((0, 32),)),
        "up_weight": scatter_about(splits[12], (D, FF), D ** -0.5, 0.1875, ((0, 32),)),
        "up_bias": scatter_about(splits[13], (FF,), 0.3, 3.0, ((0, 32),)),
        "down_weight": scatter_about(splits[14], (FF, D), FF ** -0.5, 0.09375, ((0, 32),)),
        "down_bias": scatter_about(splits[15], (D,), 0.3, 3.0, ((0, 32),)),
    }


@jax.custom_vjp
def low(v):
    return lax.optimization_barrier(v.astype(jnp.bfloat16)).astype(jnp.float32)

@jax.custom_vjp
def low_back(v):
    return v

def low_keep(v):
    return (low(v), None)

def low_pass(kept, grad):
    return (grad,)

def back_keep(v):
    return (v, None)

def back_low(kept, grad):
    return (low(grad),)
low.defvjp(low_keep, low_pass)
low_back.defvjp(back_keep, back_low)

def matmul(left_side, right_side):
    return jnp.dot(left_side, right_side, precision=lax.Precision.HIGHEST, preferred_element_type=jnp.float32)

def layer_norm(values, norm_gain, norm_shift):
    average = lax.optimization_barrier(jnp.mean(values, axis=-1, keepdims=True))
    centered = values - average
    variance = lax.optimization_barrier(jnp.mean(centered * centered, axis=-1, keepdims=True))
    return centered * lax.rsqrt(variance + 1e-06) * norm_gain + norm_shift

def attend_clip(operands):
    clip_queries, clip_keys, clip_values, clip_marks = operands
    slot_count = clip_queries.shape[0]
    query_heads = clip_queries.reshape(slot_count, HEADS, HEAD)
    key_heads = clip_keys.reshape(slot_count, HEADS, HEAD)
    value_heads = clip_values.reshape(slot_count, HEADS, HEAD)
    scores = jnp.einsum('qhd,khd->hqk', query_heads, key_heads, precision=lax.Precision.HIGHEST)
    penalty = jnp.where(clip_marks > 0, 0.0, -1000000000.0)
    scores = low_back(HEAD ** (-0.5) * scores) + penalty[None, None, :]
    probabilities = low(jax.nn.softmax(scores, axis=-1))
    attended = jnp.einsum('hqk,khd->qhd', probabilities, value_heads, precision=lax.Precision.HIGHEST)
    return attended.reshape(slot_count, D)

def forward(inputs, valid_slots, params):
    first_gain, first_shift, qkv_weight, query_bias, value_bias, proj_weight, proj_bias, second_gain, second_shift, up_weight, up_bias, down_weight, down_bias = params
    norm_one = low(layer_norm(inputs, first_gain, first_shift))
    qkv_bias = jnp.concatenate([query_bias, jnp.zeros_like(query_bias), value_bias])
    projected = low(low_back(matmul(norm_one, qkv_weight)) + qkv_bias)
    clip_total = MICRO * CLIPS
    queries = projected[..., :D].reshape(clip_total, CLIP_SLOTS, D)
    keys = projected[..., D:2 * D].reshape(clip_total, CLIP_SLOTS, D)
    values = projected[..., 2 * D:].reshape(clip_total, CLIP_SLOTS, D)
    marks = valid_slots.reshape(clip_total, CLIP_SLOTS)
    attended = lax.map(jax.checkpoint(attend_clip), (queries, keys, values, marks))
    attended = low(low_back(attended.reshape(MICRO, TOKENS, D)))
    middle = inputs + low_back(matmul(attended, proj_weight)) + proj_bias
    norm_two = low(layer_norm(middle, second_gain, second_shift))
    pre_act = low_back(matmul(norm_two, up_weight)) + up_bias
    activation = low(jax.nn.gelu(pre_act, approximate=False))
    return middle + matmul(activation, down_weight) + down_bias

def reference(tokens, valid_slots, cotangent, first_gain, first_shift, qkv_weight, query_bias, value_bias, proj_weight, proj_bias, second_gain, second_shift, up_weight, up_bias, down_weight, down_bias):
    params = (first_gain.astype(jnp.float32), first_shift.astype(jnp.float32), qkv_weight.astype(jnp.float32), query_bias.astype(jnp.float32), value_bias.astype(jnp.float32), proj_weight.astype(jnp.float32), proj_bias.astype(jnp.float32), second_gain.astype(jnp.float32), second_shift.astype(jnp.float32), up_weight.astype(jnp.float32), up_bias.astype(jnp.float32), down_weight.astype(jnp.float32), down_bias.astype(jnp.float32))

    def wrapped(inputs, weights):
        return forward(inputs, valid_slots, weights)
    block_output, pullback = jax.vjp(wrapped, tokens.astype(jnp.float32), params)
    seed_grad = cotangent.astype(jnp.float32) * valid_slots.astype(jnp.float32)[:, :, None]
    tokens_grad, weight_grads = pullback(seed_grad)
    return (block_output.astype(jnp.bfloat16), tokens_grad, weight_grads[0], weight_grads[1], weight_grads[2], weight_grads[3], weight_grads[4], weight_grads[5], weight_grads[6], weight_grads[7], weight_grads[8], weight_grads[9], weight_grads[10], weight_grads[11], weight_grads[12])
```

```python
import functools

import jax
import jax.numpy as jnp
from jax import lax
from jax.experimental import pallas as pl
from jax.experimental.pallas import tpu as pltpu
from jax.sharding import PartitionSpec as P

AX = "fsdp"
MESH = pl.DeviceIdType.MESH
HEAD = 64
EPSILON = 1e-06
ROOT_HALF = 0.7071067811865476
INV_ROOT_TWO_PI = 0.3989422804014327
BF = jnp.bfloat16
F32 = jnp.float32
PARAM_COLS = 128


def product(left_side, right_side):
    return jnp.dot(left_side, right_side, preferred_element_type=F32)


def product_left_t(left_side, right_side):
    return lax.dot_general(left_side, right_side, (((0,), (0,)), ((), ())), preferred_element_type=F32)


def product_right_t(left_side, right_side):
    return lax.dot_general(left_side, right_side, (((1,), (1,)), ((), ())), preferred_element_type=F32)


def swap(shard):
    return lax.ppermute(shard, AX, [(i, i ^ 1) for i in range(lax.axis_size(AX))])


def same_core_groups():
    count = lax.axis_size(AX)
    return [[i for i in range(count) if i % 2 == core] for core in (0, 1)]


def flip(index, step):
    return index + step - 2 * step * ((index // step) % 2)


def peers_of(me):
    return flip(me, 1), flip(me, 2), flip(me, 4), [flip(me, 8), flip(me, 16), flip(flip(me, 8), 16)]


def zflip(chip, j):
    return [chip, flip(chip, 4), flip(chip, 8), flip(flip(chip, 4), 8)][j]


def meet(peers):
    barrier = pltpu.get_barrier_semaphore()
    for peer in peers:
        pl.semaphore_signal(barrier, inc=1, device_id=(peer,), device_id_type=MESH)
    pl.semaphore_wait(barrier, len(peers))


def gather_kernel(count, *refs):
    ins, outs = refs[:count], refs[count : 2 * count]
    local_sem, send_sem, recv_sem = refs[2 * count :]
    me = lax.axis_index(AX)
    chip, core = me // 2, me % 2
    mate, peer_x, peer_y, peers_z = peers_of(me)
    meet([mate, peer_x, peer_y] + peers_z)
    chip_x, chip_y = flip(chip, 1), flip(chip, 2)
    chip_xy = flip(chip_x, 2)
    pending = []

    def send(w, slot, block, target, peer):
        copy = pltpu.make_async_remote_copy(
            src_ref=block, dst_ref=target, send_sem=send_sem.at[w, slot], recv_sem=recv_sem.at[w, slot],
            device_id=(peer,), device_id_type=MESH,
        )
        copy.start()
        pending.append(copy)

    def arrive(w, slot, block):
        pltpu.make_async_remote_copy(
            src_ref=block, dst_ref=block, send_sem=send_sem.at[w, slot], recv_sem=recv_sem.at[w, slot],
            device_id=(mate,), device_id_type=MESH,
        ).wait_recv()

    local = []
    for w in range(count):
        copy = pltpu.make_async_copy(ins[w].at[core], outs[w].at[chip, core], local_sem.at[w])
        copy.start()
        local.append(copy)
        send(w, 0, ins[w].at[1 - core], outs[w].at[chip, core], mate)
    for w in range(count):
        local[w].wait()
        arrive(w, 0, outs[w].at[chip, 1 - core])
        block = outs[w].at[chip]
        for j in range(3):
            send(w, 1 + j, block, block, peers_z[j])
        send(w, 4, block, block, peer_x)
        send(w, 8, block, block, peer_y)
    for w in range(count):
        for j in (1, 2, 3):
            block = outs[w].at[zflip(chip, j)]
            arrive(w, j, block)
            send(w, 4 + j, block, block, peer_x)
            send(w, 8 + j, block, block, peer_y)
        for j in range(4):
            block = outs[w].at[zflip(chip_x, j)]
            arrive(w, 4 + j, block)
            send(w, 12 + j, block.at[0], block.at[0], peer_y)
            block = outs[w].at[zflip(chip_y, j)]
            arrive(w, 8 + j, block)
            send(w, 16 + j, block.at[1], block.at[1], peer_x)
    for w in range(count):
        for j in range(4):
            block = outs[w].at[zflip(chip_xy, j)]
            arrive(w, 12 + j, block.at[0])
            arrive(w, 16 + j, block.at[1])
    for copy in pending:
        copy.wait_send()


def gather_chips(shards):
    devices = lax.axis_size(AX)
    if devices != 32:
        core = lax.axis_index(AX) % 2
        gathered = []
        for shard in shards:
            own = lax.dynamic_index_in_dim(shard, core, 0, keepdims=False)
            other = swap(lax.dynamic_index_in_dim(shard, 1 - core, 0, keepdims=False))
            block = jnp.where(core == 0, jnp.stack([own, other]), jnp.stack([other, own]))
            gathered.append(lax.all_gather(block, AX, axis=0, axis_index_groups=same_core_groups()))
        return gathered
    count = len(shards)
    return pl.pallas_call(
        functools.partial(gather_kernel, count),
        out_shape=[jax.ShapeDtypeStruct((devices // 2,) + s.shape, s.dtype) for s in shards],
        in_specs=[pl.BlockSpec(memory_space=pltpu.VMEM)] * count,
        out_specs=[pl.BlockSpec(memory_space=pl.ANY)] * count,
        scratch_shapes=[
            pltpu.SemaphoreType.DMA((count,)),
            pltpu.SemaphoreType.DMA((count, 20)),
            pltpu.SemaphoreType.DMA((count, 20)),
        ],
        compiler_params=pltpu.CompilerParams(collective_id=0, has_side_effects=True),
        name="gather_chips",
    )(*shards)


def scatter_kernel(count, *refs):
    ins, outs = refs[:count], refs[count : 2 * count]
    scratch = refs[2 * count :]
    recv_a, recv_b = scratch[:count], scratch[count : 2 * count]
    recv_x, recv_y = scratch[2 * count : 3 * count], scratch[3 * count : 4 * count]
    recv_z, stage = scratch[4 * count : 5 * count], scratch[5 * count : 6 * count]
    send_sem, recv_sem = scratch[6 * count :]
    me = lax.axis_index(AX)
    chip, core = me // 2, me % 2
    mate, peer_x, peer_y, peers_z = peers_of(me)
    meet([mate, peer_x, peer_y] + peers_z)
    chip_x, chip_y = flip(chip, 1), flip(chip, 2)
    chip_xy = flip(chip_x, 2)
    pending = []

    def send(w, slot, block, target, peer):
        copy = pltpu.make_async_remote_copy(
            src_ref=block, dst_ref=target, send_sem=send_sem.at[w, slot], recv_sem=recv_sem.at[w, slot],
            device_id=(peer,), device_id_type=MESH,
        )
        copy.start()
        pending.append(copy)

    def arrive(w, slot, block):
        pltpu.make_async_remote_copy(
            src_ref=block, dst_ref=block, send_sem=send_sem.at[w, slot], recv_sem=recv_sem.at[w, slot],
            device_id=(mate,), device_id_type=MESH,
        ).wait_recv()

    order = (1, 2, 3, 0)

    def first(w):
        for j in order:
            block = ins[w].at[zflip(chip_xy, j)]
            send(w, j, block.at[0], recv_a[w].at[j], peer_y)
            send(w, 4 + j, block.at[1], recv_b[w].at[j], peer_x)
        for j in order:
            send(w, 8 + j, ins[w].at[zflip(chip_x, j), 1], recv_x[w].at[j, 1], peer_x)
            send(w, 12 + j, ins[w].at[zflip(chip_y, j), 0], recv_y[w].at[j, 0], peer_y)

    def second(w):
        rows = ins[w].shape[2]
        for j in order:
            arrive(w, j, recv_a[w].at[j])

            @pl.loop(0, rows // 16)
            def _(i):
                part = pl.ds(pl.multiple_of(i * 16, 16), 16)
                total = recv_a[w][j, part].astype(F32) + ins[w][zflip(chip_x, j), 0, part].astype(F32)
                recv_a[w][j, part] = total.astype(BF)

            send(w, 16 + j, recv_a[w].at[j], recv_x[w].at[j, 0], peer_x)
            arrive(w, 4 + j, recv_b[w].at[j])

            @pl.loop(0, rows // 16)
            def _(i):
                part = pl.ds(pl.multiple_of(i * 16, 16), 16)
                total = recv_b[w][j, part].astype(F32) + ins[w][zflip(chip_y, j), 1, part].astype(F32)
                recv_b[w][j, part] = total.astype(BF)

            send(w, 20 + j, recv_b[w].at[j], recv_y[w].at[j, 1], peer_y)

    def third(w):
        rows = ins[w].shape[2]
        for j in (1, 2, 3):
            arrive(w, 8 + j, recv_x[w].at[j, 1])
            arrive(w, 12 + j, recv_y[w].at[j, 0])
            arrive(w, 16 + j, recv_x[w].at[j, 0])
            arrive(w, 20 + j, recv_y[w].at[j, 1])

            @pl.loop(0, 2 * (rows // 16))
            def _(i):
                half = i // (rows // 16)
                part = pl.ds(pl.multiple_of((i % (rows // 16)) * 16, 16), 16)
                total = recv_x[w][j, half, part].astype(F32) + recv_y[w][j, half, part].astype(F32)
                total = total + ins[w][zflip(chip, j), half, part].astype(F32)
                recv_x[w][j, half, part] = total.astype(BF)

            send(w, 23 + j, recv_x[w].at[j], recv_z[w].at[j - 1], peers_z[j - 1])

    def last(w):
        rows = ins[w].shape[2]
        for slot, block in ((8, recv_x[w].at[0, 1]), (12, recv_y[w].at[0, 0]), (16, recv_x[w].at[0, 0]), (20, recv_y[w].at[0, 1])):
            arrive(w, slot, block)
        for j in range(3):
            arrive(w, 24 + j, recv_z[w].at[j])

        def total_of(half, part):
            total = recv_x[w][0, half, part].astype(F32) + recv_y[w][0, half, part].astype(F32)
            total = total + ins[w][chip, half, part].astype(F32)
            for j in range(3):
                total = total + recv_z[w][j, half, part].astype(F32)
            return total

        @pl.loop(0, rows // 16)
        def _(i):
            part = pl.ds(pl.multiple_of(i * 16, 16), 16)
            stage[w][part] = total_of(1 - core, part)

        send(w, 27, stage[w], outs[w].at[core], mate)

        @pl.loop(0, rows // 16)
        def _(i):
            part = pl.ds(pl.multiple_of(i * 16, 16), 16)
            outs[w][core, part] = total_of(core, part)

    for w in range(count):
        first(w)
        if w >= 1:
            second(w - 1)
        if w >= 2:
            third(w - 2)
    second(count - 1)
    for w in range(max(count - 2, 0), count):
        third(w)
    for w in range(count):
        last(w)
    for w in range(count):
        arrive(w, 27, outs[w].at[1 - core])
    for copy in pending:
        copy.wait_send()


def scatter_chips(grads):
    devices = lax.axis_size(AX)
    if devices != 32:
        core = lax.axis_index(AX) % 2
        summed = []
        for grad in grads:
            block = lax.psum_scatter(grad, AX, scatter_dimension=0, axis_index_groups=same_core_groups())
            block = block.astype(F32)
            own = lax.dynamic_index_in_dim(block, core, 0, keepdims=False)
            other = swap(lax.dynamic_index_in_dim(block, 1 - core, 0, keepdims=False))
            summed.append(jnp.where(core == 0, jnp.stack([own, other]), jnp.stack([other, own])))
        return summed
    count = len(grads)
    shapes = [g.shape for g in grads]
    scratch = [pltpu.VMEM((4,) + s[2:], BF) for s in shapes] * 2
    scratch += [pltpu.VMEM((4, 2) + s[2:], BF) for s in shapes] * 2
    scratch += [pltpu.VMEM((3, 2) + s[2:], BF) for s in shapes]
    scratch += [pltpu.VMEM(s[2:], F32) for s in shapes]
    scratch += [pltpu.SemaphoreType.DMA((count, 28)), pltpu.SemaphoreType.DMA((count, 28))]
    return pl.pallas_call(
        functools.partial(scatter_kernel, count),
        out_shape=[jax.ShapeDtypeStruct((2,) + s[2:], F32) for s in shapes],
        in_specs=[pl.BlockSpec(memory_space=pltpu.VMEM)] * count,
        out_specs=[pl.BlockSpec(memory_space=pltpu.VMEM)] * count,
        scratch_shapes=scratch,
        compiler_params=pltpu.CompilerParams(
            collective_id=1, has_side_effects=True, vmem_limit_bytes=56 << 20
        ),
        name="scatter_chips",
    )(*grads)


def head_masks():
    lane = lax.broadcasted_iota(jnp.int32, (1, 2 * HEAD), 1)
    return [(lane < HEAD).astype(BF), (lane >= HEAD).astype(BF)]


def attend_kernel(chunk, q_ref, k_ref, v_ref, penalty_ref, out_ref, log_ref):
    slots = q_ref.shape[1]
    keys, values = k_ref[0], v_ref[0]
    values_t = values.T
    penalty = penalty_ref[0]
    masks = head_masks()
    for start in range(0, slots, chunk):
        queries = q_ref[0, start : start + chunk] * jnp.asarray(0.125, BF)
        parts = []
        for h in range(2):
            scores = product_right_t(keys, queries * masks[h]) + penalty
            top = jnp.max(scores, axis=0, keepdims=True)
            exponent = jnp.exp(scores - top)
            total = jnp.sum(exponent, axis=0, keepdims=True)
            mixed = product(values_t[h * HEAD : (h + 1) * HEAD], exponent.astype(BF))
            parts.append(mixed * (1.0 / total))
            log_ref[0, 0, h : h + 1, start : start + chunk] = top + jnp.log(total)
        out_ref[0, start : start + chunk] = jnp.concatenate(parts, 0).T.astype(BF)


def attend(projected, penalty):
    clips, slots, triple = projected.shape
    width = triple // 3
    pairs = width // (2 * HEAD)

    def block(offset):
        return pl.BlockSpec((1, slots, 2 * HEAD), lambda i, j: (i, 0, offset * pairs + j))

    return pl.pallas_call(
        functools.partial(attend_kernel, 256),
        grid=(clips, pairs),
        in_specs=[block(0), block(1), block(2), pl.BlockSpec((1, slots, 1), lambda i, j: (i, 0, 0))],
        out_specs=[block(0), pl.BlockSpec((1, 1, 2, slots), lambda i, j: (i, j, 0, 0))],
        out_shape=[
            jax.ShapeDtypeStruct((clips, slots, width), BF),
            jax.ShapeDtypeStruct((clips, pairs, 2, slots), F32),
        ],
        compiler_params=pltpu.CompilerParams(vmem_limit_bytes=48 << 20),
        cost_estimate=pl.CostEstimate(
            flops=4 * clips * pairs * slots * slots * 2 * HEAD, bytes_accessed=8 * clips * slots * width,
            transcendentals=clips * pairs * 2 * slots * slots,
        ),
        name="attend",
    )(projected, projected, projected, penalty)


def attend_back_kernel(chunk, q_ref, k_ref, v_ref, penalty_ref, log_ref, att_ref, grad_ref, out_ref, bias_ref):
    slots = q_ref.shape[1]
    pair = pl.program_id(1)
    width = out_ref.shape[2] // 3
    keys, values = k_ref[0], v_ref[0]
    keys_t = keys.T
    penalty = penalty_ref[0]
    masks = head_masks()
    grad_keys = jnp.zeros((slots, 2 * HEAD), F32)
    grad_values = jnp.zeros((slots, 2 * HEAD), F32)
    query_bias = jnp.zeros((1, 2 * HEAD), F32)
    for start in range(0, slots, chunk):
        queries = q_ref[0, start : start + chunk] * jnp.asarray(0.125, BF)
        grads = grad_ref[0, start : start + chunk]
        overlap = (grads.astype(F32) * att_ref[0, start : start + chunk].astype(F32)).T
        parts = []
        for h in range(2):
            head_queries = queries * masks[h]
            head_grads = grads * masks[h]
            correction = jnp.sum(overlap[h * HEAD : (h + 1) * HEAD], axis=0, keepdims=True)
            logs = log_ref[0, 0, h : h + 1, start : start + chunk]
            soft = jnp.exp(product_right_t(keys, head_queries) + penalty - logs)
            grad_soft = product_right_t(values, head_grads)
            grad_values += product(soft.astype(BF), head_grads)
            grad_scores = (soft * (grad_soft - correction)).astype(BF)
            grad_keys += product(grad_scores, head_queries)
            parts.append(product(keys_t[h * HEAD : (h + 1) * HEAD], grad_scores))
        grad_queries = jnp.concatenate(parts, 0).T * 0.125
        query_bias += jnp.sum(grad_queries, axis=0, keepdims=True)
        out_ref[0, start : start + chunk, pl.ds(pl.multiple_of(pair * 2 * HEAD, 128), 2 * HEAD)] = grad_queries.astype(BF)
    out_ref[0, :, pl.ds(pl.multiple_of(width + pair * 2 * HEAD, 128), 2 * HEAD)] = grad_keys.astype(BF)
    out_ref[0, :, pl.ds(pl.multiple_of(2 * width + pair * 2 * HEAD, 128), 2 * HEAD)] = grad_values.astype(BF)
    bias_ref[0, 0, 0:1] = query_bias
    bias_ref[0, 0, 1:2] = jnp.sum(grad_values, axis=0, keepdims=True)


def attend_back(projected, penalty, logs, attended, grad_attended):
    clips, slots, triple = projected.shape
    width = triple // 3
    pairs = width // (2 * HEAD)

    def block(offset):
        return pl.BlockSpec((1, slots, 2 * HEAD), lambda i, j: (i, 0, offset * pairs + j))

    return pl.pallas_call(
        functools.partial(attend_back_kernel, 256),
        grid=(clips, pairs),
        in_specs=[
            block(0), block(1), block(2),
            pl.BlockSpec((1, slots, 1), lambda i, j: (i, 0, 0)),
            pl.BlockSpec((1, 1, 2, slots), lambda i, j: (i, j, 0, 0)),
            block(0), block(0),
        ],
        out_specs=[
            pl.BlockSpec((1, slots, triple), lambda i, j: (i, 0, 0)),
            pl.BlockSpec((1, 1, 2, 2 * HEAD), lambda i, j: (i, j, 0, 0)),
        ],
        out_shape=[
            jax.ShapeDtypeStruct((clips, slots, triple), BF),
            jax.ShapeDtypeStruct((clips, pairs, 2, 2 * HEAD), F32),
        ],
        compiler_params=pltpu.CompilerParams(vmem_limit_bytes=56 << 20),
        cost_estimate=pl.CostEstimate(
            flops=10 * clips * pairs * slots * slots * 2 * HEAD, bytes_accessed=18 * clips * slots * width,
            transcendentals=clips * pairs * 2 * slots * slots,
        ),
        name="attend_back",
    )(projected, projected, projected, penalty, logs, attended, grad_attended)


def normalize(values, norm_gain, norm_shift):
    average = jnp.mean(values, axis=-1, keepdims=True)
    centered = values - average
    variance = jnp.mean(centered * centered, axis=-1, keepdims=True)
    inverse = lax.rsqrt(variance + EPSILON)
    scaled = centered * inverse
    return scaled * norm_gain + norm_shift, scaled, inverse


def normalize_back(grad_normed, scaled, inverse, norm_gain):
    grad_scaled = grad_normed * norm_gain
    first_mean = jnp.mean(grad_scaled, axis=-1, keepdims=True)
    second_mean = jnp.mean(grad_scaled * scaled, axis=-1, keepdims=True)
    return inverse * (grad_scaled - first_mean - scaled * second_mean)


def by_core(core, own, other, axis):
    return jnp.where(core == 0, jnp.concatenate([own, other], axis), jnp.concatenate([other, own], axis))


def per_device(
    tokens, valid_slots, cotangent, first_gain, first_shift, qkv_weight, query_bias, value_bias, proj_weight,
    proj_bias, second_gain, second_shift, up_weight, up_bias, down_weight, down_bias,
):
    devices = lax.axis_size(AX)
    chips = devices // 2
    core = lax.axis_index(AX) % 2
    micro, rows, features = tokens.shape
    shard = qkv_weight.shape[0]
    width = features // 2
    hidden = up_weight.shape[1] // 2
    unit = hidden // chips
    slots = 2 * rows
    every = micro * slots

    vectors = jnp.stack(
        [first_gain, first_shift, query_bias, value_bias, proj_bias, second_gain, second_shift, down_bias], 1
    )
    packed = jnp.concatenate([vectors, up_bias.reshape(shard, 4)], 1)
    packed = jnp.pad(packed, ((0, 0), (0, PARAM_COLS - packed.shape[1])))
    split = qkv_weight.reshape(shard, 3, 2, width).transpose(2, 0, 1, 3).reshape(2, shard, 3 * width)
    qkv_in = jnp.concatenate([split, jnp.broadcast_to(packed, (2,) + packed.shape)], 2)
    up_in = up_weight.reshape(shard, chips, 2, unit).transpose(2, 0, 1, 3).reshape(2, shard, hidden)
    proj_in = proj_weight.reshape(shard, 2, width).transpose(1, 0, 2)
    weight_down = lax.all_gather(down_weight, AX, axis=0, tiled=True, axis_index_groups=same_core_groups())
    qkv_all, proj_all, up_all = gather_chips([qkv_in, proj_in, up_in])
    qkv_all = qkv_all.reshape(features, 3 * width + PARAM_COLS)
    weight_qkv = qkv_all[:, : 3 * width]
    params = qkv_all[:, 3 * width : 3 * width + 12].astype(F32).T
    gain_one, shift_one, bias_query, bias_value, bias_proj, gain_two, shift_two, bias_down = params[:8]
    bias_up = params[8:].T.reshape(chips, 2, unit)
    bias_up = lax.dynamic_index_in_dim(bias_up, core, 1, keepdims=False).reshape(hidden)
    weight_up = up_all.reshape(features, hidden)
    proj_cols = proj_all.reshape(2, width, width)
    proj_own = lax.dynamic_index_in_dim(proj_cols, core, 0, keepdims=False)
    proj_other = swap(lax.dynamic_index_in_dim(proj_cols, 1 - core, 0, keepdims=False))
    weight_proj = by_core(core, proj_own, proj_other, 1)
    qkv_bias = jnp.concatenate(
        [
            lax.dynamic_slice_in_dim(bias_query, core * width, width),
            jnp.zeros((width,), F32),
            lax.dynamic_slice_in_dim(bias_value, core * width, width),
        ]
    )

    def both(own):
        return jnp.concatenate([own, swap(own)], 1)

    inputs_low = both(tokens)
    marks = both(valid_slots)
    grad_out = both(cotangent)
    inputs = tokens.astype(F32)
    norm_one, hat_one, inverse_one = normalize(inputs_low.astype(F32), gain_one, shift_one)
    norm_one = norm_one.astype(BF).reshape(every, features)
    projected = (product(norm_one, weight_qkv) + qkv_bias).astype(BF).reshape(micro, slots, 3 * width)
    penalty = jnp.where(marks > 0, 0.0, -1000000000.0).astype(F32)[:, :, None]
    attended, logs = attend(projected, penalty)
    attended_flat = attended.reshape(every, width)
    mixed = product(attended_flat, weight_proj).reshape(micro, slots, features)
    middle = inputs + mixed[:, :rows] + swap(mixed[:, rows:].astype(BF)).astype(F32) + bias_proj
    norm_two, hat_two, inverse_two = normalize(middle, gain_two, shift_two)
    norm_two = both(norm_two.astype(BF)).reshape(every, features)
    pre_act = product(norm_two, weight_up) + bias_up
    normal_cdf = 0.5 * (1.0 + jax.scipy.special.erf(pre_act * ROOT_HALF))
    density = jnp.exp(-0.5 * pre_act * pre_act) * INV_ROOT_TWO_PI
    activation = (pre_act * normal_cdf).astype(BF)
    slope = (normal_cdf + pre_act * density).astype(BF)
    lifted = product(activation, weight_down).reshape(micro, slots, features)
    block_output = (middle + lifted[:, :rows] + swap(lifted[:, rows:].astype(BF)).astype(F32) + bias_down).astype(BF)

    grad_out = (grad_out * (marks > 0).astype(BF)[:, :, None])
    grad_out_own = grad_out[:, :rows].astype(F32)
    grad_out = grad_out.reshape(every, features)
    grad_down = product_left_t(activation, grad_out).astype(BF)
    down_weight_grad = lax.psum_scatter(
        grad_down, AX, scatter_dimension=0, tiled=True, axis_index_groups=same_core_groups()
    ).astype(F32)
    grad_pre_full = product_right_t(grad_out, weight_down) * slope.astype(F32)
    grad_bias_up = jnp.sum(grad_pre_full, axis=0)
    grad_pre = grad_pre_full.astype(BF)
    grad_up = product_left_t(norm_two, grad_pre).astype(BF)
    grad_norm_two = product_right_t(grad_pre, weight_up).reshape(micro, slots, features)
    grad_norm_two = grad_norm_two[:, :rows] + swap(grad_norm_two[:, rows:].astype(BF)).astype(F32)
    grad_middle = grad_out_own + normalize_back(grad_norm_two, hat_two, inverse_two, gain_two)
    grad_middle_low = both(grad_middle.astype(BF)).reshape(every, features)
    grad_proj = product_left_t(attended_flat, grad_middle_low).astype(BF)
    grad_proj_own = lax.dynamic_slice_in_dim(grad_proj, core * width, width, 1)
    grad_proj_other = swap(lax.dynamic_slice_in_dim(grad_proj, (1 - core) * width, width, 1))
    grad_proj = by_core(core, grad_proj_own, grad_proj_other, 0)
    grad_attended = product_right_t(grad_middle_low, weight_proj).astype(BF).reshape(micro, slots, width)
    grad_projected, grad_bias = attend_back(projected, penalty, logs, attended, grad_attended)
    grad_projected = grad_projected.reshape(every, 3 * width)
    grad_bias = jnp.sum(grad_bias, axis=0)
    grad_qkv = product_left_t(norm_one, grad_projected).astype(BF)
    grad_norm_one = product_right_t(grad_projected, weight_qkv).reshape(micro, slots, features)
    grad_norm_one = grad_norm_one[:, :rows] + swap(grad_norm_one[:, rows:].astype(BF)).astype(F32)
    hat_own, inverse_own = hat_one[:, :rows], inverse_one[:, :rows]
    tokens_grad = grad_middle + normalize_back(grad_norm_one, hat_own, inverse_own, gain_one)

    def over_rows(value):
        return jnp.sum(value, axis=(0, 1))

    def whole(half):
        empty = jnp.zeros_like(half)
        return by_core(core, half, empty, 0)

    up_units = grad_bias_up.reshape(chips, 1, unit)
    up_units = by_core(core, up_units, jnp.zeros_like(up_units), 1).reshape(features, 4)
    sums = jnp.stack(
        [
            over_rows(grad_norm_one * hat_own),
            over_rows(grad_norm_one),
            whole(grad_bias[:, 0].reshape(width)),
            whole(grad_bias[:, 1].reshape(width)),
            over_rows(grad_middle),
            over_rows(grad_norm_two * hat_two),
            over_rows(grad_norm_two),
            over_rows(grad_out_own),
        ],
        1,
    )
    sums = jnp.concatenate([sums, up_units], 1)
    sums = jnp.pad(sums, ((0, 0), (0, PARAM_COLS - sums.shape[1]))).astype(BF)
    qkv_part = jnp.concatenate([grad_qkv, sums], 1).reshape(chips, 2, shard, 3 * width + PARAM_COLS)
    up_sum, qkv_sum, proj_sum = scatter_chips(
        [
            grad_up.reshape(chips, 2, shard, hidden),
            qkv_part,
            grad_proj.reshape(chips, 2, shard, width),
        ]
    )
    qkv_weight_grad = qkv_sum[:, :, : 3 * width].reshape(2, shard, 3, width).transpose(1, 2, 0, 3)
    qkv_weight_grad = qkv_weight_grad.reshape(shard, 6 * width)
    up_weight_grad = up_sum.reshape(2, shard, chips, unit).transpose(1, 2, 0, 3).reshape(shard, 2 * hidden)
    proj_weight_grad = jnp.concatenate([proj_sum[0], proj_sum[1]], 1)
    vector_sum = qkv_sum[0, :, 3 * width : 3 * width + 12] + qkv_sum[1, :, 3 * width : 3 * width + 12]
    up_bias_grad = vector_sum[:, 8:].reshape(4 * shard)
    vector_sum = vector_sum.T
    return (
        block_output, tokens_grad, vector_sum[0], vector_sum[1], qkv_weight_grad, vector_sum[2], vector_sum[3],
        proj_weight_grad, vector_sum[4], vector_sum[5], vector_sum[6], up_weight_grad, up_bias_grad,
        down_weight_grad, vector_sum[7],
    )


def solution(mesh):
    row = P(None, AX, None)
    vec = P(AX)
    mat = P(AX, None)
    return jax.shard_map(
        per_device,
        mesh=mesh,
        in_specs=(row, P(None, AX), row, vec, vec, mat, vec, vec, mat, vec, vec, vec, mat, vec, mat, vec),
        out_specs=(row, row, vec, vec, mat, vec, vec, mat, vec, vec, vec, mat, vec, mat, vec),
        check_vma=False,
    )
```

```python
import functools

import jax
import jax.numpy as jnp
from jax import lax
from jax.experimental import pallas as pl
from jax.experimental.pallas import tpu as pltpu
from jax.sharding import PartitionSpec as P

AX = "fsdp"
MESH = pl.DeviceIdType.MESH
HEAD = 64
EPSILON = 1e-06
ROOT_HALF = 0.7071067811865476
INV_ROOT_TWO_PI = 0.3989422804014327
BF = jnp.bfloat16
F32 = jnp.float32
PARAM_COLS = 128


def product(left_side, right_side):
    return jnp.dot(left_side, right_side, preferred_element_type=F32)


def product_left_t(left_side, right_side):
    return lax.dot_general(left_side, right_side, (((0,), (0,)), ((), ())), preferred_element_type=F32)


def product_right_t(left_side, right_side):
    return lax.dot_general(left_side, right_side, (((1,), (1,)), ((), ())), preferred_element_type=F32)


def swap(shard):
    return lax.ppermute(shard, AX, [(i, i ^ 1) for i in range(lax.axis_size(AX))])


def same_core_groups():
    count = lax.axis_size(AX)
    return [[i for i in range(count) if i % 2 == core] for core in (0, 1)]


def flip(index, step):
    return index + step - 2 * step * ((index // step) % 2)


def peers_of(me):
    return flip(me, 1), flip(me, 2), flip(me, 4), [flip(me, 8), flip(me, 16), flip(flip(me, 8), 16)]


def zflip(chip, j):
    return [chip, flip(chip, 4), flip(chip, 8), flip(flip(chip, 4), 8)][j]


def meet(peers):
    barrier = pltpu.get_barrier_semaphore()
    for peer in peers:
        pl.semaphore_signal(barrier, inc=1, device_id=(peer,), device_id_type=MESH)
    pl.semaphore_wait(barrier, len(peers))


def gather_kernel(qkv_ref, proj_ref, packed_ref, qkv_out, proj_out, packed_out, local_sem, send_sem, recv_sem):
    me = lax.axis_index(AX)
    chip, core = me // 2, me % 2
    mate, peer_x, peer_y, peers_z = peers_of(me)
    meet([mate, peer_x, peer_y] + peers_z)
    chip_x, chip_y = flip(chip, 1), flip(chip, 2)
    chip_xy = flip(chip_x, 2)
    outs = (qkv_out, packed_out, proj_out)
    count = len(outs)
    width = qkv_ref.shape[1] // 6
    pending = []

    def remote(w, slot, block, target, peer):
        return pltpu.make_async_remote_copy(
            src_ref=block, dst_ref=target, send_sem=send_sem.at[w, slot], recv_sem=recv_sem.at[w, slot],
            device_id=(peer,), device_id_type=MESH,
        )

    def send(w, slot, block, target, peer):
        copy = remote(w, slot, block, target, peer)
        copy.start()
        pending.append(copy)

    def arrive(w, slot, block):
        remote(w, slot, block, block, mate).wait_recv()

    def columns(start, size):
        return pl.ds(pl.multiple_of(start, 128), size)

    def pieces(w, half, target):
        if w == 0:
            return [
                (qkv_ref.at[:, columns((2 * t + half) * width, width)], target.at[:, pl.ds(t * width, width)])
                for t in range(3)
            ]
        if w == 1:
            return [(packed_ref, target)]
        return [(proj_ref.at[:, columns(half * width, width)], target)]

    for w in range(count):
        for source, target in pieces(w, 1 - core, outs[w].at[chip, core]):
            remote(w, 0, source, target, mate).start()
        for source, target in pieces(w, core, outs[w].at[chip, core]):
            pltpu.make_async_copy(source, target, local_sem.at[w]).start()
    for w in range(count):
        own = outs[w].at[chip, core]
        pltpu.make_async_copy(own, own, local_sem.at[w]).wait()
        arrive(w, 0, outs[w].at[chip, 1 - core])
        block = outs[w].at[chip]
        for j in range(3):
            send(w, 1 + j, block, block, peers_z[j])
        send(w, 4, block, block, peer_x)
        send(w, 8, block, block, peer_y)
    for w in range(count):
        for j in (1, 2, 3):
            block = outs[w].at[zflip(chip, j)]
            arrive(w, j, block)
            send(w, 4 + j, block, block, peer_x)
            send(w, 8 + j, block, block, peer_y)
        for j in range(4):
            block = outs[w].at[zflip(chip_x, j)]
            arrive(w, 4 + j, block)
            send(w, 12 + j, block.at[0], block.at[0], peer_y)
            block = outs[w].at[zflip(chip_y, j)]
            arrive(w, 8 + j, block)
            send(w, 16 + j, block.at[1], block.at[1], peer_x)
    for w in range(count):
        for j in range(4):
            block = outs[w].at[zflip(chip_xy, j)]
            arrive(w, 12 + j, block.at[0])
            arrive(w, 16 + j, block.at[1])
    for w in range(count):
        own = outs[w].at[chip, core]
        remote(w, 0, own, own, mate).wait_send()
    for copy in pending:
        copy.wait_send()


def gather_chips(qkv, proj, packed):
    devices = lax.axis_size(AX)
    shard, features = proj.shape
    width = features // 2
    if devices != 32:
        core = lax.axis_index(AX) % 2
        split = qkv.reshape(shard, 3, 2, width).transpose(2, 0, 1, 3).reshape(2, shard, 3 * width)
        gathered = []
        for halves in (split, proj.reshape(shard, 2, width).transpose(1, 0, 2), jnp.stack([packed, packed])):
            own = lax.dynamic_index_in_dim(halves, core, 0, keepdims=False)
            other = swap(lax.dynamic_index_in_dim(halves, 1 - core, 0, keepdims=False))
            block = jnp.where(core == 0, jnp.stack([own, other]), jnp.stack([other, own]))
            gathered.append(lax.all_gather(block, AX, axis=0, axis_index_groups=same_core_groups()))
        return gathered
    chips = devices // 2
    return pl.pallas_call(
        gather_kernel,
        out_shape=[
            jax.ShapeDtypeStruct((chips, 2, shard, 3 * width), BF),
            jax.ShapeDtypeStruct((chips, 2, shard, width), BF),
            jax.ShapeDtypeStruct((chips, 2) + packed.shape, BF),
        ],
        in_specs=[pl.BlockSpec(memory_space=pltpu.VMEM)] * 3,
        out_specs=[pl.BlockSpec(memory_space=pl.ANY)] * 3,
        scratch_shapes=[
            pltpu.SemaphoreType.DMA((3,)),
            pltpu.SemaphoreType.DMA((3, 20)),
            pltpu.SemaphoreType.DMA((3, 20)),
        ],
        compiler_params=pltpu.CompilerParams(collective_id=0, has_side_effects=True),
        cost_estimate=pl.CostEstimate(flops=int(4e10), bytes_accessed=int(1.5e8), transcendentals=0),
        name="gather_chips",
    )(qkv, proj, packed)


def scatter_kernel(kinds, *refs):
    count = len(kinds)
    ins, outs = refs[:count], refs[count : 2 * count]
    scratch = refs[2 * count :]
    recv_a, recv_b = scratch[:count], scratch[count : 2 * count]
    recv_x, recv_y = scratch[2 * count : 3 * count], scratch[3 * count : 4 * count]
    recv_z, stage = scratch[4 * count : 5 * count], scratch[5 * count : 6 * count]
    land = scratch[6 * count : 7 * count]
    send_sem, recv_sem = scratch[7 * count :]
    me = lax.axis_index(AX)
    chip, core = me // 2, me % 2
    mate, peer_x, peer_y, peers_z = peers_of(me)
    meet([mate, peer_x, peer_y] + peers_z)
    chip_x, chip_y = flip(chip, 1), flip(chip, 2)
    chip_xy = flip(chip_x, 2)
    pending = []

    def send(w, slot, block, target, peer):
        copy = pltpu.make_async_remote_copy(
            src_ref=block, dst_ref=target, send_sem=send_sem.at[w, slot], recv_sem=recv_sem.at[w, slot],
            device_id=(peer,), device_id_type=MESH,
        )
        copy.start()
        pending.append(copy)

    def arrive(w, slot, block):
        pltpu.make_async_remote_copy(
            src_ref=block, dst_ref=block, send_sem=send_sem.at[w, slot], recv_sem=recv_sem.at[w, slot],
            device_id=(mate,), device_id_type=MESH,
        ).wait_recv()

    order = (1, 2, 3, 0)

    def first(w):
        for j in order:
            block = ins[w].at[zflip(chip_xy, j)]
            send(w, j, block.at[0], recv_a[w].at[j], peer_y)
            send(w, 4 + j, block.at[1], recv_b[w].at[j], peer_x)
        for j in order:
            send(w, 8 + j, ins[w].at[zflip(chip_x, j), 1], recv_x[w].at[j, 1], peer_x)
            send(w, 12 + j, ins[w].at[zflip(chip_y, j), 0], recv_y[w].at[j, 0], peer_y)

    def second(w):
        rows = ins[w].shape[2]
        for j in order:
            arrive(w, j, recv_a[w].at[j])

            @pl.loop(0, rows // 16)
            def _(i):
                part = pl.ds(pl.multiple_of(i * 16, 16), 16)
                total = recv_a[w][j, part].astype(F32) + ins[w][zflip(chip_x, j), 0, part].astype(F32)
                recv_a[w][j, part] = total.astype(BF)

            send(w, 16 + j, recv_a[w].at[j], recv_x[w].at[j, 0], peer_x)
            arrive(w, 4 + j, recv_b[w].at[j])

            @pl.loop(0, rows // 16)
            def _(i):
                part = pl.ds(pl.multiple_of(i * 16, 16), 16)
                total = recv_b[w][j, part].astype(F32) + ins[w][zflip(chip_y, j), 1, part].astype(F32)
                recv_b[w][j, part] = total.astype(BF)

            send(w, 20 + j, recv_b[w].at[j], recv_y[w].at[j, 1], peer_y)

    def third(w):
        rows = ins[w].shape[2]
        for j in (1, 2, 3):
            arrive(w, 8 + j, recv_x[w].at[j, 1])
            arrive(w, 12 + j, recv_y[w].at[j, 0])
            arrive(w, 16 + j, recv_x[w].at[j, 0])
            arrive(w, 20 + j, recv_y[w].at[j, 1])

            @pl.loop(0, 2 * (rows // 16))
            def _(i):
                half = i // (rows // 16)
                part = pl.ds(pl.multiple_of((i % (rows // 16)) * 16, 16), 16)
                total = recv_x[w][j, half, part].astype(F32) + recv_y[w][j, half, part].astype(F32)
                total = total + ins[w][zflip(chip, j), half, part].astype(F32)
                recv_x[w][j, half, part] = total.astype(BF)

            send(w, 23 + j, recv_x[w].at[j], recv_z[w].at[j - 1], peers_z[j - 1])

    def last(w):
        rows = ins[w].shape[2]
        for slot, block in ((8, recv_x[w].at[0, 1]), (12, recv_y[w].at[0, 0]), (16, recv_x[w].at[0, 0]), (20, recv_y[w].at[0, 1])):
            arrive(w, slot, block)
        for j in range(3):
            arrive(w, 24 + j, recv_z[w].at[j])

        def total_of(half, part):
            total = recv_x[w][0, half, part].astype(F32) + recv_y[w][0, half, part].astype(F32)
            total = total + ins[w][chip, half, part].astype(F32)
            for j in range(3):
                total = total + recv_z[w][j, half, part].astype(F32)
            return total

        @pl.loop(0, rows // 16)
        def _(i):
            part = pl.ds(pl.multiple_of(i * 16, 16), 16)
            stage[w][part] = total_of(1 - core, part)

        send(w, 27, stage[w], land[w], mate)

        @pl.loop(0, rows // 16)
        def _(i):
            part = pl.ds(pl.multiple_of(i * 16, 16), 16)
            place(w, part, total_of(core, part), core)

    def place(w, part, total, half):
        if kinds[w] == "sum":
            outs[w][part] = total
            return
        size = total.shape[1] // kinds[w]
        for t in range(kinds[w]):
            start = pl.multiple_of((2 * t + half) * size, 128)
            outs[w][part, pl.ds(start, size)] = total[:, t * size : (t + 1) * size]

    for w in range(count):
        first(w)
        if w >= 1:
            second(w - 1)
        if w >= 2:
            third(w - 2)
    second(count - 1)
    for w in range(max(count - 2, 0), count):
        third(w)
    for w in range(count):
        last(w)
    for w in range(count):
        arrive(w, 27, land[w])

        @pl.loop(0, stage[w].shape[0] // 16)
        def _(i):
            part = pl.ds(pl.multiple_of(i * 16, 16), 16)
            other = land[w][part]
            if kinds[w] == "sum":
                other = other + outs[w][part]
            place(w, part, other, 1 - core)

    for copy in pending:
        copy.wait_send()


def scatter_chips(grads, kinds):
    devices = lax.axis_size(AX)
    shapes = [g.shape for g in grads]
    if devices != 32:
        core = lax.axis_index(AX) % 2
        summed = []
        for grad, kind in zip(grads, kinds):
            block = lax.psum_scatter(grad, AX, scatter_dimension=0, axis_index_groups=same_core_groups())
            block = block.astype(F32)
            own = lax.dynamic_index_in_dim(block, core, 0, keepdims=False)
            other = swap(lax.dynamic_index_in_dim(block, 1 - core, 0, keepdims=False))
            if kind == "sum":
                summed.append(own + other)
                continue
            rows, columns = own.shape
            own = own.reshape(rows, kind, 1, columns // kind)
            other = other.reshape(rows, kind, 1, columns // kind)
            summed.append(by_core(core, own, other, 2).reshape(rows, 2 * columns))
        return summed
    count = len(grads)
    scratch = [pltpu.VMEM((4,) + s[2:], BF) for s in shapes] * 2
    scratch += [pltpu.VMEM((4, 2) + s[2:], BF) for s in shapes] * 2
    scratch += [pltpu.VMEM((3, 2) + s[2:], BF) for s in shapes]
    scratch += [pltpu.VMEM(s[2:], F32) for s in shapes] * 2
    scratch += [pltpu.SemaphoreType.DMA((count, 28)), pltpu.SemaphoreType.DMA((count, 28))]
    return pl.pallas_call(
        functools.partial(scatter_kernel, kinds),
        out_shape=[
            jax.ShapeDtypeStruct((s[2], s[3] * (1 if kind == "sum" else 2)), F32) for s, kind in zip(shapes, kinds)
        ],
        in_specs=[pl.BlockSpec(memory_space=pltpu.VMEM)] * count,
        out_specs=[pl.BlockSpec(memory_space=pltpu.VMEM)] * count,
        scratch_shapes=scratch,
        compiler_params=pltpu.CompilerParams(
            collective_id=1, has_side_effects=True, vmem_limit_bytes=56 << 20
        ),
        name="scatter_chips",
    )(*grads)


def flat(ref):
    return ref[...].reshape(-1, ref.shape[-1])


def head_masks():
    lane = lax.broadcasted_iota(jnp.int32, (1, 2 * HEAD), 1)
    return [(lane < HEAD).astype(BF), (lane >= HEAD).astype(BF)]


def attend_kernel(chunk, q_ref, k_ref, v_ref, penalty_ref, out_ref, log_ref):
    slots = 2 * q_ref.shape[2]
    all_queries, keys, values = flat(q_ref), flat(k_ref), flat(v_ref)
    values_t = values.T
    penalty = flat(penalty_ref)
    masks = head_masks()
    mixed_all = []
    for start in range(0, slots, chunk):
        queries = all_queries[start : start + chunk] * jnp.asarray(0.125, BF)
        parts = []
        for h in range(2):
            scores = product_right_t(keys, queries * masks[h]) + penalty
            top = jnp.max(scores, axis=0, keepdims=True)
            exponent = jnp.exp(scores - top)
            total = jnp.sum(exponent, axis=0, keepdims=True)
            mixed = product(values_t[h * HEAD : (h + 1) * HEAD], exponent.astype(BF))
            parts.append(mixed * (1.0 / total))
            log_ref[0, 0, h : h + 1, start : start + chunk] = top + jnp.log(total)
        mixed_all.append(jnp.concatenate(parts, 0).T.astype(BF))
    out_ref[...] = jnp.concatenate(mixed_all, 0).reshape(out_ref.shape)


def attend(projected, penalty):
    _, clips, rows, triple = projected.shape
    slots = 2 * rows
    width = triple // 3
    pairs = width // (2 * HEAD)

    def block(offset):
        return pl.BlockSpec((2, 1, rows, 2 * HEAD), lambda i, j: (0, i, 0, offset * pairs + j))

    return pl.pallas_call(
        functools.partial(attend_kernel, 256),
        grid=(clips, pairs),
        in_specs=[block(0), block(1), block(2), pl.BlockSpec((2, 1, rows, 1), lambda i, j: (0, i, 0, 0))],
        out_specs=[block(0), pl.BlockSpec((1, 1, 2, slots), lambda i, j: (i, j, 0, 0))],
        out_shape=[
            jax.ShapeDtypeStruct((2, clips, rows, width), BF),
            jax.ShapeDtypeStruct((clips, pairs, 2, slots), F32),
        ],
        compiler_params=pltpu.CompilerParams(vmem_limit_bytes=48 << 20),
        cost_estimate=pl.CostEstimate(
            flops=4 * clips * pairs * slots * slots * 2 * HEAD, bytes_accessed=8 * clips * slots * width,
            transcendentals=clips * pairs * 2 * slots * slots,
        ),
        name="attend",
    )(projected, projected, projected, penalty)


def attend_back_kernel(chunk, q_ref, k_ref, v_ref, penalty_ref, log_ref, att_ref, grad_ref, out_ref, bias_ref):
    rows = q_ref.shape[2]
    slots = 2 * rows
    pair = pl.program_id(1)
    width = out_ref.shape[3] // 3
    all_queries, keys, values = flat(q_ref), flat(k_ref), flat(v_ref)
    all_grads, all_mixed = flat(grad_ref), flat(att_ref)
    keys_t = keys.T
    penalty = flat(penalty_ref)
    query_grads = []

    def keep(offset, value):
        columns = pl.ds(pl.multiple_of(offset + pair * 2 * HEAD, 128), 2 * HEAD)
        for side in range(2):
            out_ref[side, 0, :, columns] = value[side * rows : (side + 1) * rows]

    masks = head_masks()
    grad_keys = jnp.zeros((slots, 2 * HEAD), F32)
    grad_values = jnp.zeros((slots, 2 * HEAD), F32)
    query_bias = jnp.zeros((1, 2 * HEAD), F32)
    for start in range(0, slots, chunk):
        queries = all_queries[start : start + chunk] * jnp.asarray(0.125, BF)
        grads = all_grads[start : start + chunk]
        overlap = (grads.astype(F32) * all_mixed[start : start + chunk].astype(F32)).T
        parts = []
        for h in range(2):
            head_queries = queries * masks[h]
            head_grads = grads * masks[h]
            correction = jnp.sum(overlap[h * HEAD : (h + 1) * HEAD], axis=0, keepdims=True)
            logs = log_ref[0, 0, h : h + 1, start : start + chunk]
            soft = jnp.exp(product_right_t(keys, head_queries) + penalty - logs)
            grad_soft = product_right_t(values, head_grads)
            grad_values += product(soft.astype(BF), head_grads)
            grad_scores = (soft * (grad_soft - correction)).astype(BF)
            grad_keys += product(grad_scores, head_queries)
            parts.append(product(keys_t[h * HEAD : (h + 1) * HEAD], grad_scores))
        grad_queries = jnp.concatenate(parts, 0).T * 0.125
        query_bias += jnp.sum(grad_queries, axis=0, keepdims=True)
        query_grads.append(grad_queries.astype(BF))
    keep(0, jnp.concatenate(query_grads, 0))
    keep(width, grad_keys.astype(BF))
    keep(2 * width, grad_values.astype(BF))
    bias_ref[0, 0, 0:1] = query_bias
    bias_ref[0, 0, 1:2] = jnp.sum(grad_values, axis=0, keepdims=True)


def attend_back(projected, penalty, logs, attended, grad_attended):
    _, clips, rows, triple = projected.shape
    slots = 2 * rows
    width = triple // 3
    pairs = width // (2 * HEAD)

    def block(offset):
        return pl.BlockSpec((2, 1, rows, 2 * HEAD), lambda i, j: (0, i, 0, offset * pairs + j))

    return pl.pallas_call(
        functools.partial(attend_back_kernel, 256),
        grid=(clips, pairs),
        in_specs=[
            block(0), block(1), block(2),
            pl.BlockSpec((2, 1, rows, 1), lambda i, j: (0, i, 0, 0)),
            pl.BlockSpec((1, 1, 2, slots), lambda i, j: (i, j, 0, 0)),
            block(0), block(0),
        ],
        out_specs=[
            pl.BlockSpec((2, 1, rows, triple), lambda i, j: (0, i, 0, 0)),
            pl.BlockSpec((1, 1, 2, 2 * HEAD), lambda i, j: (i, j, 0, 0)),
        ],
        out_shape=[
            jax.ShapeDtypeStruct((2, clips, rows, triple), BF),
            jax.ShapeDtypeStruct((clips, pairs, 2, 2 * HEAD), F32),
        ],
        compiler_params=pltpu.CompilerParams(vmem_limit_bytes=56 << 20),
        cost_estimate=pl.CostEstimate(
            flops=10 * clips * pairs * slots * slots * 2 * HEAD, bytes_accessed=18 * clips * slots * width,
            transcendentals=clips * pairs * 2 * slots * slots,
        ),
        name="attend_back",
    )(projected, projected, projected, penalty, logs, attended, grad_attended)


def normal_parts(values):
    average = jnp.mean(values, axis=-1, keepdims=True)
    centered = values - average
    inverse = lax.rsqrt(jnp.mean(centered * centered, axis=-1, keepdims=True) + EPSILON)
    return centered * inverse, inverse


def normal_back(grad_normed, scaled, inverse, gain):
    grad_scaled = grad_normed * gain
    first_mean = jnp.mean(grad_scaled, axis=-1, keepdims=True)
    second_mean = jnp.mean(grad_scaled * scaled, axis=-1, keepdims=True)
    return inverse * (grad_scaled - first_mean - scaled * second_mean)


def rows_spec(size, columns):
    return pl.BlockSpec((size, columns), lambda i: (i, 0))


def whole_spec(shape):
    return pl.BlockSpec(shape, lambda i: (0,) * len(shape), pipeline_mode=pl.Buffered(1))


PARAMS = pltpu.CompilerParams(vmem_limit_bytes=56 << 20)


def first_norm_kernel(steps, own_ref, other_ref, gain_ref, shift_ref, out_ref):
    def put(ref):
        scaled, _ = normal_parts(ref[...].astype(F32))
        out_ref[...] = (scaled * gain_ref[...] + shift_ref[...]).astype(BF)

    pl.when(pl.program_id(0) < steps)(lambda: put(own_ref))
    pl.when(pl.program_id(0) >= steps)(lambda: put(other_ref))


def first_norm(own, other, gain, shift):
    rows, features = own.shape
    steps = 3
    size = rows // steps
    return pl.pallas_call(
        functools.partial(first_norm_kernel, steps),
        grid=(2 * steps,),
        in_specs=[
            pl.BlockSpec((size, features), lambda i: (jnp.minimum(i, steps - 1), 0)),
            pl.BlockSpec((size, features), lambda i: (jnp.maximum(i - steps, 0), 0)),
            whole_spec((1, features)),
            whole_spec((1, features)),
        ],
        out_specs=rows_spec(size, features),
        out_shape=jax.ShapeDtypeStruct((2 * rows, features), BF),
        compiler_params=PARAMS,
        name="first_norm",
    )(own, other, gain, shift)


def second_norm_kernel(att_ref, weight_ref, token_ref, recv_ref, bias_ref, gain_ref, shift_ref, middle_ref, out_ref):
    middle = token_ref[...].astype(F32) + product(att_ref[...], weight_ref[...])
    middle = middle + recv_ref[...].astype(F32) + bias_ref[...]
    middle_ref[...] = middle
    scaled, _ = normal_parts(middle)
    out_ref[...] = (scaled * gain_ref[...] + shift_ref[...]).astype(BF)


def second_norm(attended, weight, tokens, received, bias, gain, shift):
    rows, features = tokens.shape
    width = weight.shape[0]
    size = rows // 4
    return pl.pallas_call(
        second_norm_kernel,
        grid=(4,),
        in_specs=[
            rows_spec(size, width), whole_spec((width, features)), rows_spec(size, features), rows_spec(size, features),
            whole_spec((1, features)), whole_spec((1, features)), whole_spec((1, features)),
        ],
        out_specs=[rows_spec(size, features), rows_spec(size, features)],
        out_shape=[jax.ShapeDtypeStruct((rows, features), F32), jax.ShapeDtypeStruct((rows, features), BF)],
        compiler_params=PARAMS,
        name="second_norm",
    )(attended, weight, tokens, received, bias, gain, shift)


def lift_kernel(steps, unit, own_ref, other_ref, weight_ref, bias_ref, act_ref, slope_ref, norm_ref, half_ref):
    step = pl.program_id(0)
    hidden = half_ref.shape[1]

    @pl.when(step == 0)
    def _():
        if weight_ref.shape[1] == hidden:
            half_ref[...] = weight_ref[...]
        else:
            core = lax.axis_index(AX) % 2
            for k in range(hidden // unit):
                start = pl.multiple_of((2 * k + core) * unit, unit)
                half_ref[:, k * unit : (k + 1) * unit] = weight_ref[:, pl.ds(start, unit)]

    def put(ref):
        rows = ref[...]
        norm_ref[...] = rows
        size = 512
        for start in range(0, hidden, size):
            part = slice(start, start + size)
            pre = product(rows, half_ref[:, part]) + bias_ref[:, part]
            normal_cdf = 0.5 * (1.0 + lax.erf(pre * ROOT_HALF))
            density = jnp.exp(-0.5 * pre * pre) * INV_ROOT_TWO_PI
            act_ref[:, part] = (pre * normal_cdf).astype(BF)
            slope_ref[:, part] = (normal_cdf + pre * density).astype(BF)

    pl.when(step < steps)(lambda: put(own_ref))
    pl.when(step >= steps)(lambda: put(other_ref))


def lift(own, other, weight, bias, unit):
    rows, features = own.shape
    hidden = bias.shape[1]
    steps = 3
    size = rows // steps
    return pl.pallas_call(
        functools.partial(lift_kernel, steps, unit),
        grid=(2 * steps,),
        in_specs=[
            pl.BlockSpec((size, features), lambda i: (jnp.minimum(i, steps - 1), 0)),
            pl.BlockSpec((size, features), lambda i: (jnp.maximum(i - steps, 0), 0)),
            whole_spec(weight.shape),
            whole_spec((1, hidden)),
        ],
        out_specs=[
            rows_spec(size, hidden), rows_spec(size, hidden), rows_spec(size, features),
            pl.BlockSpec((features, hidden), lambda i: (0, 0)),
        ],
        out_shape=[
            jax.ShapeDtypeStruct((2 * rows, hidden), BF), jax.ShapeDtypeStruct((2 * rows, hidden), BF),
            jax.ShapeDtypeStruct((2 * rows, features), BF), jax.ShapeDtypeStruct((features, hidden), BF),
        ],
        compiler_params=PARAMS,
        cost_estimate=pl.CostEstimate(
            flops=4 * rows * features * hidden, bytes_accessed=4 * features * hidden, transcendentals=4 * rows * hidden
        ),
        name="lift",
    )(own, other, weight, bias)


def gather_sums(sums_ref, values):
    @pl.when(pl.program_id(0) == 0)
    def _():
        sums_ref[...] = jnp.zeros_like(sums_ref)

    for index, value in enumerate(values):
        sums_ref[index : index + 1] += jnp.sum(value, axis=0, keepdims=True)


def second_back_kernel(
    grad_ref, weight_ref, recv_ref, middle_ref, out_ref, gain_ref, full_ref, low_ref, sums_ref
):
    grad_normed = product_right_t(grad_ref[...], weight_ref[...]) + recv_ref[...].astype(F32)
    scaled, inverse = normal_parts(middle_ref[...])
    grad_out = out_ref[...].astype(F32)
    grad_middle = grad_out + normal_back(grad_normed, scaled, inverse, gain_ref[...])
    full_ref[...] = grad_middle
    low_ref[...] = grad_middle.astype(BF)
    gather_sums(sums_ref, [grad_normed * scaled, grad_normed, grad_middle, grad_out])


def second_back(grad_pre, weight, received, middle, grad_out, gain):
    rows, features = middle.shape
    hidden = weight.shape[1]
    size = rows // 4
    return pl.pallas_call(
        second_back_kernel,
        grid=(4,),
        in_specs=[
            rows_spec(size, hidden), whole_spec((features, hidden)), rows_spec(size, features),
            rows_spec(size, features), rows_spec(size, features), whole_spec((1, features)),
        ],
        out_specs=[rows_spec(size, features), rows_spec(size, features), pl.BlockSpec((8, features), lambda i: (0, 0))],
        out_shape=[
            jax.ShapeDtypeStruct((rows, features), F32), jax.ShapeDtypeStruct((rows, features), BF),
            jax.ShapeDtypeStruct((8, features), F32),
        ],
        compiler_params=PARAMS,
        name="second_back",
    )(grad_pre, weight, received, middle, grad_out, gain)


def first_back_kernel(grad_ref, weight_ref, recv_ref, token_ref, middle_ref, gain_ref, full_ref, sums_ref):
    grad_normed = product_right_t(grad_ref[...], weight_ref[...]) + recv_ref[...].astype(F32)
    scaled, inverse = normal_parts(token_ref[...].astype(F32))
    full_ref[...] = middle_ref[...] + normal_back(grad_normed, scaled, inverse, gain_ref[...])
    gather_sums(sums_ref, [grad_normed * scaled, grad_normed])


def first_back(grad_projected, weight, received, tokens, grad_middle, gain):
    rows, features = tokens.shape
    triple = weight.shape[1]
    size = rows // 4
    return pl.pallas_call(
        first_back_kernel,
        grid=(4,),
        in_specs=[
            rows_spec(size, triple), whole_spec((features, triple)), rows_spec(size, features),
            rows_spec(size, features), rows_spec(size, features), whole_spec((1, features)),
        ],
        out_specs=[rows_spec(size, features), pl.BlockSpec((8, features), lambda i: (0, 0))],
        out_shape=[jax.ShapeDtypeStruct((rows, features), F32), jax.ShapeDtypeStruct((8, features), F32)],
        compiler_params=PARAMS,
        name="first_back",
    )(grad_projected, weight, received, tokens, grad_middle, gain)


def by_core(core, own, other, axis):
    return jnp.where(core == 0, jnp.concatenate([own, other], axis), jnp.concatenate([other, own], axis))


def per_device(
    tokens, valid_slots, cotangent, first_gain, first_shift, qkv_weight, query_bias, value_bias, proj_weight,
    proj_bias, second_gain, second_shift, up_weight, up_bias, down_weight, down_bias,
):
    devices = lax.axis_size(AX)
    chips = devices // 2
    core = lax.axis_index(AX) % 2
    micro, rows, features = tokens.shape
    shard = qkv_weight.shape[0]
    width = features // 2
    hidden = up_weight.shape[1] // 2
    unit = hidden // chips
    own_rows = micro * rows
    every = 2 * own_rows

    weight_up = lax.all_gather(up_weight, AX, axis=0, tiled=True)
    weight_down = lax.all_gather(down_weight, AX, axis=0, tiled=True, axis_index_groups=same_core_groups())
    if unit % 128 != 0:
        weight_up = lax.dynamic_index_in_dim(weight_up.reshape(features, chips, 2, unit), core, 2, keepdims=False)
        weight_up = weight_up.reshape(features, hidden)
    vectors = jnp.stack(
        [first_gain, first_shift, query_bias, value_bias, proj_bias, second_gain, second_shift, down_bias], 0
    )
    lanes = max(PARAM_COLS, unit)
    vectors = jnp.pad(vectors.T, ((0, 16), (0, lanes - 8)))
    packed = lax.dynamic_update_slice(vectors, up_bias[None, :], (shard, 0))
    qkv_all, proj_all, packed_all = gather_chips(qkv_weight, proj_weight, packed)
    weight_qkv = qkv_all.reshape(features, 3 * width)
    params = packed_all[:, :, :shard, :8].astype(F32).reshape(features, 8).T
    gain_one, shift_one, bias_query, bias_value, bias_proj, gain_two, shift_two, bias_down = [
        params[i : i + 1] for i in range(8)
    ]
    bias_up = lax.dynamic_index_in_dim(packed_all[:, :, shard, :unit], core, 1, keepdims=False)
    bias_up = bias_up.astype(F32).reshape(1, hidden)
    proj_cols = proj_all.reshape(2, width, width)
    proj_own = lax.dynamic_index_in_dim(proj_cols, core, 0, keepdims=False)
    proj_other = swap(lax.dynamic_index_in_dim(proj_cols, 1 - core, 0, keepdims=False))
    weight_proj = by_core(core, proj_own, proj_other, 1)
    qkv_bias = jnp.concatenate(
        [
            lax.dynamic_slice_in_dim(bias_query, core * width, width, 1),
            jnp.zeros((1, width), F32),
            lax.dynamic_slice_in_dim(bias_value, core * width, width, 1),
        ],
        1,
    )

    own_tokens = tokens.reshape(own_rows, features)
    other_tokens = swap(own_tokens)
    marks = jnp.stack([valid_slots, swap(valid_slots)])
    own_cotangent = cotangent.reshape(own_rows, features)
    grad_out = jnp.concatenate([own_cotangent, swap(own_cotangent)], 0)
    grad_out = grad_out * (marks > 0).astype(BF).reshape(every, 1)
    penalty = jnp.where(marks > 0, 0.0, -1000000000.0).astype(F32)[..., None]
    norm_one = first_norm(own_tokens, other_tokens, gain_one, shift_one)
    projected = (product(norm_one, weight_qkv) + qkv_bias).astype(BF).reshape(2, micro, rows, 3 * width)
    attended, logs = attend(projected, penalty)
    attended_flat = attended.reshape(every, width)
    mixed = swap(product(attended_flat[own_rows:], weight_proj).astype(BF))
    middle, norm_own = second_norm(
        attended_flat, weight_proj, own_tokens, mixed, bias_proj, gain_two, shift_two
    )
    activation, slope, norm_two, weight_half = lift(norm_own, swap(norm_own), weight_up, bias_up, unit)
    lifted = swap(product(activation[own_rows:], weight_down).astype(BF))
    lifted = product(activation[:own_rows], weight_down) + lifted.astype(F32)
    block_output = (middle + lifted + bias_down).astype(BF).reshape(micro, rows, features)

    grad_pre_full = product_right_t(grad_out, weight_down) * slope.astype(F32)
    grad_bias_up = jnp.sum(grad_pre_full, axis=0)
    grad_pre = grad_pre_full.astype(BF)
    grad_down = product_left_t(activation, grad_out).astype(BF)
    down_weight_grad = lax.psum_scatter(
        grad_down, AX, scatter_dimension=0, tiled=True, axis_index_groups=same_core_groups()
    ).astype(F32)
    passed = swap(product_right_t(grad_pre[own_rows:], weight_half).astype(BF))
    grad_middle, grad_low, second_sums = second_back(
        grad_pre, weight_half, passed, middle, grad_out, gain_two
    )
    grad_up = product_left_t(norm_two, grad_pre).astype(BF)
    grad_low = jnp.concatenate([grad_low, swap(grad_low)], 0)
    grad_attended = product_right_t(grad_low, weight_proj).astype(BF).reshape(2, micro, rows, width)
    grad_proj = product_left_t(attended_flat, grad_low).astype(BF)
    grad_proj_own = lax.dynamic_slice_in_dim(grad_proj, core * width, width, 1)
    grad_proj_other = swap(lax.dynamic_slice_in_dim(grad_proj, (1 - core) * width, width, 1))
    grad_proj = by_core(core, grad_proj_own, grad_proj_other, 0)
    grad_projected, grad_bias = attend_back(projected, penalty, logs, attended, grad_attended)
    grad_projected = grad_projected.reshape(every, 3 * width)
    passed = swap(product_right_t(grad_projected[own_rows:], weight_qkv).astype(BF))
    grad_qkv = product_left_t(norm_one, grad_projected).astype(BF)
    tokens_grad, first_sums = first_back(
        grad_projected, weight_qkv, passed, own_tokens, grad_middle, gain_one
    )
    tokens_grad = tokens_grad.reshape(micro, rows, features)

    grad_bias = jnp.sum(grad_bias, axis=0).transpose(1, 0, 2).reshape(2, width)
    grad_bias = by_core(core, grad_bias, jnp.zeros_like(grad_bias), 1)
    sums = jnp.concatenate([first_sums[:2], grad_bias, second_sums[2:3], second_sums[:2], second_sums[3:4]], 0)
    sums = sums.astype(BF).T.reshape(chips, 2, shard, 8)
    sums = jnp.pad(sums, ((0, 0), (0, 0), (0, 16), (0, lanes - 8)))
    up_units = grad_bias_up.astype(BF).reshape(chips, 1, unit)
    up_units = by_core(core, up_units, jnp.zeros_like(up_units), 1)
    sums = lax.dynamic_update_slice(sums, up_units.reshape(chips, 2, 1, unit), (0, 0, shard, 0))
    up_weight_grad, qkv_weight_grad, proj_weight_grad, packed_sum = scatter_chips(
        [
            grad_up.reshape(chips, 2, shard, hidden),
            grad_qkv.reshape(chips, 2, shard, 3 * width),
            grad_proj.reshape(chips, 2, shard, width),
            sums,
        ],
        (chips, 3, 1, "sum"),
    )
    up_bias_grad = packed_sum[shard, :unit]
    vector_sum = packed_sum[:shard, :8].T
    return (
        block_output, tokens_grad, vector_sum[0], vector_sum[1], qkv_weight_grad, vector_sum[2], vector_sum[3],
        proj_weight_grad, vector_sum[4], vector_sum[5], vector_sum[6], up_weight_grad, up_bias_grad,
        down_weight_grad, vector_sum[7],
    )


def solution(mesh):
    row = P(None, AX, None)
    vec = P(AX)
    mat = P(AX, None)
    return jax.shard_map(
        per_device,
        mesh=mesh,
        in_specs=(row, P(None, AX), row, vec, vec, mat, vec, vec, mat, vec, vec, vec, mat, vec, mat, vec),
        out_specs=(row, row, vec, vec, mat, vec, vec, mat, vec, vec, vec, mat, vec, mat, vec),
        check_vma=False,
    )
```

```python
import functools

import jax
import jax.numpy as jnp
from jax import lax
from jax.experimental import pallas as pl
from jax.experimental.pallas import tpu as pltpu
from jax.sharding import PartitionSpec as P

AX = "fsdp"
MESH = pl.DeviceIdType.MESH
HEAD = 64
EPSILON = 1e-06
ROOT_HALF = 0.7071067811865476
INV_ROOT_TWO_PI = 0.3989422804014327
BF = jnp.bfloat16
F32 = jnp.float32
PARAM_COLS = 128


def product(left_side, right_side):
    return jnp.dot(left_side, right_side, preferred_element_type=F32)


def product_left_t(left_side, right_side):
    return lax.dot_general(left_side, right_side, (((0,), (0,)), ((), ())), preferred_element_type=F32)


def product_right_t(left_side, right_side):
    return lax.dot_general(left_side, right_side, (((1,), (1,)), ((), ())), preferred_element_type=F32)


def swap(shard):
    return lax.ppermute(shard, AX, [(i, i ^ 1) for i in range(lax.axis_size(AX))])


def same_core_groups():
    count = lax.axis_size(AX)
    return [[i for i in range(count) if i % 2 == core] for core in (0, 1)]


def flip(index, step):
    return index + step - 2 * step * ((index // step) % 2)


def peers_of(me):
    return flip(me, 1), flip(me, 2), flip(me, 4), [flip(me, 8), flip(me, 16), flip(flip(me, 8), 16)]


def zflip(chip, j):
    return [chip, flip(chip, 4), flip(chip, 8), flip(flip(chip, 4), 8)][j]


def meet(peers):
    barrier = pltpu.get_barrier_semaphore()
    for peer in peers:
        pl.semaphore_signal(barrier, inc=1, device_id=(peer,), device_id_type=MESH)
    pl.semaphore_wait(barrier, len(peers))


def gather_kernel(qkv_ref, proj_ref, packed_ref, qkv_out, proj_out, packed_out, local_sem, send_sem, recv_sem):
    me = lax.axis_index(AX)
    chip, core = me // 2, me % 2
    mate, peer_x, peer_y, peers_z = peers_of(me)
    meet([mate, peer_x, peer_y] + peers_z)
    chip_x, chip_y = flip(chip, 1), flip(chip, 2)
    chip_xy = flip(chip_x, 2)
    outs = (qkv_out, packed_out, proj_out)
    count = len(outs)
    width = qkv_ref.shape[1] // 6
    pending = []

    def remote(w, slot, block, target, peer):
        return pltpu.make_async_remote_copy(
            src_ref=block, dst_ref=target, send_sem=send_sem.at[w, slot], recv_sem=recv_sem.at[w, slot],
            device_id=(peer,), device_id_type=MESH,
        )

    def send(w, slot, block, target, peer):
        copy = remote(w, slot, block, target, peer)
        copy.start()
        pending.append(copy)

    def arrive(w, slot, block):
        remote(w, slot, block, block, mate).wait_recv()

    def columns(start, size):
        return pl.ds(pl.multiple_of(start, 128), size)

    def pieces(w, half, target):
        if w == 0:
            return [
                (qkv_ref.at[:, columns((2 * t + half) * width, width)], target.at[:, pl.ds(t * width, width)])
                for t in range(3)
            ]
        if w == 1:
            return [(packed_ref, target)]
        return [(proj_ref.at[:, columns(half * width, width)], target)]

    for w in range(count):
        for source, target in pieces(w, 1 - core, outs[w].at[chip, core]):
            remote(w, 0, source, target, mate).start()
        for source, target in pieces(w, core, outs[w].at[chip, core]):
            pltpu.make_async_copy(source, target, local_sem.at[w]).start()
    for w in range(count):
        own = outs[w].at[chip, core]
        pltpu.make_async_copy(own, own, local_sem.at[w]).wait()
        arrive(w, 0, outs[w].at[chip, 1 - core])
        block = outs[w].at[chip]
        for j in range(3):
            send(w, 1 + j, block, block, peers_z[j])
        send(w, 4, block, block, peer_x)
        send(w, 8, block, block, peer_y)
    for w in range(count):
        for j in (1, 2, 3):
            block = outs[w].at[zflip(chip, j)]
            arrive(w, j, block)
            send(w, 4 + j, block, block, peer_x)
            send(w, 8 + j, block, block, peer_y)
        for j in range(4):
            block = outs[w].at[zflip(chip_x, j)]
            arrive(w, 4 + j, block)
            send(w, 12 + j, block.at[0], block.at[0], peer_y)
            block = outs[w].at[zflip(chip_y, j)]
            arrive(w, 8 + j, block)
            send(w, 16 + j, block.at[1], block.at[1], peer_x)
    for w in range(count):
        for j in range(4):
            block = outs[w].at[zflip(chip_xy, j)]
            arrive(w, 12 + j, block.at[0])
            arrive(w, 16 + j, block.at[1])
    for w in range(count):
        own = outs[w].at[chip, core]
        remote(w, 0, own, own, mate).wait_send()
    for copy in pending:
        copy.wait_send()


def gather_chips(qkv, proj, packed):
    devices = lax.axis_size(AX)
    shard, features = proj.shape
    width = features // 2
    if devices != 32:
        core = lax.axis_index(AX) % 2
        split = qkv.reshape(shard, 3, 2, width).transpose(2, 0, 1, 3).reshape(2, shard, 3 * width)
        gathered = []
        for halves in (split, proj.reshape(shard, 2, width).transpose(1, 0, 2), jnp.stack([packed, packed])):
            own = lax.dynamic_index_in_dim(halves, core, 0, keepdims=False)
            other = swap(lax.dynamic_index_in_dim(halves, 1 - core, 0, keepdims=False))
            block = jnp.where(core == 0, jnp.stack([own, other]), jnp.stack([other, own]))
            gathered.append(lax.all_gather(block, AX, axis=0, axis_index_groups=same_core_groups()))
        return gathered
    chips = devices // 2
    return pl.pallas_call(
        gather_kernel,
        out_shape=[
            jax.ShapeDtypeStruct((chips, 2, shard, 3 * width), BF),
            jax.ShapeDtypeStruct((chips, 2, shard, width), BF),
            jax.ShapeDtypeStruct((chips, 2) + packed.shape, BF),
        ],
        in_specs=[pl.BlockSpec(memory_space=pltpu.VMEM)] * 3,
        out_specs=[pl.BlockSpec(memory_space=pl.ANY)] * 3,
        scratch_shapes=[
            pltpu.SemaphoreType.DMA((3,)),
            pltpu.SemaphoreType.DMA((3, 20)),
            pltpu.SemaphoreType.DMA((3, 20)),
        ],
        compiler_params=pltpu.CompilerParams(collective_id=0, has_side_effects=True),
        cost_estimate=pl.CostEstimate(flops=int(4e10), bytes_accessed=int(1.5e8), transcendentals=0),
        name="gather_chips",
    )(qkv, proj, packed)


class Scatter:
    def __init__(self, kinds, ins, outs, scratch):
        count = len(kinds)
        self.kinds, self.ins, self.outs = kinds, ins, outs
        names = ("recv_a", "recv_b", "recv_x", "recv_y", "recv_z", "stage", "land")
        for place, name in enumerate(names):
            setattr(self, name, scratch[place * count : (place + 1) * count])
        self.send_sem, self.recv_sem = scratch[len(names) * count :]
        me = lax.axis_index(AX)
        self.chip, self.core = me // 2, me % 2
        self.mate, self.peer_x, self.peer_y, self.peers_z = peers_of(me)
        chip_x, chip_y = flip(self.chip, 1), flip(self.chip, 2)
        self.own = [zflip(self.chip, j) for j in range(4)]
        self.at_x = [zflip(chip_x, j) for j in range(4)]
        self.at_y = [zflip(chip_y, j) for j in range(4)]
        self.at_xy = [zflip(flip(chip_x, 2), j) for j in range(4)]
        self.sent = []

    def meet(self):
        meet([self.mate, self.peer_x, self.peer_y] + self.peers_z)

    def remote(self, w, slot, block, target, peer):
        return pltpu.make_async_remote_copy(
            src_ref=block, dst_ref=target, send_sem=self.send_sem.at[w, slot], recv_sem=self.recv_sem.at[w, slot],
            device_id=(peer,), device_id_type=MESH,
        )

    def send(self, w, slot, block, target, peer):
        self.remote(w, slot, block, target, peer).start()
        self.sent.append((w, slot))

    def arrive(self, w, slot, block):
        self.remote(w, slot, block, block, self.mate).wait_recv()

    def far(self, w, j):
        block = self.ins[w].at[self.at_xy[j]]
        self.send(w, j, block.at[0], self.recv_a[w].at[j], self.peer_y)
        self.send(w, 4 + j, block.at[1], self.recv_b[w].at[j], self.peer_x)

    def near(self, w, j):
        self.send(w, 8 + j, self.ins[w].at[self.at_x[j], 1], self.recv_x[w].at[j, 1], self.peer_x)
        self.send(w, 12 + j, self.ins[w].at[self.at_y[j], 0], self.recv_y[w].at[j, 0], self.peer_y)

    def strips(self, w, body):
        @pl.loop(0, self.ins[w].shape[2] // 16)
        def _(i):
            body(pl.ds(pl.multiple_of(i * 16, 16), 16))

    def relay(self, w, j):
        for slot, recv, block, half in (
            (j, self.recv_a[w], self.at_x[j], 0),
            (4 + j, self.recv_b[w], self.at_y[j], 1),
        ):
            self.arrive(w, slot, recv.at[j])

            def body(part):
                total = recv[j, part].astype(F32) + self.ins[w][block, half, part].astype(F32)
                recv[j, part] = total.astype(BF)

            self.strips(w, body)
            if half == 0:
                self.send(w, 16 + j, recv.at[j], self.recv_x[w].at[j, 0], self.peer_x)
            else:
                self.send(w, 20 + j, recv.at[j], self.recv_y[w].at[j, 1], self.peer_y)

    def arrive_near(self, w, j):
        self.arrive(w, 8 + j, self.recv_x[w].at[j, 1])
        self.arrive(w, 12 + j, self.recv_y[w].at[j, 0])
        self.arrive(w, 16 + j, self.recv_x[w].at[j, 0])
        self.arrive(w, 20 + j, self.recv_y[w].at[j, 1])

    def near_sum(self, w, j, half, part):
        total = self.recv_x[w][j, half, part].astype(F32) + self.recv_y[w][j, half, part].astype(F32)
        return total + self.ins[w][self.own[j], half, part].astype(F32)

    def cross(self, w, j):
        self.arrive_near(w, j)

        def body(part):
            for half in range(2):
                self.recv_x[w][j, half, part] = self.near_sum(w, j, half, part).astype(BF)

        self.strips(w, body)
        self.send(w, 23 + j, self.recv_x[w].at[j], self.recv_z[w].at[j - 1], self.peers_z[j - 1])

    def place(self, w, part, total, half):
        kind = self.kinds[w]
        if kind == "sum":
            self.outs[w][part] = total
            return
        size = total.shape[1] // kind
        for t in range(kind):
            start = pl.multiple_of((2 * t + half) * size, 128)
            self.outs[w][part, pl.ds(start, size)] = total[:, t * size : (t + 1) * size]

    def last(self, w):
        self.arrive_near(w, 0)
        for j in range(3):
            self.arrive(w, 24 + j, self.recv_z[w].at[j])

        def total_of(half, part):
            total = self.near_sum(w, 0, half, part)
            for j in range(3):
                total = total + self.recv_z[w][j, half, part].astype(F32)
            return total

        def other(part):
            self.stage[w][part] = total_of(1 - self.core, part)

        self.strips(w, other)
        self.send(w, 27, self.stage[w], self.land[w], self.mate)
        self.strips(w, lambda part: self.place(w, part, total_of(self.core, part), self.core))

    def finish(self, w):
        self.arrive(w, 27, self.land[w])

        def body(part):
            other = self.land[w][part]
            if self.kinds[w] == "sum":
                other = other + self.outs[w][part]
            self.place(w, part, other, 1 - self.core)

        self.strips(w, body)

    def drain(self):
        for w, slot in self.sent:
            if slot == 27:
                block = self.stage[w]
            elif slot >= 24:
                block = self.recv_x[w].at[0]
            else:
                block = self.recv_a[w].at[0]
            self.remote(w, slot, block, block, self.mate).wait_send()

    def run(self):
        small = range(2, len(self.kinds))

        def opening(w):
            self.far(w, 1), self.far(w, 2), self.near(w, 1)

        self.meet()
        opening(0)
        for w in small:
            for j in (1, 2, 3, 0):
                self.far(w, j), self.near(w, j)
        self.relay(0, 1), self.far(0, 3), self.near(0, 2)
        self.relay(0, 2), self.far(0, 0), self.near(0, 3)
        for w in small:
            for j in (1, 2, 3, 0):
                self.relay(w, j)
        self.relay(0, 3), self.near(0, 0), self.cross(0, 1)
        opening(1)
        for w in small:
            for j in (1, 2, 3):
                self.cross(w, j)
        self.relay(0, 0), self.cross(0, 2), self.cross(0, 3)
        self.relay(1, 1), self.far(1, 3), self.near(1, 2)
        self.relay(1, 2), self.far(1, 0), self.near(1, 3)
        for w in small:
            self.last(w)
        self.relay(1, 3), self.near(1, 0), self.cross(1, 1)
        self.relay(1, 0)
        self.last(0)
        self.cross(1, 2), self.cross(1, 3)
        for w in small:
            self.finish(w)
        self.finish(0)
        self.last(1)
        self.finish(1)
        self.drain()


def scatter_scratch(shapes):
    count = len(shapes)
    scratch = [pltpu.VMEM((4,) + s[2:], BF) for s in shapes] * 2
    scratch += [pltpu.VMEM((4, 2) + s[2:], BF) for s in shapes] * 2
    scratch += [pltpu.VMEM((3, 2) + s[2:], BF) for s in shapes]
    scratch += [pltpu.VMEM(s[2:], F32) for s in shapes] * 2
    return scratch + [pltpu.SemaphoreType.DMA((count, 28)), pltpu.SemaphoreType.DMA((count, 28))]


def scatter_shapes(shapes, kinds):
    return [
        jax.ShapeDtypeStruct((s[2], s[3] * (1 if kind == "sum" else 2)), F32) for s, kind in zip(shapes, kinds)
    ]


def scatter_kernel(kinds, *refs):
    count = len(kinds)
    Scatter(kinds, refs[:count], refs[count : 2 * count], refs[2 * count :]).run()


def scatter_chips(grads, kinds):
    devices = lax.axis_size(AX)
    shapes = [g.shape for g in grads]
    if devices != 32:
        core = lax.axis_index(AX) % 2
        summed = []
        for grad, kind in zip(grads, kinds):
            block = lax.psum_scatter(grad, AX, scatter_dimension=0, axis_index_groups=same_core_groups())
            block = block.astype(F32)
            own = lax.dynamic_index_in_dim(block, core, 0, keepdims=False)
            other = swap(lax.dynamic_index_in_dim(block, 1 - core, 0, keepdims=False))
            if kind == "sum":
                summed.append(own + other)
                continue
            rows, columns = own.shape
            own = own.reshape(rows, kind, 1, columns // kind)
            other = other.reshape(rows, kind, 1, columns // kind)
            summed.append(by_core(core, own, other, 2).reshape(rows, 2 * columns))
        return summed
    count = len(grads)
    return pl.pallas_call(
        functools.partial(scatter_kernel, kinds),
        out_shape=scatter_shapes(shapes, kinds),
        in_specs=[pl.BlockSpec(memory_space=pltpu.VMEM)] * count,
        out_specs=[pl.BlockSpec(memory_space=pltpu.VMEM)] * count,
        scratch_shapes=scatter_scratch(shapes),
        compiler_params=pltpu.CompilerParams(
            collective_id=1, has_side_effects=True, vmem_limit_bytes=56 << 20
        ),
        name="scatter_chips",
    )(*grads)


def flat(ref):
    return ref[...].reshape(-1, ref.shape[-1])


def head_masks():
    lane = lax.broadcasted_iota(jnp.int32, (1, 2 * HEAD), 1)
    return [(lane < HEAD).astype(BF), (lane >= HEAD).astype(BF)]


def attend_kernel(chunk, q_ref, k_ref, v_ref, penalty_ref, out_ref, log_ref, query_buf, mixed_buf):
    query_buf[...] = flat(q_ref) * jnp.asarray(0.125, BF)
    keys, values = flat(k_ref), flat(v_ref)
    values_t = values.T
    penalty = flat(penalty_ref)
    masks = head_masks()

    @pl.loop(0, query_buf.shape[0] // chunk)
    def _(i):
        part = pl.ds(pl.multiple_of(i * chunk, chunk), chunk)
        queries = query_buf[part]
        parts = []
        for h in range(2):
            scores = product_right_t(keys, queries * masks[h]) + penalty
            top = jnp.max(scores, axis=0, keepdims=True)
            exponent = jnp.exp(scores - top)
            total = jnp.sum(exponent, axis=0, keepdims=True)
            mixed = product(values_t[h * HEAD : (h + 1) * HEAD], exponent.astype(BF))
            parts.append(mixed * (1.0 / total))
            log_ref[0, 0, h : h + 1, part] = top + jnp.log(total)
        mixed_buf[part] = jnp.concatenate(parts, 0).T.astype(BF)

    out_ref[...] = mixed_buf[...].reshape(out_ref.shape)


def attend(projected, penalty):
    _, clips, rows, triple = projected.shape
    slots = 2 * rows
    width = triple // 3
    pairs = width // (2 * HEAD)

    def block(offset):
        return pl.BlockSpec((2, 1, rows, 2 * HEAD), lambda i, j: (0, i, 0, offset * pairs + j))

    return pl.pallas_call(
        functools.partial(attend_kernel, 256),
        grid=(clips, pairs),
        in_specs=[block(0), block(1), block(2), pl.BlockSpec((2, 1, rows, 1), lambda i, j: (0, i, 0, 0))],
        out_specs=[block(0), pl.BlockSpec((1, 1, 2, slots), lambda i, j: (i, j, 0, 0))],
        out_shape=[
            jax.ShapeDtypeStruct((2, clips, rows, width), BF),
            jax.ShapeDtypeStruct((clips, pairs, 2, slots), F32),
        ],
        scratch_shapes=[pltpu.VMEM((slots, 2 * HEAD), BF)] * 2,
        compiler_params=pltpu.CompilerParams(vmem_limit_bytes=48 << 20),
        cost_estimate=pl.CostEstimate(
            flops=4 * clips * pairs * slots * slots * 2 * HEAD, bytes_accessed=8 * clips * slots * width,
            transcendentals=clips * pairs * 2 * slots * slots,
        ),
        name="attend",
    )(projected, projected, projected, penalty)


def attend_back_kernel(
    chunk, q_ref, k_ref, v_ref, penalty_ref, log_ref, att_ref, grad_ref, out_ref, bias_ref,
    query_buf, grad_buf, mixed_buf, back_buf, key_sum, value_sum, bias_sum,
):
    rows = q_ref.shape[2]
    pair = pl.program_id(1)
    width = out_ref.shape[3] // 3
    query_buf[...] = flat(q_ref) * jnp.asarray(0.125, BF)
    grad_buf[...] = flat(grad_ref)
    mixed_buf[...] = flat(att_ref)
    keys, values = flat(k_ref), flat(v_ref)
    keys_t = keys.T
    penalty = flat(penalty_ref)
    masks = head_masks()
    for total in (key_sum, value_sum, bias_sum):
        total[...] = jnp.zeros_like(total)

    def keep(offset, value):
        columns = pl.ds(pl.multiple_of(offset + pair * 2 * HEAD, 128), 2 * HEAD)
        for side in range(2):
            out_ref[side, 0, :, columns] = value[side * rows : (side + 1) * rows]

    for start in range(0, query_buf.shape[0], chunk):
        part = pl.ds(start, chunk)
        queries, grads = query_buf[part], grad_buf[part]
        overlap = (grads.astype(F32) * mixed_buf[part].astype(F32)).T
        parts = []
        for h in range(2):
            head_queries = queries * masks[h]
            head_grads = grads * masks[h]
            correction = jnp.sum(overlap[h * HEAD : (h + 1) * HEAD], axis=0, keepdims=True)
            logs = log_ref[0, 0, h : h + 1, part]
            soft = jnp.exp(product_right_t(keys, head_queries) + penalty - logs)
            grad_soft = product_right_t(values, head_grads)
            value_sum[...] += product(soft.astype(BF), head_grads)
            grad_scores = (soft * (grad_soft - correction)).astype(BF)
            key_sum[...] += product(grad_scores, head_queries)
            parts.append(product(keys_t[h * HEAD : (h + 1) * HEAD], grad_scores))
        grad_queries = jnp.concatenate(parts, 0).T * 0.125
        bias_sum[0:1] += jnp.sum(grad_queries, axis=0, keepdims=True)
        back_buf[part] = grad_queries.astype(BF)

    keep(0, back_buf[...])
    keep(width, key_sum[...].astype(BF))
    keep(2 * width, value_sum[...].astype(BF))
    bias_ref[0, 0, 0:1] = bias_sum[0:1]
    bias_ref[0, 0, 1:2] = jnp.sum(value_sum[...], axis=0, keepdims=True)


def attend_back(projected, penalty, logs, attended, grad_attended):
    _, clips, rows, triple = projected.shape
    slots = 2 * rows
    width = triple // 3
    pairs = width // (2 * HEAD)

    def block(offset):
        return pl.BlockSpec((2, 1, rows, 2 * HEAD), lambda i, j: (0, i, 0, offset * pairs + j))

    return pl.pallas_call(
        functools.partial(attend_back_kernel, 256),
        grid=(clips, pairs),
        in_specs=[
            block(0), block(1), block(2),
            pl.BlockSpec((2, 1, rows, 1), lambda i, j: (0, i, 0, 0)),
            pl.BlockSpec((1, 1, 2, slots), lambda i, j: (i, j, 0, 0)),
            block(0), block(0),
        ],
        out_specs=[
            pl.BlockSpec((2, 1, rows, triple), lambda i, j: (0, i, 0, 0)),
            pl.BlockSpec((1, 1, 2, 2 * HEAD), lambda i, j: (i, j, 0, 0)),
        ],
        out_shape=[
            jax.ShapeDtypeStruct((2, clips, rows, triple), BF),
            jax.ShapeDtypeStruct((clips, pairs, 2, 2 * HEAD), F32),
        ],
        scratch_shapes=[pltpu.VMEM((slots, 2 * HEAD), BF)] * 4
        + [pltpu.VMEM((slots, 2 * HEAD), F32)] * 2
        + [pltpu.VMEM((8, 2 * HEAD), F32)],
        compiler_params=pltpu.CompilerParams(vmem_limit_bytes=56 << 20),
        cost_estimate=pl.CostEstimate(
            flops=10 * clips * pairs * slots * slots * 2 * HEAD, bytes_accessed=18 * clips * slots * width,
            transcendentals=clips * pairs * 2 * slots * slots,
        ),
        name="attend_back",
    )(projected, projected, projected, penalty, logs, attended, grad_attended)


def normal_parts(values):
    average = jnp.mean(values, axis=-1, keepdims=True)
    centered = values - average
    inverse = lax.rsqrt(jnp.mean(centered * centered, axis=-1, keepdims=True) + EPSILON)
    return centered * inverse, inverse


def normal_back(grad_normed, scaled, inverse, gain):
    grad_scaled = grad_normed * gain
    first_mean = jnp.mean(grad_scaled, axis=-1, keepdims=True)
    second_mean = jnp.mean(grad_scaled * scaled, axis=-1, keepdims=True)
    return inverse * (grad_scaled - first_mean - scaled * second_mean)


def rows_spec(size, columns):
    return pl.BlockSpec((size, columns), lambda i: (i, 0))


def whole_spec(shape):
    return pl.BlockSpec(shape, lambda i: (0,) * len(shape), pipeline_mode=pl.Buffered(1))


PARAMS = pltpu.CompilerParams(vmem_limit_bytes=56 << 20)


def strips_of(ref):
    return [pl.ds(start, 32) for start in range(0, ref.shape[0], 32)]


def project_kernel(steps, own_ref, other_ref, gain_ref, shift_ref, weight_ref, bias_ref, norm_ref, out_ref):
    is_own = pl.program_id(0) < steps
    for part in strips_of(own_ref):
        rows = jnp.where(is_own, own_ref[part].astype(F32), other_ref[part].astype(F32))
        scaled, _ = normal_parts(rows)
        norm_ref[part] = (scaled * gain_ref[...] + shift_ref[...]).astype(BF)
    out_ref[...] = (product(norm_ref[...], weight_ref[...]) + bias_ref[...]).astype(BF)


def project(own, other, gain, shift, weight, bias):
    rows, features = own.shape
    columns = weight.shape[1]
    steps = 3
    size = rows // steps
    return pl.pallas_call(
        functools.partial(project_kernel, steps),
        grid=(2 * steps,),
        in_specs=[
            pl.BlockSpec((size, features), lambda i: (jnp.minimum(i, steps - 1), 0)),
            pl.BlockSpec((size, features), lambda i: (jnp.maximum(i - steps, 0), 0)),
            whole_spec((1, features)),
            whole_spec((1, features)),
            whole_spec((features, columns)),
            whole_spec((1, columns)),
        ],
        out_specs=[rows_spec(size, features), rows_spec(size, columns)],
        out_shape=[
            jax.ShapeDtypeStruct((2 * rows, features), BF),
            jax.ShapeDtypeStruct((2 * rows, columns), BF),
        ],
        compiler_params=PARAMS,
        name="project",
    )(own, other, gain, shift, weight, bias)


def second_norm_kernel(att_ref, weight_ref, token_ref, recv_ref, bias_ref, gain_ref, shift_ref, middle_ref, out_ref):
    mixed = product(att_ref[...], weight_ref[...])
    for part in strips_of(token_ref):
        middle = token_ref[part].astype(F32) + mixed[part.start : part.start + part.size]
        middle = middle + recv_ref[part].astype(F32) + bias_ref[...]
        middle_ref[part] = middle
        scaled, _ = normal_parts(middle)
        out_ref[part] = (scaled * gain_ref[...] + shift_ref[...]).astype(BF)


def second_norm(attended, weight, tokens, received, bias, gain, shift):
    rows, features = tokens.shape
    width = weight.shape[0]
    size = rows // 4
    return pl.pallas_call(
        second_norm_kernel,
        grid=(4,),
        in_specs=[
            rows_spec(size, width), whole_spec((width, features)), rows_spec(size, features), rows_spec(size, features),
            whole_spec((1, features)), whole_spec((1, features)), whole_spec((1, features)),
        ],
        out_specs=[rows_spec(size, features), rows_spec(size, features)],
        out_shape=[jax.ShapeDtypeStruct((rows, features), F32), jax.ShapeDtypeStruct((rows, features), BF)],
        compiler_params=PARAMS,
        name="second_norm",
    )(attended, weight, tokens, received, bias, gain, shift)


def feed_kernel(
    steps, unit, own_ref, other_ref, grad_own_ref, grad_other_ref, mark_ref, bias_ref, *refs
):
    if len(refs) == 14:
        both_ref, refs = refs[0], refs[1:]
        sources = None
    else:
        sources, refs = refs[:2], refs[2:]
    act_ref, pre_ref, norm_ref, grad_ref, lift_own_ref, lift_other_ref, pass_own_ref, pass_other_ref = refs[:8]
    sums_ref, up_ref, down_ref, up_sem, down_sem = refs[8:]
    step = pl.program_id(0)
    features, hidden = up_ref.shape

    @pl.when(step == 0)
    def _():
        sums_ref[...] = jnp.zeros_like(sums_ref)
        if sources is not None:
            pltpu.make_async_copy(sources[0], up_ref, up_sem).start()
            pltpu.make_async_copy(sources[1], down_ref, down_sem).start()
        else:
            core = lax.axis_index(AX) % 2
            chips = hidden // unit
            shard = features // (2 * chips)
            for k in range(chips):
                device = 2 * k + core
                pltpu.make_async_copy(
                    both_ref.at[:, pl.ds(pl.multiple_of(device * unit, 128), unit)],
                    up_ref.at[:, k * unit : (k + 1) * unit],
                    up_sem,
                ).start()
            for k in range(chips):
                device = 2 * k + core
                for q in range(unit // shard):
                    pltpu.make_async_copy(
                        both_ref.at[
                            pl.ds(pl.multiple_of(device * shard, 16), shard),
                            pl.ds(2 * hidden + q * features, features),
                        ],
                        down_ref.at[k * unit + q * shard : k * unit + (q + 1) * shard],
                        down_sem,
                    ).start()
        pltpu.make_async_copy(up_ref, up_ref, up_sem).wait()
        pltpu.make_async_copy(down_ref, down_ref, down_sem).wait()

    rows = jnp.where(step < steps, other_ref[...], own_ref[...])
    grads = jnp.where(step < steps, grad_other_ref[...], grad_own_ref[...]) * mark_ref[...].astype(BF)
    norm_ref[...] = rows
    grad_ref[...] = grads
    size = 512
    for start in range(0, hidden, size):
        part = slice(start, start + size)
        pre = product(rows, up_ref[:, part]) + bias_ref[:, part]
        normal_cdf = 0.5 * (1.0 + lax.erf(pre * ROOT_HALF))
        density = jnp.exp(-0.5 * pre * pre) * INV_ROOT_TWO_PI
        act_ref[:, part] = (pre * normal_cdf).astype(BF)
        grad_pre = product_right_t(grads, down_ref[part]) * (normal_cdf + pre * density)
        sums_ref[0:1, part] += jnp.sum(grad_pre, axis=0, keepdims=True)
        pre_ref[:, part] = grad_pre.astype(BF)
    lifted = product(act_ref[...], down_ref[...])
    passed = product_right_t(pre_ref[...], up_ref[...])
    lift_own_ref[...] = lifted
    pass_own_ref[...] = passed

    @pl.when(step < steps)
    def _():
        lift_other_ref[...] = lifted.astype(BF)
        pass_other_ref[...] = passed.astype(BF)


def feed(own, other, grad_own, grad_other, marks, weights, bias, unit):
    rows, features = own.shape
    hidden = bias.shape[1]
    steps = 3
    size = rows // steps

    def side(i):
        return jnp.where(i < steps, i + steps, i - steps)

    def both_spec(columns):
        return pl.BlockSpec((size, columns), lambda i: (side(i), 0))

    own_spec = pl.BlockSpec((size, features), lambda i: (jnp.maximum(i - steps, 0), 0))
    other_spec = pl.BlockSpec((size, features), lambda i: (jnp.minimum(i, steps - 1), 0))
    return pl.pallas_call(
        functools.partial(feed_kernel, steps, unit),
        grid=(2 * steps,),
        in_specs=[own_spec, other_spec, own_spec, other_spec, both_spec(1), whole_spec((1, hidden))]
        + [pl.BlockSpec(memory_space=pl.ANY)] * len(weights),
        out_specs=[
            both_spec(hidden), both_spec(hidden), both_spec(features), both_spec(features),
            own_spec, other_spec, own_spec, other_spec,
            pl.BlockSpec((8, hidden), lambda i: (0, 0)),
        ],
        out_shape=[
            jax.ShapeDtypeStruct((2 * rows, hidden), BF), jax.ShapeDtypeStruct((2 * rows, hidden), BF),
            jax.ShapeDtypeStruct((2 * rows, features), BF), jax.ShapeDtypeStruct((2 * rows, features), BF),
            jax.ShapeDtypeStruct((rows, features), F32), jax.ShapeDtypeStruct((rows, features), BF),
            jax.ShapeDtypeStruct((rows, features), F32), jax.ShapeDtypeStruct((rows, features), BF),
            jax.ShapeDtypeStruct((8, hidden), F32),
        ],
        scratch_shapes=[
            pltpu.VMEM((features, hidden), BF), pltpu.VMEM((hidden, features), BF),
            pltpu.SemaphoreType.DMA(()), pltpu.SemaphoreType.DMA(()),
        ],
        compiler_params=PARAMS,
        cost_estimate=pl.CostEstimate(
            flops=16 * rows * features * hidden, bytes_accessed=8 * features * hidden,
            transcendentals=4 * rows * hidden,
        ),
        name="feed",
    )(own, other, grad_own, grad_other, marks, bias, *weights)


def outer_kernel(left_ref, right_ref, out_ref):
    out_ref[...] = product_left_t(left_ref[...], right_ref[...]).astype(BF)


def outer(left, right):
    rows, columns = left.shape
    width = right.shape[1]
    size = 256
    return pl.pallas_call(
        outer_kernel,
        grid=(columns // size,),
        in_specs=[pl.BlockSpec((rows, size), lambda i: (0, i)), whole_spec((rows, width))],
        out_specs=rows_spec(size, width),
        out_shape=jax.ShapeDtypeStruct((columns, width), BF),
        compiler_params=PARAMS,
        cost_estimate=pl.CostEstimate(
            flops=2 * rows * columns * width, bytes_accessed=2 * (rows * columns + rows * width + columns * width),
            transcendentals=0,
        ),
        name="outer",
    )(left, right)


def gather_sums(sums_ref, values):
    for index, value in enumerate(values):
        sums_ref[index : index + 1] += jnp.sum(value, axis=0, keepdims=True)


def clear_first(sums_ref):
    @pl.when(pl.program_id(0) == 0)
    def _():
        sums_ref[...] = jnp.zeros_like(sums_ref)


def second_back_kernel(
    grad_ref, recv_ref, middle_ref, out_ref, lift_ref, lift_recv_ref, gain_ref, bias_ref,
    full_ref, low_ref, block_ref, sums_ref,
):
    clear_first(sums_ref)
    for part in strips_of(grad_ref):
        lifted = lift_ref[part] + lift_recv_ref[part].astype(F32)
        block_ref[part] = (middle_ref[part] + lifted + bias_ref[...]).astype(BF)
        grad_normed = grad_ref[part] + recv_ref[part].astype(F32)
        scaled, inverse = normal_parts(middle_ref[part])
        grad_out = out_ref[part].astype(F32)
        grad_middle = grad_out + normal_back(grad_normed, scaled, inverse, gain_ref[...])
        full_ref[part] = grad_middle
        low_ref[part] = grad_middle.astype(BF)
        gather_sums(sums_ref, [grad_normed * scaled, grad_normed, grad_middle, grad_out])


def second_back(passed, received, middle, grad_out, lifted, lift_received, gain, bias):
    rows, features = middle.shape
    size = rows // 4
    return pl.pallas_call(
        second_back_kernel,
        grid=(4,),
        in_specs=[rows_spec(size, features)] * 6 + [whole_spec((1, features))] * 2,
        out_specs=[rows_spec(size, features)] * 3 + [pl.BlockSpec((8, features), lambda i: (0, 0))],
        out_shape=[
            jax.ShapeDtypeStruct((rows, features), F32), jax.ShapeDtypeStruct((rows, features), BF),
            jax.ShapeDtypeStruct((rows, features), BF), jax.ShapeDtypeStruct((8, features), F32),
        ],
        compiler_params=PARAMS,
        name="second_back",
    )(passed, received, middle, grad_out, lifted, lift_received, gain, bias)


def first_back_kernel(grad_ref, weight_ref, recv_ref, token_ref, middle_ref, gain_ref, full_ref, sums_ref):
    clear_first(sums_ref)
    passed = product_right_t(grad_ref[...], weight_ref[...])
    for part in strips_of(grad_ref):
        grad_normed = passed[part.start : part.start + part.size] + recv_ref[part].astype(F32)
        scaled, inverse = normal_parts(token_ref[part].astype(F32))
        full_ref[part] = middle_ref[part] + normal_back(grad_normed, scaled, inverse, gain_ref[...])
        gather_sums(sums_ref, [grad_normed * scaled, grad_normed])


def first_back(grad_projected, weight, received, tokens, grad_middle, gain):
    rows, features = tokens.shape
    triple = weight.shape[1]
    size = rows // 4
    return pl.pallas_call(
        first_back_kernel,
        grid=(4,),
        in_specs=[
            rows_spec(size, triple), whole_spec((features, triple)), rows_spec(size, features),
            rows_spec(size, features), rows_spec(size, features), whole_spec((1, features)),
        ],
        out_specs=[rows_spec(size, features), pl.BlockSpec((8, features), lambda i: (0, 0))],
        out_shape=[jax.ShapeDtypeStruct((rows, features), F32), jax.ShapeDtypeStruct((8, features), F32)],
        compiler_params=PARAMS,
        name="first_back",
    )(grad_projected, weight, received, tokens, grad_middle, gain)


def pack_kernel(up_ref, down_ref, out_ref):
    shard, columns = up_ref.shape
    features = down_ref.shape[1]
    out_ref[:, :columns] = up_ref[...]
    for i in range(down_ref.shape[0] // shard):
        out_ref[:, columns + i * features : columns + (i + 1) * features] = down_ref[i * shard : (i + 1) * shard]


def pack(up, down):
    shard, columns = up.shape
    fold = down.shape[0] // shard
    if shard % 16 != 0:
        return jnp.concatenate([up] + [down[shard * i : shard * (i + 1)] for i in range(fold)], 1)
    return pl.pallas_call(
        pack_kernel,
        out_shape=jax.ShapeDtypeStruct((shard, columns + fold * down.shape[1]), BF),
        in_specs=[pl.BlockSpec(memory_space=pltpu.VMEM)] * 2,
        out_specs=pl.BlockSpec(memory_space=pltpu.VMEM),
        name="pack",
    )(up, down)


def finish_kernel(up_ref, qkv_ref, proj_ref, down_ref, packed_ref, up_out, qkv_out, proj_out, down_out, vec_out, bias_out):
    up_out[...] = up_ref[...]
    qkv_out[...] = qkv_ref[...]
    proj_out[...] = proj_ref[...]
    down_out[...] = down_ref[...].astype(F32)
    shard = vec_out.shape[1]
    vec_out[...] = packed_ref[:shard].T[:8]
    bias_out[...] = packed_ref[shard : shard + 1]


def finish(up, qkv, proj, down, packed, shard, unit):
    if lax.axis_size(AX) != 32:
        return up, qkv, proj, down.astype(F32), packed[:shard, :8].T, packed[shard : shard + 1, :unit]
    return pl.pallas_call(
        finish_kernel,
        out_shape=[jax.ShapeDtypeStruct(a.shape, F32) for a in (up, qkv, proj, down)]
        + [jax.ShapeDtypeStruct((8, shard), F32), jax.ShapeDtypeStruct((1, unit), F32)],
        in_specs=[pl.BlockSpec(memory_space=pltpu.VMEM)] * 5,
        out_specs=[pl.BlockSpec(memory_space=pltpu.VMEM)] * 6,
        compiler_params=PARAMS,
        name="finish",
    )(up, qkv, proj, down, packed)


def by_core(core, own, other, axis):
    return jnp.where(core == 0, jnp.concatenate([own, other], axis), jnp.concatenate([other, own], axis))


def per_device(
    tokens, valid_slots, cotangent, first_gain, first_shift, qkv_weight, query_bias, value_bias, proj_weight,
    proj_bias, second_gain, second_shift, up_weight, up_bias, down_weight, down_bias,
):
    devices = lax.axis_size(AX)
    chips = devices // 2
    core = lax.axis_index(AX) % 2
    micro, rows, features = tokens.shape
    shard = qkv_weight.shape[0]
    width = features // 2
    hidden = up_weight.shape[1] // 2
    unit = hidden // chips
    own_rows = micro * rows
    every = 2 * own_rows

    fold = unit // shard
    both_weights = lax.all_gather(pack(up_weight, down_weight), AX, axis=0, tiled=True)
    feed_weights = [both_weights]
    if unit % 128 != 0 or shard % 16 != 0:
        half_up = both_weights[:, : 2 * hidden].reshape(features, chips, 2, unit)
        half_up = lax.dynamic_index_in_dim(half_up, core, 2, keepdims=False).reshape(features, hidden)
        half_down = both_weights[:, 2 * hidden :].reshape(chips, 2, shard, fold, features)
        half_down = lax.dynamic_index_in_dim(half_down, core, 1, keepdims=False)
        half_down = half_down.transpose(0, 2, 1, 3).reshape(hidden, features)
        feed_weights = [half_up, half_down]
    vectors = jnp.stack(
        [first_gain, first_shift, query_bias, value_bias, proj_bias, second_gain, second_shift, down_bias], 0
    )
    lanes = max(PARAM_COLS, unit)
    vectors = jnp.pad(vectors.T, ((0, 16), (0, lanes - 8)))
    packed = lax.dynamic_update_slice(vectors, up_bias[None, :], (shard, 0))
    qkv_all, proj_all, packed_all = gather_chips(qkv_weight, proj_weight, packed)
    weight_qkv = qkv_all.reshape(features, 3 * width)
    params = packed_all[:, :, :shard, :8].astype(F32).reshape(features, 8).T
    gain_one, shift_one, bias_query, bias_value, bias_proj, gain_two, shift_two, bias_down = [
        params[i : i + 1] for i in range(8)
    ]
    bias_up = lax.dynamic_index_in_dim(packed_all[:, :, shard, :unit], core, 1, keepdims=False)
    bias_up = bias_up.astype(F32).reshape(1, hidden)
    proj_cols = proj_all.reshape(2, width, width)
    proj_own = lax.dynamic_index_in_dim(proj_cols, core, 0, keepdims=False)
    proj_other = swap(lax.dynamic_index_in_dim(proj_cols, 1 - core, 0, keepdims=False))
    weight_proj = by_core(core, proj_own, proj_other, 1)
    qkv_bias = jnp.concatenate(
        [
            lax.dynamic_slice_in_dim(bias_query, core * width, width, 1),
            jnp.zeros((1, width), F32),
            lax.dynamic_slice_in_dim(bias_value, core * width, width, 1),
        ],
        1,
    )

    own_tokens = tokens.reshape(own_rows, features)
    other_tokens = swap(own_tokens)
    marks = jnp.stack([valid_slots, swap(valid_slots)])
    own_cotangent = cotangent.reshape(own_rows, features)
    penalty = jnp.where(marks > 0, 0.0, -1000000000.0).astype(F32)[..., None]
    norm_one, projected = project(own_tokens, other_tokens, gain_one, shift_one, weight_qkv, qkv_bias)
    projected = projected.reshape(2, micro, rows, 3 * width)
    attended, logs = attend(projected, penalty)
    attended_flat = attended.reshape(every, width)
    mixed = swap(product(attended_flat[own_rows:], weight_proj).astype(BF))
    middle, norm_own = second_norm(
        attended_flat, weight_proj, own_tokens, mixed, bias_proj, gain_two, shift_two
    )
    activation, grad_pre, norm_two, grad_out, lifted, lifted_other, passed, passed_other, up_sums = feed(
        norm_own, swap(norm_own), own_cotangent, swap(own_cotangent),
        (marks > 0).astype(F32).reshape(every, 1), feed_weights, bias_up, unit,
    )
    grad_bias_up = up_sums[0]
    passed_other = swap(passed_other)
    lifted_other = swap(lifted_other)

    grad_down = outer(activation, grad_out)
    down_weight_grad = lax.psum_scatter(
        grad_down, AX, scatter_dimension=0, tiled=True, axis_index_groups=same_core_groups()
    )
    grad_middle, grad_low, block_output, second_sums = second_back(
        passed, passed_other, middle, grad_out, lifted, lifted_other, gain_two, bias_down
    )
    block_output = block_output.reshape(micro, rows, features)
    grad_up = outer(norm_two, grad_pre)
    grad_low = jnp.concatenate([grad_low, swap(grad_low)], 0)
    grad_attended = product_right_t(grad_low, weight_proj).astype(BF).reshape(2, micro, rows, width)
    grad_proj = product_left_t(attended_flat, grad_low).astype(BF)
    grad_proj_own = lax.dynamic_slice_in_dim(grad_proj, core * width, width, 1)
    grad_proj_other = swap(lax.dynamic_slice_in_dim(grad_proj, (1 - core) * width, width, 1))
    grad_proj = by_core(core, grad_proj_own, grad_proj_other, 0)
    grad_projected, grad_bias = attend_back(projected, penalty, logs, attended, grad_attended)
    grad_projected = grad_projected.reshape(every, 3 * width)
    passed = swap(product_right_t(grad_projected[own_rows:], weight_qkv).astype(BF))
    grad_qkv = outer(norm_one, grad_projected)
    tokens_grad, first_sums = first_back(
        grad_projected, weight_qkv, passed, own_tokens, grad_middle, gain_one
    )
    tokens_grad = tokens_grad.reshape(micro, rows, features)

    grad_bias = jnp.sum(grad_bias, axis=0).transpose(1, 0, 2).reshape(2, width)
    grad_bias = by_core(core, grad_bias, jnp.zeros_like(grad_bias), 1)
    sums = jnp.concatenate([first_sums[:2], grad_bias, second_sums[2:3], second_sums[:2], second_sums[3:4]], 0)
    sums = sums.astype(BF).T.reshape(chips, 2, shard, 8)
    sums = jnp.pad(sums, ((0, 0), (0, 0), (0, 16), (0, lanes - 8)))
    up_units = grad_bias_up.astype(BF).reshape(chips, 1, unit)
    up_units = by_core(core, up_units, jnp.zeros_like(up_units), 1)
    sums = lax.dynamic_update_slice(sums, up_units.reshape(chips, 2, 1, unit), (0, 0, shard, 0))
    up_weight_grad, qkv_weight_grad, proj_weight_grad, packed_sum = scatter_chips(
        [
            grad_up.reshape(chips, 2, shard, hidden),
            grad_qkv.reshape(chips, 2, shard, 3 * width),
            grad_proj.reshape(chips, 2, shard, width),
            sums,
        ],
        (chips, 3, 1, "sum"),
    )
    up_weight_grad, qkv_weight_grad, proj_weight_grad, down_weight_grad, vector_sum, up_bias_grad = finish(
        up_weight_grad, qkv_weight_grad, proj_weight_grad, down_weight_grad, packed_sum, shard, unit
    )
    up_bias_grad = up_bias_grad[0]
    return (
        block_output, tokens_grad, vector_sum[0], vector_sum[1], qkv_weight_grad, vector_sum[2], vector_sum[3],
        proj_weight_grad, vector_sum[4], vector_sum[5], vector_sum[6], up_weight_grad, up_bias_grad,
        down_weight_grad, vector_sum[7],
    )


def solution(mesh):
    row = P(None, AX, None)
    vec = P(AX)
    mat = P(AX, None)
    return jax.shard_map(
        per_device,
        mesh=mesh,
        in_specs=(row, P(None, AX), row, vec, vec, mat, vec, vec, mat, vec, vec, vec, mat, vec, mat, vec),
        out_specs=(row, row, vec, vec, mat, vec, vec, mat, vec, vec, vec, mat, vec, mat, vec),
        check_vma=False,
    )
```

```python
import functools

import jax
import jax.numpy as jnp
from jax import lax
from jax.experimental import pallas as pl
from jax.experimental.pallas import tpu as pltpu
from jax.sharding import PartitionSpec as P

AX = "fsdp"
MESH = pl.DeviceIdType.MESH
HEAD = 64
EPSILON = 1e-06
ROOT_HALF = 0.7071067811865476
INV_ROOT_TWO_PI = 0.3989422804014327
BF = jnp.bfloat16
F32 = jnp.float32
PARAM_COLS = 128


def product(left_side, right_side):
    return jnp.dot(left_side, right_side, preferred_element_type=F32)


def product_left_t(left_side, right_side):
    return lax.dot_general(left_side, right_side, (((0,), (0,)), ((), ())), preferred_element_type=F32)


def product_right_t(left_side, right_side):
    return lax.dot_general(left_side, right_side, (((1,), (1,)), ((), ())), preferred_element_type=F32)


def swap(shard):
    return lax.ppermute(shard, AX, [(i, i ^ 1) for i in range(lax.axis_size(AX))])


def same_core_groups():
    count = lax.axis_size(AX)
    return [[i for i in range(count) if i % 2 == core] for core in (0, 1)]


def flip(index, step):
    return index + step - 2 * step * ((index // step) % 2)


def peers_of(me):
    return flip(me, 1), flip(me, 2), flip(me, 4), [flip(me, 8), flip(me, 16), flip(flip(me, 8), 16)]


def zflip(chip, j):
    return [chip, flip(chip, 4), flip(chip, 8), flip(flip(chip, 4), 8)][j]


def meet(peers):
    barrier = pltpu.get_barrier_semaphore()
    for peer in peers:
        pl.semaphore_signal(barrier, inc=1, device_id=(peer,), device_id_type=MESH)
    pl.semaphore_wait(barrier, len(peers))


def gather_kernel(qkv_ref, proj_ref, packed_ref, qkv_out, proj_out, packed_out, local_sem, send_sem, recv_sem):
    me = lax.axis_index(AX)
    chip, core = me // 2, me % 2
    mate, peer_x, peer_y, peers_z = peers_of(me)
    meet([mate, peer_x, peer_y] + peers_z)
    chip_x, chip_y = flip(chip, 1), flip(chip, 2)
    chip_xy = flip(chip_x, 2)
    outs = (qkv_out, packed_out, proj_out)
    count = len(outs)
    width = qkv_ref.shape[1] // 6
    pending = []

    def remote(w, slot, block, target, peer):
        return pltpu.make_async_remote_copy(
            src_ref=block, dst_ref=target, send_sem=send_sem.at[w, slot], recv_sem=recv_sem.at[w, slot],
            device_id=(peer,), device_id_type=MESH,
        )

    def send(w, slot, block, target, peer):
        copy = remote(w, slot, block, target, peer)
        copy.start()
        pending.append(copy)

    def arrive(w, slot, block):
        remote(w, slot, block, block, mate).wait_recv()

    def columns(start, size):
        return pl.ds(pl.multiple_of(start, 128), size)

    def pieces(w, half, target):
        if w == 0:
            return [
                (qkv_ref.at[:, columns((2 * t + half) * width, width)], target.at[:, pl.ds(t * width, width)])
                for t in range(3)
            ]
        if w == 1:
            return [(packed_ref, target)]
        return [(proj_ref.at[:, columns(half * width, width)], target)]

    for w in range(count):
        for source, target in pieces(w, 1 - core, outs[w].at[chip, core]):
            remote(w, 0, source, target, mate).start()
        for source, target in pieces(w, core, outs[w].at[chip, core]):
            pltpu.make_async_copy(source, target, local_sem.at[w]).start()
    for w in range(count):
        own = outs[w].at[chip, core]
        pltpu.make_async_copy(own, own, local_sem.at[w]).wait()
        arrive(w, 0, outs[w].at[chip, 1 - core])
        block = outs[w].at[chip]
        for j in range(3):
            send(w, 1 + j, block, block, peers_z[j])
        send(w, 4, block, block, peer_x)
        send(w, 8, block, block, peer_y)
    for w in range(count):
        for j in (1, 2, 3):
            block = outs[w].at[zflip(chip, j)]
            arrive(w, j, block)
            send(w, 4 + j, block, block, peer_x)
            send(w, 8 + j, block, block, peer_y)
        for j in range(4):
            block = outs[w].at[zflip(chip_x, j)]
            arrive(w, 4 + j, block)
            send(w, 12 + j, block.at[0], block.at[0], peer_y)
            block = outs[w].at[zflip(chip_y, j)]
            arrive(w, 8 + j, block)
            send(w, 16 + j, block.at[1], block.at[1], peer_x)
    for w in range(count):
        for j in range(4):
            block = outs[w].at[zflip(chip_xy, j)]
            arrive(w, 12 + j, block.at[0])
            arrive(w, 16 + j, block.at[1])
    for w in range(count):
        own = outs[w].at[chip, core]
        remote(w, 0, own, own, mate).wait_send()
    for copy in pending:
        copy.wait_send()


def gather_chips(qkv, proj, packed):
    devices = lax.axis_size(AX)
    shard, features = proj.shape
    width = features // 2
    if devices != 32:
        core = lax.axis_index(AX) % 2
        split = qkv.reshape(shard, 3, 2, width).transpose(2, 0, 1, 3).reshape(2, shard, 3 * width)
        gathered = []
        for halves in (split, proj.reshape(shard, 2, width).transpose(1, 0, 2), jnp.stack([packed, packed])):
            own = lax.dynamic_index_in_dim(halves, core, 0, keepdims=False)
            other = swap(lax.dynamic_index_in_dim(halves, 1 - core, 0, keepdims=False))
            block = jnp.where(core == 0, jnp.stack([own, other]), jnp.stack([other, own]))
            gathered.append(lax.all_gather(block, AX, axis=0, axis_index_groups=same_core_groups()))
        return gathered
    chips = devices // 2
    return pl.pallas_call(
        gather_kernel,
        out_shape=[
            jax.ShapeDtypeStruct((chips, 2, shard, 3 * width), BF),
            jax.ShapeDtypeStruct((chips, 2, shard, width), BF),
            jax.ShapeDtypeStruct((chips, 2) + packed.shape, BF),
        ],
        in_specs=[pl.BlockSpec(memory_space=pltpu.VMEM)] * 3,
        out_specs=[pl.BlockSpec(memory_space=pl.ANY)] * 3,
        scratch_shapes=[
            pltpu.SemaphoreType.DMA((3,)),
            pltpu.SemaphoreType.DMA((3, 20)),
            pltpu.SemaphoreType.DMA((3, 20)),
        ],
        compiler_params=pltpu.CompilerParams(collective_id=0, has_side_effects=True),
        cost_estimate=pl.CostEstimate(flops=int(4e10), bytes_accessed=int(1.5e8), transcendentals=0),
        name="gather_chips",
    )(qkv, proj, packed)


class Scatter:
    def __init__(self, kinds, ins, outs, scratch):
        count = len(kinds)
        self.kinds, self.ins, self.outs = kinds, ins, outs
        names = ("recv_a", "recv_b", "recv_x", "recv_y", "recv_z", "stage", "land")
        for place, name in enumerate(names):
            setattr(self, name, scratch[place * count : (place + 1) * count])
        self.send_sem, self.recv_sem = scratch[len(names) * count :]
        me = lax.axis_index(AX)
        self.chip, self.core = me // 2, me % 2
        self.mate, self.peer_x, self.peer_y, self.peers_z = peers_of(me)
        chip_x, chip_y = flip(self.chip, 1), flip(self.chip, 2)
        self.own = [zflip(self.chip, j) for j in range(4)]
        self.at_x = [zflip(chip_x, j) for j in range(4)]
        self.at_y = [zflip(chip_y, j) for j in range(4)]
        self.at_xy = [zflip(flip(chip_x, 2), j) for j in range(4)]
        self.sent = []

    def meet(self):
        meet([self.mate, self.peer_x, self.peer_y] + self.peers_z)

    def remote(self, w, slot, block, target, peer):
        return pltpu.make_async_remote_copy(
            src_ref=block, dst_ref=target, send_sem=self.send_sem.at[w, slot], recv_sem=self.recv_sem.at[w, slot],
            device_id=(peer,), device_id_type=MESH,
        )

    def send(self, w, slot, block, target, peer):
        self.remote(w, slot, block, target, peer).start()
        self.sent.append((w, slot))

    def arrive(self, w, slot, block):
        self.remote(w, slot, block, block, self.mate).wait_recv()

    def far(self, w, j):
        block = self.ins[w].at[self.at_xy[j]]
        self.send(w, j, block.at[0], self.recv_a[w].at[j], self.peer_y)
        self.send(w, 4 + j, block.at[1], self.recv_b[w].at[j], self.peer_x)

    def near(self, w, j):
        self.send(w, 8 + j, self.ins[w].at[self.at_x[j], 1], self.recv_x[w].at[j, 1], self.peer_x)
        self.send(w, 12 + j, self.ins[w].at[self.at_y[j], 0], self.recv_y[w].at[j, 0], self.peer_y)

    def strips(self, w, body):
        @pl.loop(0, self.ins[w].shape[2] // 16)
        def _(i):
            body(pl.ds(pl.multiple_of(i * 16, 16), 16))

    def relay(self, w, j):
        for slot, recv, block, half in (
            (j, self.recv_a[w], self.at_x[j], 0),
            (4 + j, self.recv_b[w], self.at_y[j], 1),
        ):
            self.arrive(w, slot, recv.at[j])

            def body(part):
                total = recv[j, part].astype(F32) + self.ins[w][block, half, part].astype(F32)
                recv[j, part] = total.astype(BF)

            self.strips(w, body)
            if half == 0:
                self.send(w, 16 + j, recv.at[j], self.recv_x[w].at[j, 0], self.peer_x)
            else:
                self.send(w, 20 + j, recv.at[j], self.recv_y[w].at[j, 1], self.peer_y)

    def arrive_near(self, w, j):
        self.arrive(w, 8 + j, self.recv_x[w].at[j, 1])
        self.arrive(w, 12 + j, self.recv_y[w].at[j, 0])
        self.arrive(w, 16 + j, self.recv_x[w].at[j, 0])
        self.arrive(w, 20 + j, self.recv_y[w].at[j, 1])

    def near_sum(self, w, j, half, part):
        total = self.recv_x[w][j, half, part].astype(F32) + self.recv_y[w][j, half, part].astype(F32)
        return total + self.ins[w][self.own[j], half, part].astype(F32)

    def cross(self, w, j):
        self.arrive_near(w, j)

        def body(part):
            for half in range(2):
                self.recv_x[w][j, half, part] = self.near_sum(w, j, half, part).astype(BF)

        self.strips(w, body)
        self.send(w, 23 + j, self.recv_x[w].at[j], self.recv_z[w].at[j - 1], self.peers_z[j - 1])

    def place(self, w, part, total, half):
        kind = self.kinds[w]
        if kind == "sum":
            self.outs[w][part] = total
            return
        size = total.shape[1] // kind
        for t in range(kind):
            start = pl.multiple_of((2 * t + half) * size, 128)
            self.outs[w][part, pl.ds(start, size)] = total[:, t * size : (t + 1) * size]

    def last(self, w):
        self.arrive_near(w, 0)
        for j in range(3):
            self.arrive(w, 24 + j, self.recv_z[w].at[j])

        def total_of(half, part):
            total = self.near_sum(w, 0, half, part)
            for j in range(3):
                total = total + self.recv_z[w][j, half, part].astype(F32)
            return total

        def other(part):
            self.stage[w][part] = total_of(1 - self.core, part)

        self.strips(w, other)
        self.send(w, 27, self.stage[w], self.land[w], self.mate)
        self.strips(w, lambda part: self.place(w, part, total_of(self.core, part), self.core))

    def finish(self, w):
        self.arrive(w, 27, self.land[w])

        def body(part):
            other = self.land[w][part]
            if self.kinds[w] == "sum":
                other = other + self.outs[w][part]
            self.place(w, part, other, 1 - self.core)

        self.strips(w, body)

    def drain(self):
        for w, slot in self.sent:
            if slot == 27:
                block = self.stage[w]
            elif slot >= 24:
                block = self.recv_x[w].at[0]
            else:
                block = self.recv_a[w].at[0]
            self.remote(w, slot, block, block, self.mate).wait_send()

    def opening(self, w):
        self.far(w, 1), self.far(w, 2), self.near(w, 1)

    def run(self):
        small = range(2, len(self.kinds))
        opening = self.opening
        self.meet()
        opening(0)
        for w in small:
            for j in (1, 2, 3, 0):
                self.far(w, j), self.near(w, j)
        self.relay(0, 1), self.far(0, 3), self.near(0, 2)
        self.relay(0, 2), self.far(0, 0), self.near(0, 3)
        for w in small:
            for j in (1, 2, 3, 0):
                self.relay(w, j)
        self.relay(0, 3), self.near(0, 0), self.cross(0, 1)
        opening(1)
        for w in small:
            for j in (1, 2, 3):
                self.cross(w, j)
        self.relay(0, 0), self.cross(0, 2), self.cross(0, 3)
        self.relay(1, 1), self.far(1, 3), self.near(1, 2)
        self.relay(1, 2), self.far(1, 0), self.near(1, 3)
        for w in small:
            self.last(w)
        self.relay(1, 3), self.near(1, 0), self.cross(1, 1)
        self.relay(1, 0)
        self.last(0)
        self.cross(1, 2), self.cross(1, 3)
        for w in small:
            self.finish(w)
        self.finish(0)
        self.last(1)
        self.finish(1)
        self.drain()


def scatter_scratch(shapes):
    count = len(shapes)
    scratch = [pltpu.VMEM((4,) + s[2:], BF) for s in shapes] * 2
    scratch += [pltpu.VMEM((4, 2) + s[2:], BF) for s in shapes] * 2
    scratch += [pltpu.VMEM((3, 2) + s[2:], BF) for s in shapes]
    scratch += [pltpu.VMEM(s[2:], F32) for s in shapes] * 2
    return scratch + [pltpu.SemaphoreType.DMA((count, 28)), pltpu.SemaphoreType.DMA((count, 28))]


def scatter_shapes(shapes, kinds):
    return [
        jax.ShapeDtypeStruct((s[2], s[3] * (1 if kind == "sum" else 2)), F32) for s, kind in zip(shapes, kinds)
    ]


def scatter_kernel(kinds, *refs):
    count = len(kinds)
    Scatter(kinds, refs[:count], refs[count : 2 * count], refs[2 * count :]).run()


def scatter_chips(grads, kinds):
    devices = lax.axis_size(AX)
    shapes = [g.shape for g in grads]
    if devices != 32:
        core = lax.axis_index(AX) % 2
        summed = []
        for grad, kind in zip(grads, kinds):
            block = lax.psum_scatter(grad, AX, scatter_dimension=0, axis_index_groups=same_core_groups())
            block = block.astype(F32)
            own = lax.dynamic_index_in_dim(block, core, 0, keepdims=False)
            other = swap(lax.dynamic_index_in_dim(block, 1 - core, 0, keepdims=False))
            if kind == "sum":
                summed.append(own + other)
                continue
            rows, columns = own.shape
            own = own.reshape(rows, kind, 1, columns // kind)
            other = other.reshape(rows, kind, 1, columns // kind)
            summed.append(by_core(core, own, other, 2).reshape(rows, 2 * columns))
        return summed
    count = len(grads)
    return pl.pallas_call(
        functools.partial(scatter_kernel, kinds),
        out_shape=scatter_shapes(shapes, kinds),
        in_specs=[pl.BlockSpec(memory_space=pltpu.VMEM)] * count,
        out_specs=[pl.BlockSpec(memory_space=pltpu.VMEM)] * count,
        scratch_shapes=scatter_scratch(shapes),
        compiler_params=pltpu.CompilerParams(
            collective_id=1, has_side_effects=True, vmem_limit_bytes=56 << 20
        ),
        name="scatter_chips",
    )(*grads)


def flat(ref):
    return ref[...].reshape(-1, ref.shape[-1])


def head_masks():
    lane = lax.broadcasted_iota(jnp.int32, (1, 2 * HEAD), 1)
    return [(lane < HEAD).astype(BF), (lane >= HEAD).astype(BF)]


def attend_kernel(chunk, q_ref, k_ref, v_ref, penalty_ref, out_ref, log_ref, query_buf, mixed_buf):
    query_buf[...] = flat(q_ref) * jnp.asarray(0.125, BF)
    keys, values = flat(k_ref), flat(v_ref)
    values_t = values.T
    penalty = flat(penalty_ref)
    masks = head_masks()

    @pl.loop(0, query_buf.shape[0] // chunk)
    def _(i):
        part = pl.ds(pl.multiple_of(i * chunk, chunk), chunk)
        queries = query_buf[part]
        parts = []
        for h in range(2):
            scores = product_right_t(keys, queries * masks[h]) + penalty
            top = jnp.max(scores, axis=0, keepdims=True)
            exponent = jnp.exp(scores - top)
            total = jnp.sum(exponent, axis=0, keepdims=True)
            mixed = product(values_t[h * HEAD : (h + 1) * HEAD], exponent.astype(BF))
            parts.append(mixed * (1.0 / total))
            log_ref[0, 0, h : h + 1, part] = top + jnp.log(total)
        mixed_buf[part] = jnp.concatenate(parts, 0).T.astype(BF)

    out_ref[...] = mixed_buf[...].reshape(out_ref.shape)


def attend(projected, penalty):
    _, clips, rows, triple = projected.shape
    slots = 2 * rows
    width = triple // 3
    pairs = width // (2 * HEAD)

    def block(offset):
        return pl.BlockSpec((2, 1, rows, 2 * HEAD), lambda i, j: (0, i, 0, offset * pairs + j))

    return pl.pallas_call(
        functools.partial(attend_kernel, 256),
        grid=(clips, pairs),
        in_specs=[block(0), block(1), block(2), pl.BlockSpec((2, 1, rows, 1), lambda i, j: (0, i, 0, 0))],
        out_specs=[block(0), pl.BlockSpec((1, 1, 2, slots), lambda i, j: (i, j, 0, 0))],
        out_shape=[
            jax.ShapeDtypeStruct((2, clips, rows, width), BF),
            jax.ShapeDtypeStruct((clips, pairs, 2, slots), F32),
        ],
        scratch_shapes=[pltpu.VMEM((slots, 2 * HEAD), BF)] * 2,
        compiler_params=pltpu.CompilerParams(vmem_limit_bytes=48 << 20),
        cost_estimate=pl.CostEstimate(
            flops=4 * clips * pairs * slots * slots * 2 * HEAD, bytes_accessed=8 * clips * slots * width,
            transcendentals=clips * pairs * 2 * slots * slots,
        ),
        name="attend",
    )(projected, projected, projected, penalty)


def attend_back_kernel(
    chunk, q_ref, k_ref, v_ref, penalty_ref, log_ref, att_ref, grad_ref, out_ref, bias_ref,
    query_buf, grad_buf, mixed_buf, back_buf, key_sum, value_sum, bias_sum,
):
    rows = q_ref.shape[2]
    pair = pl.program_id(1)
    width = out_ref.shape[3] // 3
    query_buf[...] = flat(q_ref) * jnp.asarray(0.125, BF)
    grad_buf[...] = flat(grad_ref)
    mixed_buf[...] = flat(att_ref)
    keys, values = flat(k_ref), flat(v_ref)
    keys_t = keys.T
    penalty = flat(penalty_ref)
    masks = head_masks()
    for total in (key_sum, value_sum, bias_sum):
        total[...] = jnp.zeros_like(total)

    def keep(offset, value):
        columns = pl.ds(pl.multiple_of(offset + pair * 2 * HEAD, 128), 2 * HEAD)
        for side in range(2):
            out_ref[side, 0, :, columns] = value[side * rows : (side + 1) * rows]

    for start in range(0, query_buf.shape[0], chunk):
        part = pl.ds(start, chunk)
        queries, grads = query_buf[part], grad_buf[part]
        overlap = (grads.astype(F32) * mixed_buf[part].astype(F32)).T
        parts = []
        for h in range(2):
            head_queries = queries * masks[h]
            head_grads = grads * masks[h]
            correction = jnp.sum(overlap[h * HEAD : (h + 1) * HEAD], axis=0, keepdims=True)
            logs = log_ref[0, 0, h : h + 1, part]
            soft = jnp.exp(product_right_t(keys, head_queries) + penalty - logs)
            grad_soft = product_right_t(values, head_grads)
            value_sum[...] += product(soft.astype(BF), head_grads)
            grad_scores = (soft * (grad_soft - correction)).astype(BF)
            key_sum[...] += product(grad_scores, head_queries)
            parts.append(product(keys_t[h * HEAD : (h + 1) * HEAD], grad_scores))
        grad_queries = jnp.concatenate(parts, 0).T * 0.125
        bias_sum[0:1] += jnp.sum(grad_queries, axis=0, keepdims=True)
        back_buf[part] = grad_queries.astype(BF)

    keep(0, back_buf[...])
    keep(width, key_sum[...].astype(BF))
    keep(2 * width, value_sum[...].astype(BF))
    bias_ref[0, 0, 0:1] = bias_sum[0:1]
    bias_ref[0, 0, 1:2] = jnp.sum(value_sum[...], axis=0, keepdims=True)


def attend_back(projected, penalty, logs, attended, grad_attended):
    _, clips, rows, triple = projected.shape
    slots = 2 * rows
    width = triple // 3
    pairs = width // (2 * HEAD)

    def block(offset):
        return pl.BlockSpec((2, 1, rows, 2 * HEAD), lambda i, j: (0, i, 0, offset * pairs + j))

    return pl.pallas_call(
        functools.partial(attend_back_kernel, 256),
        grid=(clips, pairs),
        in_specs=[
            block(0), block(1), block(2),
            pl.BlockSpec((2, 1, rows, 1), lambda i, j: (0, i, 0, 0)),
            pl.BlockSpec((1, 1, 2, slots), lambda i, j: (i, j, 0, 0)),
            block(0), block(0),
        ],
        out_specs=[
            pl.BlockSpec((2, 1, rows, triple), lambda i, j: (0, i, 0, 0)),
            pl.BlockSpec((1, 1, 2, 2 * HEAD), lambda i, j: (i, j, 0, 0)),
        ],
        out_shape=[
            jax.ShapeDtypeStruct((2, clips, rows, triple), BF),
            jax.ShapeDtypeStruct((clips, pairs, 2, 2 * HEAD), F32),
        ],
        scratch_shapes=[pltpu.VMEM((slots, 2 * HEAD), BF)] * 4
        + [pltpu.VMEM((slots, 2 * HEAD), F32)] * 2
        + [pltpu.VMEM((8, 2 * HEAD), F32)],
        compiler_params=pltpu.CompilerParams(vmem_limit_bytes=56 << 20),
        cost_estimate=pl.CostEstimate(
            flops=10 * clips * pairs * slots * slots * 2 * HEAD, bytes_accessed=18 * clips * slots * width,
            transcendentals=clips * pairs * 2 * slots * slots,
        ),
        name="attend_back",
    )(projected, projected, projected, penalty, logs, attended, grad_attended)


def normal_parts(values):
    average = jnp.mean(values, axis=-1, keepdims=True)
    centered = values - average
    inverse = lax.rsqrt(jnp.mean(centered * centered, axis=-1, keepdims=True) + EPSILON)
    return centered * inverse, inverse


def normal_back(grad_normed, scaled, inverse, gain):
    grad_scaled = grad_normed * gain
    first_mean = jnp.mean(grad_scaled, axis=-1, keepdims=True)
    second_mean = jnp.mean(grad_scaled * scaled, axis=-1, keepdims=True)
    return inverse * (grad_scaled - first_mean - scaled * second_mean)


def rows_spec(size, columns):
    return pl.BlockSpec((size, columns), lambda i: (i, 0))


def whole_spec(shape):
    return pl.BlockSpec(shape, lambda i: (0,) * len(shape), pipeline_mode=pl.Buffered(1))


PARAMS = pltpu.CompilerParams(vmem_limit_bytes=56 << 20)


def strips_of(ref):
    return [pl.ds(start, 32) for start in range(0, ref.shape[0], 32)]


def project_kernel(steps, own_ref, other_ref, gain_ref, shift_ref, weight_ref, bias_ref, norm_ref, out_ref):
    is_own = pl.program_id(0) < steps
    for part in strips_of(own_ref):
        rows = jnp.where(is_own, own_ref[part].astype(F32), other_ref[part].astype(F32))
        scaled, _ = normal_parts(rows)
        norm_ref[part] = (scaled * gain_ref[...] + shift_ref[...]).astype(BF)
    out_ref[...] = (product(norm_ref[...], weight_ref[...]) + bias_ref[...]).astype(BF)


def project(own, other, gain, shift, weight, bias):
    rows, features = own.shape
    columns = weight.shape[1]
    steps = 3
    size = rows // steps
    return pl.pallas_call(
        functools.partial(project_kernel, steps),
        grid=(2 * steps,),
        in_specs=[
            pl.BlockSpec((size, features), lambda i: (jnp.minimum(i, steps - 1), 0)),
            pl.BlockSpec((size, features), lambda i: (jnp.maximum(i - steps, 0), 0)),
            whole_spec((1, features)),
            whole_spec((1, features)),
            whole_spec((features, columns)),
            whole_spec((1, columns)),
        ],
        out_specs=[rows_spec(size, features), rows_spec(size, columns)],
        out_shape=[
            jax.ShapeDtypeStruct((2 * rows, features), BF),
            jax.ShapeDtypeStruct((2 * rows, columns), BF),
        ],
        compiler_params=PARAMS,
        name="project",
    )(own, other, gain, shift, weight, bias)


def second_norm_kernel(att_ref, weight_ref, token_ref, recv_ref, bias_ref, gain_ref, shift_ref, middle_ref, out_ref):
    mixed = product(att_ref[...], weight_ref[...])
    for part in strips_of(token_ref):
        middle = token_ref[part].astype(F32) + mixed[part.start : part.start + part.size]
        middle = middle + recv_ref[part].astype(F32) + bias_ref[...]
        middle_ref[part] = middle
        scaled, _ = normal_parts(middle)
        out_ref[part] = (scaled * gain_ref[...] + shift_ref[...]).astype(BF)


def second_norm(attended, weight, tokens, received, bias, gain, shift):
    rows, features = tokens.shape
    width = weight.shape[0]
    size = rows // 4
    return pl.pallas_call(
        second_norm_kernel,
        grid=(4,),
        in_specs=[
            rows_spec(size, width), whole_spec((width, features)), rows_spec(size, features), rows_spec(size, features),
            whole_spec((1, features)), whole_spec((1, features)), whole_spec((1, features)),
        ],
        out_specs=[rows_spec(size, features), rows_spec(size, features)],
        out_shape=[jax.ShapeDtypeStruct((rows, features), F32), jax.ShapeDtypeStruct((rows, features), BF)],
        compiler_params=PARAMS,
        name="second_norm",
    )(attended, weight, tokens, received, bias, gain, shift)


def feed_kernel(
    steps, unit, own_ref, other_ref, grad_own_ref, grad_other_ref, mark_ref, bias_ref, *refs
):
    if len(refs) == 14:
        both_ref, refs = refs[0], refs[1:]
        sources = None
    else:
        sources, refs = refs[:2], refs[2:]
    act_ref, pre_ref, norm_ref, grad_ref, lift_own_ref, lift_other_ref, pass_own_ref, pass_other_ref = refs[:8]
    sums_ref, up_ref, down_ref, up_sem, down_sem = refs[8:]
    step = pl.program_id(0)
    features, hidden = up_ref.shape

    @pl.when(step == 0)
    def _():
        sums_ref[...] = jnp.zeros_like(sums_ref)
        if sources is not None:
            pltpu.make_async_copy(sources[0], up_ref, up_sem).start()
            pltpu.make_async_copy(sources[1], down_ref, down_sem).start()
        else:
            core = lax.axis_index(AX) % 2
            chips = hidden // unit
            shard = features // (2 * chips)
            for k in range(chips):
                device = 2 * k + core
                pltpu.make_async_copy(
                    both_ref.at[:, pl.ds(pl.multiple_of(device * unit, 128), unit)],
                    up_ref.at[:, k * unit : (k + 1) * unit],
                    up_sem,
                ).start()
            for k in range(chips):
                device = 2 * k + core
                for q in range(unit // shard):
                    pltpu.make_async_copy(
                        both_ref.at[
                            pl.ds(pl.multiple_of(device * shard, 16), shard),
                            pl.ds(2 * hidden + q * features, features),
                        ],
                        down_ref.at[k * unit + q * shard : k * unit + (q + 1) * shard],
                        down_sem,
                    ).start()
        pltpu.make_async_copy(up_ref, up_ref, up_sem).wait()
        pltpu.make_async_copy(down_ref, down_ref, down_sem).wait()

    rows = jnp.where(step < steps, other_ref[...], own_ref[...])
    grads = jnp.where(step < steps, grad_other_ref[...], grad_own_ref[...]) * mark_ref[...].astype(BF)
    norm_ref[...] = rows
    grad_ref[...] = grads
    size = 512
    for start in range(0, hidden, size):
        part = slice(start, start + size)
        pre = product(rows, up_ref[:, part]) + bias_ref[:, part]
        normal_cdf = 0.5 * (1.0 + lax.erf(pre * ROOT_HALF))
        density = jnp.exp(-0.5 * pre * pre) * INV_ROOT_TWO_PI
        act_ref[:, part] = (pre * normal_cdf).astype(BF)
        grad_pre = product_right_t(grads, down_ref[part]) * (normal_cdf + pre * density)
        sums_ref[0:1, part] += jnp.sum(grad_pre, axis=0, keepdims=True)
        pre_ref[:, part] = grad_pre.astype(BF)
    lifted = product(act_ref[...], down_ref[...])
    passed = product_right_t(pre_ref[...], up_ref[...])
    lift_own_ref[...] = lifted
    pass_own_ref[...] = passed

    @pl.when(step < steps)
    def _():
        lift_other_ref[...] = lifted.astype(BF)
        pass_other_ref[...] = passed.astype(BF)


def feed(own, other, grad_own, grad_other, marks, weights, bias, unit):
    rows, features = own.shape
    hidden = bias.shape[1]
    steps = 3
    size = rows // steps

    def side(i):
        return jnp.where(i < steps, i + steps, i - steps)

    def both_spec(columns):
        return pl.BlockSpec((size, columns), lambda i: (side(i), 0))

    own_spec = pl.BlockSpec((size, features), lambda i: (jnp.maximum(i - steps, 0), 0))
    other_spec = pl.BlockSpec((size, features), lambda i: (jnp.minimum(i, steps - 1), 0))
    return pl.pallas_call(
        functools.partial(feed_kernel, steps, unit),
        grid=(2 * steps,),
        in_specs=[own_spec, other_spec, own_spec, other_spec, both_spec(1), whole_spec((1, hidden))]
        + [pl.BlockSpec(memory_space=pl.ANY)] * len(weights),
        out_specs=[
            both_spec(hidden), both_spec(hidden), both_spec(features), both_spec(features),
            own_spec, other_spec, own_spec, other_spec,
            pl.BlockSpec((8, hidden), lambda i: (0, 0)),
        ],
        out_shape=[
            jax.ShapeDtypeStruct((2 * rows, hidden), BF), jax.ShapeDtypeStruct((2 * rows, hidden), BF),
            jax.ShapeDtypeStruct((2 * rows, features), BF), jax.ShapeDtypeStruct((2 * rows, features), BF),
            jax.ShapeDtypeStruct((rows, features), F32), jax.ShapeDtypeStruct((rows, features), BF),
            jax.ShapeDtypeStruct((rows, features), F32), jax.ShapeDtypeStruct((rows, features), BF),
            jax.ShapeDtypeStruct((8, hidden), F32),
        ],
        scratch_shapes=[
            pltpu.VMEM((features, hidden), BF), pltpu.VMEM((hidden, features), BF),
            pltpu.SemaphoreType.DMA(()), pltpu.SemaphoreType.DMA(()),
        ],
        compiler_params=PARAMS,
        cost_estimate=pl.CostEstimate(
            flops=16 * rows * features * hidden, bytes_accessed=8 * features * hidden,
            transcendentals=4 * rows * hidden,
        ),
        name="feed",
    )(own, other, grad_own, grad_other, marks, bias, *weights)


def outer_kernel(left_ref, right_ref, out_ref):
    out_ref[...] = product_left_t(left_ref[...], right_ref[...]).astype(BF)


def outer(left, right):
    rows, columns = left.shape
    width = right.shape[1]
    size = 256
    return pl.pallas_call(
        outer_kernel,
        grid=(columns // size,),
        in_specs=[pl.BlockSpec((rows, size), lambda i: (0, i)), whole_spec((rows, width))],
        out_specs=rows_spec(size, width),
        out_shape=jax.ShapeDtypeStruct((columns, width), BF),
        compiler_params=PARAMS,
        cost_estimate=pl.CostEstimate(
            flops=2 * rows * columns * width, bytes_accessed=2 * (rows * columns + rows * width + columns * width),
            transcendentals=0,
        ),
        name="outer",
    )(left, right)


def gather_sums(sums_ref, values):
    for index, value in enumerate(values):
        sums_ref[index : index + 1] += jnp.sum(value, axis=0, keepdims=True)


def clear_first(sums_ref):
    @pl.when(pl.program_id(0) == 0)
    def _():
        sums_ref[...] = jnp.zeros_like(sums_ref)


def second_back_kernel(
    grad_ref, recv_ref, middle_ref, out_ref, lift_ref, lift_recv_ref, gain_ref, bias_ref,
    full_ref, low_ref, block_ref, sums_ref,
):
    clear_first(sums_ref)
    for part in strips_of(grad_ref):
        lifted = lift_ref[part] + lift_recv_ref[part].astype(F32)
        block_ref[part] = (middle_ref[part] + lifted + bias_ref[...]).astype(BF)
        grad_normed = grad_ref[part] + recv_ref[part].astype(F32)
        scaled, inverse = normal_parts(middle_ref[part])
        grad_out = out_ref[part].astype(F32)
        grad_middle = grad_out + normal_back(grad_normed, scaled, inverse, gain_ref[...])
        full_ref[part] = grad_middle
        low_ref[part] = grad_middle.astype(BF)
        gather_sums(sums_ref, [grad_normed * scaled, grad_normed, grad_middle, grad_out])


def second_back(passed, received, middle, grad_out, lifted, lift_received, gain, bias):
    rows, features = middle.shape
    size = rows // 4
    return pl.pallas_call(
        second_back_kernel,
        grid=(4,),
        in_specs=[rows_spec(size, features)] * 6 + [whole_spec((1, features))] * 2,
        out_specs=[rows_spec(size, features)] * 3 + [pl.BlockSpec((8, features), lambda i: (0, 0))],
        out_shape=[
            jax.ShapeDtypeStruct((rows, features), F32), jax.ShapeDtypeStruct((rows, features), BF),
            jax.ShapeDtypeStruct((rows, features), BF), jax.ShapeDtypeStruct((8, features), F32),
        ],
        compiler_params=PARAMS,
        name="second_back",
    )(passed, received, middle, grad_out, lifted, lift_received, gain, bias)


def first_back_kernel(grad_ref, weight_ref, recv_ref, token_ref, middle_ref, gain_ref, full_ref, sums_ref):
    clear_first(sums_ref)
    passed = product_right_t(grad_ref[...], weight_ref[...])
    for part in strips_of(grad_ref):
        grad_normed = passed[part.start : part.start + part.size] + recv_ref[part].astype(F32)
        scaled, inverse = normal_parts(token_ref[part].astype(F32))
        full_ref[part] = middle_ref[part] + normal_back(grad_normed, scaled, inverse, gain_ref[...])
        gather_sums(sums_ref, [grad_normed * scaled, grad_normed])


def first_back(grad_projected, weight, received, tokens, grad_middle, gain):
    rows, features = tokens.shape
    triple = weight.shape[1]
    size = rows // 4
    return pl.pallas_call(
        first_back_kernel,
        grid=(4,),
        in_specs=[
            rows_spec(size, triple), whole_spec((features, triple)), rows_spec(size, features),
            rows_spec(size, features), rows_spec(size, features), whole_spec((1, features)),
        ],
        out_specs=[rows_spec(size, features), pl.BlockSpec((8, features), lambda i: (0, 0))],
        out_shape=[jax.ShapeDtypeStruct((rows, features), F32), jax.ShapeDtypeStruct((8, features), F32)],
        compiler_params=PARAMS,
        name="first_back",
    )(grad_projected, weight, received, tokens, grad_middle, gain)


def tail_kernel(
    kinds, up_ref, proj_ref, sums_ref, bias_ref, gain_ref, back_hbm, weight_hbm, norm_hbm, token_hbm, middle_hbm,
    up_out, qkv_out, proj_out, packed_out, tokens_out, *refs
):
    back, weight, norm, token, middle, qkv, packed, vectors, stage, land, load_sem, pass_sem = refs[:12]
    scatter = Scatter(kinds, (up_ref, qkv, proj_ref, packed), (up_out, qkv_out, proj_out, packed_out), refs[12:])
    chips, _, shard, triple = qkv.shape
    own_rows = token.shape[0]
    loads = [
        pltpu.make_async_copy(source, target, load_sem.at[i])
        for i, (source, target) in enumerate(
            ((back_hbm, back), (weight_hbm, weight), (norm_hbm, norm), (token_hbm, token), (middle_hbm, middle))
        )
    ]
    for load in loads:
        load.start()
    scatter.meet()
    scatter.opening(0)
    for j in (1, 2, 3, 0):
        scatter.far(2, j), scatter.near(2, j)
    vectors[...] = jnp.zeros_like(vectors)
    vectors[0:8] = sums_ref[...]
    loads[0].wait(), loads[1].wait()

    @pl.loop(0, own_rows // 256)
    def _(i):
        part = pl.ds(pl.multiple_of(own_rows + i * 256, 256), 256)
        stage[pl.ds(pl.multiple_of(i * 256, 256), 256)] = product_right_t(back[part], weight[...]).astype(BF)

    passing = pltpu.make_async_remote_copy(
        src_ref=stage, dst_ref=land, send_sem=pass_sem.at[0], recv_sem=pass_sem.at[1],
        device_id=(scatter.mate,), device_id_type=MESH,
    )
    passing.start()
    scatter.relay(0, 1), scatter.far(0, 3), scatter.near(0, 2)
    loads[2].wait()

    @pl.loop(0, norm.shape[1] // 256)
    def _(i):
        part = pl.ds(pl.multiple_of(i * 256, 256), 256)
        count = 256 // (2 * shard)
        grad = product_left_t(norm[:, part], back[...]).astype(BF)
        qkv[pl.ds(i * count, count)] = grad.reshape(count, 2, shard, triple)

    scatter.relay(0, 2), scatter.far(0, 0), scatter.near(0, 3)
    for j in (1, 2, 3, 0):
        scatter.relay(2, j)
    scatter.opening(1)
    loads[3].wait(), loads[4].wait()
    passing.wait()

    @pl.loop(0, own_rows // 256)
    def _(i):
        start = pl.multiple_of(i * 256, 256)
        passed = product_right_t(back[pl.ds(start, 256)], weight[...])
        for strip in range(0, 256, 32):
            part = pl.ds(start + strip, 32)
            grad_normed = passed[strip : strip + 32] + land[part].astype(F32)
            scaled, inverse = normal_parts(token[part].astype(F32))
            tokens_out[part] = middle[part] + normal_back(grad_normed, scaled, inverse, gain_ref[...])
            vectors[0:1] += jnp.sum(grad_normed * scaled, axis=0, keepdims=True)
            vectors[1:2] += jnp.sum(grad_normed, axis=0, keepdims=True)

    scatter.relay(0, 3), scatter.near(0, 0), scatter.cross(0, 1), scatter.cross(0, 2)
    packed[:, :, :shard] = vectors[...].T.astype(BF).reshape(chips, 2, shard, PARAM_COLS)
    packed[:, :, shard:] = bias_ref[...]
    for j in (1, 2, 3, 0):
        scatter.far(3, j), scatter.near(3, j)
    scatter.relay(0, 0), scatter.cross(0, 3)
    for j in (1, 2, 3):
        scatter.cross(2, j)
    scatter.relay(1, 1), scatter.far(1, 3), scatter.near(1, 2)
    scatter.relay(1, 2), scatter.far(1, 0), scatter.near(1, 3)
    for j in (1, 2, 3, 0):
        scatter.relay(3, j)
    scatter.last(2)
    scatter.relay(1, 3), scatter.near(1, 0), scatter.cross(1, 1)
    for j in (1, 2, 3):
        scatter.cross(3, j)
    scatter.relay(1, 0)
    scatter.last(0)
    scatter.cross(1, 2), scatter.cross(1, 3)
    scatter.finish(2), scatter.finish(0)
    scatter.last(3)
    scatter.last(1)
    scatter.finish(3), scatter.finish(1)
    scatter.drain()


def tail(grad_up, grad_proj, sums, bias_rows, gain, back, weight, norm, tokens, middle):
    chips, _, shard, hidden = grad_up.shape
    rows, triple = back.shape
    own_rows, features = tokens.shape
    extra = bias_rows.shape[2]
    kinds = (chips, 3, 1, "sum")
    shapes = [
        grad_up.shape, (chips, 2, shard, triple), grad_proj.shape, (chips, 2, shard + extra, PARAM_COLS),
    ]
    vmem = pl.BlockSpec(memory_space=pltpu.VMEM)
    return pl.pallas_call(
        functools.partial(tail_kernel, kinds),
        out_shape=scatter_shapes(shapes, kinds) + [jax.ShapeDtypeStruct((own_rows, features), F32)],
        in_specs=[vmem] * 5 + [pl.BlockSpec(memory_space=pl.ANY)] * 5,
        out_specs=[vmem] * 5,
        scratch_shapes=[
            pltpu.VMEM(back.shape, BF), pltpu.VMEM(weight.shape, BF), pltpu.VMEM(norm.shape, BF),
            pltpu.VMEM(tokens.shape, BF), pltpu.VMEM(middle.shape, F32),
            pltpu.VMEM(shapes[1], BF), pltpu.VMEM(shapes[3], BF), pltpu.VMEM((PARAM_COLS, features), F32),
            pltpu.VMEM((own_rows, features), BF), pltpu.VMEM((own_rows, features), BF),
            pltpu.SemaphoreType.DMA((5,)), pltpu.SemaphoreType.DMA((2,)),
        ]
        + scatter_scratch(shapes),
        compiler_params=pltpu.CompilerParams(collective_id=1, has_side_effects=True, vmem_limit_bytes=62 << 20),
        name="tail",
    )(grad_up, grad_proj, sums, bias_rows, gain, back, weight, norm, tokens, middle)


def pack_kernel(up_ref, down_ref, out_ref):
    shard, columns = up_ref.shape
    features = down_ref.shape[1]
    out_ref[:, :columns] = up_ref[...]
    for i in range(down_ref.shape[0] // shard):
        out_ref[:, columns + i * features : columns + (i + 1) * features] = down_ref[i * shard : (i + 1) * shard]


def pack(up, down):
    shard, columns = up.shape
    fold = down.shape[0] // shard
    if shard % 16 != 0:
        return jnp.concatenate([up] + [down[shard * i : shard * (i + 1)] for i in range(fold)], 1)
    return pl.pallas_call(
        pack_kernel,
        out_shape=jax.ShapeDtypeStruct((shard, columns + fold * down.shape[1]), BF),
        in_specs=[pl.BlockSpec(memory_space=pltpu.VMEM)] * 2,
        out_specs=pl.BlockSpec(memory_space=pltpu.VMEM),
        name="pack",
    )(up, down)


def finish_kernel(up_ref, qkv_ref, proj_ref, down_ref, packed_ref, up_out, qkv_out, proj_out, down_out, vec_out, bias_out):
    up_out[...] = up_ref[...]
    qkv_out[...] = qkv_ref[...]
    proj_out[...] = proj_ref[...]
    down_out[...] = down_ref[...].astype(F32)
    shard = vec_out.shape[1]
    vec_out[...] = packed_ref[:shard].T[:8]
    bias_out[...] = packed_ref[shard : shard + 1]


def finish(up, qkv, proj, down, packed, shard, unit):
    if lax.axis_size(AX) != 32:
        return up, qkv, proj, down.astype(F32), packed[:shard, :8].T, packed[shard : shard + 1, :unit]
    return pl.pallas_call(
        finish_kernel,
        out_shape=[jax.ShapeDtypeStruct(a.shape, F32) for a in (up, qkv, proj, down)]
        + [jax.ShapeDtypeStruct((8, shard), F32), jax.ShapeDtypeStruct((1, unit), F32)],
        in_specs=[pl.BlockSpec(memory_space=pltpu.VMEM)] * 5,
        out_specs=[pl.BlockSpec(memory_space=pltpu.VMEM)] * 6,
        compiler_params=PARAMS,
        name="finish",
    )(up, qkv, proj, down, packed)


def by_core(core, own, other, axis):
    return jnp.where(core == 0, jnp.concatenate([own, other], axis), jnp.concatenate([other, own], axis))


def per_device(
    tokens, valid_slots, cotangent, first_gain, first_shift, qkv_weight, query_bias, value_bias, proj_weight,
    proj_bias, second_gain, second_shift, up_weight, up_bias, down_weight, down_bias,
):
    devices = lax.axis_size(AX)
    chips = devices // 2
    core = lax.axis_index(AX) % 2
    micro, rows, features = tokens.shape
    shard = qkv_weight.shape[0]
    width = features // 2
    hidden = up_weight.shape[1] // 2
    unit = hidden // chips
    own_rows = micro * rows
    every = 2 * own_rows

    fold = unit // shard
    both_weights = lax.all_gather(pack(up_weight, down_weight), AX, axis=0, tiled=True)
    feed_weights = [both_weights]
    if unit % 128 != 0 or shard % 16 != 0:
        half_up = both_weights[:, : 2 * hidden].reshape(features, chips, 2, unit)
        half_up = lax.dynamic_index_in_dim(half_up, core, 2, keepdims=False).reshape(features, hidden)
        half_down = both_weights[:, 2 * hidden :].reshape(chips, 2, shard, fold, features)
        half_down = lax.dynamic_index_in_dim(half_down, core, 1, keepdims=False)
        half_down = half_down.transpose(0, 2, 1, 3).reshape(hidden, features)
        feed_weights = [half_up, half_down]
    vectors = jnp.stack(
        [first_gain, first_shift, query_bias, value_bias, proj_bias, second_gain, second_shift, down_bias], 0
    )
    lanes = max(PARAM_COLS, unit)
    vectors = jnp.pad(vectors.T, ((0, 16), (0, lanes - 8)))
    packed = lax.dynamic_update_slice(vectors, up_bias[None, :], (shard, 0))
    qkv_all, proj_all, packed_all = gather_chips(qkv_weight, proj_weight, packed)
    weight_qkv = qkv_all.reshape(features, 3 * width)
    params = packed_all[:, :, :shard, :8].astype(F32).reshape(features, 8).T
    gain_one, shift_one, bias_query, bias_value, bias_proj, gain_two, shift_two, bias_down = [
        params[i : i + 1] for i in range(8)
    ]
    bias_up = lax.dynamic_index_in_dim(packed_all[:, :, shard, :unit], core, 1, keepdims=False)
    bias_up = bias_up.astype(F32).reshape(1, hidden)
    proj_cols = proj_all.reshape(2, width, width)
    proj_own = lax.dynamic_index_in_dim(proj_cols, core, 0, keepdims=False)
    proj_other = swap(lax.dynamic_index_in_dim(proj_cols, 1 - core, 0, keepdims=False))
    weight_proj = by_core(core, proj_own, proj_other, 1)
    qkv_bias = jnp.concatenate(
        [
            lax.dynamic_slice_in_dim(bias_query, core * width, width, 1),
            jnp.zeros((1, width), F32),
            lax.dynamic_slice_in_dim(bias_value, core * width, width, 1),
        ],
        1,
    )

    own_tokens = tokens.reshape(own_rows, features)
    other_tokens = swap(own_tokens)
    marks = jnp.stack([valid_slots, swap(valid_slots)])
    own_cotangent = cotangent.reshape(own_rows, features)
    penalty = jnp.where(marks > 0, 0.0, -1000000000.0).astype(F32)[..., None]
    norm_one, projected = project(own_tokens, other_tokens, gain_one, shift_one, weight_qkv, qkv_bias)
    projected = projected.reshape(2, micro, rows, 3 * width)
    attended, logs = attend(projected, penalty)
    attended_flat = attended.reshape(every, width)
    mixed = swap(product(attended_flat[own_rows:], weight_proj).astype(BF))
    middle, norm_own = second_norm(
        attended_flat, weight_proj, own_tokens, mixed, bias_proj, gain_two, shift_two
    )
    activation, grad_pre, norm_two, grad_out, lifted, lifted_other, passed, passed_other, up_sums = feed(
        norm_own, swap(norm_own), own_cotangent, swap(own_cotangent),
        (marks > 0).astype(F32).reshape(every, 1), feed_weights, bias_up, unit,
    )
    grad_bias_up = up_sums[0]
    passed_other = swap(passed_other)
    lifted_other = swap(lifted_other)

    grad_down = outer(activation, grad_out)
    down_weight_grad = lax.psum_scatter(
        grad_down, AX, scatter_dimension=0, tiled=True, axis_index_groups=same_core_groups()
    )
    grad_middle, grad_low, block_output, second_sums = second_back(
        passed, passed_other, middle, grad_out, lifted, lifted_other, gain_two, bias_down
    )
    block_output = block_output.reshape(micro, rows, features)
    grad_up = outer(norm_two, grad_pre)
    grad_low = jnp.concatenate([grad_low, swap(grad_low)], 0)
    grad_attended = product_right_t(grad_low, weight_proj).astype(BF).reshape(2, micro, rows, width)
    grad_proj = product_left_t(attended_flat, grad_low).astype(BF)
    grad_attended, grad_proj, grad_up = lax.optimization_barrier((grad_attended, grad_proj, grad_up))
    grad_proj_own = lax.dynamic_slice_in_dim(grad_proj, core * width, width, 1)
    grad_proj_other = swap(lax.dynamic_slice_in_dim(grad_proj, (1 - core) * width, width, 1))
    grad_proj = by_core(core, grad_proj_own, grad_proj_other, 0)
    grad_projected, grad_bias = attend_back(projected, penalty, logs, attended, grad_attended)
    grad_projected = grad_projected.reshape(every, 3 * width)

    grad_bias = jnp.sum(grad_bias, axis=0).transpose(1, 0, 2).reshape(2, width)
    grad_bias = by_core(core, grad_bias, jnp.zeros_like(grad_bias), 1)
    sums = [grad_bias, second_sums[2:3], second_sums[:2], second_sums[3:4]]
    up_units = grad_bias_up.astype(BF).reshape(chips, 1, unit)
    up_units = by_core(core, up_units, jnp.zeros_like(up_units), 1).reshape(chips, 2, 1, unit)
    grad_up = grad_up.reshape(chips, 2, shard, hidden)
    grad_proj = grad_proj.reshape(chips, 2, shard, width)
    if devices == 32:
        bias_rows = jnp.pad(up_units, ((0, 0), (0, 0), (0, 15), (0, 0)))
        sums = jnp.concatenate([jnp.zeros((2, features), F32)] + sums, 0)
        up_weight_grad, qkv_weight_grad, proj_weight_grad, packed_sum, tokens_grad = tail(
            grad_up, grad_proj, sums, bias_rows, gain_one, grad_projected, weight_qkv, norm_one, own_tokens, grad_middle
        )
    else:
        passed = swap(product_right_t(grad_projected[own_rows:], weight_qkv).astype(BF))
        grad_qkv = outer(norm_one, grad_projected)
        tokens_grad, first_sums = first_back(
            grad_projected, weight_qkv, passed, own_tokens, grad_middle, gain_one
        )
        sums = jnp.concatenate([first_sums[:2]] + sums, 0)
        sums = sums.astype(BF).T.reshape(chips, 2, shard, 8)
        sums = jnp.pad(sums, ((0, 0), (0, 0), (0, 16), (0, lanes - 8)))
        sums = lax.dynamic_update_slice(sums, up_units, (0, 0, shard, 0))
        up_weight_grad, qkv_weight_grad, proj_weight_grad, packed_sum = scatter_chips(
            [grad_up, grad_qkv.reshape(chips, 2, shard, 3 * width), grad_proj, sums], (chips, 3, 1, "sum")
        )
    tokens_grad = tokens_grad.reshape(micro, rows, features)
    up_weight_grad, qkv_weight_grad, proj_weight_grad, down_weight_grad, vector_sum, up_bias_grad = finish(
        up_weight_grad, qkv_weight_grad, proj_weight_grad, down_weight_grad, packed_sum, shard, unit
    )
    up_bias_grad = up_bias_grad[0]
    return (
        block_output, tokens_grad, vector_sum[0], vector_sum[1], qkv_weight_grad, vector_sum[2], vector_sum[3],
        proj_weight_grad, vector_sum[4], vector_sum[5], vector_sum[6], up_weight_grad, up_bias_grad,
        down_weight_grad, vector_sum[7],
    )


def solution(mesh):
    row = P(None, AX, None)
    vec = P(AX)
    mat = P(AX, None)
    return jax.shard_map(
        per_device,
        mesh=mesh,
        in_specs=(row, P(None, AX), row, vec, vec, mat, vec, vec, mat, vec, vec, vec, mat, vec, mat, vec),
        out_specs=(row, row, vec, vec, mat, vec, vec, mat, vec, vec, vec, mat, vec, mat, vec),
        check_vma=False,
    )
```

```python
import functools

import jax
import jax.numpy as jnp
from jax import lax
from jax.experimental import pallas as pl
from jax.experimental.pallas import tpu as pltpu
from jax.sharding import PartitionSpec as P

AX = "fsdp"
MESH = pl.DeviceIdType.MESH
HEAD = 64
EPSILON = 1e-06
ROOT_HALF = 0.7071067811865476
INV_ROOT_TWO_PI = 0.3989422804014327
BF = jnp.bfloat16
F32 = jnp.float32
PARAM_COLS = 128


def product(left_side, right_side):
    return jnp.dot(left_side, right_side, preferred_element_type=F32)


def product_left_t(left_side, right_side):
    return lax.dot_general(left_side, right_side, (((0,), (0,)), ((), ())), preferred_element_type=F32)


def product_right_t(left_side, right_side):
    return lax.dot_general(left_side, right_side, (((1,), (1,)), ((), ())), preferred_element_type=F32)


def swap(shard):
    return lax.ppermute(shard, AX, [(i, i ^ 1) for i in range(lax.axis_size(AX))])


def same_core_groups():
    count = lax.axis_size(AX)
    return [[i for i in range(count) if i % 2 == core] for core in (0, 1)]


def flip(index, step):
    return index + step - 2 * step * ((index // step) % 2)


def peers_of(me):
    return flip(me, 1), flip(me, 2), flip(me, 4), [flip(me, 8), flip(me, 16), flip(flip(me, 8), 16)]


def zflip(chip, j):
    return [chip, flip(chip, 4), flip(chip, 8), flip(flip(chip, 4), 8)][j]


def meet(peers):
    barrier = pltpu.get_barrier_semaphore()
    for peer in peers:
        pl.semaphore_signal(barrier, inc=1, device_id=(peer,), device_id_type=MESH)
    pl.semaphore_wait(barrier, len(peers))


def gather_kernel(qkv_ref, proj_ref, packed_ref, qkv_out, proj_out, packed_out, local_sem, send_sem, recv_sem):
    me = lax.axis_index(AX)
    chip, core = me // 2, me % 2
    mate, peer_x, peer_y, peers_z = peers_of(me)
    meet([mate, peer_x, peer_y] + peers_z)
    chip_x, chip_y = flip(chip, 1), flip(chip, 2)
    chip_xy = flip(chip_x, 2)
    outs = (qkv_out, packed_out, proj_out)
    count = len(outs)
    width = qkv_ref.shape[1] // 6
    pending = []

    def remote(w, slot, block, target, peer):
        return pltpu.make_async_remote_copy(
            src_ref=block, dst_ref=target, send_sem=send_sem.at[w, slot], recv_sem=recv_sem.at[w, slot],
            device_id=(peer,), device_id_type=MESH,
        )

    def send(w, slot, block, target, peer):
        copy = remote(w, slot, block, target, peer)
        copy.start()
        pending.append(copy)

    def arrive(w, slot, block):
        remote(w, slot, block, block, mate).wait_recv()

    def columns(start, size):
        return pl.ds(pl.multiple_of(start, 128), size)

    def pieces(w, half, target):
        if w == 0:
            return [
                (qkv_ref.at[:, columns((2 * t + half) * width, width)], target.at[:, pl.ds(t * width, width)])
                for t in range(3)
            ]
        if w == 1:
            return [(packed_ref, target)]
        return [(proj_ref.at[:, columns(half * width, width)], target)]

    for w in range(count):
        for source, target in pieces(w, 1 - core, outs[w].at[chip, core]):
            remote(w, 0, source, target, mate).start()
        for source, target in pieces(w, core, outs[w].at[chip, core]):
            pltpu.make_async_copy(source, target, local_sem.at[w]).start()
    for w in range(count):
        own = outs[w].at[chip, core]
        pltpu.make_async_copy(own, own, local_sem.at[w]).wait()
        arrive(w, 0, outs[w].at[chip, 1 - core])
        block = outs[w].at[chip]
        for j in range(3):
            send(w, 1 + j, block, block, peers_z[j])
        send(w, 4, block, block, peer_x)
        send(w, 8, block, block, peer_y)
    for w in range(count):
        for j in (1, 2, 3):
            block = outs[w].at[zflip(chip, j)]
            arrive(w, j, block)
            send(w, 4 + j, block, block, peer_x)
            send(w, 8 + j, block, block, peer_y)
        for j in range(4):
            block = outs[w].at[zflip(chip_x, j)]
            arrive(w, 4 + j, block)
            send(w, 12 + j, block.at[0], block.at[0], peer_y)
            block = outs[w].at[zflip(chip_y, j)]
            arrive(w, 8 + j, block)
            send(w, 16 + j, block.at[1], block.at[1], peer_x)
    for w in range(count):
        for j in range(4):
            block = outs[w].at[zflip(chip_xy, j)]
            arrive(w, 12 + j, block.at[0])
            arrive(w, 16 + j, block.at[1])
    for w in range(count):
        own = outs[w].at[chip, core]
        remote(w, 0, own, own, mate).wait_send()
    for copy in pending:
        copy.wait_send()


def gather_chips(qkv, proj, packed):
    devices = lax.axis_size(AX)
    shard, features = proj.shape
    width = features // 2
    if devices != 32:
        core = lax.axis_index(AX) % 2
        split = qkv.reshape(shard, 3, 2, width).transpose(2, 0, 1, 3).reshape(2, shard, 3 * width)
        gathered = []
        for halves in (split, proj.reshape(shard, 2, width).transpose(1, 0, 2), jnp.stack([packed, packed])):
            own = lax.dynamic_index_in_dim(halves, core, 0, keepdims=False)
            other = swap(lax.dynamic_index_in_dim(halves, 1 - core, 0, keepdims=False))
            block = jnp.where(core == 0, jnp.stack([own, other]), jnp.stack([other, own]))
            gathered.append(lax.all_gather(block, AX, axis=0, axis_index_groups=same_core_groups()))
        return gathered
    chips = devices // 2
    return pl.pallas_call(
        gather_kernel,
        out_shape=[
            jax.ShapeDtypeStruct((chips, 2, shard, 3 * width), BF),
            jax.ShapeDtypeStruct((chips, 2, shard, width), BF),
            jax.ShapeDtypeStruct((chips, 2) + packed.shape, BF),
        ],
        in_specs=[pl.BlockSpec(memory_space=pltpu.VMEM)] * 3,
        out_specs=[pl.BlockSpec(memory_space=pl.ANY)] * 3,
        scratch_shapes=[
            pltpu.SemaphoreType.DMA((3,)),
            pltpu.SemaphoreType.DMA((3, 20)),
            pltpu.SemaphoreType.DMA((3, 20)),
        ],
        compiler_params=pltpu.CompilerParams(collective_id=0, has_side_effects=True),
        cost_estimate=pl.CostEstimate(flops=int(4e10), bytes_accessed=int(1.5e8), transcendentals=0),
        name="gather_chips",
    )(qkv, proj, packed)


class Scatter:
    def __init__(self, kinds, ins, outs, scratch):
        count = len(kinds)
        self.kinds, self.ins, self.outs = kinds, ins, outs
        names = ("recv_a", "recv_b", "recv_x", "recv_y", "recv_z", "stage", "land")
        for place, name in enumerate(names):
            setattr(self, name, scratch[place * count : (place + 1) * count])
        self.send_sem, self.recv_sem = scratch[len(names) * count :]
        me = lax.axis_index(AX)
        self.chip, self.core = me // 2, me % 2
        self.mate, self.peer_x, self.peer_y, self.peers_z = peers_of(me)
        chip_x, chip_y = flip(self.chip, 1), flip(self.chip, 2)
        self.own = [zflip(self.chip, j) for j in range(4)]
        self.at_x = [zflip(chip_x, j) for j in range(4)]
        self.at_y = [zflip(chip_y, j) for j in range(4)]
        self.at_xy = [zflip(flip(chip_x, 2), j) for j in range(4)]
        self.sent = []

    def meet(self):
        meet([self.mate, self.peer_x, self.peer_y] + self.peers_z)

    def remote(self, w, slot, block, target, peer):
        return pltpu.make_async_remote_copy(
            src_ref=block, dst_ref=target, send_sem=self.send_sem.at[w, slot], recv_sem=self.recv_sem.at[w, slot],
            device_id=(peer,), device_id_type=MESH,
        )

    def send(self, w, slot, block, target, peer):
        self.remote(w, slot, block, target, peer).start()
        self.sent.append((w, slot))

    def arrive(self, w, slot, block):
        self.remote(w, slot, block, block, self.mate).wait_recv()

    def far(self, w, j):
        block = self.ins[w].at[self.at_xy[j]]
        self.send(w, j, block.at[0], self.recv_a[w].at[j], self.peer_y)
        self.send(w, 4 + j, block.at[1], self.recv_b[w].at[j], self.peer_x)

    def near(self, w, j):
        self.send(w, 8 + j, self.ins[w].at[self.at_x[j], 1], self.recv_x[w].at[j, 1], self.peer_x)
        self.send(w, 12 + j, self.ins[w].at[self.at_y[j], 0], self.recv_y[w].at[j, 0], self.peer_y)

    def strips(self, w, body):
        @pl.loop(0, self.ins[w].shape[2] // 16)
        def _(i):
            body(pl.ds(pl.multiple_of(i * 16, 16), 16))

    def relay(self, w, j):
        for slot, recv, block, half in (
            (j, self.recv_a[w], self.at_x[j], 0),
            (4 + j, self.recv_b[w], self.at_y[j], 1),
        ):
            self.arrive(w, slot, recv.at[j])

            def body(part):
                total = recv[j, part].astype(F32) + self.ins[w][block, half, part].astype(F32)
                recv[j, part] = total.astype(BF)

            self.strips(w, body)
            if half == 0:
                self.send(w, 16 + j, recv.at[j], self.recv_x[w].at[j, 0], self.peer_x)
            else:
                self.send(w, 20 + j, recv.at[j], self.recv_y[w].at[j, 1], self.peer_y)

    def arrive_near(self, w, j):
        self.arrive(w, 8 + j, self.recv_x[w].at[j, 1])
        self.arrive(w, 12 + j, self.recv_y[w].at[j, 0])
        self.arrive(w, 16 + j, self.recv_x[w].at[j, 0])
        self.arrive(w, 20 + j, self.recv_y[w].at[j, 1])

    def near_sum(self, w, j, half, part):
        total = self.recv_x[w][j, half, part].astype(F32) + self.recv_y[w][j, half, part].astype(F32)
        return total + self.ins[w][self.own[j], half, part].astype(F32)

    def cross(self, w, j):
        self.arrive_near(w, j)

        def body(part):
            for half in range(2):
                self.recv_x[w][j, half, part] = self.near_sum(w, j, half, part).astype(BF)

        self.strips(w, body)
        self.send(w, 23 + j, self.recv_x[w].at[j], self.recv_z[w].at[j - 1], self.peers_z[j - 1])

    def place(self, w, part, total, half):
        kind = self.kinds[w]
        if kind == "sum":
            self.outs[w][part] = total
            return
        size = total.shape[1] // kind
        for t in range(kind):
            start = pl.multiple_of((2 * t + half) * size, 128)
            self.outs[w][part, pl.ds(start, size)] = total[:, t * size : (t + 1) * size]

    def last(self, w):
        self.arrive_near(w, 0)
        for j in range(3):
            self.arrive(w, 24 + j, self.recv_z[w].at[j])
        rows = self.ins[w].shape[2]

        def total_of(half, part):
            total = self.near_sum(w, 0, half, part)
            for j in range(3):
                total = total + self.recv_z[w][j, half, part].astype(F32)
            return total

        if self.kinds[w] == "rows":

            @pl.loop(0, rows // 16)
            def _(i):
                for half in range(2):
                    part = pl.ds(pl.multiple_of(i * 16, 16), 16)
                    self.outs[w][pl.ds(pl.multiple_of(half * rows + i * 16, 16), 16)] = total_of(half, part)

            return

        def other(part):
            self.stage[w][part] = total_of(1 - self.core, part)

        self.strips(w, other)
        self.send(w, 27, self.stage[w], self.land[w], self.mate)
        self.strips(w, lambda part: self.place(w, part, total_of(self.core, part), self.core))

    def finish(self, w):
        self.arrive(w, 27, self.land[w])

        def body(part):
            other = self.land[w][part]
            if self.kinds[w] == "sum":
                other = other + self.outs[w][part]
            self.place(w, part, other, 1 - self.core)

        self.strips(w, body)

    def drain(self):
        for w, slot in self.sent:
            if slot == 27:
                block = self.stage[w]
            elif slot >= 24:
                block = self.recv_x[w].at[0]
            else:
                block = self.recv_a[w].at[0]
            self.remote(w, slot, block, block, self.mate).wait_send()

    def opening(self, w):
        self.far(w, 1), self.far(w, 2), self.near(w, 1)

    def run(self):
        small = range(2, len(self.kinds))
        opening = self.opening
        self.meet()
        opening(0)
        for w in small:
            for j in (1, 2, 3, 0):
                self.far(w, j), self.near(w, j)
        self.relay(0, 1), self.far(0, 3), self.near(0, 2)
        self.relay(0, 2), self.far(0, 0), self.near(0, 3)
        for w in small:
            for j in (1, 2, 3, 0):
                self.relay(w, j)
        self.relay(0, 3), self.near(0, 0), self.cross(0, 1)
        opening(1)
        for w in small:
            for j in (1, 2, 3):
                self.cross(w, j)
        self.relay(0, 0), self.cross(0, 2), self.cross(0, 3)
        self.relay(1, 1), self.far(1, 3), self.near(1, 2)
        self.relay(1, 2), self.far(1, 0), self.near(1, 3)
        for w in small:
            self.last(w)
        self.relay(1, 3), self.near(1, 0), self.cross(1, 1)
        self.relay(1, 0)
        self.last(0)
        self.cross(1, 2), self.cross(1, 3)
        for w in small:
            self.finish(w)
        self.finish(0)
        self.last(1)
        self.finish(1)
        self.drain()


def scatter_scratch(shapes):
    count = len(shapes)
    scratch = [pltpu.VMEM((4,) + s[2:], BF) for s in shapes] * 2
    scratch += [pltpu.VMEM((4, 2) + s[2:], BF) for s in shapes] * 2
    scratch += [pltpu.VMEM((3, 2) + s[2:], BF) for s in shapes]
    scratch += [pltpu.VMEM(s[2:], F32) for s in shapes] * 2
    return scratch + [pltpu.SemaphoreType.DMA((count, 28)), pltpu.SemaphoreType.DMA((count, 28))]


def scatter_shapes(shapes, kinds):
    factors = {"sum": (1, 1), "rows": (2, 1)}
    sizes = [factors.get(kind, (1, 2)) for kind in kinds]
    return [jax.ShapeDtypeStruct((s[2] * a, s[3] * b), F32) for s, (a, b) in zip(shapes, sizes)]


def scatter_kernel(kinds, *refs):
    count = len(kinds)
    Scatter(kinds, refs[:count], refs[count : 2 * count], refs[2 * count :]).run()


def scatter_chips(grads, kinds):
    devices = lax.axis_size(AX)
    shapes = [g.shape for g in grads]
    if devices != 32:
        core = lax.axis_index(AX) % 2
        summed = []
        for grad, kind in zip(grads, kinds):
            block = lax.psum_scatter(grad, AX, scatter_dimension=0, axis_index_groups=same_core_groups())
            block = block.astype(F32)
            own = lax.dynamic_index_in_dim(block, core, 0, keepdims=False)
            other = swap(lax.dynamic_index_in_dim(block, 1 - core, 0, keepdims=False))
            if kind == "sum":
                summed.append(own + other)
                continue
            rows, columns = own.shape
            own = own.reshape(rows, kind, 1, columns // kind)
            other = other.reshape(rows, kind, 1, columns // kind)
            summed.append(by_core(core, own, other, 2).reshape(rows, 2 * columns))
        return summed
    count = len(grads)
    return pl.pallas_call(
        functools.partial(scatter_kernel, kinds),
        out_shape=scatter_shapes(shapes, kinds),
        in_specs=[pl.BlockSpec(memory_space=pltpu.VMEM)] * count,
        out_specs=[pl.BlockSpec(memory_space=pltpu.VMEM)] * count,
        scratch_shapes=scatter_scratch(shapes),
        compiler_params=pltpu.CompilerParams(
            collective_id=1, has_side_effects=True, vmem_limit_bytes=56 << 20
        ),
        name="scatter_chips",
    )(*grads)


def flat(ref):
    return ref[...].reshape(-1, ref.shape[-1])


def head_masks():
    lane = lax.broadcasted_iota(jnp.int32, (1, 2 * HEAD), 1)
    return [(lane < HEAD).astype(BF), (lane >= HEAD).astype(BF)]


def attend_kernel(chunk, q_ref, k_ref, v_ref, penalty_ref, out_ref, log_ref, query_buf, mixed_buf):
    query_buf[...] = flat(q_ref) * jnp.asarray(0.125, BF)
    keys, values = flat(k_ref), flat(v_ref)
    values_t = values.T
    penalty = flat(penalty_ref)
    masks = head_masks()

    @pl.loop(0, query_buf.shape[0] // chunk)
    def _(i):
        part = pl.ds(pl.multiple_of(i * chunk, chunk), chunk)
        queries = query_buf[part]
        parts = []
        for h in range(2):
            scores = product_right_t(keys, queries * masks[h]) + penalty
            top = jnp.max(scores, axis=0, keepdims=True)
            exponent = jnp.exp(scores - top)
            total = jnp.sum(exponent, axis=0, keepdims=True)
            mixed = product(values_t[h * HEAD : (h + 1) * HEAD], exponent.astype(BF))
            parts.append(mixed * (1.0 / total))
            log_ref[0, 0, h : h + 1, part] = top + jnp.log(total)
        mixed_buf[part] = jnp.concatenate(parts, 0).T.astype(BF)

    out_ref[...] = mixed_buf[...].reshape(out_ref.shape)


def attend(projected, penalty):
    _, clips, rows, triple = projected.shape
    slots = 2 * rows
    width = triple // 3
    pairs = width // (2 * HEAD)

    def block(offset):
        return pl.BlockSpec((2, 1, rows, 2 * HEAD), lambda i, j: (0, i, 0, offset * pairs + j))

    return pl.pallas_call(
        functools.partial(attend_kernel, 256),
        grid=(clips, pairs),
        in_specs=[block(0), block(1), block(2), pl.BlockSpec((2, 1, rows, 1), lambda i, j: (0, i, 0, 0))],
        out_specs=[block(0), pl.BlockSpec((1, 1, 2, slots), lambda i, j: (i, j, 0, 0))],
        out_shape=[
            jax.ShapeDtypeStruct((2, clips, rows, width), BF),
            jax.ShapeDtypeStruct((clips, pairs, 2, slots), F32),
        ],
        scratch_shapes=[pltpu.VMEM((slots, 2 * HEAD), BF)] * 2,
        compiler_params=pltpu.CompilerParams(vmem_limit_bytes=48 << 20),
        cost_estimate=pl.CostEstimate(
            flops=4 * clips * pairs * slots * slots * 2 * HEAD, bytes_accessed=8 * clips * slots * width,
            transcendentals=clips * pairs * 2 * slots * slots,
        ),
        name="attend",
    )(projected, projected, projected, penalty)


def attend_back_kernel(chunk, *refs):
    if len(refs) == 16:
        attend_back_step(chunk, *refs)
        return
    inputs, (down_ref, norm_hbm, pre_hbm), (back_out, bias_out, down_out, up_out) = refs[:7], refs[7:10], refs[10:14]
    buffers, (norm, pre, load_sem), scratch = refs[14:21], refs[21:24], refs[24:]
    scatter = Scatter(("rows",), (down_ref,), (down_out,), scratch)
    step = pl.program_id(0) * pl.num_programs(1) + pl.program_id(1)
    total = pl.num_programs(0) * pl.num_programs(1)

    def start():
        pltpu.make_async_copy(norm_hbm, norm, load_sem.at[0]).start()
        pltpu.make_async_copy(pre_hbm, pre, load_sem.at[1]).start()
        scatter.meet()
        scatter.opening(0)

    def two():
        scatter.relay(0, 1), scatter.far(0, 3), scatter.near(0, 2)

    def four():
        scatter.relay(0, 2), scatter.far(0, 0), scatter.near(0, 3), scatter.cross(0, 1)

    def five():
        scatter.relay(0, 3), scatter.near(0, 0)

    def six():
        scatter.cross(0, 2)

    def seven():
        scatter.relay(0, 0)

    def end():
        scatter.cross(0, 3)
        pltpu.make_async_copy(norm_hbm, norm, load_sem.at[0]).wait()
        pltpu.make_async_copy(pre_hbm, pre, load_sem.at[1]).wait()

        @pl.loop(0, norm.shape[1] // 256)
        def _(i):
            part = pl.ds(pl.multiple_of(i * 256, 256), 256)
            up_out[part] = product_left_t(norm[:, part], pre[...]).astype(BF)

        scatter.last(0)
        scatter.drain()

    for place, work in ((0, start), (2, two), (4, four), (5, five), (6, six), (7, seven)):
        pl.when(step == place)(work)
    attend_back_step(chunk, *inputs, back_out, bias_out, *buffers)
    pl.when(step == total - 1)(end)


def attend_back_step(
    chunk, q_ref, k_ref, v_ref, penalty_ref, log_ref, att_ref, grad_ref, out_ref, bias_ref,
    query_buf, grad_buf, mixed_buf, back_buf, key_sum, value_sum, bias_sum,
):
    rows = q_ref.shape[2]
    pair = pl.program_id(1)
    width = out_ref.shape[3] // 3
    query_buf[...] = flat(q_ref) * jnp.asarray(0.125, BF)
    grad_buf[...] = flat(grad_ref)
    mixed_buf[...] = flat(att_ref)
    keys, values = flat(k_ref), flat(v_ref)
    keys_t = keys.T
    penalty = flat(penalty_ref)
    masks = head_masks()
    for total in (key_sum, value_sum, bias_sum):
        total[...] = jnp.zeros_like(total)

    def keep(offset, value):
        columns = pl.ds(pl.multiple_of(offset + pair * 2 * HEAD, 128), 2 * HEAD)
        for side in range(2):
            out_ref[side, 0, :, columns] = value[side * rows : (side + 1) * rows]

    for start in range(0, query_buf.shape[0], chunk):
        part = pl.ds(start, chunk)
        queries, grads = query_buf[part], grad_buf[part]
        overlap = (grads.astype(F32) * mixed_buf[part].astype(F32)).T
        parts = []
        for h in range(2):
            head_queries = queries * masks[h]
            head_grads = grads * masks[h]
            correction = jnp.sum(overlap[h * HEAD : (h + 1) * HEAD], axis=0, keepdims=True)
            logs = log_ref[0, 0, h : h + 1, part]
            soft = jnp.exp(product_right_t(keys, head_queries) + penalty - logs)
            grad_soft = product_right_t(values, head_grads)
            value_sum[...] += product(soft.astype(BF), head_grads)
            grad_scores = (soft * (grad_soft - correction)).astype(BF)
            key_sum[...] += product(grad_scores, head_queries)
            parts.append(product(keys_t[h * HEAD : (h + 1) * HEAD], grad_scores))
        grad_queries = jnp.concatenate(parts, 0).T * 0.125
        bias_sum[0:1] += jnp.sum(grad_queries, axis=0, keepdims=True)
        back_buf[part] = grad_queries.astype(BF)

    keep(0, back_buf[...])
    keep(width, key_sum[...].astype(BF))
    keep(2 * width, value_sum[...].astype(BF))
    bias_ref[0, 0, 0:1] = bias_sum[0:1]
    bias_ref[0, 0, 1:2] = jnp.sum(value_sum[...], axis=0, keepdims=True)


def attend_back(projected, penalty, logs, attended, grad_attended, grad_down, norm_two, grad_pre):
    _, clips, rows, triple = projected.shape
    slots = 2 * rows
    width = triple // 3
    pairs = width // (2 * HEAD)
    fused = lax.axis_size(AX) == 32 and clips * pairs == 8

    def block(offset):
        return pl.BlockSpec((2, 1, rows, 2 * HEAD), lambda i, j: (0, i, 0, offset * pairs + j))

    in_specs = [
        block(0), block(1), block(2),
        pl.BlockSpec((2, 1, rows, 1), lambda i, j: (0, i, 0, 0)),
        pl.BlockSpec((1, 1, 2, slots), lambda i, j: (i, j, 0, 0)),
        block(0), block(0),
    ]
    out_specs = [
        pl.BlockSpec((2, 1, rows, triple), lambda i, j: (0, i, 0, 0)),
        pl.BlockSpec((1, 1, 2, 2 * HEAD), lambda i, j: (i, j, 0, 0)),
    ]
    out_shape = [
        jax.ShapeDtypeStruct((2, clips, rows, triple), BF),
        jax.ShapeDtypeStruct((clips, pairs, 2, 2 * HEAD), F32),
    ]
    operands = [projected, projected, projected, penalty, logs, attended, grad_attended]
    scratch = [pltpu.VMEM((slots, 2 * HEAD), BF)] * 4 + [pltpu.VMEM((slots, 2 * HEAD), F32)] * 2
    scratch += [pltpu.VMEM((8, 2 * HEAD), F32)]
    params = pltpu.CompilerParams(vmem_limit_bytes=60 << 20)
    if fused:
        up_shape = (norm_two.shape[1], grad_pre.shape[1])
        sums = scatter_shapes([grad_down.shape], ("rows",))
        in_specs += [pl.BlockSpec(grad_down.shape, lambda i, j: (0, 0, 0, 0), pipeline_mode=pl.Buffered(1))]
        in_specs += [pl.BlockSpec(memory_space=pl.ANY)] * 2
        out_specs += [pl.BlockSpec(sums[0].shape, lambda i, j: (0, 0)), pl.BlockSpec(up_shape, lambda i, j: (0, 0))]
        out_shape += [sums[0], jax.ShapeDtypeStruct(up_shape, BF)]
        operands += [grad_down, norm_two, grad_pre]
        scratch += [pltpu.VMEM(norm_two.shape, BF), pltpu.VMEM(grad_pre.shape, BF), pltpu.SemaphoreType.DMA((2,))]
        scratch += scatter_scratch([grad_down.shape])
        params = pltpu.CompilerParams(vmem_limit_bytes=60 << 20, collective_id=2, has_side_effects=True)
    outs = pl.pallas_call(
        functools.partial(attend_back_kernel, 256),
        grid=(clips, pairs),
        in_specs=in_specs,
        out_specs=out_specs,
        out_shape=out_shape,
        scratch_shapes=scratch,
        compiler_params=params,
        cost_estimate=pl.CostEstimate(
            flops=10 * clips * pairs * slots * slots * 2 * HEAD, bytes_accessed=18 * clips * slots * width,
            transcendentals=clips * pairs * 2 * slots * slots,
        ),
        name="attend_back",
    )(*operands)
    if not fused:
        total = lax.psum_scatter(grad_down, AX, scatter_dimension=0, axis_index_groups=same_core_groups())
        total = total.astype(F32).reshape(-1, total.shape[-1])
        outs = [*outs, total, outer(norm_two, grad_pre)]
    return outs


def normal_parts(values):
    average = jnp.mean(values, axis=-1, keepdims=True)
    centered = values - average
    inverse = lax.rsqrt(jnp.mean(centered * centered, axis=-1, keepdims=True) + EPSILON)
    return centered * inverse, inverse


def normal_back(grad_normed, scaled, inverse, gain):
    grad_scaled = grad_normed * gain
    first_mean = jnp.mean(grad_scaled, axis=-1, keepdims=True)
    second_mean = jnp.mean(grad_scaled * scaled, axis=-1, keepdims=True)
    return inverse * (grad_scaled - first_mean - scaled * second_mean)


def rows_spec(size, columns):
    return pl.BlockSpec((size, columns), lambda i: (i, 0))


def whole_spec(shape):
    return pl.BlockSpec(shape, lambda i: (0,) * len(shape), pipeline_mode=pl.Buffered(1))


PARAMS = pltpu.CompilerParams(vmem_limit_bytes=56 << 20)


def strips_of(ref):
    return [pl.ds(start, 32) for start in range(0, ref.shape[0], 32)]


def project_kernel(steps, own_ref, other_ref, gain_ref, shift_ref, weight_ref, bias_ref, norm_ref, out_ref):
    is_own = pl.program_id(0) < steps
    for part in strips_of(own_ref):
        rows = jnp.where(is_own, own_ref[part].astype(F32), other_ref[part].astype(F32))
        scaled, _ = normal_parts(rows)
        norm_ref[part] = (scaled * gain_ref[...] + shift_ref[...]).astype(BF)
    out_ref[...] = (product(norm_ref[...], weight_ref[...]) + bias_ref[...]).astype(BF)


def project(own, other, gain, shift, weight, bias):
    rows, features = own.shape
    columns = weight.shape[1]
    steps = 3
    size = rows // steps
    return pl.pallas_call(
        functools.partial(project_kernel, steps),
        grid=(2 * steps,),
        in_specs=[
            pl.BlockSpec((size, features), lambda i: (jnp.minimum(i, steps - 1), 0)),
            pl.BlockSpec((size, features), lambda i: (jnp.maximum(i - steps, 0), 0)),
            whole_spec((1, features)),
            whole_spec((1, features)),
            whole_spec((features, columns)),
            whole_spec((1, columns)),
        ],
        out_specs=[rows_spec(size, features), rows_spec(size, columns)],
        out_shape=[
            jax.ShapeDtypeStruct((2 * rows, features), BF),
            jax.ShapeDtypeStruct((2 * rows, columns), BF),
        ],
        compiler_params=PARAMS,
        name="project",
    )(own, other, gain, shift, weight, bias)


def second_norm_kernel(att_ref, weight_ref, token_ref, recv_ref, bias_ref, gain_ref, shift_ref, middle_ref, out_ref):
    mixed = product(att_ref[...], weight_ref[...])
    for part in strips_of(token_ref):
        middle = token_ref[part].astype(F32) + mixed[part.start : part.start + part.size]
        middle = middle + recv_ref[part].astype(F32) + bias_ref[...]
        middle_ref[part] = middle
        scaled, _ = normal_parts(middle)
        out_ref[part] = (scaled * gain_ref[...] + shift_ref[...]).astype(BF)


def second_norm(attended, weight, tokens, received, bias, gain, shift):
    rows, features = tokens.shape
    width = weight.shape[0]
    size = rows // 4
    return pl.pallas_call(
        second_norm_kernel,
        grid=(4,),
        in_specs=[
            rows_spec(size, width), whole_spec((width, features)), rows_spec(size, features), rows_spec(size, features),
            whole_spec((1, features)), whole_spec((1, features)), whole_spec((1, features)),
        ],
        out_specs=[rows_spec(size, features), rows_spec(size, features)],
        out_shape=[jax.ShapeDtypeStruct((rows, features), F32), jax.ShapeDtypeStruct((rows, features), BF)],
        compiler_params=PARAMS,
        name="second_norm",
    )(attended, weight, tokens, received, bias, gain, shift)


def feed_kernel(
    steps, unit, own_ref, other_ref, grad_own_ref, grad_other_ref, mark_ref, bias_ref, *refs
):
    if len(refs) == 14:
        both_ref, refs = refs[0], refs[1:]
        sources = None
    else:
        sources, refs = refs[:2], refs[2:]
    act_ref, pre_ref, norm_ref, grad_ref, pass_own_ref, pass_other_ref, sums_ref, down_hbm = refs[:8]
    up_ref, down_ref, up_sem, down_sem, out_sem = refs[8:]
    step = pl.program_id(0)
    features, hidden = up_ref.shape

    @pl.when(step == 0)
    def _():
        sums_ref[...] = jnp.zeros_like(sums_ref)
        if sources is not None:
            pltpu.make_async_copy(sources[0], up_ref, up_sem).start()
            pltpu.make_async_copy(sources[1], down_ref, down_sem).start()
        else:
            core = lax.axis_index(AX) % 2
            chips = hidden // unit
            shard = features // (2 * chips)
            for k in range(chips):
                device = 2 * k + core
                pltpu.make_async_copy(
                    both_ref.at[:, pl.ds(pl.multiple_of(device * unit, 128), unit)],
                    up_ref.at[:, k * unit : (k + 1) * unit],
                    up_sem,
                ).start()
            for k in range(chips):
                device = 2 * k + core
                for q in range(unit // shard):
                    pltpu.make_async_copy(
                        both_ref.at[
                            pl.ds(pl.multiple_of(device * shard, 16), shard),
                            pl.ds(2 * hidden + q * features, features),
                        ],
                        down_ref.at[k * unit + q * shard : k * unit + (q + 1) * shard],
                        down_sem,
                    ).start()
        pltpu.make_async_copy(up_ref, up_ref, up_sem).wait()
        pltpu.make_async_copy(down_ref, down_ref, down_sem).wait()
        pltpu.make_async_copy(down_ref, down_hbm, out_sem).start()

    rows = jnp.where(step < steps, other_ref[...], own_ref[...])
    grads = jnp.where(step < steps, grad_other_ref[...], grad_own_ref[...]) * mark_ref[...].astype(BF)
    norm_ref[...] = rows
    grad_ref[...] = grads
    size = 512
    for start in range(0, hidden, size):
        part = slice(start, start + size)
        pre = product(rows, up_ref[:, part]) + bias_ref[:, part]
        normal_cdf = 0.5 * (1.0 + lax.erf(pre * ROOT_HALF))
        density = jnp.exp(-0.5 * pre * pre) * INV_ROOT_TWO_PI
        act_ref[:, part] = (pre * normal_cdf).astype(BF)
        grad_pre = product_right_t(grads, down_ref[part]) * (normal_cdf + pre * density)
        sums_ref[0:1, part] += jnp.sum(grad_pre, axis=0, keepdims=True)
        pre_ref[:, part] = grad_pre.astype(BF)
    passed = product_right_t(pre_ref[...], up_ref[...])
    pass_own_ref[...] = passed

    @pl.when(step < steps)
    def _():
        pass_other_ref[...] = passed.astype(BF)

    @pl.when(step == 2 * steps - 1)
    def _():
        pltpu.make_async_copy(down_ref, down_hbm, out_sem).wait()


def feed(own, other, grad_own, grad_other, marks, weights, bias, unit):
    rows, features = own.shape
    hidden = bias.shape[1]
    steps = 3
    size = rows // steps

    def side(i):
        return jnp.where(i < steps, i + steps, i - steps)

    def both_spec(columns):
        return pl.BlockSpec((size, columns), lambda i: (side(i), 0))

    own_spec = pl.BlockSpec((size, features), lambda i: (jnp.maximum(i - steps, 0), 0))
    other_spec = pl.BlockSpec((size, features), lambda i: (jnp.minimum(i, steps - 1), 0))
    return pl.pallas_call(
        functools.partial(feed_kernel, steps, unit),
        grid=(2 * steps,),
        in_specs=[own_spec, other_spec, own_spec, other_spec, both_spec(1), whole_spec((1, hidden))]
        + [pl.BlockSpec(memory_space=pl.ANY)] * len(weights),
        out_specs=[
            both_spec(hidden), both_spec(hidden), both_spec(features), both_spec(features),
            own_spec, other_spec,
            pl.BlockSpec((8, hidden), lambda i: (0, 0)), pl.BlockSpec(memory_space=pl.ANY),
        ],
        out_shape=[
            jax.ShapeDtypeStruct((2 * rows, hidden), BF), jax.ShapeDtypeStruct((2 * rows, hidden), BF),
            jax.ShapeDtypeStruct((2 * rows, features), BF), jax.ShapeDtypeStruct((2 * rows, features), BF),
            jax.ShapeDtypeStruct((rows, features), F32), jax.ShapeDtypeStruct((rows, features), BF),
            jax.ShapeDtypeStruct((8, hidden), F32), jax.ShapeDtypeStruct((hidden, features), BF),
        ],
        scratch_shapes=[
            pltpu.VMEM((features, hidden), BF), pltpu.VMEM((hidden, features), BF),
            pltpu.SemaphoreType.DMA(()), pltpu.SemaphoreType.DMA(()), pltpu.SemaphoreType.DMA(()),
        ],
        compiler_params=PARAMS,
        cost_estimate=pl.CostEstimate(
            flops=12 * rows * features * hidden, bytes_accessed=8 * features * hidden,
            transcendentals=4 * rows * hidden,
        ),
        name="feed",
    )(own, other, grad_own, grad_other, marks, bias, *weights)


def outer_kernel(left_ref, right_ref, out_ref):
    out_ref[...] = product_left_t(left_ref[...], right_ref[...]).astype(BF)


def outer(left, right):
    rows, columns = left.shape
    width = right.shape[1]
    size = 256
    return pl.pallas_call(
        outer_kernel,
        grid=(columns // size,),
        in_specs=[pl.BlockSpec((rows, size), lambda i: (0, i)), whole_spec((rows, width))],
        out_specs=rows_spec(size, width),
        out_shape=jax.ShapeDtypeStruct((columns, width), BF),
        compiler_params=PARAMS,
        cost_estimate=pl.CostEstimate(
            flops=2 * rows * columns * width, bytes_accessed=2 * (rows * columns + rows * width + columns * width),
            transcendentals=0,
        ),
        name="outer",
    )(left, right)


def gather_sums(sums_ref, values):
    for index, value in enumerate(values):
        sums_ref[index : index + 1] += jnp.sum(value, axis=0, keepdims=True)


def clear_first(sums_ref):
    @pl.when(pl.program_id(0) == 0)
    def _():
        sums_ref[...] = jnp.zeros_like(sums_ref)


def second_back_kernel(
    grad_ref, recv_ref, middle_ref, out_ref, gain_ref, full_ref, low_ref, sums_ref
):
    clear_first(sums_ref)
    for part in strips_of(grad_ref):
        grad_normed = grad_ref[part] + recv_ref[part].astype(F32)
        scaled, inverse = normal_parts(middle_ref[part])
        grad_out = out_ref[part].astype(F32)
        grad_middle = grad_out + normal_back(grad_normed, scaled, inverse, gain_ref[...])
        full_ref[part] = grad_middle
        low_ref[part] = grad_middle.astype(BF)
        gather_sums(sums_ref, [grad_normed * scaled, grad_normed, grad_middle, grad_out])


def second_back(passed, received, middle, grad_out, gain):
    rows, features = middle.shape
    size = rows // 4
    return pl.pallas_call(
        second_back_kernel,
        grid=(4,),
        in_specs=[rows_spec(size, features)] * 4 + [whole_spec((1, features))],
        out_specs=[rows_spec(size, features)] * 2 + [pl.BlockSpec((8, features), lambda i: (0, 0))],
        out_shape=[
            jax.ShapeDtypeStruct((rows, features), F32), jax.ShapeDtypeStruct((rows, features), BF),
            jax.ShapeDtypeStruct((8, features), F32),
        ],
        compiler_params=PARAMS,
        name="second_back",
    )(passed, received, middle, grad_out, gain)


def first_back_kernel(grad_ref, weight_ref, recv_ref, token_ref, middle_ref, gain_ref, full_ref, sums_ref):
    clear_first(sums_ref)
    passed = product_right_t(grad_ref[...], weight_ref[...])
    for part in strips_of(grad_ref):
        grad_normed = passed[part.start : part.start + part.size] + recv_ref[part].astype(F32)
        scaled, inverse = normal_parts(token_ref[part].astype(F32))
        full_ref[part] = middle_ref[part] + normal_back(grad_normed, scaled, inverse, gain_ref[...])
        gather_sums(sums_ref, [grad_normed * scaled, grad_normed])


def first_back(grad_projected, weight, received, tokens, grad_middle, gain):
    rows, features = tokens.shape
    triple = weight.shape[1]
    size = rows // 4
    return pl.pallas_call(
        first_back_kernel,
        grid=(4,),
        in_specs=[
            rows_spec(size, triple), whole_spec((features, triple)), rows_spec(size, features),
            rows_spec(size, features), rows_spec(size, features), whole_spec((1, features)),
        ],
        out_specs=[rows_spec(size, features), pl.BlockSpec((8, features), lambda i: (0, 0))],
        out_shape=[jax.ShapeDtypeStruct((rows, features), F32), jax.ShapeDtypeStruct((8, features), F32)],
        compiler_params=PARAMS,
        name="first_back",
    )(grad_projected, weight, received, tokens, grad_middle, gain)


def tail_kernel(
    kinds, up_ref, proj_ref, sums_ref, bias_ref, gain_ref, shift_ref,
    back_hbm, weight_hbm, norm_hbm, token_hbm, middle_hbm, down_hbm, act_hbm, sum_hbm,
    up_out, qkv_out, proj_out, packed_out, tokens_out, block_out, *refs
):
    back, weight, norm, token, middle, down, qkv, packed, vectors, stage, land, load_sem, pass_sem = refs[:13]
    act, total, lift_stage, lift_land, block_sem = refs[13:18]
    scatter = Scatter(kinds, (up_ref, qkv, proj_ref, packed), (up_out, qkv_out, proj_out, packed_out), refs[18:])
    chips, _, shard, triple = qkv.shape
    own_rows = token.shape[0]
    loads = [
        pltpu.make_async_copy(source, target, load_sem.at[i])
        for i, (source, target) in enumerate(
            (
                (back_hbm, back), (weight_hbm, weight), (norm_hbm, norm), (token_hbm, token), (middle_hbm, middle),
                (down_hbm, down),
            )
        )
    ]
    for load in loads:
        load.start()
    scatter.meet()
    scatter.opening(0)
    for j in (1, 2, 3, 0):
        scatter.far(2, j), scatter.near(2, j)
    vectors[...] = jnp.zeros_like(vectors)
    vectors[0:8] = sums_ref[...]
    loads[0].wait(), loads[1].wait()

    @pl.loop(0, own_rows // 256)
    def _(i):
        part = pl.ds(pl.multiple_of(own_rows + i * 256, 256), 256)
        stage[pl.ds(pl.multiple_of(i * 256, 256), 256)] = product_right_t(back[part], weight[...]).astype(BF)

    passing = pltpu.make_async_remote_copy(
        src_ref=stage, dst_ref=land, send_sem=pass_sem.at[0], recv_sem=pass_sem.at[1],
        device_id=(scatter.mate,), device_id_type=MESH,
    )
    passing.start()
    scatter.relay(0, 1), scatter.far(0, 3), scatter.near(0, 2)
    loads[2].wait()

    @pl.loop(0, norm.shape[1] // 256)
    def _(i):
        part = pl.ds(pl.multiple_of(i * 256, 256), 256)
        count = 256 // (2 * shard)
        grad = product_left_t(norm[:, part], back[...]).astype(BF)
        qkv[pl.ds(i * count, count)] = grad.reshape(count, 2, shard, triple)

    scatter.relay(0, 2), scatter.far(0, 0), scatter.near(0, 3)
    for j in (1, 2, 3, 0):
        scatter.relay(2, j)
    scatter.opening(1)
    loads[3].wait(), loads[4].wait()
    passing.wait()

    @pl.loop(0, own_rows // 256)
    def _(i):
        start = pl.multiple_of(i * 256, 256)
        passed = product_right_t(back[pl.ds(start, 256)], weight[...])
        for strip in range(0, 256, 32):
            part = pl.ds(start + strip, 32)
            grad_normed = passed[strip : strip + 32] + land[part].astype(F32)
            scaled, inverse = normal_parts(token[part].astype(F32))
            tokens_out[part] = middle[part] + normal_back(grad_normed, scaled, inverse, gain_ref[...])
            vectors[0:1] += jnp.sum(grad_normed * scaled, axis=0, keepdims=True)
            vectors[1:2] += jnp.sum(grad_normed, axis=0, keepdims=True)

    scatter.relay(0, 3), scatter.near(0, 0), scatter.cross(0, 1), scatter.cross(0, 2)
    packed[:, :, :shard] = vectors[...].T.astype(BF).reshape(chips, 2, shard, PARAM_COLS)
    packed[:, :, shard:] = bias_ref[...]
    for j in (1, 2, 3, 0):
        scatter.far(3, j), scatter.near(3, j)
    scatter.relay(0, 0), scatter.cross(0, 3)
    for j in (1, 2, 3):
        scatter.cross(2, j)
    loads[5].wait()

    def fetch(source, start, target, slot):
        copy = pltpu.make_async_copy(source.at[pl.ds(start, 256)], target, block_sem.at[slot])
        copy.start()
        return copy

    @pl.loop(0, own_rows // 256)
    def _(i):
        fetch(act_hbm, pl.multiple_of(own_rows + i * 256, 256), act, 0).wait()
        lift_stage[pl.ds(pl.multiple_of(i * 256, 256), 256)] = product(act[...], down[...]).astype(BF)

    lifting = pltpu.make_async_remote_copy(
        src_ref=lift_stage, dst_ref=lift_land, send_sem=pass_sem.at[2], recv_sem=pass_sem.at[3],
        device_id=(scatter.mate,), device_id_type=MESH,
    )
    lifting.start()
    scatter.relay(1, 1), scatter.far(1, 3), scatter.near(1, 2)
    scatter.relay(1, 2), scatter.far(1, 0), scatter.near(1, 3)
    lifting.wait()

    @pl.loop(0, own_rows // 256)
    def _(i):
        start = pl.multiple_of(i * 256, 256)
        copies = fetch(act_hbm, start, act, 0), fetch(sum_hbm, start, total, 1)
        for copy in copies:
            copy.wait()
        lifted = product(act[...], down[...]) + lift_land[pl.ds(start, 256)].astype(F32)
        block_out[pl.ds(start, 256)] = (total[...] + lifted + shift_ref[...]).astype(BF)

    for j in (1, 2, 3, 0):
        scatter.relay(3, j)
    scatter.last(2)
    scatter.relay(1, 3), scatter.near(1, 0), scatter.cross(1, 1)
    for j in (1, 2, 3):
        scatter.cross(3, j)
    scatter.relay(1, 0)
    scatter.last(0)
    scatter.cross(1, 2), scatter.cross(1, 3)
    scatter.finish(2), scatter.finish(0)
    scatter.last(3)
    scatter.last(1)
    scatter.finish(3), scatter.finish(1)
    scatter.drain()


def tail(grad_up, grad_proj, sums, bias_rows, gain, shift, back, weight, norm, tokens, grad_middle, down, act, middle):
    chips, _, shard, hidden = grad_up.shape
    rows, triple = back.shape
    own_rows, features = tokens.shape
    extra = bias_rows.shape[2]
    kinds = (chips, 3, 1, "sum")
    shapes = [
        grad_up.shape, (chips, 2, shard, triple), grad_proj.shape, (chips, 2, shard + extra, PARAM_COLS),
    ]
    vmem = pl.BlockSpec(memory_space=pltpu.VMEM)
    return pl.pallas_call(
        functools.partial(tail_kernel, kinds),
        out_shape=scatter_shapes(shapes, kinds)
        + [jax.ShapeDtypeStruct((own_rows, features), F32), jax.ShapeDtypeStruct((own_rows, features), BF)],
        in_specs=[vmem] * 6 + [pl.BlockSpec(memory_space=pl.ANY)] * 8,
        out_specs=[vmem] * 6,
        scratch_shapes=[
            pltpu.VMEM(back.shape, BF), pltpu.VMEM(weight.shape, BF), pltpu.VMEM(norm.shape, BF),
            pltpu.VMEM(tokens.shape, BF), pltpu.VMEM(middle.shape, F32), pltpu.VMEM(down.shape, BF),
            pltpu.VMEM(shapes[1], BF), pltpu.VMEM(shapes[3], BF), pltpu.VMEM((PARAM_COLS, features), F32),
            pltpu.VMEM((own_rows, features), BF), pltpu.VMEM((own_rows, features), BF),
            pltpu.SemaphoreType.DMA((6,)), pltpu.SemaphoreType.DMA((4,)),
            pltpu.VMEM((256, act.shape[1]), BF), pltpu.VMEM((256, features), F32),
            pltpu.VMEM((own_rows, features), BF), pltpu.VMEM((own_rows, features), BF), pltpu.SemaphoreType.DMA((2,)),
        ]
        + scatter_scratch(shapes),
        compiler_params=pltpu.CompilerParams(collective_id=1, has_side_effects=True, vmem_limit_bytes=62 << 20),
        name="tail",
    )(grad_up, grad_proj, sums, bias_rows, gain, shift, back, weight, norm, tokens, grad_middle, down, act, middle)


def pack_kernel(up_ref, down_ref, out_ref):
    shard, columns = up_ref.shape
    features = down_ref.shape[1]
    out_ref[:, :columns] = up_ref[...]
    for i in range(down_ref.shape[0] // shard):
        out_ref[:, columns + i * features : columns + (i + 1) * features] = down_ref[i * shard : (i + 1) * shard]


def pack(up, down):
    shard, columns = up.shape
    fold = down.shape[0] // shard
    if shard % 16 != 0:
        return jnp.concatenate([up] + [down[shard * i : shard * (i + 1)] for i in range(fold)], 1)
    return pl.pallas_call(
        pack_kernel,
        out_shape=jax.ShapeDtypeStruct((shard, columns + fold * down.shape[1]), BF),
        in_specs=[pl.BlockSpec(memory_space=pltpu.VMEM)] * 2,
        out_specs=pl.BlockSpec(memory_space=pltpu.VMEM),
        name="pack",
    )(up, down)


def finish_kernel(
    up_ref, qkv_ref, proj_ref, down_ref, token_ref, block_ref, packed_ref,
    up_out, qkv_out, proj_out, down_out, token_out, block_out, vec_out, bias_out,
):
    token_out[...] = token_ref[...]
    block_out[...] = block_ref[...]
    up_out[...] = up_ref[...]
    qkv_out[...] = qkv_ref[...]
    proj_out[...] = proj_ref[...]
    down_out[...] = down_ref[...]
    shard = vec_out.shape[1]
    vec_out[...] = packed_ref[:shard].T[:8]
    bias_out[...] = packed_ref[shard : shard + 1]


def finish(up, qkv, proj, down, tokens, block, packed, shard, unit):
    if lax.axis_size(AX) != 32:
        return up, qkv, proj, down, tokens, block, packed[:shard, :8].T, packed[shard : shard + 1, :unit]
    return pl.pallas_call(
        finish_kernel,
        out_shape=[jax.ShapeDtypeStruct(a.shape, a.dtype) for a in (up, qkv, proj, down, tokens, block)]
        + [jax.ShapeDtypeStruct((8, shard), F32), jax.ShapeDtypeStruct((1, unit), F32)],
        in_specs=[pl.BlockSpec(memory_space=pltpu.VMEM)] * 7,
        out_specs=[pl.BlockSpec(memory_space=pltpu.VMEM)] * 8,
        compiler_params=PARAMS,
        name="finish",
    )(up, qkv, proj, down, tokens, block, packed)


def by_core(core, own, other, axis):
    return jnp.where(core == 0, jnp.concatenate([own, other], axis), jnp.concatenate([other, own], axis))


def per_device(
    tokens, valid_slots, cotangent, first_gain, first_shift, qkv_weight, query_bias, value_bias, proj_weight,
    proj_bias, second_gain, second_shift, up_weight, up_bias, down_weight, down_bias,
):
    devices = lax.axis_size(AX)
    chips = devices // 2
    core = lax.axis_index(AX) % 2
    micro, rows, features = tokens.shape
    shard = qkv_weight.shape[0]
    width = features // 2
    hidden = up_weight.shape[1] // 2
    unit = hidden // chips
    own_rows = micro * rows
    every = 2 * own_rows

    fold = unit // shard
    both_weights = lax.all_gather(pack(up_weight, down_weight), AX, axis=0, tiled=True)
    feed_weights = [both_weights]
    if unit % 128 != 0 or shard % 16 != 0:
        half_up = both_weights[:, : 2 * hidden].reshape(features, chips, 2, unit)
        half_up = lax.dynamic_index_in_dim(half_up, core, 2, keepdims=False).reshape(features, hidden)
        half_down = both_weights[:, 2 * hidden :].reshape(chips, 2, shard, fold, features)
        half_down = lax.dynamic_index_in_dim(half_down, core, 1, keepdims=False)
        half_down = half_down.transpose(0, 2, 1, 3).reshape(hidden, features)
        feed_weights = [half_up, half_down]
    vectors = jnp.stack(
        [first_gain, first_shift, query_bias, value_bias, proj_bias, second_gain, second_shift, down_bias], 0
    )
    lanes = max(PARAM_COLS, unit)
    vectors = jnp.pad(vectors.T, ((0, 16), (0, lanes - 8)))
    packed = lax.dynamic_update_slice(vectors, up_bias[None, :], (shard, 0))
    qkv_all, proj_all, packed_all = gather_chips(qkv_weight, proj_weight, packed)
    weight_qkv = qkv_all.reshape(features, 3 * width)
    params = packed_all[:, :, :shard, :8].astype(F32).reshape(features, 8).T
    gain_one, shift_one, bias_query, bias_value, bias_proj, gain_two, shift_two, bias_down = [
        params[i : i + 1] for i in range(8)
    ]
    bias_up = lax.dynamic_index_in_dim(packed_all[:, :, shard, :unit], core, 1, keepdims=False)
    bias_up = bias_up.astype(F32).reshape(1, hidden)
    proj_cols = proj_all.reshape(2, width, width)
    proj_own = lax.dynamic_index_in_dim(proj_cols, core, 0, keepdims=False)
    proj_other = swap(lax.dynamic_index_in_dim(proj_cols, 1 - core, 0, keepdims=False))
    weight_proj = by_core(core, proj_own, proj_other, 1)
    qkv_bias = jnp.concatenate(
        [
            lax.dynamic_slice_in_dim(bias_query, core * width, width, 1),
            jnp.zeros((1, width), F32),
            lax.dynamic_slice_in_dim(bias_value, core * width, width, 1),
        ],
        1,
    )

    own_tokens = tokens.reshape(own_rows, features)
    other_tokens = swap(own_tokens)
    marks = jnp.stack([valid_slots, swap(valid_slots)])
    own_cotangent = cotangent.reshape(own_rows, features)
    penalty = jnp.where(marks > 0, 0.0, -1000000000.0).astype(F32)[..., None]
    norm_one, projected = project(own_tokens, other_tokens, gain_one, shift_one, weight_qkv, qkv_bias)
    projected = projected.reshape(2, micro, rows, 3 * width)
    attended, logs = attend(projected, penalty)
    attended_flat = attended.reshape(every, width)
    mixed = swap(product(attended_flat[own_rows:], weight_proj).astype(BF))
    middle, norm_own = second_norm(
        attended_flat, weight_proj, own_tokens, mixed, bias_proj, gain_two, shift_two
    )
    activation, grad_pre, norm_two, grad_out, passed, passed_other, up_sums, weight_down = feed(
        norm_own, swap(norm_own), own_cotangent, swap(own_cotangent),
        (marks > 0).astype(F32).reshape(every, 1), feed_weights, bias_up, unit,
    )
    grad_bias_up = up_sums[0]
    passed_other = swap(passed_other)

    grad_down = outer(activation, grad_out)
    passed_other, grad_down = lax.optimization_barrier((passed_other, grad_down))
    grad_middle, grad_low, second_sums = second_back(passed, passed_other, middle, grad_out, gain_two)
    grad_low = jnp.concatenate([grad_low, swap(grad_low)], 0)
    grad_attended = product_right_t(grad_low, weight_proj).astype(BF).reshape(2, micro, rows, width)
    grad_proj = product_left_t(attended_flat, grad_low).astype(BF)
    grad_attended, grad_proj = lax.optimization_barrier((grad_attended, grad_proj))
    grad_proj_own = lax.dynamic_slice_in_dim(grad_proj, core * width, width, 1)
    grad_proj_other = swap(lax.dynamic_slice_in_dim(grad_proj, (1 - core) * width, width, 1))
    grad_proj = by_core(core, grad_proj_own, grad_proj_other, 0)
    grad_projected, grad_bias, down_weight_grad, grad_up = attend_back(
        projected, penalty, logs, attended, grad_attended, grad_down.reshape(chips, 2, unit // 2, features),
        norm_two, grad_pre,
    )
    grad_projected = grad_projected.reshape(every, 3 * width)

    grad_bias = jnp.sum(grad_bias, axis=0).transpose(1, 0, 2).reshape(2, width)
    grad_bias = by_core(core, grad_bias, jnp.zeros_like(grad_bias), 1)
    sums = [grad_bias, second_sums[2:3], second_sums[:2], second_sums[3:4]]
    up_units = grad_bias_up.astype(BF).reshape(chips, 1, unit)
    up_units = by_core(core, up_units, jnp.zeros_like(up_units), 1).reshape(chips, 2, 1, unit)
    grad_up = grad_up.reshape(chips, 2, shard, hidden)
    grad_proj = grad_proj.reshape(chips, 2, shard, width)
    if devices == 32:
        bias_rows = jnp.pad(up_units, ((0, 0), (0, 0), (0, 15), (0, 0)))
        sums = jnp.concatenate([jnp.zeros((2, features), F32)] + sums, 0)
        up_weight_grad, qkv_weight_grad, proj_weight_grad, packed_sum, tokens_grad, block_output = tail(
            grad_up, grad_proj, sums, bias_rows, gain_one, bias_down, grad_projected, weight_qkv, norm_one, own_tokens,
            grad_middle, weight_down, activation, middle,
        )
    else:
        lifted = swap(product(activation[own_rows:], weight_down).astype(BF)).astype(F32)
        block_output = (middle + product(activation[:own_rows], weight_down) + lifted + bias_down).astype(BF)
        passed = swap(product_right_t(grad_projected[own_rows:], weight_qkv).astype(BF))
        grad_qkv = outer(norm_one, grad_projected)
        tokens_grad, first_sums = first_back(
            grad_projected, weight_qkv, passed, own_tokens, grad_middle, gain_one
        )
        sums = jnp.concatenate([first_sums[:2]] + sums, 0)
        sums = sums.astype(BF).T.reshape(chips, 2, shard, 8)
        sums = jnp.pad(sums, ((0, 0), (0, 0), (0, 16), (0, lanes - 8)))
        sums = lax.dynamic_update_slice(sums, up_units, (0, 0, shard, 0))
        up_weight_grad, qkv_weight_grad, proj_weight_grad, packed_sum = scatter_chips(
            [grad_up, grad_qkv.reshape(chips, 2, shard, 3 * width), grad_proj, sums], (chips, 3, 1, "sum")
        )
    (
        up_weight_grad, qkv_weight_grad, proj_weight_grad, down_weight_grad, tokens_grad, block_output,
        vector_sum, up_bias_grad,
    ) = finish(
        up_weight_grad, qkv_weight_grad, proj_weight_grad, down_weight_grad, tokens_grad, block_output,
        packed_sum, shard, unit,
    )
    tokens_grad = tokens_grad.reshape(micro, rows, features)
    block_output = block_output.reshape(micro, rows, features)
    up_bias_grad = up_bias_grad[0]
    return (
        block_output, tokens_grad, vector_sum[0], vector_sum[1], qkv_weight_grad, vector_sum[2], vector_sum[3],
        proj_weight_grad, vector_sum[4], vector_sum[5], vector_sum[6], up_weight_grad, up_bias_grad,
        down_weight_grad, vector_sum[7],
    )


def solution(mesh):
    row = P(None, AX, None)
    vec = P(AX)
    mat = P(AX, None)
    return jax.shard_map(
        per_device,
        mesh=mesh,
        in_specs=(row, P(None, AX), row, vec, vec, mat, vec, vec, mat, vec, vec, vec, mat, vec, mat, vec),
        out_specs=(row, row, vec, vec, mat, vec, vec, mat, vec, vec, vec, mat, vec, mat, vec),
        check_vma=False,
    )
```

```python
import functools

import jax
import jax.numpy as jnp
from jax import lax
from jax.experimental import pallas as pl
from jax.experimental.pallas import tpu as pltpu
from jax.sharding import PartitionSpec as P

AX = "fsdp"
MESH = pl.DeviceIdType.MESH
HEAD = 64
EPSILON = 1e-06
ROOT_HALF = 0.7071067811865476
INV_ROOT_TWO_PI = 0.3989422804014327
BF = jnp.bfloat16
F32 = jnp.float32
PARAM_COLS = 128


def product(left_side, right_side):
    return jnp.dot(left_side, right_side, preferred_element_type=F32)


def product_left_t(left_side, right_side):
    return lax.dot_general(left_side, right_side, (((0,), (0,)), ((), ())), preferred_element_type=F32)


def product_right_t(left_side, right_side):
    return lax.dot_general(left_side, right_side, (((1,), (1,)), ((), ())), preferred_element_type=F32)


def swap(shard):
    return lax.ppermute(shard, AX, [(i, i ^ 1) for i in range(lax.axis_size(AX))])


def same_core_groups():
    count = lax.axis_size(AX)
    return [[i for i in range(count) if i % 2 == core] for core in (0, 1)]


def flip(index, step):
    return index + step - 2 * step * ((index // step) % 2)


def peers_of(me):
    return flip(me, 1), flip(me, 2), flip(me, 4), [flip(me, 8), flip(me, 16), flip(flip(me, 8), 16)]


def zflip(chip, j):
    return [chip, flip(chip, 4), flip(chip, 8), flip(flip(chip, 4), 8)][j]


def meet(peers):
    barrier = pltpu.get_barrier_semaphore()
    for peer in peers:
        pl.semaphore_signal(barrier, inc=1, device_id=(peer,), device_id_type=MESH)
    pl.semaphore_wait(barrier, len(peers))


def gather_kernel(qkv_ref, proj_ref, packed_ref, qkv_out, proj_out, packed_out, local_sem, send_sem, recv_sem):
    me = lax.axis_index(AX)
    chip, core = me // 2, me % 2
    mate, peer_x, peer_y, peers_z = peers_of(me)
    meet([mate, peer_x, peer_y] + peers_z)
    chip_x, chip_y = flip(chip, 1), flip(chip, 2)
    chip_xy = flip(chip_x, 2)
    outs = (qkv_out, packed_out, proj_out)
    count = len(outs)
    width = qkv_ref.shape[1] // 6
    pending = []

    def remote(w, slot, block, target, peer):
        return pltpu.make_async_remote_copy(
            src_ref=block, dst_ref=target, send_sem=send_sem.at[w, slot], recv_sem=recv_sem.at[w, slot],
            device_id=(peer,), device_id_type=MESH,
        )

    def send(w, slot, block, target, peer):
        copy = remote(w, slot, block, target, peer)
        copy.start()
        pending.append(copy)

    def arrive(w, slot, block):
        remote(w, slot, block, block, mate).wait_recv()

    def columns(start, size):
        return pl.ds(pl.multiple_of(start, 128), size)

    def pieces(w, half, target):
        if w == 0:
            return [
                (qkv_ref.at[:, columns((2 * t + half) * width, width)], target.at[:, pl.ds(t * width, width)])
                for t in range(3)
            ]
        if w == 1:
            return [(packed_ref, target)]
        return [(proj_ref.at[:, columns(half * width, width)], target)]

    for w in range(count):
        for source, target in pieces(w, 1 - core, outs[w].at[chip, core]):
            remote(w, 0, source, target, mate).start()
        for source, target in pieces(w, core, outs[w].at[chip, core]):
            pltpu.make_async_copy(source, target, local_sem.at[w]).start()
    for w in range(count):
        own = outs[w].at[chip, core]
        pltpu.make_async_copy(own, own, local_sem.at[w]).wait()
        arrive(w, 0, outs[w].at[chip, 1 - core])
        block = outs[w].at[chip]
        for j in range(3):
            send(w, 1 + j, block, block, peers_z[j])
        send(w, 4, block, block, peer_x)
        send(w, 8, block, block, peer_y)
    for w in range(count):
        for j in (1, 2, 3):
            block = outs[w].at[zflip(chip, j)]
            arrive(w, j, block)
            send(w, 4 + j, block, block, peer_x)
            send(w, 8 + j, block, block, peer_y)
        for j in range(4):
            block = outs[w].at[zflip(chip_x, j)]
            arrive(w, 4 + j, block)
            send(w, 12 + j, block.at[0], block.at[0], peer_y)
            block = outs[w].at[zflip(chip_y, j)]
            arrive(w, 8 + j, block)
            send(w, 16 + j, block.at[1], block.at[1], peer_x)
    for w in range(count):
        for j in range(4):
            block = outs[w].at[zflip(chip_xy, j)]
            arrive(w, 12 + j, block.at[0])
            arrive(w, 16 + j, block.at[1])
    for w in range(count):
        own = outs[w].at[chip, core]
        remote(w, 0, own, own, mate).wait_send()
    for copy in pending:
        copy.wait_send()


def gather_chips(qkv, proj, packed):
    devices = lax.axis_size(AX)
    shard, features = proj.shape
    width = features // 2
    if devices != 32:
        core = lax.axis_index(AX) % 2
        split = qkv.reshape(shard, 3, 2, width).transpose(2, 0, 1, 3).reshape(2, shard, 3 * width)
        gathered = []
        for halves in (split, proj.reshape(shard, 2, width).transpose(1, 0, 2), jnp.stack([packed, packed])):
            own = lax.dynamic_index_in_dim(halves, core, 0, keepdims=False)
            other = swap(lax.dynamic_index_in_dim(halves, 1 - core, 0, keepdims=False))
            block = jnp.where(core == 0, jnp.stack([own, other]), jnp.stack([other, own]))
            gathered.append(lax.all_gather(block, AX, axis=0, axis_index_groups=same_core_groups()))
        return gathered
    chips = devices // 2
    return pl.pallas_call(
        gather_kernel,
        out_shape=[
            jax.ShapeDtypeStruct((chips, 2, shard, 3 * width), BF),
            jax.ShapeDtypeStruct((chips, 2, shard, width), BF),
            jax.ShapeDtypeStruct((chips, 2) + packed.shape, BF),
        ],
        in_specs=[pl.BlockSpec(memory_space=pltpu.VMEM)] * 3,
        out_specs=[pl.BlockSpec(memory_space=pl.ANY)] * 3,
        scratch_shapes=[
            pltpu.SemaphoreType.DMA((3,)),
            pltpu.SemaphoreType.DMA((3, 20)),
            pltpu.SemaphoreType.DMA((3, 20)),
        ],
        compiler_params=pltpu.CompilerParams(collective_id=0, has_side_effects=True),
        cost_estimate=pl.CostEstimate(flops=int(4e10), bytes_accessed=int(1.5e8), transcendentals=0),
        name="gather_chips",
    )(qkv, proj, packed)


class Scatter:
    def __init__(self, kinds, ins, outs, scratch, early=None):
        count = len(kinds)
        self.early = early
        if early is not None:
            self.plane, scratch = scratch[-1], scratch[:-1]
        self.kinds, self.ins, self.outs = kinds, ins, outs
        names = ("recv_a", "recv_b", "recv_x", "recv_y", "recv_z", "stage", "land")
        for place, name in enumerate(names):
            setattr(self, name, scratch[place * count : (place + 1) * count])
        self.send_sem, self.recv_sem = scratch[len(names) * count :]
        me = lax.axis_index(AX)
        self.chip, self.core = me // 2, me % 2
        self.mate, self.peer_x, self.peer_y, self.peers_z = peers_of(me)
        chip_x, chip_y = flip(self.chip, 1), flip(self.chip, 2)
        self.own = [zflip(self.chip, j) for j in range(4)]
        self.at_x = [zflip(chip_x, j) for j in range(4)]
        self.at_y = [zflip(chip_y, j) for j in range(4)]
        self.at_xy = [zflip(flip(chip_x, 2), j) for j in range(4)]
        self.sent = []

    def meet(self):
        meet([self.mate, self.peer_x, self.peer_y] + self.peers_z)

    def remote(self, w, slot, block, target, peer):
        return pltpu.make_async_remote_copy(
            src_ref=block, dst_ref=target, send_sem=self.send_sem.at[w, slot], recv_sem=self.recv_sem.at[w, slot],
            device_id=(peer,), device_id_type=MESH,
        )

    def send(self, w, slot, block, target, peer):
        self.remote(w, slot, block, target, peer).start()
        self.sent.append((w, slot))

    def arrive(self, w, slot, block):
        self.remote(w, slot, block, block, self.mate).wait_recv()

    def source(self, w, chip):
        return (self.plane, chip % 4) if w == self.early else (self.ins[w], chip)

    def along(self, w):
        for j in (1, 2, 3):
            layer = pl.multiple_of(self.own[j] // 4 * 4, 4)
            self.send(w, 23 + j, self.ins[w].at[pl.ds(layer, 4)], self.recv_z[w].at[j - 1], self.peers_z[j - 1])

    def layer_sum(self, w):
        for j in range(3):
            self.arrive(w, 24 + j, self.recv_z[w].at[j])
        layer = self.chip // 4 * 4

        @pl.loop(0, 4)
        def _(block):
            def body(part):
                for half in range(2):
                    total = self.ins[w][layer + block, half, part].astype(F32)
                    for j in range(3):
                        total = total + self.recv_z[w][j, block, half, part].astype(F32)
                    self.plane[block, half, part] = total.astype(BF)

            self.strips(w, body)

    def far(self, w, j):
        ref, at = self.source(w, self.at_xy[j])
        block = ref.at[at]
        self.send(w, j, block.at[0], self.recv_a[w].at[j], self.peer_y)
        self.send(w, 4 + j, block.at[1], self.recv_b[w].at[j], self.peer_x)

    def near(self, w, j):
        ref, at = self.source(w, self.at_x[j])
        self.send(w, 8 + j, ref.at[at, 1], self.recv_x[w].at[j, 1], self.peer_x)
        ref, at = self.source(w, self.at_y[j])
        self.send(w, 12 + j, ref.at[at, 0], self.recv_y[w].at[j, 0], self.peer_y)

    def strips(self, w, body):
        @pl.loop(0, self.ins[w].shape[2] // 16)
        def _(i):
            body(pl.ds(pl.multiple_of(i * 16, 16), 16))

    def relay(self, w, j):
        for slot, recv, block, half in (
            (j, self.recv_a[w], self.at_x[j], 0),
            (4 + j, self.recv_b[w], self.at_y[j], 1),
        ):
            self.arrive(w, slot, recv.at[j])

            ref, at = self.source(w, block)

            def body(part):
                total = recv[j, part].astype(F32) + ref[at, half, part].astype(F32)
                recv[j, part] = total.astype(BF)

            self.strips(w, body)
            if half == 0:
                self.send(w, 16 + j, recv.at[j], self.recv_x[w].at[j, 0], self.peer_x)
            else:
                self.send(w, 20 + j, recv.at[j], self.recv_y[w].at[j, 1], self.peer_y)

    def arrive_near(self, w, j):
        self.arrive(w, 8 + j, self.recv_x[w].at[j, 1])
        self.arrive(w, 12 + j, self.recv_y[w].at[j, 0])
        self.arrive(w, 16 + j, self.recv_x[w].at[j, 0])
        self.arrive(w, 20 + j, self.recv_y[w].at[j, 1])

    def near_sum(self, w, j, half, part):
        total = self.recv_x[w][j, half, part].astype(F32) + self.recv_y[w][j, half, part].astype(F32)
        ref, at = self.source(w, self.own[j])
        return total + ref[at, half, part].astype(F32)

    def cross(self, w, j):
        self.arrive_near(w, j)

        def body(part):
            for half in range(2):
                self.recv_x[w][j, half, part] = self.near_sum(w, j, half, part).astype(BF)

        self.strips(w, body)
        self.send(w, 23 + j, self.recv_x[w].at[j], self.recv_z[w].at[j - 1], self.peers_z[j - 1])

    def place(self, w, part, total, half):
        kind = self.kinds[w]
        if kind == "sum":
            self.outs[w][part] = total
            return
        size = total.shape[1] // kind
        for t in range(kind):
            start = pl.multiple_of((2 * t + half) * size, 128)
            self.outs[w][part, pl.ds(start, size)] = total[:, t * size : (t + 1) * size]

    def last(self, w):
        self.arrive_near(w, 0)
        layers = 0 if w == self.early else 3
        for j in range(layers):
            self.arrive(w, 24 + j, self.recv_z[w].at[j])
        rows = self.ins[w].shape[2]

        def total_of(half, part):
            total = self.near_sum(w, 0, half, part)
            for j in range(layers):
                total = total + self.recv_z[w][j, half, part].astype(F32)
            return total

        if self.kinds[w] == "rows":

            @pl.loop(0, rows // 16)
            def _(i):
                for half in range(2):
                    part = pl.ds(pl.multiple_of(i * 16, 16), 16)
                    self.outs[w][pl.ds(pl.multiple_of(half * rows + i * 16, 16), 16)] = total_of(half, part)

            return

        def other(part):
            self.stage[w][part] = total_of(1 - self.core, part)

        self.strips(w, other)
        self.send(w, 27, self.stage[w], self.land[w], self.mate)
        self.strips(w, lambda part: self.place(w, part, total_of(self.core, part), self.core))

    def finish(self, w):
        self.arrive(w, 27, self.land[w])

        def body(part):
            other = self.land[w][part]
            if self.kinds[w] == "sum":
                other = other + self.outs[w][part]
            self.place(w, part, other, 1 - self.core)

        self.strips(w, body)

    def drain(self):
        for w, slot in self.sent:
            if slot == 27:
                block = self.stage[w]
            elif slot >= 24:
                block = self.recv_z[w].at[0]
            else:
                block = self.recv_a[w].at[0]
            self.remote(w, slot, block, block, self.mate).wait_send()

    def opening(self, w):
        self.far(w, 1), self.far(w, 2), self.near(w, 1)

    def run(self):
        small = range(2, len(self.kinds))
        opening = self.opening
        self.meet()
        opening(0)
        for w in small:
            for j in (1, 2, 3, 0):
                self.far(w, j), self.near(w, j)
        self.relay(0, 1), self.far(0, 3), self.near(0, 2)
        self.relay(0, 2), self.far(0, 0), self.near(0, 3)
        for w in small:
            for j in (1, 2, 3, 0):
                self.relay(w, j)
        self.relay(0, 3), self.near(0, 0), self.cross(0, 1)
        opening(1)
        for w in small:
            for j in (1, 2, 3):
                self.cross(w, j)
        self.relay(0, 0), self.cross(0, 2), self.cross(0, 3)
        self.relay(1, 1), self.far(1, 3), self.near(1, 2)
        self.relay(1, 2), self.far(1, 0), self.near(1, 3)
        for w in small:
            self.last(w)
        self.relay(1, 3), self.near(1, 0), self.cross(1, 1)
        self.relay(1, 0)
        self.last(0)
        self.cross(1, 2), self.cross(1, 3)
        for w in small:
            self.finish(w)
        self.finish(0)
        self.last(1)
        self.finish(1)
        self.drain()


def scatter_scratch(shapes, early=None):
    count = len(shapes)
    scratch = [pltpu.VMEM((4,) + s[2:], BF) for s in shapes] * 2
    scratch += [pltpu.VMEM((4, 2) + s[2:], BF) for s in shapes] * 2
    scratch += [pltpu.VMEM(((3, 4, 2) if w == early else (3, 2)) + s[2:], BF) for w, s in enumerate(shapes)]
    scratch += [pltpu.VMEM(s[2:], F32) for s in shapes] * 2
    scratch += [pltpu.SemaphoreType.DMA((count, 28)), pltpu.SemaphoreType.DMA((count, 28))]
    if early is not None:
        scratch += [pltpu.VMEM((4, 2) + shapes[early][2:], BF)]
    return scratch


def scatter_shapes(shapes, kinds):
    factors = {"sum": (1, 1), "rows": (2, 1)}
    sizes = [factors.get(kind, (1, 2)) for kind in kinds]
    return [jax.ShapeDtypeStruct((s[2] * a, s[3] * b), F32) for s, (a, b) in zip(shapes, sizes)]


def scatter_kernel(kinds, *refs):
    count = len(kinds)
    Scatter(kinds, refs[:count], refs[count : 2 * count], refs[2 * count :]).run()


def scatter_chips(grads, kinds):
    devices = lax.axis_size(AX)
    shapes = [g.shape for g in grads]
    if devices != 32:
        core = lax.axis_index(AX) % 2
        summed = []
        for grad, kind in zip(grads, kinds):
            block = lax.psum_scatter(grad, AX, scatter_dimension=0, axis_index_groups=same_core_groups())
            block = block.astype(F32)
            own = lax.dynamic_index_in_dim(block, core, 0, keepdims=False)
            other = swap(lax.dynamic_index_in_dim(block, 1 - core, 0, keepdims=False))
            if kind == "sum":
                summed.append(own + other)
                continue
            rows, columns = own.shape
            own = own.reshape(rows, kind, 1, columns // kind)
            other = other.reshape(rows, kind, 1, columns // kind)
            summed.append(by_core(core, own, other, 2).reshape(rows, 2 * columns))
        return summed
    count = len(grads)
    return pl.pallas_call(
        functools.partial(scatter_kernel, kinds),
        out_shape=scatter_shapes(shapes, kinds),
        in_specs=[pl.BlockSpec(memory_space=pltpu.VMEM)] * count,
        out_specs=[pl.BlockSpec(memory_space=pltpu.VMEM)] * count,
        scratch_shapes=scatter_scratch(shapes),
        compiler_params=pltpu.CompilerParams(
            collective_id=1, has_side_effects=True, vmem_limit_bytes=56 << 20
        ),
        name="scatter_chips",
    )(*grads)


def flat(ref):
    return ref[...].reshape(-1, ref.shape[-1])


def head_masks():
    lane = lax.broadcasted_iota(jnp.int32, (1, 2 * HEAD), 1)
    return [(lane < HEAD).astype(BF), (lane >= HEAD).astype(BF)]


def attend_kernel(chunk, q_ref, k_ref, v_ref, penalty_ref, out_ref, log_ref, query_buf, mixed_buf):
    query_buf[...] = flat(q_ref) * jnp.asarray(0.125, BF)
    keys, values = flat(k_ref), flat(v_ref)
    values_t = values.T
    penalty = flat(penalty_ref)
    masks = head_masks()

    @pl.loop(0, query_buf.shape[0] // chunk)
    def _(i):
        part = pl.ds(pl.multiple_of(i * chunk, chunk), chunk)
        queries = query_buf[part]
        parts = []
        for h in range(2):
            scores = product_right_t(keys, queries * masks[h]) + penalty
            top = jnp.max(scores, axis=0, keepdims=True)
            exponent = jnp.exp(scores - top)
            total = jnp.sum(exponent, axis=0, keepdims=True)
            mixed = product(values_t[h * HEAD : (h + 1) * HEAD], exponent.astype(BF))
            parts.append(mixed * (1.0 / total))
            log_ref[0, 0, h : h + 1, part] = top + jnp.log(total)
        mixed_buf[part] = jnp.concatenate(parts, 0).T.astype(BF)

    out_ref[...] = mixed_buf[...].reshape(out_ref.shape)


def attend(projected, penalty):
    _, clips, rows, triple = projected.shape
    slots = 2 * rows
    width = triple // 3
    pairs = width // (2 * HEAD)

    def block(offset):
        return pl.BlockSpec((2, 1, rows, 2 * HEAD), lambda i, j: (0, i, 0, offset * pairs + j))

    return pl.pallas_call(
        functools.partial(attend_kernel, 256),
        grid=(clips, pairs),
        in_specs=[block(0), block(1), block(2), pl.BlockSpec((2, 1, rows, 1), lambda i, j: (0, i, 0, 0))],
        out_specs=[block(0), pl.BlockSpec((1, 1, 2, slots), lambda i, j: (i, j, 0, 0))],
        out_shape=[
            jax.ShapeDtypeStruct((2, clips, rows, width), BF),
            jax.ShapeDtypeStruct((clips, pairs, 2, slots), F32),
        ],
        scratch_shapes=[pltpu.VMEM((slots, 2 * HEAD), BF)] * 2,
        compiler_params=pltpu.CompilerParams(vmem_limit_bytes=48 << 20),
        cost_estimate=pl.CostEstimate(
            flops=4 * clips * pairs * slots * slots * 2 * HEAD, bytes_accessed=8 * clips * slots * width,
            transcendentals=clips * pairs * 2 * slots * slots,
        ),
        name="attend",
    )(projected, projected, projected, penalty)


def attend_back_kernel(chunk, *refs):
    if len(refs) == 16:
        attend_back_step(chunk, *refs)
        return
    inputs, (down_ref, norm_hbm, pre_hbm), (back_out, bias_out, down_out, up_out) = refs[:7], refs[7:10], refs[10:14]
    buffers, (norm, pre, load_sem), scratch = refs[14:21], refs[21:24], refs[24:]
    scatter = Scatter(("rows",), (down_ref,), (down_out,), scratch)
    step = pl.program_id(0) * pl.num_programs(1) + pl.program_id(1)
    total = pl.num_programs(0) * pl.num_programs(1)

    def start():
        pltpu.make_async_copy(norm_hbm, norm, load_sem.at[0]).start()
        pltpu.make_async_copy(pre_hbm, pre, load_sem.at[1]).start()
        scatter.meet()
        scatter.opening(0)

    def two():
        scatter.relay(0, 1), scatter.far(0, 3), scatter.near(0, 2)

    def four():
        scatter.relay(0, 2), scatter.far(0, 0), scatter.near(0, 3), scatter.cross(0, 1)

    def five():
        scatter.relay(0, 3), scatter.near(0, 0)

    def six():
        scatter.cross(0, 2)

    def seven():
        scatter.relay(0, 0)

    def end():
        scatter.cross(0, 3)
        pltpu.make_async_copy(norm_hbm, norm, load_sem.at[0]).wait()
        pltpu.make_async_copy(pre_hbm, pre, load_sem.at[1]).wait()

        @pl.loop(0, norm.shape[1] // 256)
        def _(i):
            part = pl.ds(pl.multiple_of(i * 256, 256), 256)
            up_out[part] = product_left_t(norm[:, part], pre[...]).astype(BF)

        scatter.last(0)
        scatter.drain()

    for place, work in ((0, start), (2, two), (4, four), (5, five), (6, six), (7, seven)):
        pl.when(step == place)(work)
    attend_back_step(chunk, *inputs, back_out, bias_out, *buffers)
    pl.when(step == total - 1)(end)


def attend_back_step(
    chunk, q_ref, k_ref, v_ref, penalty_ref, log_ref, att_ref, grad_ref, out_ref, bias_ref,
    query_buf, grad_buf, mixed_buf, back_buf, key_sum, value_sum, bias_sum,
):
    rows = q_ref.shape[2]
    pair = pl.program_id(1)
    width = out_ref.shape[3] // 3
    query_buf[...] = flat(q_ref) * jnp.asarray(0.125, BF)
    grad_buf[...] = flat(grad_ref)
    mixed_buf[...] = flat(att_ref)
    keys, values = flat(k_ref), flat(v_ref)
    keys_t = keys.T
    penalty = flat(penalty_ref)
    masks = head_masks()
    for total in (key_sum, value_sum, bias_sum):
        total[...] = jnp.zeros_like(total)

    def keep(offset, value):
        columns = pl.ds(pl.multiple_of(offset + pair * 2 * HEAD, 128), 2 * HEAD)
        for side in range(2):
            out_ref[side, 0, :, columns] = value[side * rows : (side + 1) * rows]

    for start in range(0, query_buf.shape[0], chunk):
        part = pl.ds(start, chunk)
        queries, grads = query_buf[part], grad_buf[part]
        overlap = (grads.astype(F32) * mixed_buf[part].astype(F32)).T
        parts = []
        for h in range(2):
            head_queries = queries * masks[h]
            head_grads = grads * masks[h]
            correction = jnp.sum(overlap[h * HEAD : (h + 1) * HEAD], axis=0, keepdims=True)
            logs = log_ref[0, 0, h : h + 1, part]
            soft = jnp.exp(product_right_t(keys, head_queries) + penalty - logs)
            grad_soft = product_right_t(values, head_grads)
            value_sum[...] += product(soft.astype(BF), head_grads)
            grad_scores = (soft * (grad_soft - correction)).astype(BF)
            key_sum[...] += product(grad_scores, head_queries)
            parts.append(product(keys_t[h * HEAD : (h + 1) * HEAD], grad_scores))
        grad_queries = jnp.concatenate(parts, 0).T * 0.125
        bias_sum[0:1] += jnp.sum(grad_queries, axis=0, keepdims=True)
        back_buf[part] = grad_queries.astype(BF)

    keep(0, back_buf[...])
    keep(width, key_sum[...].astype(BF))
    keep(2 * width, value_sum[...].astype(BF))
    bias_ref[0, 0, 0:1] = bias_sum[0:1]
    bias_ref[0, 0, 1:2] = jnp.sum(value_sum[...], axis=0, keepdims=True)


def attend_back(projected, penalty, logs, attended, grad_attended, grad_down, norm_two, grad_pre):
    _, clips, rows, triple = projected.shape
    slots = 2 * rows
    width = triple // 3
    pairs = width // (2 * HEAD)
    fused = lax.axis_size(AX) == 32 and clips * pairs == 8

    def block(offset):
        return pl.BlockSpec((2, 1, rows, 2 * HEAD), lambda i, j: (0, i, 0, offset * pairs + j))

    in_specs = [
        block(0), block(1), block(2),
        pl.BlockSpec((2, 1, rows, 1), lambda i, j: (0, i, 0, 0)),
        pl.BlockSpec((1, 1, 2, slots), lambda i, j: (i, j, 0, 0)),
        block(0), block(0),
    ]
    out_specs = [
        pl.BlockSpec((2, 1, rows, triple), lambda i, j: (0, i, 0, 0)),
        pl.BlockSpec((1, 1, 2, 2 * HEAD), lambda i, j: (i, j, 0, 0)),
    ]
    out_shape = [
        jax.ShapeDtypeStruct((2, clips, rows, triple), BF),
        jax.ShapeDtypeStruct((clips, pairs, 2, 2 * HEAD), F32),
    ]
    operands = [projected, projected, projected, penalty, logs, attended, grad_attended]
    scratch = [pltpu.VMEM((slots, 2 * HEAD), BF)] * 4 + [pltpu.VMEM((slots, 2 * HEAD), F32)] * 2
    scratch += [pltpu.VMEM((8, 2 * HEAD), F32)]
    params = pltpu.CompilerParams(vmem_limit_bytes=60 << 20)
    if fused:
        up_shape = (norm_two.shape[1], grad_pre.shape[1])
        sums = scatter_shapes([grad_down.shape], ("rows",))
        in_specs += [pl.BlockSpec(grad_down.shape, lambda i, j: (0, 0, 0, 0), pipeline_mode=pl.Buffered(1))]
        in_specs += [pl.BlockSpec(memory_space=pl.ANY)] * 2
        out_specs += [pl.BlockSpec(sums[0].shape, lambda i, j: (0, 0)), pl.BlockSpec(up_shape, lambda i, j: (0, 0))]
        out_shape += [sums[0], jax.ShapeDtypeStruct(up_shape, BF)]
        operands += [grad_down, norm_two, grad_pre]
        scratch += [pltpu.VMEM(norm_two.shape, BF), pltpu.VMEM(grad_pre.shape, BF), pltpu.SemaphoreType.DMA((2,))]
        scratch += scatter_scratch([grad_down.shape])
        params = pltpu.CompilerParams(vmem_limit_bytes=60 << 20, collective_id=2, has_side_effects=True)
    outs = pl.pallas_call(
        functools.partial(attend_back_kernel, 256),
        grid=(clips, pairs),
        in_specs=in_specs,
        out_specs=out_specs,
        out_shape=out_shape,
        scratch_shapes=scratch,
        compiler_params=params,
        cost_estimate=pl.CostEstimate(
            flops=10 * clips * pairs * slots * slots * 2 * HEAD, bytes_accessed=18 * clips * slots * width,
            transcendentals=clips * pairs * 2 * slots * slots,
        ),
        name="attend_back",
    )(*operands)
    if not fused:
        total = lax.psum_scatter(grad_down, AX, scatter_dimension=0, axis_index_groups=same_core_groups())
        total = total.astype(F32).reshape(-1, total.shape[-1])
        outs = [*outs, total, outer(norm_two, grad_pre)]
    return outs


def normal_parts(values):
    average = jnp.mean(values, axis=-1, keepdims=True)
    centered = values - average
    inverse = lax.rsqrt(jnp.mean(centered * centered, axis=-1, keepdims=True) + EPSILON)
    return centered * inverse, inverse


def normal_back(grad_normed, scaled, inverse, gain):
    grad_scaled = grad_normed * gain
    first_mean = jnp.mean(grad_scaled, axis=-1, keepdims=True)
    second_mean = jnp.mean(grad_scaled * scaled, axis=-1, keepdims=True)
    return inverse * (grad_scaled - first_mean - scaled * second_mean)


def rows_spec(size, columns):
    return pl.BlockSpec((size, columns), lambda i: (i, 0))


def whole_spec(shape):
    return pl.BlockSpec(shape, lambda i: (0,) * len(shape), pipeline_mode=pl.Buffered(1))


PARAMS = pltpu.CompilerParams(vmem_limit_bytes=56 << 20)


def strips_of(ref):
    return [pl.ds(start, 32) for start in range(0, ref.shape[0], 32)]


def project_kernel(steps, own_ref, other_ref, gain_ref, shift_ref, weight_ref, bias_ref, norm_ref, out_ref):
    is_own = pl.program_id(0) < steps
    for part in strips_of(own_ref):
        rows = jnp.where(is_own, own_ref[part].astype(F32), other_ref[part].astype(F32))
        scaled, _ = normal_parts(rows)
        norm_ref[part] = (scaled * gain_ref[...] + shift_ref[...]).astype(BF)
    out_ref[...] = (product(norm_ref[...], weight_ref[...]) + bias_ref[...]).astype(BF)


def project(own, other, gain, shift, weight, bias):
    rows, features = own.shape
    columns = weight.shape[1]
    steps = 3
    size = rows // steps
    return pl.pallas_call(
        functools.partial(project_kernel, steps),
        grid=(2 * steps,),
        in_specs=[
            pl.BlockSpec((size, features), lambda i: (jnp.minimum(i, steps - 1), 0)),
            pl.BlockSpec((size, features), lambda i: (jnp.maximum(i - steps, 0), 0)),
            whole_spec((1, features)),
            whole_spec((1, features)),
            whole_spec((features, columns)),
            whole_spec((1, columns)),
        ],
        out_specs=[rows_spec(size, features), rows_spec(size, columns)],
        out_shape=[
            jax.ShapeDtypeStruct((2 * rows, features), BF),
            jax.ShapeDtypeStruct((2 * rows, columns), BF),
        ],
        compiler_params=PARAMS,
        name="project",
    )(own, other, gain, shift, weight, bias)


def second_norm_kernel(att_ref, weight_ref, token_ref, recv_ref, bias_ref, gain_ref, shift_ref, middle_ref, out_ref):
    mixed = product(att_ref[...], weight_ref[...])
    for part in strips_of(token_ref):
        middle = token_ref[part].astype(F32) + mixed[part.start : part.start + part.size]
        middle = middle + recv_ref[part].astype(F32) + bias_ref[...]
        middle_ref[part] = middle
        scaled, _ = normal_parts(middle)
        out_ref[part] = (scaled * gain_ref[...] + shift_ref[...]).astype(BF)


def second_norm(attended, weight, tokens, received, bias, gain, shift):
    rows, features = tokens.shape
    width = weight.shape[0]
    size = rows // 4
    return pl.pallas_call(
        second_norm_kernel,
        grid=(4,),
        in_specs=[
            rows_spec(size, width), whole_spec((width, features)), rows_spec(size, features), rows_spec(size, features),
            whole_spec((1, features)), whole_spec((1, features)), whole_spec((1, features)),
        ],
        out_specs=[rows_spec(size, features), rows_spec(size, features)],
        out_shape=[jax.ShapeDtypeStruct((rows, features), F32), jax.ShapeDtypeStruct((rows, features), BF)],
        compiler_params=PARAMS,
        name="second_norm",
    )(attended, weight, tokens, received, bias, gain, shift)


def feed_kernel(
    steps, unit, own_ref, other_ref, grad_own_ref, grad_other_ref, mark_ref, bias_ref, *refs
):
    if len(refs) == 14:
        both_ref, refs = refs[0], refs[1:]
        sources = None
    else:
        sources, refs = refs[:2], refs[2:]
    act_ref, pre_ref, norm_ref, grad_ref, pass_own_ref, pass_other_ref, sums_ref, down_hbm = refs[:8]
    up_ref, down_ref, up_sem, down_sem, out_sem = refs[8:]
    step = pl.program_id(0)
    features, hidden = up_ref.shape

    @pl.when(step == 0)
    def _():
        sums_ref[...] = jnp.zeros_like(sums_ref)
        if sources is not None:
            pltpu.make_async_copy(sources[0], up_ref, up_sem).start()
            pltpu.make_async_copy(sources[1], down_ref, down_sem).start()
        else:
            core = lax.axis_index(AX) % 2
            chips = hidden // unit
            shard = features // (2 * chips)
            for k in range(chips):
                device = 2 * k + core
                pltpu.make_async_copy(
                    both_ref.at[:, pl.ds(pl.multiple_of(device * unit, 128), unit)],
                    up_ref.at[:, k * unit : (k + 1) * unit],
                    up_sem,
                ).start()
            for k in range(chips):
                device = 2 * k + core
                for q in range(unit // shard):
                    pltpu.make_async_copy(
                        both_ref.at[
                            pl.ds(pl.multiple_of(device * shard, 16), shard),
                            pl.ds(2 * hidden + q * features, features),
                        ],
                        down_ref.at[k * unit + q * shard : k * unit + (q + 1) * shard],
                        down_sem,
                    ).start()
        pltpu.make_async_copy(up_ref, up_ref, up_sem).wait()
        pltpu.make_async_copy(down_ref, down_ref, down_sem).wait()
        pltpu.make_async_copy(down_ref, down_hbm, out_sem).start()

    rows = jnp.where(step < steps, other_ref[...], own_ref[...])
    grads = jnp.where(step < steps, grad_other_ref[...], grad_own_ref[...]) * mark_ref[...].astype(BF)
    norm_ref[...] = rows
    grad_ref[...] = grads
    size = 512
    for start in range(0, hidden, size):
        part = slice(start, start + size)
        pre = product(rows, up_ref[:, part]) + bias_ref[:, part]
        normal_cdf = 0.5 * (1.0 + lax.erf(pre * ROOT_HALF))
        density = jnp.exp(-0.5 * pre * pre) * INV_ROOT_TWO_PI
        act_ref[:, part] = (pre * normal_cdf).astype(BF)
        grad_pre = product_right_t(grads, down_ref[part]) * (normal_cdf + pre * density)
        sums_ref[0:1, part] += jnp.sum(grad_pre, axis=0, keepdims=True)
        pre_ref[:, part] = grad_pre.astype(BF)
    passed = product_right_t(pre_ref[...], up_ref[...])
    pass_own_ref[...] = passed

    @pl.when(step < steps)
    def _():
        pass_other_ref[...] = passed.astype(BF)

    @pl.when(step == 2 * steps - 1)
    def _():
        pltpu.make_async_copy(down_ref, down_hbm, out_sem).wait()


def feed(own, other, grad_own, grad_other, marks, weights, bias, unit):
    rows, features = own.shape
    hidden = bias.shape[1]
    steps = 3
    size = rows // steps

    def side(i):
        return jnp.where(i < steps, i + steps, i - steps)

    def both_spec(columns):
        return pl.BlockSpec((size, columns), lambda i: (side(i), 0))

    own_spec = pl.BlockSpec((size, features), lambda i: (jnp.maximum(i - steps, 0), 0))
    other_spec = pl.BlockSpec((size, features), lambda i: (jnp.minimum(i, steps - 1), 0))
    return pl.pallas_call(
        functools.partial(feed_kernel, steps, unit),
        grid=(2 * steps,),
        in_specs=[own_spec, other_spec, own_spec, other_spec, both_spec(1), whole_spec((1, hidden))]
        + [pl.BlockSpec(memory_space=pl.ANY)] * len(weights),
        out_specs=[
            both_spec(hidden), both_spec(hidden), both_spec(features), both_spec(features),
            own_spec, other_spec,
            pl.BlockSpec((8, hidden), lambda i: (0, 0)), pl.BlockSpec(memory_space=pl.ANY),
        ],
        out_shape=[
            jax.ShapeDtypeStruct((2 * rows, hidden), BF), jax.ShapeDtypeStruct((2 * rows, hidden), BF),
            jax.ShapeDtypeStruct((2 * rows, features), BF), jax.ShapeDtypeStruct((2 * rows, features), BF),
            jax.ShapeDtypeStruct((rows, features), F32), jax.ShapeDtypeStruct((rows, features), BF),
            jax.ShapeDtypeStruct((8, hidden), F32), jax.ShapeDtypeStruct((hidden, features), BF),
        ],
        scratch_shapes=[
            pltpu.VMEM((features, hidden), BF), pltpu.VMEM((hidden, features), BF),
            pltpu.SemaphoreType.DMA(()), pltpu.SemaphoreType.DMA(()), pltpu.SemaphoreType.DMA(()),
        ],
        compiler_params=PARAMS,
        cost_estimate=pl.CostEstimate(
            flops=12 * rows * features * hidden, bytes_accessed=8 * features * hidden,
            transcendentals=4 * rows * hidden,
        ),
        name="feed",
    )(own, other, grad_own, grad_other, marks, bias, *weights)


def outer_kernel(left_ref, right_ref, out_ref):
    out_ref[...] = product_left_t(left_ref[...], right_ref[...]).astype(BF)


def outer(left, right):
    rows, columns = left.shape
    width = right.shape[1]
    size = 512
    return pl.pallas_call(
        outer_kernel,
        grid=(columns // size,),
        in_specs=[pl.BlockSpec((rows, size), lambda i: (0, i)), whole_spec((rows, width))],
        out_specs=rows_spec(size, width),
        out_shape=jax.ShapeDtypeStruct((columns, width), BF),
        compiler_params=PARAMS,
        cost_estimate=pl.CostEstimate(
            flops=2 * rows * columns * width, bytes_accessed=2 * (rows * columns + rows * width + columns * width),
            transcendentals=0,
        ),
        name="outer",
    )(left, right)


def gather_sums(sums_ref, values):
    for index, value in enumerate(values):
        sums_ref[index : index + 1] += jnp.sum(value, axis=0, keepdims=True)


def clear_first(sums_ref):
    @pl.when(pl.program_id(0) == 0)
    def _():
        sums_ref[...] = jnp.zeros_like(sums_ref)


def second_back_kernel(
    grad_ref, recv_ref, middle_ref, out_ref, gain_ref, full_ref, low_ref, sums_ref
):
    clear_first(sums_ref)
    for part in strips_of(grad_ref):
        grad_normed = grad_ref[part] + recv_ref[part].astype(F32)
        scaled, inverse = normal_parts(middle_ref[part])
        grad_out = out_ref[part].astype(F32)
        grad_middle = grad_out + normal_back(grad_normed, scaled, inverse, gain_ref[...])
        full_ref[part] = grad_middle
        low_ref[part] = grad_middle.astype(BF)
        gather_sums(sums_ref, [grad_normed * scaled, grad_normed, grad_middle, grad_out])


def second_back(passed, received, middle, grad_out, gain):
    rows, features = middle.shape
    size = rows // 4
    return pl.pallas_call(
        second_back_kernel,
        grid=(4,),
        in_specs=[rows_spec(size, features)] * 4 + [whole_spec((1, features))],
        out_specs=[rows_spec(size, features)] * 2 + [pl.BlockSpec((8, features), lambda i: (0, 0))],
        out_shape=[
            jax.ShapeDtypeStruct((rows, features), F32), jax.ShapeDtypeStruct((rows, features), BF),
            jax.ShapeDtypeStruct((8, features), F32),
        ],
        compiler_params=PARAMS,
        name="second_back",
    )(passed, received, middle, grad_out, gain)


def first_back_kernel(grad_ref, weight_ref, recv_ref, token_ref, middle_ref, gain_ref, full_ref, sums_ref):
    clear_first(sums_ref)
    passed = product_right_t(grad_ref[...], weight_ref[...])
    for part in strips_of(grad_ref):
        grad_normed = passed[part.start : part.start + part.size] + recv_ref[part].astype(F32)
        scaled, inverse = normal_parts(token_ref[part].astype(F32))
        full_ref[part] = middle_ref[part] + normal_back(grad_normed, scaled, inverse, gain_ref[...])
        gather_sums(sums_ref, [grad_normed * scaled, grad_normed])


def first_back(grad_projected, weight, received, tokens, grad_middle, gain):
    rows, features = tokens.shape
    triple = weight.shape[1]
    size = rows // 4
    return pl.pallas_call(
        first_back_kernel,
        grid=(4,),
        in_specs=[
            rows_spec(size, triple), whole_spec((features, triple)), rows_spec(size, features),
            rows_spec(size, features), rows_spec(size, features), whole_spec((1, features)),
        ],
        out_specs=[rows_spec(size, features), pl.BlockSpec((8, features), lambda i: (0, 0))],
        out_shape=[jax.ShapeDtypeStruct((rows, features), F32), jax.ShapeDtypeStruct((8, features), F32)],
        compiler_params=PARAMS,
        name="first_back",
    )(grad_projected, weight, received, tokens, grad_middle, gain)


def tail_kernel(
    kinds, up_ref, proj_ref, sums_ref, bias_ref, gain_ref, shift_ref,
    back_hbm, weight_hbm, norm_hbm, token_hbm, middle_hbm, down_hbm, act_hbm, sum_hbm,
    up_out, qkv_out, proj_out, packed_out, tokens_out, block_out, *refs
):
    back, weight, norm, token, middle, down, qkv, packed, vectors, stage, land, load_sem, pass_sem = refs[:13]
    act, total, lift_stage, lift_land, block_sem = refs[13:18]
    scatter = Scatter(kinds, (up_ref, qkv, proj_ref, packed), (up_out, qkv_out, proj_out, packed_out), refs[18:], 2)
    chips, _, shard, triple = qkv.shape
    own_rows = token.shape[0]
    loads = [
        pltpu.make_async_copy(source, target, load_sem.at[i])
        for i, (source, target) in enumerate(
            (
                (back_hbm, back), (weight_hbm, weight), (norm_hbm, norm), (token_hbm, token), (middle_hbm, middle),
                (down_hbm, down),
            )
        )
    ]
    for load in loads:
        load.start()
    scatter.meet()
    scatter.opening(0)
    scatter.along(2)
    vectors[...] = jnp.zeros_like(vectors)
    vectors[0:8] = sums_ref[...]
    loads[0].wait(), loads[1].wait()

    @pl.loop(0, own_rows // 256)
    def _(i):
        part = pl.ds(pl.multiple_of(own_rows + i * 256, 256), 256)
        stage[pl.ds(pl.multiple_of(i * 256, 256), 256)] = product_right_t(back[part], weight[...]).astype(BF)

    passing = pltpu.make_async_remote_copy(
        src_ref=stage, dst_ref=land, send_sem=pass_sem.at[0], recv_sem=pass_sem.at[1],
        device_id=(scatter.mate,), device_id_type=MESH,
    )
    passing.start()
    scatter.relay(0, 1), scatter.far(0, 3), scatter.near(0, 2)
    loads[2].wait()

    @pl.loop(0, norm.shape[1] // 256)
    def _(i):
        part = pl.ds(pl.multiple_of(i * 256, 256), 256)
        count = 256 // (2 * shard)
        grad = product_left_t(norm[:, part], back[...]).astype(BF)
        qkv[pl.ds(i * count, count)] = grad.reshape(count, 2, shard, triple)

    scatter.relay(0, 2), scatter.far(0, 0), scatter.near(0, 3)
    scatter.opening(1)
    loads[3].wait(), loads[4].wait()
    passing.wait()

    @pl.loop(0, own_rows // 256)
    def _(i):
        start = pl.multiple_of(i * 256, 256)
        passed = product_right_t(back[pl.ds(start, 256)], weight[...])
        for strip in range(0, 256, 32):
            part = pl.ds(start + strip, 32)
            grad_normed = passed[strip : strip + 32] + land[part].astype(F32)
            scaled, inverse = normal_parts(token[part].astype(F32))
            tokens_out[part] = middle[part] + normal_back(grad_normed, scaled, inverse, gain_ref[...])
            vectors[0:1] += jnp.sum(grad_normed * scaled, axis=0, keepdims=True)
            vectors[1:2] += jnp.sum(grad_normed, axis=0, keepdims=True)

    scatter.relay(0, 3), scatter.near(0, 0), scatter.cross(0, 1), scatter.cross(0, 2)
    packed[:, :, :shard] = vectors[...].T.astype(BF).reshape(chips, 2, shard, PARAM_COLS)
    packed[:, :, shard:] = bias_ref[...]
    for j in (1, 2, 3, 0):
        scatter.far(3, j), scatter.near(3, j)
    scatter.layer_sum(2)
    scatter.far(2, 0), scatter.near(2, 0)
    scatter.relay(0, 0), scatter.cross(0, 3)
    loads[5].wait()

    def fetch(source, start, target, slot):
        copy = pltpu.make_async_copy(source.at[pl.ds(start, 256)], target, block_sem.at[slot])
        copy.start()
        return copy

    @pl.loop(0, own_rows // 256)
    def _(i):
        fetch(act_hbm, pl.multiple_of(own_rows + i * 256, 256), act, 0).wait()
        lift_stage[pl.ds(pl.multiple_of(i * 256, 256), 256)] = product(act[...], down[...]).astype(BF)

    lifting = pltpu.make_async_remote_copy(
        src_ref=lift_stage, dst_ref=lift_land, send_sem=pass_sem.at[2], recv_sem=pass_sem.at[3],
        device_id=(scatter.mate,), device_id_type=MESH,
    )
    lifting.start()
    scatter.relay(2, 0)
    scatter.relay(1, 1), scatter.far(1, 3), scatter.near(1, 2)
    scatter.relay(1, 2), scatter.far(1, 0), scatter.near(1, 3)
    lifting.wait()

    @pl.loop(0, own_rows // 256)
    def _(i):
        start = pl.multiple_of(i * 256, 256)
        copies = fetch(act_hbm, start, act, 0), fetch(sum_hbm, start, total, 1)
        for copy in copies:
            copy.wait()
        lifted = product(act[...], down[...]) + lift_land[pl.ds(start, 256)].astype(F32)
        block_out[pl.ds(start, 256)] = (total[...] + lifted + shift_ref[...]).astype(BF)

    for j in (1, 2, 3, 0):
        scatter.relay(3, j)
    scatter.last(2)
    scatter.relay(1, 3), scatter.near(1, 0), scatter.cross(1, 1)
    for j in (1, 2, 3):
        scatter.cross(3, j)
    scatter.relay(1, 0)
    scatter.last(0)
    scatter.cross(1, 2), scatter.cross(1, 3)
    scatter.finish(2), scatter.finish(0)
    scatter.last(3)
    scatter.last(1)
    scatter.finish(3), scatter.finish(1)
    scatter.drain()


def tail(grad_up, grad_proj, sums, bias_rows, gain, shift, back, weight, norm, tokens, grad_middle, down, act, middle):
    chips, _, shard, hidden = grad_up.shape
    rows, triple = back.shape
    own_rows, features = tokens.shape
    extra = bias_rows.shape[2]
    kinds = (chips, 3, 1, "sum")
    shapes = [
        grad_up.shape, (chips, 2, shard, triple), grad_proj.shape, (chips, 2, shard + extra, PARAM_COLS),
    ]
    vmem = pl.BlockSpec(memory_space=pltpu.VMEM)
    return pl.pallas_call(
        functools.partial(tail_kernel, kinds),
        out_shape=scatter_shapes(shapes, kinds)
        + [jax.ShapeDtypeStruct((own_rows, features), F32), jax.ShapeDtypeStruct((own_rows, features), BF)],
        in_specs=[vmem] * 6 + [pl.BlockSpec(memory_space=pl.ANY)] * 8,
        out_specs=[vmem] * 6,
        scratch_shapes=[
            pltpu.VMEM(back.shape, BF), pltpu.VMEM(weight.shape, BF), pltpu.VMEM(norm.shape, BF),
            pltpu.VMEM(tokens.shape, BF), pltpu.VMEM(middle.shape, F32), pltpu.VMEM(down.shape, BF),
            pltpu.VMEM(shapes[1], BF), pltpu.VMEM(shapes[3], BF), pltpu.VMEM((PARAM_COLS, features), F32),
            pltpu.VMEM((own_rows, features), BF), pltpu.VMEM((own_rows, features), BF),
            pltpu.SemaphoreType.DMA((6,)), pltpu.SemaphoreType.DMA((4,)),
            pltpu.VMEM((256, act.shape[1]), BF), pltpu.VMEM((256, features), F32),
            pltpu.VMEM((own_rows, features), BF), pltpu.VMEM((own_rows, features), BF), pltpu.SemaphoreType.DMA((2,)),
        ]
        + scatter_scratch(shapes, 2),
        compiler_params=pltpu.CompilerParams(collective_id=1, has_side_effects=True, vmem_limit_bytes=62 << 20),
        name="tail",
    )(grad_up, grad_proj, sums, bias_rows, gain, shift, back, weight, norm, tokens, grad_middle, down, act, middle)


def pack_kernel(up_ref, down_ref, out_ref):
    shard, columns = up_ref.shape
    features = down_ref.shape[1]
    out_ref[:, :columns] = up_ref[...]
    for i in range(down_ref.shape[0] // shard):
        out_ref[:, columns + i * features : columns + (i + 1) * features] = down_ref[i * shard : (i + 1) * shard]


def pack(up, down):
    shard, columns = up.shape
    fold = down.shape[0] // shard
    if shard % 16 != 0:
        return jnp.concatenate([up] + [down[shard * i : shard * (i + 1)] for i in range(fold)], 1)
    return pl.pallas_call(
        pack_kernel,
        out_shape=jax.ShapeDtypeStruct((shard, columns + fold * down.shape[1]), BF),
        in_specs=[pl.BlockSpec(memory_space=pltpu.VMEM)] * 2,
        out_specs=pl.BlockSpec(memory_space=pltpu.VMEM),
        name="pack",
    )(up, down)


def finish_kernel(
    up_ref, qkv_ref, proj_ref, down_ref, token_ref, block_ref, packed_ref,
    up_out, qkv_out, proj_out, down_out, token_out, block_out, vec_out, bias_out,
):
    token_out[...] = token_ref[...]
    block_out[...] = block_ref[...]

    @pl.when(pl.program_id(0) == 0)
    def _():
        up_out[...] = up_ref[...]
        qkv_out[...] = qkv_ref[...]
        proj_out[...] = proj_ref[...]
        down_out[...] = down_ref[...]
        shard = vec_out.shape[1]
        vec_out[...] = packed_ref[:shard].T[:8]
        bias_out[...] = packed_ref[shard : shard + 1]


def finish(up, qkv, proj, down, tokens, block, packed, shard, unit):
    if lax.axis_size(AX) != 32:
        return up, qkv, proj, down, tokens, block, packed[:shard, :8].T, packed[shard : shard + 1, :unit]
    size = tokens.shape[0] // 4
    passed = [rows_spec(size, tokens.shape[1])] * 2

    def kept(shape):
        return pl.BlockSpec(shape, lambda i: (0, 0))

    summed = [whole_spec(a.shape) for a in (up, qkv, proj, down)]
    return pl.pallas_call(
        finish_kernel,
        grid=(4,),
        out_shape=[jax.ShapeDtypeStruct(a.shape, a.dtype) for a in (up, qkv, proj, down, tokens, block)]
        + [jax.ShapeDtypeStruct((8, shard), F32), jax.ShapeDtypeStruct((1, unit), F32)],
        in_specs=summed + passed + [whole_spec(packed.shape)],
        out_specs=[kept(a.shape) for a in (up, qkv, proj, down)] + passed + [kept((8, shard)), kept((1, unit))],
        compiler_params=PARAMS,
        name="finish",
    )(up, qkv, proj, down, tokens, block, packed)


def by_core(core, own, other, axis):
    return jnp.where(core == 0, jnp.concatenate([own, other], axis), jnp.concatenate([other, own], axis))


def per_device(
    tokens, valid_slots, cotangent, first_gain, first_shift, qkv_weight, query_bias, value_bias, proj_weight,
    proj_bias, second_gain, second_shift, up_weight, up_bias, down_weight, down_bias,
):
    devices = lax.axis_size(AX)
    chips = devices // 2
    core = lax.axis_index(AX) % 2
    micro, rows, features = tokens.shape
    shard = qkv_weight.shape[0]
    width = features // 2
    hidden = up_weight.shape[1] // 2
    unit = hidden // chips
    own_rows = micro * rows
    every = 2 * own_rows

    fold = unit // shard
    both_weights = lax.all_gather(pack(up_weight, down_weight), AX, axis=0, tiled=True)
    feed_weights = [both_weights]
    if unit % 128 != 0 or shard % 16 != 0:
        half_up = both_weights[:, : 2 * hidden].reshape(features, chips, 2, unit)
        half_up = lax.dynamic_index_in_dim(half_up, core, 2, keepdims=False).reshape(features, hidden)
        half_down = both_weights[:, 2 * hidden :].reshape(chips, 2, shard, fold, features)
        half_down = lax.dynamic_index_in_dim(half_down, core, 1, keepdims=False)
        half_down = half_down.transpose(0, 2, 1, 3).reshape(hidden, features)
        feed_weights = [half_up, half_down]
    vectors = jnp.stack(
        [first_gain, first_shift, query_bias, value_bias, proj_bias, second_gain, second_shift, down_bias], 0
    )
    lanes = max(PARAM_COLS, unit)
    vectors = jnp.pad(vectors.T, ((0, 16), (0, lanes - 8)))
    packed = lax.dynamic_update_slice(vectors, up_bias[None, :], (shard, 0))
    qkv_all, proj_all, packed_all = gather_chips(qkv_weight, proj_weight, packed)
    weight_qkv = qkv_all.reshape(features, 3 * width)
    params = packed_all[:, :, :shard, :8].astype(F32).reshape(features, 8).T
    gain_one, shift_one, bias_query, bias_value, bias_proj, gain_two, shift_two, bias_down = [
        params[i : i + 1] for i in range(8)
    ]
    bias_up = lax.dynamic_index_in_dim(packed_all[:, :, shard, :unit], core, 1, keepdims=False)
    bias_up = bias_up.astype(F32).reshape(1, hidden)
    proj_cols = proj_all.reshape(2, width, width)
    proj_own = lax.dynamic_index_in_dim(proj_cols, core, 0, keepdims=False)
    proj_other = swap(lax.dynamic_index_in_dim(proj_cols, 1 - core, 0, keepdims=False))
    weight_proj = by_core(core, proj_own, proj_other, 1)
    qkv_bias = jnp.concatenate(
        [
            lax.dynamic_slice_in_dim(bias_query, core * width, width, 1),
            jnp.zeros((1, width), F32),
            lax.dynamic_slice_in_dim(bias_value, core * width, width, 1),
        ],
        1,
    )

    own_tokens = tokens.reshape(own_rows, features)
    other_tokens = swap(own_tokens)
    marks = jnp.stack([valid_slots, swap(valid_slots)])
    own_cotangent = cotangent.reshape(own_rows, features)
    penalty = jnp.where(marks > 0, 0.0, -1000000000.0).astype(F32)[..., None]
    norm_one, projected = project(own_tokens, other_tokens, gain_one, shift_one, weight_qkv, qkv_bias)
    projected = projected.reshape(2, micro, rows, 3 * width)
    attended, logs = attend(projected, penalty)
    attended_flat = attended.reshape(every, width)
    mixed = swap(product(attended_flat[own_rows:], weight_proj).astype(BF))
    middle, norm_own = second_norm(
        attended_flat, weight_proj, own_tokens, mixed, bias_proj, gain_two, shift_two
    )
    activation, grad_pre, norm_two, grad_out, passed, passed_other, up_sums, weight_down = feed(
        norm_own, swap(norm_own), own_cotangent, swap(own_cotangent),
        (marks > 0).astype(F32).reshape(every, 1), feed_weights, bias_up, unit,
    )
    grad_bias_up = up_sums[0]
    passed_other = swap(passed_other)

    grad_down = outer(activation, grad_out)
    passed_other, grad_down = lax.optimization_barrier((passed_other, grad_down))
    grad_middle, grad_low, second_sums = second_back(passed, passed_other, middle, grad_out, gain_two)
    grad_low = jnp.concatenate([grad_low, swap(grad_low)], 0)
    grad_attended = product_right_t(grad_low, weight_proj).astype(BF).reshape(2, micro, rows, width)
    grad_proj = product_left_t(attended_flat, grad_low).astype(BF)
    grad_attended, grad_proj = lax.optimization_barrier((grad_attended, grad_proj))
    grad_proj_own = lax.dynamic_slice_in_dim(grad_proj, core * width, width, 1)
    grad_proj_other = swap(lax.dynamic_slice_in_dim(grad_proj, (1 - core) * width, width, 1))
    grad_proj = by_core(core, grad_proj_own, grad_proj_other, 0)
    grad_projected, grad_bias, down_weight_grad, grad_up = attend_back(
        projected, penalty, logs, attended, grad_attended, grad_down.reshape(chips, 2, unit // 2, features),
        norm_two, grad_pre,
    )
    grad_projected = grad_projected.reshape(every, 3 * width)

    grad_bias = jnp.sum(grad_bias, axis=0).transpose(1, 0, 2).reshape(2, width)
    grad_bias = by_core(core, grad_bias, jnp.zeros_like(grad_bias), 1)
    sums = [grad_bias, second_sums[2:3], second_sums[:2], second_sums[3:4]]
    up_units = grad_bias_up.astype(BF).reshape(chips, 1, unit)
    up_units = by_core(core, up_units, jnp.zeros_like(up_units), 1).reshape(chips, 2, 1, unit)
    grad_up = grad_up.reshape(chips, 2, shard, hidden)
    grad_proj = grad_proj.reshape(chips, 2, shard, width)
    if devices == 32:
        bias_rows = jnp.pad(up_units, ((0, 0), (0, 0), (0, 15), (0, 0)))
        sums = jnp.concatenate([jnp.zeros((2, features), F32)] + sums, 0)
        up_weight_grad, qkv_weight_grad, proj_weight_grad, packed_sum, tokens_grad, block_output = tail(
            grad_up, grad_proj, sums, bias_rows, gain_one, bias_down, grad_projected, weight_qkv, norm_one, own_tokens,
            grad_middle, weight_down, activation, middle,
        )
    else:
        lifted = swap(product(activation[own_rows:], weight_down).astype(BF)).astype(F32)
        block_output = (middle + product(activation[:own_rows], weight_down) + lifted + bias_down).astype(BF)
        passed = swap(product_right_t(grad_projected[own_rows:], weight_qkv).astype(BF))
        grad_qkv = outer(norm_one, grad_projected)
        tokens_grad, first_sums = first_back(
            grad_projected, weight_qkv, passed, own_tokens, grad_middle, gain_one
        )
        sums = jnp.concatenate([first_sums[:2]] + sums, 0)
        sums = sums.astype(BF).T.reshape(chips, 2, shard, 8)
        sums = jnp.pad(sums, ((0, 0), (0, 0), (0, 16), (0, lanes - 8)))
        sums = lax.dynamic_update_slice(sums, up_units, (0, 0, shard, 0))
        up_weight_grad, qkv_weight_grad, proj_weight_grad, packed_sum = scatter_chips(
            [grad_up, grad_qkv.reshape(chips, 2, shard, 3 * width), grad_proj, sums], (chips, 3, 1, "sum")
        )
    (
        up_weight_grad, qkv_weight_grad, proj_weight_grad, down_weight_grad, tokens_grad, block_output,
        vector_sum, up_bias_grad,
    ) = finish(
        up_weight_grad, qkv_weight_grad, proj_weight_grad, down_weight_grad, tokens_grad, block_output,
        packed_sum, shard, unit,
    )
    tokens_grad = tokens_grad.reshape(micro, rows, features)
    block_output = block_output.reshape(micro, rows, features)
    up_bias_grad = up_bias_grad[0]
    return (
        block_output, tokens_grad, vector_sum[0], vector_sum[1], qkv_weight_grad, vector_sum[2], vector_sum[3],
        proj_weight_grad, vector_sum[4], vector_sum[5], vector_sum[6], up_weight_grad, up_bias_grad,
        down_weight_grad, vector_sum[7],
    )


def solution(mesh):
    row = P(None, AX, None)
    vec = P(AX)
    mat = P(AX, None)
    return jax.shard_map(
        per_device,
        mesh=mesh,
        in_specs=(row, P(None, AX), row, vec, vec, mat, vec, vec, mat, vec, vec, vec, mat, vec, mat, vec),
        out_specs=(row, row, vec, vec, mat, vec, vec, mat, vec, vec, vec, mat, vec, mat, vec),
        check_vma=False,
    )
```

```python
import functools

import jax
import jax.numpy as jnp
from jax import lax
from jax.experimental import pallas as pl
from jax.experimental.pallas import tpu as pltpu
from jax.sharding import PartitionSpec as P

AX = "fsdp"
MESH = pl.DeviceIdType.MESH
HEAD = 64
EPSILON = 1e-06
ROOT_HALF = 0.7071067811865476
INV_ROOT_TWO_PI = 0.3989422804014327
BF = jnp.bfloat16
F32 = jnp.float32
PARAM_COLS = 128


def product(left_side, right_side):
    return jnp.dot(left_side, right_side, preferred_element_type=F32)


def product_left_t(left_side, right_side):
    return lax.dot_general(left_side, right_side, (((0,), (0,)), ((), ())), preferred_element_type=F32)


def product_right_t(left_side, right_side):
    return lax.dot_general(left_side, right_side, (((1,), (1,)), ((), ())), preferred_element_type=F32)


def swap(shard):
    return lax.ppermute(shard, AX, [(i, i ^ 1) for i in range(lax.axis_size(AX))])


def same_core_groups():
    count = lax.axis_size(AX)
    return [[i for i in range(count) if i % 2 == core] for core in (0, 1)]


def flip(index, step):
    return index + step - 2 * step * ((index // step) % 2)


def peers_of(me):
    return flip(me, 1), flip(me, 2), flip(me, 4), [flip(me, 8), flip(me, 16), flip(flip(me, 8), 16)]


def zflip(chip, j):
    return [chip, flip(chip, 4), flip(chip, 8), flip(flip(chip, 4), 8)][j]


def meet(peers):
    barrier = pltpu.get_barrier_semaphore()
    for peer in peers:
        pl.semaphore_signal(barrier, inc=1, device_id=(peer,), device_id_type=MESH)
    pl.semaphore_wait(barrier, len(peers))


def gather_kernel(qkv_ref, proj_ref, packed_ref, qkv_out, proj_out, packed_out, local_sem, send_sem, recv_sem):
    me = lax.axis_index(AX)
    chip, core = me // 2, me % 2
    mate, peer_x, peer_y, peers_z = peers_of(me)
    meet([mate, peer_x, peer_y] + peers_z)
    chip_x, chip_y = flip(chip, 1), flip(chip, 2)
    chip_xy = flip(chip_x, 2)
    outs = (qkv_out, packed_out, proj_out)
    count = len(outs)
    width = qkv_ref.shape[1] // 6
    pending = []

    def remote(w, slot, block, target, peer):
        return pltpu.make_async_remote_copy(
            src_ref=block, dst_ref=target, send_sem=send_sem.at[w, slot], recv_sem=recv_sem.at[w, slot],
            device_id=(peer,), device_id_type=MESH,
        )

    def send(w, slot, block, target, peer):
        copy = remote(w, slot, block, target, peer)
        copy.start()
        pending.append(copy)

    def arrive(w, slot, block):
        remote(w, slot, block, block, mate).wait_recv()

    def columns(start, size):
        return pl.ds(pl.multiple_of(start, 128), size)

    def pieces(w, half, target):
        if w == 0:
            return [
                (qkv_ref.at[:, columns((2 * t + half) * width, width)], target.at[:, pl.ds(t * width, width)])
                for t in range(3)
            ]
        if w == 1:
            return [(packed_ref, target)]
        return [(proj_ref.at[:, columns(half * width, width)], target)]

    for w in range(count):
        for source, target in pieces(w, 1 - core, outs[w].at[chip, core]):
            remote(w, 0, source, target, mate).start()
        for source, target in pieces(w, core, outs[w].at[chip, core]):
            pltpu.make_async_copy(source, target, local_sem.at[w]).start()
    for w in range(count):
        own = outs[w].at[chip, core]
        pltpu.make_async_copy(own, own, local_sem.at[w]).wait()
        arrive(w, 0, outs[w].at[chip, 1 - core])
        block = outs[w].at[chip]
        for j in range(3):
            send(w, 1 + j, block, block, peers_z[j])
        send(w, 4, block, block, peer_x)
        send(w, 8, block, block, peer_y)
    for w in range(count):
        for j in (1, 2, 3):
            block = outs[w].at[zflip(chip, j)]
            arrive(w, j, block)
            send(w, 4 + j, block, block, peer_x)
            send(w, 8 + j, block, block, peer_y)
        for j in range(4):
            block = outs[w].at[zflip(chip_x, j)]
            arrive(w, 4 + j, block)
            send(w, 12 + j, block.at[0], block.at[0], peer_y)
            block = outs[w].at[zflip(chip_y, j)]
            arrive(w, 8 + j, block)
            send(w, 16 + j, block.at[1], block.at[1], peer_x)
    for w in range(count):
        for j in range(4):
            block = outs[w].at[zflip(chip_xy, j)]
            arrive(w, 12 + j, block.at[0])
            arrive(w, 16 + j, block.at[1])
    for w in range(count):
        own = outs[w].at[chip, core]
        remote(w, 0, own, own, mate).wait_send()
    for copy in pending:
        copy.wait_send()


def gather_chips(qkv, proj, packed):
    devices = lax.axis_size(AX)
    shard, features = proj.shape
    width = features // 2
    if devices != 32:
        core = lax.axis_index(AX) % 2
        split = qkv.reshape(shard, 3, 2, width).transpose(2, 0, 1, 3).reshape(2, shard, 3 * width)
        gathered = []
        for halves in (split, proj.reshape(shard, 2, width).transpose(1, 0, 2), jnp.stack([packed, packed])):
            own = lax.dynamic_index_in_dim(halves, core, 0, keepdims=False)
            other = swap(lax.dynamic_index_in_dim(halves, 1 - core, 0, keepdims=False))
            block = jnp.where(core == 0, jnp.stack([own, other]), jnp.stack([other, own]))
            gathered.append(lax.all_gather(block, AX, axis=0, axis_index_groups=same_core_groups()))
        return gathered
    chips = devices // 2
    return pl.pallas_call(
        gather_kernel,
        out_shape=[
            jax.ShapeDtypeStruct((chips, 2, shard, 3 * width), BF),
            jax.ShapeDtypeStruct((chips, 2, shard, width), BF),
            jax.ShapeDtypeStruct((chips, 2) + packed.shape, BF),
        ],
        in_specs=[pl.BlockSpec(memory_space=pltpu.VMEM)] * 3,
        out_specs=[pl.BlockSpec(memory_space=pl.ANY)] * 3,
        scratch_shapes=[
            pltpu.SemaphoreType.DMA((3,)),
            pltpu.SemaphoreType.DMA((3, 20)),
            pltpu.SemaphoreType.DMA((3, 20)),
        ],
        compiler_params=pltpu.CompilerParams(collective_id=0, has_side_effects=True),
        cost_estimate=pl.CostEstimate(flops=int(4e10), bytes_accessed=int(1.5e8), transcendentals=0),
        name="gather_chips",
    )(qkv, proj, packed)


class Scatter:
    def __init__(self, kinds, ins, outs, scratch, early=None, origins=None):
        count = len(kinds)
        self.origins = origins or ins
        self.early = early
        if early is not None:
            self.plane, scratch = scratch[-1], scratch[:-1]
        self.kinds, self.ins, self.outs = kinds, ins, outs
        names = ("recv_a", "recv_b", "recv_x", "recv_y", "recv_z", "stage", "land")
        for place, name in enumerate(names):
            setattr(self, name, scratch[place * count : (place + 1) * count])
        self.send_sem, self.recv_sem = scratch[len(names) * count :]
        me = lax.axis_index(AX)
        self.chip, self.core = me // 2, me % 2
        self.mate, self.peer_x, self.peer_y, self.peers_z = peers_of(me)
        chip_x, chip_y = flip(self.chip, 1), flip(self.chip, 2)
        self.own = [zflip(self.chip, j) for j in range(4)]
        self.at_x = [zflip(chip_x, j) for j in range(4)]
        self.at_y = [zflip(chip_y, j) for j in range(4)]
        self.at_xy = [zflip(flip(chip_x, 2), j) for j in range(4)]
        self.sent = []

    def meet(self):
        meet([self.mate, self.peer_x, self.peer_y] + self.peers_z)

    def remote(self, w, slot, block, target, peer):
        return pltpu.make_async_remote_copy(
            src_ref=block, dst_ref=target, send_sem=self.send_sem.at[w, slot], recv_sem=self.recv_sem.at[w, slot],
            device_id=(peer,), device_id_type=MESH,
        )

    def send(self, w, slot, block, target, peer):
        self.remote(w, slot, block, target, peer).start()
        self.sent.append((w, slot))

    def arrive(self, w, slot, block):
        self.remote(w, slot, block, block, self.mate).wait_recv()

    def source(self, w, chip):
        return (self.plane, chip % 4) if w == self.early else (self.ins[w], chip)

    def origin(self, w, chip):
        return (self.plane, chip % 4) if w == self.early else (self.origins[w], chip)

    def along(self, w):
        for j in (1, 2, 3):
            layer = pl.multiple_of(self.own[j] // 4 * 4, 4)
            self.send(w, 23 + j, self.origins[w].at[pl.ds(layer, 4)], self.recv_z[w].at[j - 1], self.peers_z[j - 1])

    def layer_sum(self, w):
        for j in range(3):
            self.arrive(w, 24 + j, self.recv_z[w].at[j])
        layer = self.chip // 4 * 4

        @pl.loop(0, 4)
        def _(block):
            def body(part):
                for half in range(2):
                    total = self.ins[w][layer + block, half, part].astype(F32)
                    for j in range(3):
                        total = total + self.recv_z[w][j, block, half, part].astype(F32)
                    self.plane[block, half, part] = total.astype(BF)

            self.strips(w, body)

    def far(self, w, j):
        ref, at = self.origin(w, self.at_xy[j])
        block = ref.at[at]
        self.send(w, j, block.at[0], self.recv_a[w].at[j], self.peer_y)
        self.send(w, 4 + j, block.at[1], self.recv_b[w].at[j], self.peer_x)

    def near(self, w, j):
        ref, at = self.origin(w, self.at_x[j])
        self.send(w, 8 + j, ref.at[at, 1], self.recv_x[w].at[j, 1], self.peer_x)
        ref, at = self.origin(w, self.at_y[j])
        self.send(w, 12 + j, ref.at[at, 0], self.recv_y[w].at[j, 0], self.peer_y)

    def strips(self, w, body):
        @pl.loop(0, self.ins[w].shape[2] // 16)
        def _(i):
            body(pl.ds(pl.multiple_of(i * 16, 16), 16))

    def relay(self, w, j):
        for slot, recv, block, half in (
            (j, self.recv_a[w], self.at_x[j], 0),
            (4 + j, self.recv_b[w], self.at_y[j], 1),
        ):
            self.arrive(w, slot, recv.at[j])

            ref, at = self.source(w, block)

            def body(part):
                total = recv[j, part].astype(F32) + ref[at, half, part].astype(F32)
                recv[j, part] = total.astype(BF)

            self.strips(w, body)
            if half == 0:
                self.send(w, 16 + j, recv.at[j], self.recv_x[w].at[j, 0], self.peer_x)
            else:
                self.send(w, 20 + j, recv.at[j], self.recv_y[w].at[j, 1], self.peer_y)

    def arrive_near(self, w, j):
        self.arrive(w, 8 + j, self.recv_x[w].at[j, 1])
        self.arrive(w, 12 + j, self.recv_y[w].at[j, 0])
        self.arrive(w, 16 + j, self.recv_x[w].at[j, 0])
        self.arrive(w, 20 + j, self.recv_y[w].at[j, 1])

    def near_sum(self, w, j, half, part):
        total = self.recv_x[w][j, half, part].astype(F32) + self.recv_y[w][j, half, part].astype(F32)
        ref, at = self.source(w, self.own[j])
        return total + ref[at, half, part].astype(F32)

    def cross(self, w, j):
        self.arrive_near(w, j)

        def body(part):
            for half in range(2):
                self.recv_x[w][j, half, part] = self.near_sum(w, j, half, part).astype(BF)

        self.strips(w, body)
        self.send(w, 23 + j, self.recv_x[w].at[j], self.recv_z[w].at[j - 1], self.peers_z[j - 1])

    def place(self, w, part, total, half):
        kind = self.kinds[w]
        if kind == "sum":
            self.outs[w][part] = total
            return
        size = total.shape[1] // kind
        for t in range(kind):
            start = pl.multiple_of((2 * t + half) * size, 128)
            self.outs[w][part, pl.ds(start, size)] = total[:, t * size : (t + 1) * size]

    def last(self, w):
        self.arrive_near(w, 0)
        layers = 0 if w == self.early else 3
        for j in range(layers):
            self.arrive(w, 24 + j, self.recv_z[w].at[j])
        rows = self.ins[w].shape[2]

        def total_of(half, part):
            total = self.near_sum(w, 0, half, part)
            for j in range(layers):
                total = total + self.recv_z[w][j, half, part].astype(F32)
            return total

        if self.kinds[w] == "rows":

            @pl.loop(0, rows // 16)
            def _(i):
                for half in range(2):
                    part = pl.ds(pl.multiple_of(i * 16, 16), 16)
                    self.outs[w][pl.ds(pl.multiple_of(half * rows + i * 16, 16), 16)] = total_of(half, part)

            return

        def other(part):
            self.stage[w][part] = total_of(1 - self.core, part)

        self.strips(w, other)
        self.send(w, 27, self.stage[w], self.land[w], self.mate)
        self.strips(w, lambda part: self.place(w, part, total_of(self.core, part), self.core))

    def finish(self, w):
        self.arrive(w, 27, self.land[w])

        def body(part):
            other = self.land[w][part]
            if self.kinds[w] == "sum":
                other = other + self.outs[w][part]
            self.place(w, part, other, 1 - self.core)

        self.strips(w, body)

    def drain(self):
        for w, slot in self.sent:
            if slot == 27:
                block = self.stage[w]
            elif slot >= 24:
                block = self.recv_z[w].at[0]
            else:
                block = self.recv_a[w].at[0]
            self.remote(w, slot, block, block, self.mate).wait_send()

    def opening(self, w):
        self.far(w, 1), self.far(w, 2), self.near(w, 1)

    def run(self):
        small = range(2, len(self.kinds))
        opening = self.opening
        self.meet()
        opening(0)
        for w in small:
            for j in (1, 2, 3, 0):
                self.far(w, j), self.near(w, j)
        self.relay(0, 1), self.far(0, 3), self.near(0, 2)
        self.relay(0, 2), self.far(0, 0), self.near(0, 3)
        for w in small:
            for j in (1, 2, 3, 0):
                self.relay(w, j)
        self.relay(0, 3), self.near(0, 0), self.cross(0, 1)
        opening(1)
        for w in small:
            for j in (1, 2, 3):
                self.cross(w, j)
        self.relay(0, 0), self.cross(0, 2), self.cross(0, 3)
        self.relay(1, 1), self.far(1, 3), self.near(1, 2)
        self.relay(1, 2), self.far(1, 0), self.near(1, 3)
        for w in small:
            self.last(w)
        self.relay(1, 3), self.near(1, 0), self.cross(1, 1)
        self.relay(1, 0)
        self.last(0)
        self.cross(1, 2), self.cross(1, 3)
        for w in small:
            self.finish(w)
        self.finish(0)
        self.last(1)
        self.finish(1)
        self.drain()


def scatter_scratch(shapes, early=None):
    count = len(shapes)
    scratch = [pltpu.VMEM((4,) + s[2:], BF) for s in shapes] * 2
    scratch += [pltpu.VMEM((4, 2) + s[2:], BF) for s in shapes] * 2
    scratch += [pltpu.VMEM(((3, 4, 2) if w == early else (3, 2)) + s[2:], BF) for w, s in enumerate(shapes)]
    scratch += [pltpu.VMEM(s[2:], F32) for s in shapes] * 2
    scratch += [pltpu.SemaphoreType.DMA((count, 28)), pltpu.SemaphoreType.DMA((count, 28))]
    if early is not None:
        scratch += [pltpu.VMEM((4, 2) + shapes[early][2:], BF)]
    return scratch


def scatter_shapes(shapes, kinds):
    factors = {"sum": (1, 1), "rows": (2, 1)}
    sizes = [factors.get(kind, (1, 2)) for kind in kinds]
    return [jax.ShapeDtypeStruct((s[2] * a, s[3] * b), F32) for s, (a, b) in zip(shapes, sizes)]


def scatter_kernel(kinds, *refs):
    count = len(kinds)
    Scatter(kinds, refs[:count], refs[count : 2 * count], refs[2 * count :]).run()


def scatter_chips(grads, kinds):
    devices = lax.axis_size(AX)
    shapes = [g.shape for g in grads]
    if devices != 32:
        core = lax.axis_index(AX) % 2
        summed = []
        for grad, kind in zip(grads, kinds):
            block = lax.psum_scatter(grad, AX, scatter_dimension=0, axis_index_groups=same_core_groups())
            block = block.astype(F32)
            own = lax.dynamic_index_in_dim(block, core, 0, keepdims=False)
            other = swap(lax.dynamic_index_in_dim(block, 1 - core, 0, keepdims=False))
            if kind == "sum":
                summed.append(own + other)
                continue
            rows, columns = own.shape
            own = own.reshape(rows, kind, 1, columns // kind)
            other = other.reshape(rows, kind, 1, columns // kind)
            summed.append(by_core(core, own, other, 2).reshape(rows, 2 * columns))
        return summed
    count = len(grads)
    return pl.pallas_call(
        functools.partial(scatter_kernel, kinds),
        out_shape=scatter_shapes(shapes, kinds),
        in_specs=[pl.BlockSpec(memory_space=pltpu.VMEM)] * count,
        out_specs=[pl.BlockSpec(memory_space=pltpu.VMEM)] * count,
        scratch_shapes=scatter_scratch(shapes),
        compiler_params=pltpu.CompilerParams(
            collective_id=1, has_side_effects=True, vmem_limit_bytes=56 << 20
        ),
        name="scatter_chips",
    )(*grads)


def flat(ref):
    return ref[...].reshape(-1, ref.shape[-1])


def head_masks():
    lane = lax.broadcasted_iota(jnp.int32, (1, 2 * HEAD), 1)
    return [(lane < HEAD).astype(BF), (lane >= HEAD).astype(BF)]


def attend_kernel(chunk, q_ref, k_ref, v_ref, penalty_ref, out_ref, log_ref, query_buf, mixed_buf):
    query_buf[...] = flat(q_ref) * jnp.asarray(0.125, BF)
    keys, values = flat(k_ref), flat(v_ref)
    values_t = values.T
    penalty = flat(penalty_ref)
    masks = head_masks()

    @pl.loop(0, query_buf.shape[0] // chunk)
    def _(i):
        part = pl.ds(pl.multiple_of(i * chunk, chunk), chunk)
        queries = query_buf[part]
        parts = []
        for h in range(2):
            scores = product_right_t(keys, queries * masks[h]) + penalty
            top = jnp.max(scores, axis=0, keepdims=True)
            exponent = jnp.exp(scores - top)
            total = jnp.sum(exponent, axis=0, keepdims=True)
            mixed = product(values_t[h * HEAD : (h + 1) * HEAD], exponent.astype(BF))
            parts.append(mixed * (1.0 / total))
            log_ref[0, 0, h : h + 1, part] = top + jnp.log(total)
        mixed_buf[part] = jnp.concatenate(parts, 0).T.astype(BF)

    out_ref[...] = mixed_buf[...].reshape(out_ref.shape)


def attend(projected, penalty):
    _, clips, rows, triple = projected.shape
    slots = 2 * rows
    width = triple // 3
    pairs = width // (2 * HEAD)

    def block(offset):
        return pl.BlockSpec((2, 1, rows, 2 * HEAD), lambda i, j: (0, i, 0, offset * pairs + j))

    return pl.pallas_call(
        functools.partial(attend_kernel, 256),
        grid=(clips, pairs),
        in_specs=[block(0), block(1), block(2), pl.BlockSpec((2, 1, rows, 1), lambda i, j: (0, i, 0, 0))],
        out_specs=[block(0), pl.BlockSpec((1, 1, 2, slots), lambda i, j: (i, j, 0, 0))],
        out_shape=[
            jax.ShapeDtypeStruct((2, clips, rows, width), BF),
            jax.ShapeDtypeStruct((clips, pairs, 2, slots), F32),
        ],
        scratch_shapes=[pltpu.VMEM((slots, 2 * HEAD), BF)] * 2,
        compiler_params=pltpu.CompilerParams(vmem_limit_bytes=48 << 20),
        cost_estimate=pl.CostEstimate(
            flops=4 * clips * pairs * slots * slots * 2 * HEAD, bytes_accessed=8 * clips * slots * width,
            transcendentals=clips * pairs * 2 * slots * slots,
        ),
        name="attend",
    )(projected, projected, projected, penalty)


def attend_back_kernel(chunk, *refs):
    if len(refs) == 16:
        attend_back_step(chunk, *refs)
        return
    inputs, (down_ref, norm_hbm, pre_hbm), (back_out, bias_out, down_out, up_out) = refs[:7], refs[7:10], refs[10:14]
    buffers, (norm, pre, up_buf, load_sem), scratch = refs[14:21], refs[21:25], refs[25:]
    scatter = Scatter(("rows",), (down_ref,), (down_out,), scratch)
    step = pl.program_id(0) * pl.num_programs(1) + pl.program_id(1)
    total = pl.num_programs(0) * pl.num_programs(1)

    def start():
        pltpu.make_async_copy(norm_hbm, norm, load_sem.at[0]).start()
        pltpu.make_async_copy(pre_hbm, pre, load_sem.at[1]).start()
        scatter.meet()
        scatter.opening(0)

    def two():
        scatter.relay(0, 1), scatter.far(0, 3), scatter.near(0, 2)

    def four():
        scatter.relay(0, 2), scatter.far(0, 0), scatter.near(0, 3), scatter.cross(0, 1)

    def five():
        scatter.relay(0, 3), scatter.near(0, 0)

    def six():
        scatter.cross(0, 2)

    def seven():
        scatter.relay(0, 0)

    def end():
        scatter.cross(0, 3)
        pltpu.make_async_copy(norm_hbm, norm, load_sem.at[0]).wait()
        pltpu.make_async_copy(pre_hbm, pre, load_sem.at[1]).wait()

        @pl.loop(0, norm.shape[1] // 512)
        def _(i):
            part = pl.ds(pl.multiple_of(i * 512, 512), 512)
            up_buf[part] = product_left_t(norm[:, part], pre[...]).astype(BF)
            pltpu.make_async_copy(up_buf.at[part], up_out.at[part], load_sem.at[2 + i]).start()

        scatter.last(0)
        scatter.drain()
        for i in range(norm.shape[1] // 512):
            part = pl.ds(i * 512, 512)
            pltpu.make_async_copy(up_buf.at[part], up_out.at[part], load_sem.at[2 + i]).wait()

    for place, work in ((0, start), (2, two), (4, four), (5, five), (6, six), (7, seven)):
        pl.when(step == place)(work)
    attend_back_step(chunk, *inputs, back_out, bias_out, *buffers)
    pl.when(step == total - 1)(end)


def attend_back_step(
    chunk, q_ref, k_ref, v_ref, penalty_ref, log_ref, att_ref, grad_ref, out_ref, bias_ref,
    query_buf, grad_buf, mixed_buf, back_buf, key_sum, value_sum, bias_sum,
):
    rows = q_ref.shape[2]
    pair = pl.program_id(1)
    width = out_ref.shape[3] // 3
    query_buf[...] = flat(q_ref) * jnp.asarray(0.125, BF)
    grad_buf[...] = flat(grad_ref)
    mixed_buf[...] = flat(att_ref)
    keys, values = flat(k_ref), flat(v_ref)
    keys_t = keys.T
    penalty = flat(penalty_ref)
    masks = head_masks()
    for total in (key_sum, value_sum, bias_sum):
        total[...] = jnp.zeros_like(total)

    def keep(offset, value):
        columns = pl.ds(pl.multiple_of(offset + pair * 2 * HEAD, 128), 2 * HEAD)
        for side in range(2):
            out_ref[side, 0, :, columns] = value[side * rows : (side + 1) * rows]

    for start in range(0, query_buf.shape[0], chunk):
        part = pl.ds(start, chunk)
        queries, grads = query_buf[part], grad_buf[part]
        overlap = (grads.astype(F32) * mixed_buf[part].astype(F32)).T
        parts = []
        for h in range(2):
            head_queries = queries * masks[h]
            head_grads = grads * masks[h]
            correction = jnp.sum(overlap[h * HEAD : (h + 1) * HEAD], axis=0, keepdims=True)
            logs = log_ref[0, 0, h : h + 1, part]
            soft = jnp.exp(product_right_t(keys, head_queries) + penalty - logs)
            grad_soft = product_right_t(values, head_grads)
            value_sum[...] += product(soft.astype(BF), head_grads)
            grad_scores = (soft * (grad_soft - correction)).astype(BF)
            key_sum[...] += product(grad_scores, head_queries)
            parts.append(product(keys_t[h * HEAD : (h + 1) * HEAD], grad_scores))
        grad_queries = jnp.concatenate(parts, 0).T * 0.125
        bias_sum[0:1] += jnp.sum(grad_queries, axis=0, keepdims=True)
        back_buf[part] = grad_queries.astype(BF)

    keep(0, back_buf[...])
    keep(width, key_sum[...].astype(BF))
    keep(2 * width, value_sum[...].astype(BF))
    bias_ref[0, 0, 0:1] = bias_sum[0:1]
    bias_ref[0, 0, 1:2] = jnp.sum(value_sum[...], axis=0, keepdims=True)


def attend_back(projected, penalty, logs, attended, grad_attended, grad_down, norm_two, grad_pre):
    _, clips, rows, triple = projected.shape
    slots = 2 * rows
    width = triple // 3
    pairs = width // (2 * HEAD)
    fused = lax.axis_size(AX) == 32 and clips * pairs == 8

    def block(offset):
        return pl.BlockSpec((2, 1, rows, 2 * HEAD), lambda i, j: (0, i, 0, offset * pairs + j))

    in_specs = [
        block(0), block(1), block(2),
        pl.BlockSpec((2, 1, rows, 1), lambda i, j: (0, i, 0, 0)),
        pl.BlockSpec((1, 1, 2, slots), lambda i, j: (i, j, 0, 0)),
        block(0), block(0),
    ]
    out_specs = [
        pl.BlockSpec((2, 1, rows, triple), lambda i, j: (0, i, 0, 0)),
        pl.BlockSpec((1, 1, 2, 2 * HEAD), lambda i, j: (i, j, 0, 0)),
    ]
    out_shape = [
        jax.ShapeDtypeStruct((2, clips, rows, triple), BF),
        jax.ShapeDtypeStruct((clips, pairs, 2, 2 * HEAD), F32),
    ]
    operands = [projected, projected, projected, penalty, logs, attended, grad_attended]
    scratch = [pltpu.VMEM((slots, 2 * HEAD), BF)] * 4 + [pltpu.VMEM((slots, 2 * HEAD), F32)] * 2
    scratch += [pltpu.VMEM((8, 2 * HEAD), F32)]
    params = pltpu.CompilerParams(vmem_limit_bytes=60 << 20)
    if fused:
        up_shape = (norm_two.shape[1], grad_pre.shape[1])
        sums = scatter_shapes([grad_down.shape], ("rows",))
        in_specs += [pl.BlockSpec(grad_down.shape, lambda i, j: (0, 0, 0, 0), pipeline_mode=pl.Buffered(1))]
        in_specs += [pl.BlockSpec(memory_space=pl.ANY)] * 2
        out_specs += [pl.BlockSpec(sums[0].shape, lambda i, j: (0, 0)), pl.BlockSpec(memory_space=pl.ANY)]
        out_shape += [sums[0], jax.ShapeDtypeStruct(up_shape, BF)]
        operands += [grad_down, norm_two, grad_pre]
        scratch += [pltpu.VMEM(norm_two.shape, BF), pltpu.VMEM(grad_pre.shape, BF), pltpu.VMEM(up_shape, BF)]
        scratch += [pltpu.SemaphoreType.DMA((2 + up_shape[0] // 512,))]
        scratch += scatter_scratch([grad_down.shape])
        params = pltpu.CompilerParams(vmem_limit_bytes=60 << 20, collective_id=2, has_side_effects=True)
    outs = pl.pallas_call(
        functools.partial(attend_back_kernel, 256),
        grid=(clips, pairs),
        in_specs=in_specs,
        out_specs=out_specs,
        out_shape=out_shape,
        scratch_shapes=scratch,
        compiler_params=params,
        cost_estimate=pl.CostEstimate(
            flops=10 * clips * pairs * slots * slots * 2 * HEAD, bytes_accessed=18 * clips * slots * width,
            transcendentals=clips * pairs * 2 * slots * slots,
        ),
        name="attend_back",
    )(*operands)
    if not fused:
        total = lax.psum_scatter(grad_down, AX, scatter_dimension=0, axis_index_groups=same_core_groups())
        total = total.astype(F32).reshape(-1, total.shape[-1])
        outs = [*outs, total, outer(norm_two, grad_pre)]
    return outs


def normal_parts(values):
    average = jnp.mean(values, axis=-1, keepdims=True)
    centered = values - average
    inverse = lax.rsqrt(jnp.mean(centered * centered, axis=-1, keepdims=True) + EPSILON)
    return centered * inverse, inverse


def normal_back(grad_normed, scaled, inverse, gain):
    grad_scaled = grad_normed * gain
    first_mean = jnp.mean(grad_scaled, axis=-1, keepdims=True)
    second_mean = jnp.mean(grad_scaled * scaled, axis=-1, keepdims=True)
    return inverse * (grad_scaled - first_mean - scaled * second_mean)


def rows_spec(size, columns):
    return pl.BlockSpec((size, columns), lambda i: (i, 0))


def whole_spec(shape):
    return pl.BlockSpec(shape, lambda i: (0,) * len(shape), pipeline_mode=pl.Buffered(1))


PARAMS = pltpu.CompilerParams(vmem_limit_bytes=56 << 20)


def strips_of(ref):
    return [pl.ds(start, 32) for start in range(0, ref.shape[0], 32)]


def project_kernel(steps, own_ref, other_ref, gain_ref, shift_ref, weight_ref, bias_ref, norm_ref, out_ref):
    is_own = pl.program_id(0) < steps
    for part in strips_of(own_ref):
        rows = jnp.where(is_own, own_ref[part].astype(F32), other_ref[part].astype(F32))
        scaled, _ = normal_parts(rows)
        norm_ref[part] = (scaled * gain_ref[...] + shift_ref[...]).astype(BF)
    out_ref[...] = (product(norm_ref[...], weight_ref[...]) + bias_ref[...]).astype(BF)


def project(own, other, gain, shift, weight, bias):
    rows, features = own.shape
    columns = weight.shape[1]
    steps = 3
    size = rows // steps
    return pl.pallas_call(
        functools.partial(project_kernel, steps),
        grid=(2 * steps,),
        in_specs=[
            pl.BlockSpec((size, features), lambda i: (jnp.minimum(i, steps - 1), 0)),
            pl.BlockSpec((size, features), lambda i: (jnp.maximum(i - steps, 0), 0)),
            whole_spec((1, features)),
            whole_spec((1, features)),
            whole_spec((features, columns)),
            whole_spec((1, columns)),
        ],
        out_specs=[rows_spec(size, features), rows_spec(size, columns)],
        out_shape=[
            jax.ShapeDtypeStruct((2 * rows, features), BF),
            jax.ShapeDtypeStruct((2 * rows, columns), BF),
        ],
        compiler_params=PARAMS,
        name="project",
    )(own, other, gain, shift, weight, bias)


def second_norm_kernel(att_ref, weight_ref, token_ref, recv_ref, bias_ref, gain_ref, shift_ref, middle_ref, out_ref):
    mixed = product(att_ref[...], weight_ref[...])
    for part in strips_of(token_ref):
        middle = token_ref[part].astype(F32) + mixed[part.start : part.start + part.size]
        middle = middle + recv_ref[part].astype(F32) + bias_ref[...]
        middle_ref[part] = middle
        scaled, _ = normal_parts(middle)
        out_ref[part] = (scaled * gain_ref[...] + shift_ref[...]).astype(BF)


def second_norm(attended, weight, tokens, received, bias, gain, shift):
    rows, features = tokens.shape
    width = weight.shape[0]
    size = rows // 4
    return pl.pallas_call(
        second_norm_kernel,
        grid=(4,),
        in_specs=[
            rows_spec(size, width), whole_spec((width, features)), rows_spec(size, features), rows_spec(size, features),
            whole_spec((1, features)), whole_spec((1, features)), whole_spec((1, features)),
        ],
        out_specs=[rows_spec(size, features), rows_spec(size, features)],
        out_shape=[jax.ShapeDtypeStruct((rows, features), F32), jax.ShapeDtypeStruct((rows, features), BF)],
        compiler_params=PARAMS,
        name="second_norm",
    )(attended, weight, tokens, received, bias, gain, shift)


def feed_kernel(
    steps, unit, own_ref, other_ref, grad_own_ref, grad_other_ref, mark_ref, bias_ref, *refs
):
    if len(refs) == 14:
        both_ref, refs = refs[0], refs[1:]
        sources = None
    else:
        sources, refs = refs[:2], refs[2:]
    act_ref, pre_ref, norm_ref, grad_ref, pass_own_ref, pass_other_ref, sums_ref, down_hbm = refs[:8]
    up_ref, down_ref, up_sem, down_sem, out_sem = refs[8:]
    step = pl.program_id(0)
    features, hidden = up_ref.shape

    @pl.when(step == 0)
    def _():
        sums_ref[...] = jnp.zeros_like(sums_ref)
        if sources is not None:
            pltpu.make_async_copy(sources[0], up_ref, up_sem).start()
            pltpu.make_async_copy(sources[1], down_ref, down_sem).start()
        else:
            core = lax.axis_index(AX) % 2
            chips = hidden // unit
            shard = features // (2 * chips)
            for k in range(chips):
                device = 2 * k + core
                pltpu.make_async_copy(
                    both_ref.at[:, pl.ds(pl.multiple_of(device * unit, 128), unit)],
                    up_ref.at[:, k * unit : (k + 1) * unit],
                    up_sem,
                ).start()
            for k in range(chips):
                device = 2 * k + core
                for q in range(unit // shard):
                    pltpu.make_async_copy(
                        both_ref.at[
                            pl.ds(pl.multiple_of(device * shard, 16), shard),
                            pl.ds(2 * hidden + q * features, features),
                        ],
                        down_ref.at[k * unit + q * shard : k * unit + (q + 1) * shard],
                        down_sem,
                    ).start()
        pltpu.make_async_copy(up_ref, up_ref, up_sem).wait()
        pltpu.make_async_copy(down_ref, down_ref, down_sem).wait()
        pltpu.make_async_copy(down_ref, down_hbm, out_sem).start()

    rows = jnp.where(step < steps, other_ref[...], own_ref[...])
    grads = jnp.where(step < steps, grad_other_ref[...], grad_own_ref[...]) * mark_ref[...].astype(BF)
    norm_ref[...] = rows
    grad_ref[...] = grads
    size = 512
    for start in range(0, hidden, size):
        part = slice(start, start + size)
        pre = product(rows, up_ref[:, part]) + bias_ref[:, part]
        normal_cdf = 0.5 * (1.0 + lax.erf(pre * ROOT_HALF))
        density = jnp.exp(-0.5 * pre * pre) * INV_ROOT_TWO_PI
        act_ref[:, part] = (pre * normal_cdf).astype(BF)
        grad_pre = product_right_t(grads, down_ref[part]) * (normal_cdf + pre * density)
        sums_ref[0:1, part] += jnp.sum(grad_pre, axis=0, keepdims=True)
        pre_ref[:, part] = grad_pre.astype(BF)
    passed = product_right_t(pre_ref[...], up_ref[...])
    pass_own_ref[...] = passed

    @pl.when(step < steps)
    def _():
        pass_other_ref[...] = passed.astype(BF)

    @pl.when(step == 2 * steps - 1)
    def _():
        pltpu.make_async_copy(down_ref, down_hbm, out_sem).wait()


def feed(own, other, grad_own, grad_other, marks, weights, bias, unit):
    rows, features = own.shape
    hidden = bias.shape[1]
    steps = 3
    size = rows // steps

    def side(i):
        return jnp.where(i < steps, i + steps, i - steps)

    def both_spec(columns):
        return pl.BlockSpec((size, columns), lambda i: (side(i), 0))

    own_spec = pl.BlockSpec((size, features), lambda i: (jnp.maximum(i - steps, 0), 0))
    other_spec = pl.BlockSpec((size, features), lambda i: (jnp.minimum(i, steps - 1), 0))
    return pl.pallas_call(
        functools.partial(feed_kernel, steps, unit),
        grid=(2 * steps,),
        in_specs=[own_spec, other_spec, own_spec, other_spec, both_spec(1), whole_spec((1, hidden))]
        + [pl.BlockSpec(memory_space=pl.ANY)] * len(weights),
        out_specs=[
            both_spec(hidden), both_spec(hidden), both_spec(features), both_spec(features),
            own_spec, other_spec,
            pl.BlockSpec((8, hidden), lambda i: (0, 0)), pl.BlockSpec(memory_space=pl.ANY),
        ],
        out_shape=[
            jax.ShapeDtypeStruct((2 * rows, hidden), BF), jax.ShapeDtypeStruct((2 * rows, hidden), BF),
            jax.ShapeDtypeStruct((2 * rows, features), BF), jax.ShapeDtypeStruct((2 * rows, features), BF),
            jax.ShapeDtypeStruct((rows, features), F32), jax.ShapeDtypeStruct((rows, features), BF),
            jax.ShapeDtypeStruct((8, hidden), F32), jax.ShapeDtypeStruct((hidden, features), BF),
        ],
        scratch_shapes=[
            pltpu.VMEM((features, hidden), BF), pltpu.VMEM((hidden, features), BF),
            pltpu.SemaphoreType.DMA(()), pltpu.SemaphoreType.DMA(()), pltpu.SemaphoreType.DMA(()),
        ],
        compiler_params=PARAMS,
        cost_estimate=pl.CostEstimate(
            flops=12 * rows * features * hidden, bytes_accessed=8 * features * hidden,
            transcendentals=4 * rows * hidden,
        ),
        name="feed",
    )(own, other, grad_own, grad_other, marks, bias, *weights)


def outer_kernel(left_ref, right_ref, out_ref):
    out_ref[...] = product_left_t(left_ref[...], right_ref[...]).astype(BF)


def outer(left, right):
    rows, columns = left.shape
    width = right.shape[1]
    size = 512
    return pl.pallas_call(
        outer_kernel,
        grid=(columns // size,),
        in_specs=[pl.BlockSpec((rows, size), lambda i: (0, i)), whole_spec((rows, width))],
        out_specs=rows_spec(size, width),
        out_shape=jax.ShapeDtypeStruct((columns, width), BF),
        compiler_params=PARAMS,
        cost_estimate=pl.CostEstimate(
            flops=2 * rows * columns * width, bytes_accessed=2 * (rows * columns + rows * width + columns * width),
            transcendentals=0,
        ),
        name="outer",
    )(left, right)


def gather_sums(sums_ref, values):
    for index, value in enumerate(values):
        sums_ref[index : index + 1] += jnp.sum(value, axis=0, keepdims=True)


def clear_first(sums_ref):
    @pl.when(pl.program_id(0) == 0)
    def _():
        sums_ref[...] = jnp.zeros_like(sums_ref)


def second_back_kernel(
    grad_ref, recv_ref, middle_ref, out_ref, gain_ref, full_ref, low_ref, sums_ref
):
    clear_first(sums_ref)
    for part in strips_of(grad_ref):
        grad_normed = grad_ref[part] + recv_ref[part].astype(F32)
        scaled, inverse = normal_parts(middle_ref[part])
        grad_out = out_ref[part].astype(F32)
        grad_middle = grad_out + normal_back(grad_normed, scaled, inverse, gain_ref[...])
        full_ref[part] = grad_middle
        low_ref[part] = grad_middle.astype(BF)
        gather_sums(sums_ref, [grad_normed * scaled, grad_normed, grad_middle, grad_out])


def second_back(passed, received, middle, grad_out, gain):
    rows, features = middle.shape
    size = rows // 4
    return pl.pallas_call(
        second_back_kernel,
        grid=(4,),
        in_specs=[rows_spec(size, features)] * 4 + [whole_spec((1, features))],
        out_specs=[rows_spec(size, features)] * 2 + [pl.BlockSpec((8, features), lambda i: (0, 0))],
        out_shape=[
            jax.ShapeDtypeStruct((rows, features), F32), jax.ShapeDtypeStruct((rows, features), BF),
            jax.ShapeDtypeStruct((8, features), F32),
        ],
        compiler_params=PARAMS,
        name="second_back",
    )(passed, received, middle, grad_out, gain)


def first_back_kernel(grad_ref, weight_ref, recv_ref, token_ref, middle_ref, gain_ref, full_ref, sums_ref):
    clear_first(sums_ref)
    passed = product_right_t(grad_ref[...], weight_ref[...])
    for part in strips_of(grad_ref):
        grad_normed = passed[part.start : part.start + part.size] + recv_ref[part].astype(F32)
        scaled, inverse = normal_parts(token_ref[part].astype(F32))
        full_ref[part] = middle_ref[part] + normal_back(grad_normed, scaled, inverse, gain_ref[...])
        gather_sums(sums_ref, [grad_normed * scaled, grad_normed])


def first_back(grad_projected, weight, received, tokens, grad_middle, gain):
    rows, features = tokens.shape
    triple = weight.shape[1]
    size = rows // 4
    return pl.pallas_call(
        first_back_kernel,
        grid=(4,),
        in_specs=[
            rows_spec(size, triple), whole_spec((features, triple)), rows_spec(size, features),
            rows_spec(size, features), rows_spec(size, features), whole_spec((1, features)),
        ],
        out_specs=[rows_spec(size, features), pl.BlockSpec((8, features), lambda i: (0, 0))],
        out_shape=[jax.ShapeDtypeStruct((rows, features), F32), jax.ShapeDtypeStruct((8, features), F32)],
        compiler_params=PARAMS,
        name="first_back",
    )(grad_projected, weight, received, tokens, grad_middle, gain)


def tail_kernel(
    kinds, sums_ref, bias_ref, gain_ref, shift_ref, up_hbm, proj_hbm,
    back_hbm, weight_hbm, norm_hbm, token_hbm, middle_hbm, down_hbm, act_hbm, sum_hbm,
    up_out, qkv_out, proj_out, packed_out, tokens_out, block_out, *refs
):
    back, weight, norm, token, middle, down, qkv, packed, vectors, stage, land, load_sem, pass_sem = refs[:13]
    act, total, lift_stage, lift_land, block_sem, up_ref, proj_ref = refs[13:20]
    scatter = Scatter(
        kinds, (up_ref, qkv, proj_ref, packed), (up_out, qkv_out, proj_out, packed_out), refs[20:], 2,
        (up_hbm, qkv, proj_hbm, packed),
    )
    chips, _, shard, triple = qkv.shape
    own_rows = token.shape[0]
    loads = [
        pltpu.make_async_copy(source, target, load_sem.at[i])
        for i, (source, target) in enumerate(
            (
                (back_hbm, back), (weight_hbm, weight), (norm_hbm, norm), (token_hbm, token), (middle_hbm, middle),
                (down_hbm, down), (up_hbm, up_ref), (proj_hbm, proj_ref),
            )
        )
    ]
    scatter.meet()
    scatter.opening(0)
    scatter.along(2)
    for place in (0, 1, 6, 2, 7, 3, 4, 5):
        loads[place].start()
    vectors[...] = jnp.zeros_like(vectors)
    vectors[0:8] = sums_ref[...]
    loads[0].wait(), loads[1].wait()

    @pl.loop(0, own_rows // 256)
    def _(i):
        part = pl.ds(pl.multiple_of(own_rows + i * 256, 256), 256)
        stage[pl.ds(pl.multiple_of(i * 256, 256), 256)] = product_right_t(back[part], weight[...]).astype(BF)

    passing = pltpu.make_async_remote_copy(
        src_ref=stage, dst_ref=land, send_sem=pass_sem.at[0], recv_sem=pass_sem.at[1],
        device_id=(scatter.mate,), device_id_type=MESH,
    )
    passing.start()
    loads[6].wait(), loads[7].wait()
    scatter.relay(0, 1), scatter.far(0, 3), scatter.near(0, 2)
    loads[2].wait()

    @pl.loop(0, norm.shape[1] // 256)
    def _(i):
        part = pl.ds(pl.multiple_of(i * 256, 256), 256)
        count = 256 // (2 * shard)
        grad = product_left_t(norm[:, part], back[...]).astype(BF)
        qkv[pl.ds(i * count, count)] = grad.reshape(count, 2, shard, triple)

    scatter.relay(0, 2), scatter.far(0, 0), scatter.near(0, 3)
    scatter.opening(1)
    loads[3].wait(), loads[4].wait()
    passing.wait()

    @pl.loop(0, own_rows // 256)
    def _(i):
        start = pl.multiple_of(i * 256, 256)
        passed = product_right_t(back[pl.ds(start, 256)], weight[...])
        for strip in range(0, 256, 32):
            part = pl.ds(start + strip, 32)
            grad_normed = passed[strip : strip + 32] + land[part].astype(F32)
            scaled, inverse = normal_parts(token[part].astype(F32))
            tokens_out[part] = middle[part] + normal_back(grad_normed, scaled, inverse, gain_ref[...])
            vectors[0:1] += jnp.sum(grad_normed * scaled, axis=0, keepdims=True)
            vectors[1:2] += jnp.sum(grad_normed, axis=0, keepdims=True)

    scatter.relay(0, 3), scatter.near(0, 0), scatter.cross(0, 1), scatter.cross(0, 2)
    packed[:, :, :shard] = vectors[...].T.astype(BF).reshape(chips, 2, shard, PARAM_COLS)
    packed[:, :, shard:] = bias_ref[...]
    for j in (1, 2, 3, 0):
        scatter.far(3, j), scatter.near(3, j)
    scatter.layer_sum(2)
    scatter.far(2, 0), scatter.near(2, 0)
    scatter.relay(0, 0), scatter.cross(0, 3)
    loads[5].wait()

    def fetch(source, start, target, slot):
        copy = pltpu.make_async_copy(source.at[pl.ds(start, 256)], target, block_sem.at[slot])
        copy.start()
        return copy

    @pl.loop(0, own_rows // 256)
    def _(i):
        fetch(act_hbm, pl.multiple_of(own_rows + i * 256, 256), act, 0).wait()
        lift_stage[pl.ds(pl.multiple_of(i * 256, 256), 256)] = product(act[...], down[...]).astype(BF)

    lifting = pltpu.make_async_remote_copy(
        src_ref=lift_stage, dst_ref=lift_land, send_sem=pass_sem.at[2], recv_sem=pass_sem.at[3],
        device_id=(scatter.mate,), device_id_type=MESH,
    )
    lifting.start()
    scatter.relay(2, 0)
    scatter.relay(1, 1), scatter.far(1, 3), scatter.near(1, 2)
    scatter.relay(1, 2), scatter.far(1, 0), scatter.near(1, 3)
    lifting.wait()

    @pl.loop(0, own_rows // 256)
    def _(i):
        start = pl.multiple_of(i * 256, 256)
        copies = fetch(act_hbm, start, act, 0), fetch(sum_hbm, start, total, 1)
        for copy in copies:
            copy.wait()
        lifted = product(act[...], down[...]) + lift_land[pl.ds(start, 256)].astype(F32)
        block_out[pl.ds(start, 256)] = (total[...] + lifted + shift_ref[...]).astype(BF)

    for j in (1, 2, 3, 0):
        scatter.relay(3, j)
    scatter.last(2)
    scatter.relay(1, 3), scatter.near(1, 0), scatter.cross(1, 1)
    for j in (1, 2, 3):
        scatter.cross(3, j)
    scatter.relay(1, 0)
    scatter.last(0)
    scatter.cross(1, 2), scatter.cross(1, 3)
    scatter.finish(2), scatter.finish(0)
    scatter.last(3)
    scatter.last(1)
    scatter.finish(3), scatter.finish(1)
    scatter.drain()


def tail(grad_up, grad_proj, sums, bias_rows, gain, shift, back, weight, norm, tokens, grad_middle, down, act, middle):
    chips, _, shard, hidden = grad_up.shape
    rows, triple = back.shape
    own_rows, features = tokens.shape
    extra = bias_rows.shape[2]
    kinds = (chips, 3, 1, "sum")
    shapes = [
        grad_up.shape, (chips, 2, shard, triple), grad_proj.shape, (chips, 2, shard + extra, PARAM_COLS),
    ]
    vmem = pl.BlockSpec(memory_space=pltpu.VMEM)
    return pl.pallas_call(
        functools.partial(tail_kernel, kinds),
        out_shape=scatter_shapes(shapes, kinds)
        + [jax.ShapeDtypeStruct((own_rows, features), F32), jax.ShapeDtypeStruct((own_rows, features), BF)],
        in_specs=[vmem] * 4 + [pl.BlockSpec(memory_space=pl.ANY)] * 10,
        out_specs=[vmem] * 6,
        scratch_shapes=[
            pltpu.VMEM(back.shape, BF), pltpu.VMEM(weight.shape, BF), pltpu.VMEM(norm.shape, BF),
            pltpu.VMEM(tokens.shape, BF), pltpu.VMEM(middle.shape, F32), pltpu.VMEM(down.shape, BF),
            pltpu.VMEM(shapes[1], BF), pltpu.VMEM(shapes[3], BF), pltpu.VMEM((PARAM_COLS, features), F32),
            pltpu.VMEM((own_rows, features), BF), pltpu.VMEM((own_rows, features), BF),
            pltpu.SemaphoreType.DMA((8,)), pltpu.SemaphoreType.DMA((4,)),
            pltpu.VMEM((256, act.shape[1]), BF), pltpu.VMEM((256, features), F32),
            pltpu.VMEM((own_rows, features), BF), pltpu.VMEM((own_rows, features), BF), pltpu.SemaphoreType.DMA((2,)),
            pltpu.VMEM(grad_up.shape, BF), pltpu.VMEM(grad_proj.shape, BF),
        ]
        + scatter_scratch(shapes, 2),
        compiler_params=pltpu.CompilerParams(collective_id=1, has_side_effects=True, vmem_limit_bytes=62 << 20),
        name="tail",
    )(sums, bias_rows, gain, shift, grad_up, grad_proj, back, weight, norm, tokens, grad_middle, down, act, middle)


def pack_kernel(up_ref, down_ref, out_ref):
    shard, columns = up_ref.shape
    features = down_ref.shape[1]
    out_ref[:, :columns] = up_ref[...]
    for i in range(down_ref.shape[0] // shard):
        out_ref[:, columns + i * features : columns + (i + 1) * features] = down_ref[i * shard : (i + 1) * shard]


def pack(up, down):
    shard, columns = up.shape
    fold = down.shape[0] // shard
    if shard % 16 != 0:
        return jnp.concatenate([up] + [down[shard * i : shard * (i + 1)] for i in range(fold)], 1)
    return pl.pallas_call(
        pack_kernel,
        out_shape=jax.ShapeDtypeStruct((shard, columns + fold * down.shape[1]), BF),
        in_specs=[pl.BlockSpec(memory_space=pltpu.VMEM)] * 2,
        out_specs=pl.BlockSpec(memory_space=pltpu.VMEM),
        name="pack",
    )(up, down)


def finish_kernel(
    up_ref, qkv_ref, proj_ref, down_ref, token_ref, block_ref, packed_ref,
    up_out, qkv_out, proj_out, down_out, token_out, block_out, vec_out, bias_out,
):
    token_out[...] = token_ref[...]
    block_out[...] = block_ref[...]
    up_out[...] = up_ref[...]
    qkv_out[...] = qkv_ref[...]
    proj_out[...] = proj_ref[...]
    down_out[...] = down_ref[...]
    shard = vec_out.shape[1]
    vec_out[...] = packed_ref[:shard].T[:8]
    bias_out[...] = packed_ref[shard : shard + 1]


def finish(up, qkv, proj, down, tokens, block, packed, shard, unit):
    if lax.axis_size(AX) != 32:
        return up, qkv, proj, down, tokens, block, packed[:shard, :8].T, packed[shard : shard + 1, :unit]
    return pl.pallas_call(
        finish_kernel,
        out_shape=[jax.ShapeDtypeStruct(a.shape, a.dtype) for a in (up, qkv, proj, down, tokens, block)]
        + [jax.ShapeDtypeStruct((8, shard), F32), jax.ShapeDtypeStruct((1, unit), F32)],
        in_specs=[pl.BlockSpec(memory_space=pltpu.VMEM)] * 7,
        out_specs=[pl.BlockSpec(memory_space=pltpu.VMEM)] * 8,
        compiler_params=PARAMS,
        name="finish",
    )(up, qkv, proj, down, tokens, block, packed)


def by_core(core, own, other, axis):
    return jnp.where(core == 0, jnp.concatenate([own, other], axis), jnp.concatenate([other, own], axis))


def per_device(
    tokens, valid_slots, cotangent, first_gain, first_shift, qkv_weight, query_bias, value_bias, proj_weight,
    proj_bias, second_gain, second_shift, up_weight, up_bias, down_weight, down_bias,
):
    devices = lax.axis_size(AX)
    chips = devices // 2
    core = lax.axis_index(AX) % 2
    micro, rows, features = tokens.shape
    shard = qkv_weight.shape[0]
    width = features // 2
    hidden = up_weight.shape[1] // 2
    unit = hidden // chips
    own_rows = micro * rows
    every = 2 * own_rows

    fold = unit // shard
    both_weights = lax.all_gather(pack(up_weight, down_weight), AX, axis=0, tiled=True)
    feed_weights = [both_weights]
    if unit % 128 != 0 or shard % 16 != 0:
        half_up = both_weights[:, : 2 * hidden].reshape(features, chips, 2, unit)
        half_up = lax.dynamic_index_in_dim(half_up, core, 2, keepdims=False).reshape(features, hidden)
        half_down = both_weights[:, 2 * hidden :].reshape(chips, 2, shard, fold, features)
        half_down = lax.dynamic_index_in_dim(half_down, core, 1, keepdims=False)
        half_down = half_down.transpose(0, 2, 1, 3).reshape(hidden, features)
        feed_weights = [half_up, half_down]
    vectors = jnp.stack(
        [first_gain, first_shift, query_bias, value_bias, proj_bias, second_gain, second_shift, down_bias], 0
    )
    lanes = max(PARAM_COLS, unit)
    vectors = jnp.pad(vectors.T, ((0, 16), (0, lanes - 8)))
    packed = lax.dynamic_update_slice(vectors, up_bias[None, :], (shard, 0))
    qkv_all, proj_all, packed_all = gather_chips(qkv_weight, proj_weight, packed)
    weight_qkv = qkv_all.reshape(features, 3 * width)
    params = packed_all[:, :, :shard, :8].astype(F32).reshape(features, 8).T
    gain_one, shift_one, bias_query, bias_value, bias_proj, gain_two, shift_two, bias_down = [
        params[i : i + 1] for i in range(8)
    ]
    bias_up = lax.dynamic_index_in_dim(packed_all[:, :, shard, :unit], core, 1, keepdims=False)
    bias_up = bias_up.astype(F32).reshape(1, hidden)
    proj_cols = proj_all.reshape(2, width, width)
    proj_own = lax.dynamic_index_in_dim(proj_cols, core, 0, keepdims=False)
    proj_other = swap(lax.dynamic_index_in_dim(proj_cols, 1 - core, 0, keepdims=False))
    weight_proj = by_core(core, proj_own, proj_other, 1)
    qkv_bias = jnp.concatenate(
        [
            lax.dynamic_slice_in_dim(bias_query, core * width, width, 1),
            jnp.zeros((1, width), F32),
            lax.dynamic_slice_in_dim(bias_value, core * width, width, 1),
        ],
        1,
    )

    own_tokens = tokens.reshape(own_rows, features)
    other_tokens = swap(own_tokens)
    marks = jnp.stack([valid_slots, swap(valid_slots)])
    own_cotangent = cotangent.reshape(own_rows, features)
    penalty = jnp.where(marks > 0, 0.0, -1000000000.0).astype(F32)[..., None]
    norm_one, projected = project(own_tokens, other_tokens, gain_one, shift_one, weight_qkv, qkv_bias)
    projected = projected.reshape(2, micro, rows, 3 * width)
    attended, logs = attend(projected, penalty)
    attended_flat = attended.reshape(every, width)
    mixed = swap(product(attended_flat[own_rows:], weight_proj).astype(BF))
    middle, norm_own = second_norm(
        attended_flat, weight_proj, own_tokens, mixed, bias_proj, gain_two, shift_two
    )
    activation, grad_pre, norm_two, grad_out, passed, passed_other, up_sums, weight_down = feed(
        norm_own, swap(norm_own), own_cotangent, swap(own_cotangent),
        (marks > 0).astype(F32).reshape(every, 1), feed_weights, bias_up, unit,
    )
    grad_bias_up = up_sums[0]
    passed_other = swap(passed_other)

    grad_down = outer(activation, grad_out)
    passed_other, grad_down = lax.optimization_barrier((passed_other, grad_down))
    grad_middle, grad_low, second_sums = second_back(passed, passed_other, middle, grad_out, gain_two)
    grad_low = jnp.concatenate([grad_low, swap(grad_low)], 0)
    grad_attended = product_right_t(grad_low, weight_proj).astype(BF).reshape(2, micro, rows, width)
    grad_proj = product_left_t(attended_flat, grad_low).astype(BF)
    grad_attended, grad_proj = lax.optimization_barrier((grad_attended, grad_proj))
    grad_proj_own = lax.dynamic_slice_in_dim(grad_proj, core * width, width, 1)
    grad_proj_other = swap(lax.dynamic_slice_in_dim(grad_proj, (1 - core) * width, width, 1))
    grad_proj = by_core(core, grad_proj_own, grad_proj_other, 0)
    grad_projected, grad_bias, down_weight_grad, grad_up = attend_back(
        projected, penalty, logs, attended, grad_attended, grad_down.reshape(chips, 2, unit // 2, features),
        norm_two, grad_pre,
    )
    grad_projected = grad_projected.reshape(every, 3 * width)

    grad_bias = jnp.sum(grad_bias, axis=0).transpose(1, 0, 2).reshape(2, width)
    grad_bias = by_core(core, grad_bias, jnp.zeros_like(grad_bias), 1)
    sums = [grad_bias, second_sums[2:3], second_sums[:2], second_sums[3:4]]
    up_units = grad_bias_up.astype(BF).reshape(chips, 1, unit)
    up_units = by_core(core, up_units, jnp.zeros_like(up_units), 1).reshape(chips, 2, 1, unit)
    grad_up = grad_up.reshape(chips, 2, shard, hidden)
    grad_proj = grad_proj.reshape(chips, 2, shard, width)
    if devices == 32:
        bias_rows = jnp.pad(up_units, ((0, 0), (0, 0), (0, 15), (0, 0)))
        sums = jnp.concatenate([jnp.zeros((2, features), F32)] + sums, 0)
        up_weight_grad, qkv_weight_grad, proj_weight_grad, packed_sum, tokens_grad, block_output = tail(
            grad_up, grad_proj, sums, bias_rows, gain_one, bias_down, grad_projected, weight_qkv, norm_one, own_tokens,
            grad_middle, weight_down, activation, middle,
        )
    else:
        lifted = swap(product(activation[own_rows:], weight_down).astype(BF)).astype(F32)
        block_output = (middle + product(activation[:own_rows], weight_down) + lifted + bias_down).astype(BF)
        passed = swap(product_right_t(grad_projected[own_rows:], weight_qkv).astype(BF))
        grad_qkv = outer(norm_one, grad_projected)
        tokens_grad, first_sums = first_back(
            grad_projected, weight_qkv, passed, own_tokens, grad_middle, gain_one
        )
        sums = jnp.concatenate([first_sums[:2]] + sums, 0)
        sums = sums.astype(BF).T.reshape(chips, 2, shard, 8)
        sums = jnp.pad(sums, ((0, 0), (0, 0), (0, 16), (0, lanes - 8)))
        sums = lax.dynamic_update_slice(sums, up_units, (0, 0, shard, 0))
        up_weight_grad, qkv_weight_grad, proj_weight_grad, packed_sum = scatter_chips(
            [grad_up, grad_qkv.reshape(chips, 2, shard, 3 * width), grad_proj, sums], (chips, 3, 1, "sum")
        )
    (
        up_weight_grad, qkv_weight_grad, proj_weight_grad, down_weight_grad, tokens_grad, block_output,
        vector_sum, up_bias_grad,
    ) = finish(
        up_weight_grad, qkv_weight_grad, proj_weight_grad, down_weight_grad, tokens_grad, block_output,
        packed_sum, shard, unit,
    )
    tokens_grad = tokens_grad.reshape(micro, rows, features)
    block_output = block_output.reshape(micro, rows, features)
    up_bias_grad = up_bias_grad[0]
    return (
        block_output, tokens_grad, vector_sum[0], vector_sum[1], qkv_weight_grad, vector_sum[2], vector_sum[3],
        proj_weight_grad, vector_sum[4], vector_sum[5], vector_sum[6], up_weight_grad, up_bias_grad,
        down_weight_grad, vector_sum[7],
    )


def solution(mesh):
    row = P(None, AX, None)
    vec = P(AX)
    mat = P(AX, None)
    return jax.shard_map(
        per_device,
        mesh=mesh,
        in_specs=(row, P(None, AX), row, vec, vec, mat, vec, vec, mat, vec, vec, vec, mat, vec, mat, vec),
        out_specs=(row, row, vec, vec, mat, vec, vec, mat, vec, vec, vec, mat, vec, mat, vec),
        check_vma=False,
    )
```

```python
import functools

import jax
import jax.numpy as jnp
from jax import lax
from jax.experimental import pallas as pl
from jax.experimental.pallas import tpu as pltpu
from jax.sharding import PartitionSpec as P

AX = "fsdp"
MESH = pl.DeviceIdType.MESH
HEAD = 64
EPSILON = 1e-06
ROOT_HALF = 0.7071067811865476
INV_ROOT_TWO_PI = 0.3989422804014327
BF = jnp.bfloat16
F32 = jnp.float32
PARAM_COLS = 128


def product(left_side, right_side):
    return jnp.dot(left_side, right_side, preferred_element_type=F32)


def product_left_t(left_side, right_side):
    return lax.dot_general(left_side, right_side, (((0,), (0,)), ((), ())), preferred_element_type=F32)


def product_right_t(left_side, right_side):
    return lax.dot_general(left_side, right_side, (((1,), (1,)), ((), ())), preferred_element_type=F32)


def swap(shard):
    return lax.ppermute(shard, AX, [(i, i ^ 1) for i in range(lax.axis_size(AX))])


def same_core_groups():
    count = lax.axis_size(AX)
    return [[i for i in range(count) if i % 2 == core] for core in (0, 1)]


def flip(index, step):
    return index + step - 2 * step * ((index // step) % 2)


def peers_of(me):
    return flip(me, 1), flip(me, 2), flip(me, 4), [flip(me, 8), flip(me, 16), flip(flip(me, 8), 16)]


def zflip(chip, j):
    return [chip, flip(chip, 4), flip(chip, 8), flip(flip(chip, 4), 8)][j]


def meet(peers):
    barrier = pltpu.get_barrier_semaphore()
    for peer in peers:
        pl.semaphore_signal(barrier, inc=1, device_id=(peer,), device_id_type=MESH)
    pl.semaphore_wait(barrier, len(peers))


def gather_kernel(qkv_ref, proj_ref, packed_ref, qkv_out, proj_out, packed_out, local_sem, send_sem, recv_sem):
    me = lax.axis_index(AX)
    chip, core = me // 2, me % 2
    mate, peer_x, peer_y, peers_z = peers_of(me)
    meet([mate, peer_x, peer_y] + peers_z)
    chip_x, chip_y = flip(chip, 1), flip(chip, 2)
    chip_xy = flip(chip_x, 2)
    outs = (qkv_out, packed_out, proj_out)
    count = len(outs)
    width = qkv_ref.shape[1] // 6
    pending = []

    def remote(w, slot, block, target, peer):
        return pltpu.make_async_remote_copy(
            src_ref=block, dst_ref=target, send_sem=send_sem.at[w, slot], recv_sem=recv_sem.at[w, slot],
            device_id=(peer,), device_id_type=MESH,
        )

    def send(w, slot, block, target, peer):
        copy = remote(w, slot, block, target, peer)
        copy.start()
        pending.append(copy)

    def arrive(w, slot, block):
        remote(w, slot, block, block, mate).wait_recv()

    def columns(start, size):
        return pl.ds(pl.multiple_of(start, 128), size)

    def pieces(w, half, target):
        if w == 0:
            return [
                (qkv_ref.at[:, columns((2 * t + half) * width, width)], target.at[:, pl.ds(t * width, width)])
                for t in range(3)
            ]
        if w == 1:
            return [(packed_ref, target)]
        return [(proj_ref.at[:, columns(half * width, width)], target)]

    for w in range(count):
        for source, target in pieces(w, 1 - core, outs[w].at[chip, core]):
            remote(w, 0, source, target, mate).start()
        for source, target in pieces(w, core, outs[w].at[chip, core]):
            pltpu.make_async_copy(source, target, local_sem.at[w]).start()
    for w in range(count):
        own = outs[w].at[chip, core]
        pltpu.make_async_copy(own, own, local_sem.at[w]).wait()
        arrive(w, 0, outs[w].at[chip, 1 - core])
        block = outs[w].at[chip]
        for j in range(3):
            send(w, 1 + j, block, block, peers_z[j])
        send(w, 4, block, block, peer_x)
        send(w, 8, block, block, peer_y)
    for w in range(count):
        for j in (1, 2, 3):
            block = outs[w].at[zflip(chip, j)]
            arrive(w, j, block)
            send(w, 4 + j, block, block, peer_x)
            send(w, 8 + j, block, block, peer_y)
        for j in range(4):
            block = outs[w].at[zflip(chip_x, j)]
            arrive(w, 4 + j, block)
            send(w, 12 + j, block.at[0], block.at[0], peer_y)
            block = outs[w].at[zflip(chip_y, j)]
            arrive(w, 8 + j, block)
            send(w, 16 + j, block.at[1], block.at[1], peer_x)
    for w in range(count):
        for j in range(4):
            block = outs[w].at[zflip(chip_xy, j)]
            arrive(w, 12 + j, block.at[0])
            arrive(w, 16 + j, block.at[1])
    for w in range(count):
        own = outs[w].at[chip, core]
        remote(w, 0, own, own, mate).wait_send()
    for copy in pending:
        copy.wait_send()


def gather_chips(qkv, proj, packed):
    devices = lax.axis_size(AX)
    shard, features = proj.shape
    width = features // 2
    if devices != 32:
        core = lax.axis_index(AX) % 2
        split = qkv.reshape(shard, 3, 2, width).transpose(2, 0, 1, 3).reshape(2, shard, 3 * width)
        gathered = []
        for halves in (split, proj.reshape(shard, 2, width).transpose(1, 0, 2), jnp.stack([packed, packed])):
            own = lax.dynamic_index_in_dim(halves, core, 0, keepdims=False)
            other = swap(lax.dynamic_index_in_dim(halves, 1 - core, 0, keepdims=False))
            block = jnp.where(core == 0, jnp.stack([own, other]), jnp.stack([other, own]))
            gathered.append(lax.all_gather(block, AX, axis=0, axis_index_groups=same_core_groups()))
        return gathered
    chips = devices // 2
    return pl.pallas_call(
        gather_kernel,
        out_shape=[
            jax.ShapeDtypeStruct((chips, 2, shard, 3 * width), BF),
            jax.ShapeDtypeStruct((chips, 2, shard, width), BF),
            jax.ShapeDtypeStruct((chips, 2) + packed.shape, BF),
        ],
        in_specs=[pl.BlockSpec(memory_space=pltpu.VMEM)] * 3,
        out_specs=[pl.BlockSpec(memory_space=pl.ANY)] * 3,
        scratch_shapes=[
            pltpu.SemaphoreType.DMA((3,)),
            pltpu.SemaphoreType.DMA((3, 20)),
            pltpu.SemaphoreType.DMA((3, 20)),
        ],
        compiler_params=pltpu.CompilerParams(collective_id=0, has_side_effects=True),
        cost_estimate=pl.CostEstimate(flops=int(4e10), bytes_accessed=int(1.5e8), transcendentals=0),
        name="gather_chips",
    )(qkv, proj, packed)


class Scatter:
    def __init__(self, kinds, ins, outs, scratch, early=None, origins=None):
        count = len(kinds)
        self.origins = origins or ins
        self.early = early
        if early is not None:
            self.plane, scratch = scratch[-1], scratch[:-1]
        self.kinds, self.ins, self.outs = kinds, ins, outs
        names = ("recv_a", "recv_b", "recv_x", "recv_y", "recv_z", "stage", "land")
        for place, name in enumerate(names):
            setattr(self, name, scratch[place * count : (place + 1) * count])
        self.send_sem, self.recv_sem = scratch[len(names) * count :]
        me = lax.axis_index(AX)
        self.chip, self.core = me // 2, me % 2
        self.mate, self.peer_x, self.peer_y, self.peers_z = peers_of(me)
        chip_x, chip_y = flip(self.chip, 1), flip(self.chip, 2)
        self.own = [zflip(self.chip, j) for j in range(4)]
        self.at_x = [zflip(chip_x, j) for j in range(4)]
        self.at_y = [zflip(chip_y, j) for j in range(4)]
        self.at_xy = [zflip(flip(chip_x, 2), j) for j in range(4)]
        self.sent = []

    def meet(self):
        meet([self.mate, self.peer_x, self.peer_y] + self.peers_z)

    def remote(self, w, slot, block, target, peer):
        return pltpu.make_async_remote_copy(
            src_ref=block, dst_ref=target, send_sem=self.send_sem.at[w, slot], recv_sem=self.recv_sem.at[w, slot],
            device_id=(peer,), device_id_type=MESH,
        )

    def send(self, w, slot, block, target, peer):
        self.remote(w, slot, block, target, peer).start()
        self.sent.append((w, slot))

    def arrive(self, w, slot, block):
        self.remote(w, slot, block, block, self.mate).wait_recv()

    def source(self, w, chip):
        return (self.plane, chip % 4) if w == self.early else (self.ins[w], chip)

    def origin(self, w, chip):
        return (self.plane, chip % 4) if w == self.early else (self.origins[w], chip)

    def along(self, w):
        for j in (1, 2, 3):
            layer = pl.multiple_of(self.own[j] // 4 * 4, 4)
            self.send(w, 23 + j, self.origins[w].at[pl.ds(layer, 4)], self.recv_z[w].at[j - 1], self.peers_z[j - 1])

    def layer_sum(self, w):
        for j in range(3):
            self.arrive(w, 24 + j, self.recv_z[w].at[j])
        layer = self.chip // 4 * 4

        @pl.loop(0, 4)
        def _(block):
            def body(part):
                for half in range(2):
                    total = self.ins[w][layer + block, half, part].astype(F32)
                    for j in range(3):
                        total = total + self.recv_z[w][j, block, half, part].astype(F32)
                    self.plane[block, half, part] = total.astype(BF)

            self.strips(w, body)

    def far(self, w, j):
        ref, at = self.origin(w, self.at_xy[j])
        block = ref.at[at]
        self.send(w, j, block.at[0], self.recv_a[w].at[j], self.peer_y)
        self.send(w, 4 + j, block.at[1], self.recv_b[w].at[j], self.peer_x)

    def near(self, w, j):
        ref, at = self.origin(w, self.at_x[j])
        self.send(w, 8 + j, ref.at[at, 1], self.recv_x[w].at[j, 1], self.peer_x)
        ref, at = self.origin(w, self.at_y[j])
        self.send(w, 12 + j, ref.at[at, 0], self.recv_y[w].at[j, 0], self.peer_y)

    def strips(self, w, body):
        @pl.loop(0, self.ins[w].shape[2] // 16)
        def _(i):
            body(pl.ds(pl.multiple_of(i * 16, 16), 16))

    def relay(self, w, j):
        for slot, recv, block, half in (
            (j, self.recv_a[w], self.at_x[j], 0),
            (4 + j, self.recv_b[w], self.at_y[j], 1),
        ):
            self.arrive(w, slot, recv.at[j])

            ref, at = self.source(w, block)

            def body(part):
                total = recv[j, part].astype(F32) + ref[at, half, part].astype(F32)
                recv[j, part] = total.astype(BF)

            self.strips(w, body)
            if half == 0:
                self.send(w, 16 + j, recv.at[j], self.recv_x[w].at[j, 0], self.peer_x)
            else:
                self.send(w, 20 + j, recv.at[j], self.recv_y[w].at[j, 1], self.peer_y)

    def arrive_near(self, w, j):
        self.arrive(w, 8 + j, self.recv_x[w].at[j, 1])
        self.arrive(w, 12 + j, self.recv_y[w].at[j, 0])
        self.arrive(w, 16 + j, self.recv_x[w].at[j, 0])
        self.arrive(w, 20 + j, self.recv_y[w].at[j, 1])

    def near_sum(self, w, j, half, part):
        total = self.recv_x[w][j, half, part].astype(F32) + self.recv_y[w][j, half, part].astype(F32)
        ref, at = self.source(w, self.own[j])
        return total + ref[at, half, part].astype(F32)

    def cross(self, w, j):
        self.arrive_near(w, j)

        def body(part):
            for half in range(2):
                self.recv_x[w][j, half, part] = self.near_sum(w, j, half, part).astype(BF)

        self.strips(w, body)
        self.send(w, 23 + j, self.recv_x[w].at[j], self.recv_z[w].at[j - 1], self.peers_z[j - 1])

    def place(self, w, part, total, half):
        kind = self.kinds[w]
        if kind == "sum":
            self.outs[w][part] = total
            return
        size = total.shape[1] // kind
        for t in range(kind):
            start = pl.multiple_of((2 * t + half) * size, 128)
            self.outs[w][part, pl.ds(start, size)] = total[:, t * size : (t + 1) * size]

    def last(self, w):
        self.arrive_near(w, 0)
        layers = 0 if w == self.early else 3
        for j in range(layers):
            self.arrive(w, 24 + j, self.recv_z[w].at[j])
        rows = self.ins[w].shape[2]

        def total_of(half, part):
            total = self.near_sum(w, 0, half, part)
            for j in range(layers):
                total = total + self.recv_z[w][j, half, part].astype(F32)
            return total

        if self.kinds[w] == "rows":

            @pl.loop(0, rows // 16)
            def _(i):
                for half in range(2):
                    part = pl.ds(pl.multiple_of(i * 16, 16), 16)
                    self.outs[w][pl.ds(pl.multiple_of(half * rows + i * 16, 16), 16)] = total_of(half, part)

            return

        def other(part):
            self.stage[w][part] = total_of(1 - self.core, part)

        self.strips(w, other)
        self.send(w, 27, self.stage[w], self.land[w], self.mate)
        self.strips(w, lambda part: self.place(w, part, total_of(self.core, part), self.core))

    def finish(self, w):
        self.arrive(w, 27, self.land[w])

        def body(part):
            other = self.land[w][part]
            if self.kinds[w] == "sum":
                other = other + self.outs[w][part]
            self.place(w, part, other, 1 - self.core)

        self.strips(w, body)

    def drain(self):
        for w, slot in self.sent:
            if slot == 27:
                block = self.stage[w]
            elif slot >= 24:
                block = self.recv_z[w].at[0]
            else:
                block = self.recv_a[w].at[0]
            self.remote(w, slot, block, block, self.mate).wait_send()

    def opening(self, w):
        self.far(w, 1), self.far(w, 2), self.near(w, 1)

    def run(self):
        small = range(2, len(self.kinds))
        opening = self.opening
        self.meet()
        opening(0)
        for w in small:
            for j in (1, 2, 3, 0):
                self.far(w, j), self.near(w, j)
        self.relay(0, 1), self.far(0, 3), self.near(0, 2)
        self.relay(0, 2), self.far(0, 0), self.near(0, 3)
        for w in small:
            for j in (1, 2, 3, 0):
                self.relay(w, j)
        self.relay(0, 3), self.near(0, 0), self.cross(0, 1)
        opening(1)
        for w in small:
            for j in (1, 2, 3):
                self.cross(w, j)
        self.relay(0, 0), self.cross(0, 2), self.cross(0, 3)
        self.relay(1, 1), self.far(1, 3), self.near(1, 2)
        self.relay(1, 2), self.far(1, 0), self.near(1, 3)
        for w in small:
            self.last(w)
        self.relay(1, 3), self.near(1, 0), self.cross(1, 1)
        self.relay(1, 0)
        self.last(0)
        self.cross(1, 2), self.cross(1, 3)
        for w in small:
            self.finish(w)
        self.finish(0)
        self.last(1)
        self.finish(1)
        self.drain()


def scatter_scratch(shapes, early=None):
    count = len(shapes)
    scratch = [pltpu.VMEM((4,) + s[2:], BF) for s in shapes] * 2
    scratch += [pltpu.VMEM((4, 2) + s[2:], BF) for s in shapes] * 2
    scratch += [pltpu.VMEM(((3, 4, 2) if w == early else (3, 2)) + s[2:], BF) for w, s in enumerate(shapes)]
    scratch += [pltpu.VMEM(s[2:], F32) for s in shapes] * 2
    scratch += [pltpu.SemaphoreType.DMA((count, 28)), pltpu.SemaphoreType.DMA((count, 28))]
    if early is not None:
        scratch += [pltpu.VMEM((4, 2) + shapes[early][2:], BF)]
    return scratch


def scatter_shapes(shapes, kinds):
    factors = {"sum": (1, 1), "rows": (2, 1)}
    sizes = [factors.get(kind, (1, 2)) for kind in kinds]
    return [jax.ShapeDtypeStruct((s[2] * a, s[3] * b), F32) for s, (a, b) in zip(shapes, sizes)]


def scatter_kernel(kinds, *refs):
    count = len(kinds)
    Scatter(kinds, refs[:count], refs[count : 2 * count], refs[2 * count :]).run()


def scatter_chips(grads, kinds):
    devices = lax.axis_size(AX)
    shapes = [g.shape for g in grads]
    if devices != 32:
        core = lax.axis_index(AX) % 2
        summed = []
        for grad, kind in zip(grads, kinds):
            block = lax.psum_scatter(grad, AX, scatter_dimension=0, axis_index_groups=same_core_groups())
            block = block.astype(F32)
            own = lax.dynamic_index_in_dim(block, core, 0, keepdims=False)
            other = swap(lax.dynamic_index_in_dim(block, 1 - core, 0, keepdims=False))
            if kind == "sum":
                summed.append(own + other)
                continue
            rows, columns = own.shape
            own = own.reshape(rows, kind, 1, columns // kind)
            other = other.reshape(rows, kind, 1, columns // kind)
            summed.append(by_core(core, own, other, 2).reshape(rows, 2 * columns))
        return summed
    count = len(grads)
    return pl.pallas_call(
        functools.partial(scatter_kernel, kinds),
        out_shape=scatter_shapes(shapes, kinds),
        in_specs=[pl.BlockSpec(memory_space=pltpu.VMEM)] * count,
        out_specs=[pl.BlockSpec(memory_space=pltpu.VMEM)] * count,
        scratch_shapes=scatter_scratch(shapes),
        compiler_params=pltpu.CompilerParams(
            collective_id=1, has_side_effects=True, vmem_limit_bytes=56 << 20
        ),
        name="scatter_chips",
    )(*grads)


def flat(ref):
    return ref[...].reshape(-1, ref.shape[-1])


def head_masks():
    lane = lax.broadcasted_iota(jnp.int32, (1, 2 * HEAD), 1)
    return [(lane < HEAD).astype(BF), (lane >= HEAD).astype(BF)]


def attend_kernel(chunk, q_ref, k_ref, v_ref, penalty_ref, out_ref, log_ref, query_buf, mixed_buf):
    query_buf[...] = flat(q_ref) * jnp.asarray(0.125, BF)
    keys, values = flat(k_ref), flat(v_ref)
    values_t = values.T
    penalty = flat(penalty_ref)
    masks = head_masks()

    @pl.loop(0, query_buf.shape[0] // chunk)
    def _(i):
        part = pl.ds(pl.multiple_of(i * chunk, chunk), chunk)
        queries = query_buf[part]
        parts = []
        for h in range(2):
            scores = product_right_t(keys, queries * masks[h]) + penalty
            top = jnp.max(scores, axis=0, keepdims=True)
            exponent = jnp.exp(scores - top)
            total = jnp.sum(exponent, axis=0, keepdims=True)
            mixed = product(values_t[h * HEAD : (h + 1) * HEAD], exponent.astype(BF))
            parts.append(mixed * (1.0 / total))
            log_ref[0, 0, h : h + 1, part] = top + jnp.log(total)
        mixed_buf[part] = jnp.concatenate(parts, 0).T.astype(BF)

    out_ref[...] = mixed_buf[...].reshape(out_ref.shape)


def attend(projected, penalty):
    _, clips, rows, triple = projected.shape
    slots = 2 * rows
    width = triple // 3
    pairs = width // (2 * HEAD)

    def block(offset):
        return pl.BlockSpec((2, 1, rows, 2 * HEAD), lambda i, j: (0, i, 0, offset * pairs + j))

    return pl.pallas_call(
        functools.partial(attend_kernel, 256),
        grid=(clips, pairs),
        in_specs=[block(0), block(1), block(2), pl.BlockSpec((2, 1, rows, 1), lambda i, j: (0, i, 0, 0))],
        out_specs=[block(0), pl.BlockSpec((1, 1, 2, slots), lambda i, j: (i, j, 0, 0))],
        out_shape=[
            jax.ShapeDtypeStruct((2, clips, rows, width), BF),
            jax.ShapeDtypeStruct((clips, pairs, 2, slots), F32),
        ],
        scratch_shapes=[pltpu.VMEM((slots, 2 * HEAD), BF)] * 2,
        compiler_params=pltpu.CompilerParams(vmem_limit_bytes=48 << 20),
        cost_estimate=pl.CostEstimate(
            flops=4 * clips * pairs * slots * slots * 2 * HEAD, bytes_accessed=8 * clips * slots * width,
            transcendentals=clips * pairs * 2 * slots * slots,
        ),
        name="attend",
    )(projected, projected, projected, penalty)


def attend_back_kernel(chunk, *refs):
    if len(refs) == 16:
        attend_back_step(chunk, *refs)
        return
    inputs, (down_hbm, norm_hbm, pre_hbm), (back_out, bias_out, down_out, up_out) = refs[:7], refs[7:10], refs[10:14]
    buffers, (norm, pre, up_buf, down_ref, load_sem), scratch = refs[14:21], refs[21:26], refs[26:]
    width = down_out.shape[1]
    parts = pl.ds(0, width - width // 8), pl.ds(width - width // 8, width // 8)
    scatter = Scatter(
        ("rows", "rows"), [down_ref.at[:, :, :, part] for part in parts], [down_out.at[:, part] for part in parts],
        scratch, 1, [down_hbm.at[:, :, :, part] for part in parts],
    )
    step = pl.program_id(0) * pl.num_programs(1) + pl.program_id(1)
    total = pl.num_programs(0) * pl.num_programs(1)

    def start():
        pltpu.make_async_copy(norm_hbm, norm, load_sem.at[0]).start()
        pltpu.make_async_copy(pre_hbm, pre, load_sem.at[1]).start()
        scatter.meet()
        scatter.opening(0)
        scatter.along(1)
        pltpu.make_async_copy(down_hbm, down_ref, load_sem.at[load_sem.shape[0] - 1]).start()

    def two():
        pltpu.make_async_copy(down_hbm, down_ref, load_sem.at[load_sem.shape[0] - 1]).wait()
        scatter.relay(0, 1), scatter.far(0, 3), scatter.near(0, 2)

    def four():
        scatter.relay(0, 2), scatter.far(0, 0), scatter.near(0, 3), scatter.cross(0, 1)

    def five():
        scatter.relay(0, 3), scatter.near(0, 0)
        scatter.layer_sum(1)
        scatter.far(1, 0), scatter.near(1, 0)

    def six():
        scatter.cross(0, 2)

    def seven():
        scatter.relay(0, 0)

    def end():
        scatter.cross(0, 3)
        scatter.relay(1, 0)
        pltpu.make_async_copy(norm_hbm, norm, load_sem.at[0]).wait()
        pltpu.make_async_copy(pre_hbm, pre, load_sem.at[1]).wait()

        @pl.loop(0, norm.shape[1] // 512)
        def _(i):
            part = pl.ds(pl.multiple_of(i * 512, 512), 512)
            up_buf[part] = product_left_t(norm[:, part], pre[...]).astype(BF)
            pltpu.make_async_copy(up_buf.at[part], up_out.at[part], load_sem.at[2 + i]).start()

        scatter.last(1)
        scatter.last(0)
        scatter.drain()
        for i in range(norm.shape[1] // 512):
            part = pl.ds(i * 512, 512)
            pltpu.make_async_copy(up_buf.at[part], up_out.at[part], load_sem.at[2 + i]).wait()

    for place, work in ((0, start), (2, two), (4, four), (5, five), (6, six), (7, seven)):
        pl.when(step == place)(work)
    attend_back_step(chunk, *inputs, back_out, bias_out, *buffers)
    pl.when(step == total - 1)(end)


def attend_back_step(
    chunk, q_ref, k_ref, v_ref, penalty_ref, log_ref, att_ref, grad_ref, out_ref, bias_ref,
    query_buf, grad_buf, mixed_buf, back_buf, key_sum, value_sum, bias_sum,
):
    rows = q_ref.shape[2]
    pair = pl.program_id(1)
    width = out_ref.shape[3] // 3
    query_buf[...] = flat(q_ref) * jnp.asarray(0.125, BF)
    grad_buf[...] = flat(grad_ref)
    mixed_buf[...] = flat(att_ref)
    keys, values = flat(k_ref), flat(v_ref)
    keys_t = keys.T
    penalty = flat(penalty_ref)
    masks = head_masks()
    for total in (key_sum, value_sum, bias_sum):
        total[...] = jnp.zeros_like(total)

    def keep(offset, value):
        columns = pl.ds(pl.multiple_of(offset + pair * 2 * HEAD, 128), 2 * HEAD)
        for side in range(2):
            out_ref[side, 0, :, columns] = value[side * rows : (side + 1) * rows]

    for start in range(0, query_buf.shape[0], chunk):
        part = pl.ds(start, chunk)
        queries, grads = query_buf[part], grad_buf[part]
        overlap = (grads.astype(F32) * mixed_buf[part].astype(F32)).T
        parts = []
        for h in range(2):
            head_queries = queries * masks[h]
            head_grads = grads * masks[h]
            correction = jnp.sum(overlap[h * HEAD : (h + 1) * HEAD], axis=0, keepdims=True)
            logs = log_ref[0, 0, h : h + 1, part]
            soft = jnp.exp(product_right_t(keys, head_queries) + penalty - logs)
            grad_soft = product_right_t(values, head_grads)
            value_sum[...] += product(soft.astype(BF), head_grads)
            grad_scores = (soft * (grad_soft - correction)).astype(BF)
            key_sum[...] += product(grad_scores, head_queries)
            parts.append(product(keys_t[h * HEAD : (h + 1) * HEAD], grad_scores))
        grad_queries = jnp.concatenate(parts, 0).T * 0.125
        bias_sum[0:1] += jnp.sum(grad_queries, axis=0, keepdims=True)
        back_buf[part] = grad_queries.astype(BF)

    keep(0, back_buf[...])
    keep(width, key_sum[...].astype(BF))
    keep(2 * width, value_sum[...].astype(BF))
    bias_ref[0, 0, 0:1] = bias_sum[0:1]
    bias_ref[0, 0, 1:2] = jnp.sum(value_sum[...], axis=0, keepdims=True)


def attend_back(projected, penalty, logs, attended, grad_attended, grad_down, norm_two, grad_pre):
    _, clips, rows, triple = projected.shape
    slots = 2 * rows
    width = triple // 3
    pairs = width // (2 * HEAD)
    fused = lax.axis_size(AX) == 32 and clips * pairs == 8

    def block(offset):
        return pl.BlockSpec((2, 1, rows, 2 * HEAD), lambda i, j: (0, i, 0, offset * pairs + j))

    in_specs = [
        block(0), block(1), block(2),
        pl.BlockSpec((2, 1, rows, 1), lambda i, j: (0, i, 0, 0)),
        pl.BlockSpec((1, 1, 2, slots), lambda i, j: (i, j, 0, 0)),
        block(0), block(0),
    ]
    out_specs = [
        pl.BlockSpec((2, 1, rows, triple), lambda i, j: (0, i, 0, 0)),
        pl.BlockSpec((1, 1, 2, 2 * HEAD), lambda i, j: (i, j, 0, 0)),
    ]
    out_shape = [
        jax.ShapeDtypeStruct((2, clips, rows, triple), BF),
        jax.ShapeDtypeStruct((clips, pairs, 2, 2 * HEAD), F32),
    ]
    operands = [projected, projected, projected, penalty, logs, attended, grad_attended]
    scratch = [pltpu.VMEM((slots, 2 * HEAD), BF)] * 4 + [pltpu.VMEM((slots, 2 * HEAD), F32)] * 2
    scratch += [pltpu.VMEM((8, 2 * HEAD), F32)]
    params = pltpu.CompilerParams(vmem_limit_bytes=60 << 20)
    if fused:
        up_shape = (norm_two.shape[1], grad_pre.shape[1])
        sums = scatter_shapes([grad_down.shape], ("rows",))
        in_specs += [pl.BlockSpec(memory_space=pl.ANY)] * 3
        out_specs += [pl.BlockSpec(sums[0].shape, lambda i, j: (0, 0)), pl.BlockSpec(memory_space=pl.ANY)]
        out_shape += [sums[0], jax.ShapeDtypeStruct(up_shape, BF)]
        operands += [grad_down, norm_two, grad_pre]
        scratch += [pltpu.VMEM(norm_two.shape, BF), pltpu.VMEM(grad_pre.shape, BF), pltpu.VMEM(up_shape, BF)]
        scratch += [pltpu.VMEM(grad_down.shape, BF), pltpu.SemaphoreType.DMA((3 + up_shape[0] // 512,))]
        most = grad_down.shape[3] - grad_down.shape[3] // 8
        scratch += scatter_scratch(
            [grad_down.shape[:3] + (most,), grad_down.shape[:3] + (grad_down.shape[3] - most,)], 1
        )
        params = pltpu.CompilerParams(vmem_limit_bytes=60 << 20, collective_id=2, has_side_effects=True)
    outs = pl.pallas_call(
        functools.partial(attend_back_kernel, 256),
        grid=(clips, pairs),
        in_specs=in_specs,
        out_specs=out_specs,
        out_shape=out_shape,
        scratch_shapes=scratch,
        compiler_params=params,
        cost_estimate=pl.CostEstimate(
            flops=10 * clips * pairs * slots * slots * 2 * HEAD, bytes_accessed=18 * clips * slots * width,
            transcendentals=clips * pairs * 2 * slots * slots,
        ),
        name="attend_back",
    )(*operands)
    if not fused:
        total = lax.psum_scatter(grad_down, AX, scatter_dimension=0, axis_index_groups=same_core_groups())
        total = total.astype(F32).reshape(-1, total.shape[-1])
        outs = [*outs, total, outer(norm_two, grad_pre)]
    return outs


def normal_parts(values):
    average = jnp.mean(values, axis=-1, keepdims=True)
    centered = values - average
    inverse = lax.rsqrt(jnp.mean(centered * centered, axis=-1, keepdims=True) + EPSILON)
    return centered * inverse, inverse


def normal_back(grad_normed, scaled, inverse, gain):
    grad_scaled = grad_normed * gain
    first_mean = jnp.mean(grad_scaled, axis=-1, keepdims=True)
    second_mean = jnp.mean(grad_scaled * scaled, axis=-1, keepdims=True)
    return inverse * (grad_scaled - first_mean - scaled * second_mean)


def rows_spec(size, columns):
    return pl.BlockSpec((size, columns), lambda i: (i, 0))


def whole_spec(shape):
    return pl.BlockSpec(shape, lambda i: (0,) * len(shape), pipeline_mode=pl.Buffered(1))


PARAMS = pltpu.CompilerParams(vmem_limit_bytes=56 << 20)


def strips_of(ref):
    return [pl.ds(start, 32) for start in range(0, ref.shape[0], 32)]


def project_kernel(steps, own_ref, other_ref, gain_ref, shift_ref, weight_ref, bias_ref, norm_ref, out_ref):
    is_own = pl.program_id(0) < steps
    for part in strips_of(own_ref):
        rows = jnp.where(is_own, own_ref[part].astype(F32), other_ref[part].astype(F32))
        scaled, _ = normal_parts(rows)
        norm_ref[part] = (scaled * gain_ref[...] + shift_ref[...]).astype(BF)
    out_ref[...] = (product(norm_ref[...], weight_ref[...]) + bias_ref[...]).astype(BF)


def project(own, other, gain, shift, weight, bias):
    rows, features = own.shape
    columns = weight.shape[1]
    steps = 3
    size = rows // steps
    return pl.pallas_call(
        functools.partial(project_kernel, steps),
        grid=(2 * steps,),
        in_specs=[
            pl.BlockSpec((size, features), lambda i: (jnp.minimum(i, steps - 1), 0)),
            pl.BlockSpec((size, features), lambda i: (jnp.maximum(i - steps, 0), 0)),
            whole_spec((1, features)),
            whole_spec((1, features)),
            whole_spec((features, columns)),
            whole_spec((1, columns)),
        ],
        out_specs=[rows_spec(size, features), rows_spec(size, columns)],
        out_shape=[
            jax.ShapeDtypeStruct((2 * rows, features), BF),
            jax.ShapeDtypeStruct((2 * rows, columns), BF),
        ],
        compiler_params=PARAMS,
        name="project",
    )(own, other, gain, shift, weight, bias)


def second_norm_kernel(att_ref, weight_ref, token_ref, recv_ref, bias_ref, gain_ref, shift_ref, middle_ref, out_ref):
    mixed = product(att_ref[...], weight_ref[...])
    for part in strips_of(token_ref):
        middle = token_ref[part].astype(F32) + mixed[part.start : part.start + part.size]
        middle = middle + recv_ref[part].astype(F32) + bias_ref[...]
        middle_ref[part] = middle
        scaled, _ = normal_parts(middle)
        out_ref[part] = (scaled * gain_ref[...] + shift_ref[...]).astype(BF)


def second_norm(attended, weight, tokens, received, bias, gain, shift):
    rows, features = tokens.shape
    width = weight.shape[0]
    size = rows // 4
    return pl.pallas_call(
        second_norm_kernel,
        grid=(4,),
        in_specs=[
            rows_spec(size, width), whole_spec((width, features)), rows_spec(size, features), rows_spec(size, features),
            whole_spec((1, features)), whole_spec((1, features)), whole_spec((1, features)),
        ],
        out_specs=[rows_spec(size, features), rows_spec(size, features)],
        out_shape=[jax.ShapeDtypeStruct((rows, features), F32), jax.ShapeDtypeStruct((rows, features), BF)],
        compiler_params=PARAMS,
        name="second_norm",
    )(attended, weight, tokens, received, bias, gain, shift)


def feed_kernel(
    steps, unit, own_ref, other_ref, grad_own_ref, grad_other_ref, mark_ref, bias_ref, *refs
):
    if len(refs) == 14:
        both_ref, refs = refs[0], refs[1:]
        sources = None
    else:
        sources, refs = refs[:2], refs[2:]
    act_ref, pre_ref, norm_ref, grad_ref, pass_own_ref, pass_other_ref, sums_ref, down_hbm = refs[:8]
    up_ref, down_ref, up_sem, down_sem, out_sem = refs[8:]
    step = pl.program_id(0)
    features, hidden = up_ref.shape

    @pl.when(step == 0)
    def _():
        sums_ref[...] = jnp.zeros_like(sums_ref)
        if sources is not None:
            pltpu.make_async_copy(sources[0], up_ref, up_sem).start()
            pltpu.make_async_copy(sources[1], down_ref, down_sem).start()
        else:
            core = lax.axis_index(AX) % 2
            chips = hidden // unit
            shard = features // (2 * chips)
            for k in range(chips):
                device = 2 * k + core
                pltpu.make_async_copy(
                    both_ref.at[:, pl.ds(pl.multiple_of(device * unit, 128), unit)],
                    up_ref.at[:, k * unit : (k + 1) * unit],
                    up_sem,
                ).start()
            for k in range(chips):
                device = 2 * k + core
                for q in range(unit // shard):
                    pltpu.make_async_copy(
                        both_ref.at[
                            pl.ds(pl.multiple_of(device * shard, 16), shard),
                            pl.ds(2 * hidden + q * features, features),
                        ],
                        down_ref.at[k * unit + q * shard : k * unit + (q + 1) * shard],
                        down_sem,
                    ).start()
        pltpu.make_async_copy(up_ref, up_ref, up_sem).wait()
        pltpu.make_async_copy(down_ref, down_ref, down_sem).wait()
        pltpu.make_async_copy(down_ref, down_hbm, out_sem).start()

    rows = jnp.where(step < steps, other_ref[...], own_ref[...])
    grads = jnp.where(step < steps, grad_other_ref[...], grad_own_ref[...]) * mark_ref[...].astype(BF)
    norm_ref[...] = rows
    grad_ref[...] = grads
    size = 512
    for start in range(0, hidden, size):
        part = slice(start, start + size)
        pre = product(rows, up_ref[:, part]) + bias_ref[:, part]
        normal_cdf = 0.5 * (1.0 + lax.erf(pre * ROOT_HALF))
        density = jnp.exp(-0.5 * pre * pre) * INV_ROOT_TWO_PI
        act_ref[:, part] = (pre * normal_cdf).astype(BF)
        grad_pre = product_right_t(grads, down_ref[part]) * (normal_cdf + pre * density)
        sums_ref[0:1, part] += jnp.sum(grad_pre, axis=0, keepdims=True)
        pre_ref[:, part] = grad_pre.astype(BF)
    passed = product_right_t(pre_ref[...], up_ref[...])
    pass_own_ref[...] = passed

    @pl.when(step < steps)
    def _():
        pass_other_ref[...] = passed.astype(BF)

    @pl.when(step == 2 * steps - 1)
    def _():
        pltpu.make_async_copy(down_ref, down_hbm, out_sem).wait()


def feed(own, other, grad_own, grad_other, marks, weights, bias, unit):
    rows, features = own.shape
    hidden = bias.shape[1]
    steps = 3
    size = rows // steps

    def side(i):
        return jnp.where(i < steps, i + steps, i - steps)

    def both_spec(columns):
        return pl.BlockSpec((size, columns), lambda i: (side(i), 0))

    own_spec = pl.BlockSpec((size, features), lambda i: (jnp.maximum(i - steps, 0), 0))
    other_spec = pl.BlockSpec((size, features), lambda i: (jnp.minimum(i, steps - 1), 0))
    return pl.pallas_call(
        functools.partial(feed_kernel, steps, unit),
        grid=(2 * steps,),
        in_specs=[own_spec, other_spec, own_spec, other_spec, both_spec(1), whole_spec((1, hidden))]
        + [pl.BlockSpec(memory_space=pl.ANY)] * len(weights),
        out_specs=[
            both_spec(hidden), both_spec(hidden), both_spec(features), both_spec(features),
            own_spec, other_spec,
            pl.BlockSpec((8, hidden), lambda i: (0, 0)), pl.BlockSpec(memory_space=pl.ANY),
        ],
        out_shape=[
            jax.ShapeDtypeStruct((2 * rows, hidden), BF), jax.ShapeDtypeStruct((2 * rows, hidden), BF),
            jax.ShapeDtypeStruct((2 * rows, features), BF), jax.ShapeDtypeStruct((2 * rows, features), BF),
            jax.ShapeDtypeStruct((rows, features), F32), jax.ShapeDtypeStruct((rows, features), BF),
            jax.ShapeDtypeStruct((8, hidden), F32), jax.ShapeDtypeStruct((hidden, features), BF),
        ],
        scratch_shapes=[
            pltpu.VMEM((features, hidden), BF), pltpu.VMEM((hidden, features), BF),
            pltpu.SemaphoreType.DMA(()), pltpu.SemaphoreType.DMA(()), pltpu.SemaphoreType.DMA(()),
        ],
        compiler_params=PARAMS,
        cost_estimate=pl.CostEstimate(
            flops=12 * rows * features * hidden, bytes_accessed=8 * features * hidden,
            transcendentals=4 * rows * hidden,
        ),
        name="feed",
    )(own, other, grad_own, grad_other, marks, bias, *weights)


def outer_kernel(left_ref, right_ref, out_ref):
    out_ref[...] = product_left_t(left_ref[...], right_ref[...]).astype(BF)


def outer(left, right):
    rows, columns = left.shape
    width = right.shape[1]
    size = 512
    return pl.pallas_call(
        outer_kernel,
        grid=(columns // size,),
        in_specs=[pl.BlockSpec((rows, size), lambda i: (0, i)), whole_spec((rows, width))],
        out_specs=rows_spec(size, width),
        out_shape=jax.ShapeDtypeStruct((columns, width), BF),
        compiler_params=PARAMS,
        cost_estimate=pl.CostEstimate(
            flops=2 * rows * columns * width, bytes_accessed=2 * (rows * columns + rows * width + columns * width),
            transcendentals=0,
        ),
        name="outer",
    )(left, right)


def gather_sums(sums_ref, values):
    for index, value in enumerate(values):
        sums_ref[index : index + 1] += jnp.sum(value, axis=0, keepdims=True)


def clear_first(sums_ref):
    @pl.when(pl.program_id(0) == 0)
    def _():
        sums_ref[...] = jnp.zeros_like(sums_ref)


def second_back_kernel(
    grad_ref, recv_ref, middle_ref, out_ref, gain_ref, full_ref, low_ref, sums_ref
):
    clear_first(sums_ref)
    for part in strips_of(grad_ref):
        grad_normed = grad_ref[part] + recv_ref[part].astype(F32)
        scaled, inverse = normal_parts(middle_ref[part])
        grad_out = out_ref[part].astype(F32)
        grad_middle = grad_out + normal_back(grad_normed, scaled, inverse, gain_ref[...])
        full_ref[part] = grad_middle
        low_ref[part] = grad_middle.astype(BF)
        gather_sums(sums_ref, [grad_normed * scaled, grad_normed, grad_middle, grad_out])


def second_back(passed, received, middle, grad_out, gain):
    rows, features = middle.shape
    size = rows // 4
    return pl.pallas_call(
        second_back_kernel,
        grid=(4,),
        in_specs=[rows_spec(size, features)] * 4 + [whole_spec((1, features))],
        out_specs=[rows_spec(size, features)] * 2 + [pl.BlockSpec((8, features), lambda i: (0, 0))],
        out_shape=[
            jax.ShapeDtypeStruct((rows, features), F32), jax.ShapeDtypeStruct((rows, features), BF),
            jax.ShapeDtypeStruct((8, features), F32),
        ],
        compiler_params=PARAMS,
        name="second_back",
    )(passed, received, middle, grad_out, gain)


def first_back_kernel(grad_ref, weight_ref, recv_ref, token_ref, middle_ref, gain_ref, full_ref, sums_ref):
    clear_first(sums_ref)
    passed = product_right_t(grad_ref[...], weight_ref[...])
    for part in strips_of(grad_ref):
        grad_normed = passed[part.start : part.start + part.size] + recv_ref[part].astype(F32)
        scaled, inverse = normal_parts(token_ref[part].astype(F32))
        full_ref[part] = middle_ref[part] + normal_back(grad_normed, scaled, inverse, gain_ref[...])
        gather_sums(sums_ref, [grad_normed * scaled, grad_normed])


def first_back(grad_projected, weight, received, tokens, grad_middle, gain):
    rows, features = tokens.shape
    triple = weight.shape[1]
    size = rows // 4
    return pl.pallas_call(
        first_back_kernel,
        grid=(4,),
        in_specs=[
            rows_spec(size, triple), whole_spec((features, triple)), rows_spec(size, features),
            rows_spec(size, features), rows_spec(size, features), whole_spec((1, features)),
        ],
        out_specs=[rows_spec(size, features), pl.BlockSpec((8, features), lambda i: (0, 0))],
        out_shape=[jax.ShapeDtypeStruct((rows, features), F32), jax.ShapeDtypeStruct((8, features), F32)],
        compiler_params=PARAMS,
        name="first_back",
    )(grad_projected, weight, received, tokens, grad_middle, gain)


def tail_kernel(
    kinds, sums_ref, bias_ref, gain_ref, shift_ref, up_hbm, proj_hbm,
    back_hbm, weight_hbm, norm_hbm, token_hbm, middle_hbm, down_hbm, act_hbm, sum_hbm,
    up_out, qkv_out, proj_out, packed_out, tokens_out, block_out, *refs
):
    back, weight, norm, token, middle, down, qkv, packed, vectors, stage, land, load_sem, pass_sem = refs[:13]
    act, total, lift_stage, lift_land, block_sem, up_ref, proj_ref = refs[13:20]
    scatter = Scatter(
        kinds, (up_ref, qkv, proj_ref, packed), (up_out, qkv_out, proj_out, packed_out), refs[20:], 2,
        (up_hbm, qkv, proj_hbm, packed),
    )
    chips, _, shard, triple = qkv.shape
    own_rows = token.shape[0]
    loads = [
        pltpu.make_async_copy(source, target, load_sem.at[i])
        for i, (source, target) in enumerate(
            (
                (back_hbm, back), (weight_hbm, weight), (norm_hbm, norm), (token_hbm, token), (middle_hbm, middle),
                (down_hbm, down), (up_hbm, up_ref), (proj_hbm, proj_ref),
            )
        )
    ]
    scatter.meet()
    scatter.opening(0)
    scatter.along(2)
    for place in (0, 1, 6, 2, 7, 3, 4, 5):
        loads[place].start()
    vectors[...] = jnp.zeros_like(vectors)
    vectors[0:8] = sums_ref[...]
    loads[0].wait(), loads[1].wait()

    @pl.loop(0, own_rows // 256)
    def _(i):
        part = pl.ds(pl.multiple_of(own_rows + i * 256, 256), 256)
        stage[pl.ds(pl.multiple_of(i * 256, 256), 256)] = product_right_t(back[part], weight[...]).astype(BF)

    passing = pltpu.make_async_remote_copy(
        src_ref=stage, dst_ref=land, send_sem=pass_sem.at[0], recv_sem=pass_sem.at[1],
        device_id=(scatter.mate,), device_id_type=MESH,
    )
    passing.start()
    loads[6].wait(), loads[7].wait()
    scatter.relay(0, 1), scatter.far(0, 3), scatter.near(0, 2)
    loads[2].wait()

    @pl.loop(0, norm.shape[1] // 256)
    def _(i):
        part = pl.ds(pl.multiple_of(i * 256, 256), 256)
        count = 256 // (2 * shard)
        grad = product_left_t(norm[:, part], back[...]).astype(BF)
        qkv[pl.ds(i * count, count)] = grad.reshape(count, 2, shard, triple)

    scatter.relay(0, 2), scatter.far(0, 0), scatter.near(0, 3)
    scatter.opening(1)
    loads[3].wait(), loads[4].wait()
    passing.wait()

    @pl.loop(0, own_rows // 256)
    def _(i):
        start = pl.multiple_of(i * 256, 256)
        passed = product_right_t(back[pl.ds(start, 256)], weight[...])
        for strip in range(0, 256, 32):
            part = pl.ds(start + strip, 32)
            grad_normed = passed[strip : strip + 32] + land[part].astype(F32)
            scaled, inverse = normal_parts(token[part].astype(F32))
            tokens_out[part] = middle[part] + normal_back(grad_normed, scaled, inverse, gain_ref[...])
            vectors[0:1] += jnp.sum(grad_normed * scaled, axis=0, keepdims=True)
            vectors[1:2] += jnp.sum(grad_normed, axis=0, keepdims=True)

    scatter.relay(0, 3), scatter.near(0, 0), scatter.cross(0, 1), scatter.cross(0, 2)
    packed[:, :, :shard] = vectors[...].T.astype(BF).reshape(chips, 2, shard, PARAM_COLS)
    packed[:, :, shard:] = bias_ref[...]
    for j in (1, 2, 3, 0):
        scatter.far(3, j), scatter.near(3, j)
    scatter.layer_sum(2)
    scatter.far(2, 0), scatter.near(2, 0)
    scatter.relay(0, 0), scatter.cross(0, 3)
    loads[5].wait()

    def fetch(source, start, target, slot):
        copy = pltpu.make_async_copy(source.at[pl.ds(start, 256)], target, block_sem.at[slot])
        copy.start()
        return copy

    @pl.loop(0, own_rows // 256)
    def _(i):
        fetch(act_hbm, pl.multiple_of(own_rows + i * 256, 256), act, 0).wait()
        lift_stage[pl.ds(pl.multiple_of(i * 256, 256), 256)] = product(act[...], down[...]).astype(BF)

    lifting = pltpu.make_async_remote_copy(
        src_ref=lift_stage, dst_ref=lift_land, send_sem=pass_sem.at[2], recv_sem=pass_sem.at[3],
        device_id=(scatter.mate,), device_id_type=MESH,
    )
    lifting.start()
    scatter.relay(2, 0)
    scatter.relay(1, 1), scatter.far(1, 3), scatter.near(1, 2)
    scatter.relay(1, 2), scatter.far(1, 0), scatter.near(1, 3)
    lifting.wait()

    @pl.loop(0, own_rows // 256)
    def _(i):
        start = pl.multiple_of(i * 256, 256)
        copies = fetch(act_hbm, start, act, 0), fetch(sum_hbm, start, total, 1)
        for copy in copies:
            copy.wait()
        lifted = product(act[...], down[...]) + lift_land[pl.ds(start, 256)].astype(F32)
        block_out[pl.ds(start, 256)] = (total[...] + lifted + shift_ref[...]).astype(BF)

    for j in (1, 2, 3, 0):
        scatter.relay(3, j)
    scatter.last(2)
    scatter.relay(1, 3), scatter.near(1, 0), scatter.cross(1, 1)
    for j in (1, 2, 3):
        scatter.cross(3, j)
    scatter.relay(1, 0)
    scatter.last(0)
    scatter.cross(1, 2), scatter.cross(1, 3)
    scatter.finish(2), scatter.finish(0)
    scatter.last(3)
    scatter.last(1)
    scatter.finish(3), scatter.finish(1)
    scatter.drain()


def tail(grad_up, grad_proj, sums, bias_rows, gain, shift, back, weight, norm, tokens, grad_middle, down, act, middle):
    chips, _, shard, hidden = grad_up.shape
    rows, triple = back.shape
    own_rows, features = tokens.shape
    extra = bias_rows.shape[2]
    kinds = (chips, 3, 1, "sum")
    shapes = [
        grad_up.shape, (chips, 2, shard, triple), grad_proj.shape, (chips, 2, shard + extra, PARAM_COLS),
    ]
    vmem = pl.BlockSpec(memory_space=pltpu.VMEM)
    return pl.pallas_call(
        functools.partial(tail_kernel, kinds),
        out_shape=scatter_shapes(shapes, kinds)
        + [jax.ShapeDtypeStruct((own_rows, features), F32), jax.ShapeDtypeStruct((own_rows, features), BF)],
        in_specs=[vmem] * 4 + [pl.BlockSpec(memory_space=pl.ANY)] * 10,
        out_specs=[vmem] * 6,
        scratch_shapes=[
            pltpu.VMEM(back.shape, BF), pltpu.VMEM(weight.shape, BF), pltpu.VMEM(norm.shape, BF),
            pltpu.VMEM(tokens.shape, BF), pltpu.VMEM(middle.shape, F32), pltpu.VMEM(down.shape, BF),
            pltpu.VMEM(shapes[1], BF), pltpu.VMEM(shapes[3], BF), pltpu.VMEM((PARAM_COLS, features), F32),
            pltpu.VMEM((own_rows, features), BF), pltpu.VMEM((own_rows, features), BF),
            pltpu.SemaphoreType.DMA((8,)), pltpu.SemaphoreType.DMA((4,)),
            pltpu.VMEM((256, act.shape[1]), BF), pltpu.VMEM((256, features), F32),
            pltpu.VMEM((own_rows, features), BF), pltpu.VMEM((own_rows, features), BF), pltpu.SemaphoreType.DMA((2,)),
            pltpu.VMEM(grad_up.shape, BF), pltpu.VMEM(grad_proj.shape, BF),
        ]
        + scatter_scratch(shapes, 2),
        compiler_params=pltpu.CompilerParams(collective_id=1, has_side_effects=True, vmem_limit_bytes=62 << 20),
        name="tail",
    )(sums, bias_rows, gain, shift, grad_up, grad_proj, back, weight, norm, tokens, grad_middle, down, act, middle)


def pack_kernel(up_ref, down_ref, out_ref):
    shard, columns = up_ref.shape
    features = down_ref.shape[1]
    out_ref[:, :columns] = up_ref[...]
    for i in range(down_ref.shape[0] // shard):
        out_ref[:, columns + i * features : columns + (i + 1) * features] = down_ref[i * shard : (i + 1) * shard]


def pack(up, down):
    shard, columns = up.shape
    fold = down.shape[0] // shard
    if shard % 16 != 0:
        return jnp.concatenate([up] + [down[shard * i : shard * (i + 1)] for i in range(fold)], 1)
    return pl.pallas_call(
        pack_kernel,
        out_shape=jax.ShapeDtypeStruct((shard, columns + fold * down.shape[1]), BF),
        in_specs=[pl.BlockSpec(memory_space=pltpu.VMEM)] * 2,
        out_specs=pl.BlockSpec(memory_space=pltpu.VMEM),
        name="pack",
    )(up, down)


def finish_kernel(
    up_ref, qkv_ref, proj_ref, down_ref, token_ref, block_ref, packed_ref,
    up_out, qkv_out, proj_out, down_out, token_out, block_out, vec_out, bias_out,
):
    token_out[...] = token_ref[...]
    block_out[...] = block_ref[...]
    up_out[...] = up_ref[...]
    qkv_out[...] = qkv_ref[...]
    proj_out[...] = proj_ref[...]
    down_out[...] = down_ref[...]
    shard = vec_out.shape[1]
    vec_out[...] = packed_ref[:shard].T[:8]
    bias_out[...] = packed_ref[shard : shard + 1]


def finish(up, qkv, proj, down, tokens, block, packed, shard, unit):
    if lax.axis_size(AX) != 32:
        return up, qkv, proj, down, tokens, block, packed[:shard, :8].T, packed[shard : shard + 1, :unit]
    return pl.pallas_call(
        finish_kernel,
        out_shape=[jax.ShapeDtypeStruct(a.shape, a.dtype) for a in (up, qkv, proj, down, tokens, block)]
        + [jax.ShapeDtypeStruct((8, shard), F32), jax.ShapeDtypeStruct((1, unit), F32)],
        in_specs=[pl.BlockSpec(memory_space=pltpu.VMEM)] * 7,
        out_specs=[pl.BlockSpec(memory_space=pltpu.VMEM)] * 8,
        compiler_params=PARAMS,
        name="finish",
    )(up, qkv, proj, down, tokens, block, packed)


def by_core(core, own, other, axis):
    return jnp.where(core == 0, jnp.concatenate([own, other], axis), jnp.concatenate([other, own], axis))


def per_device(
    tokens, valid_slots, cotangent, first_gain, first_shift, qkv_weight, query_bias, value_bias, proj_weight,
    proj_bias, second_gain, second_shift, up_weight, up_bias, down_weight, down_bias,
):
    devices = lax.axis_size(AX)
    chips = devices // 2
    core = lax.axis_index(AX) % 2
    micro, rows, features = tokens.shape
    shard = qkv_weight.shape[0]
    width = features // 2
    hidden = up_weight.shape[1] // 2
    unit = hidden // chips
    own_rows = micro * rows
    every = 2 * own_rows

    fold = unit // shard
    both_weights = lax.all_gather(pack(up_weight, down_weight), AX, axis=0, tiled=True)
    feed_weights = [both_weights]
    if unit % 128 != 0 or shard % 16 != 0:
        half_up = both_weights[:, : 2 * hidden].reshape(features, chips, 2, unit)
        half_up = lax.dynamic_index_in_dim(half_up, core, 2, keepdims=False).reshape(features, hidden)
        half_down = both_weights[:, 2 * hidden :].reshape(chips, 2, shard, fold, features)
        half_down = lax.dynamic_index_in_dim(half_down, core, 1, keepdims=False)
        half_down = half_down.transpose(0, 2, 1, 3).reshape(hidden, features)
        feed_weights = [half_up, half_down]
    vectors = jnp.stack(
        [first_gain, first_shift, query_bias, value_bias, proj_bias, second_gain, second_shift, down_bias], 0
    )
    lanes = max(PARAM_COLS, unit)
    vectors = jnp.pad(vectors.T, ((0, 16), (0, lanes - 8)))
    packed = lax.dynamic_update_slice(vectors, up_bias[None, :], (shard, 0))
    qkv_all, proj_all, packed_all = gather_chips(qkv_weight, proj_weight, packed)
    weight_qkv = qkv_all.reshape(features, 3 * width)
    params = packed_all[:, :, :shard, :8].astype(F32).reshape(features, 8).T
    gain_one, shift_one, bias_query, bias_value, bias_proj, gain_two, shift_two, bias_down = [
        params[i : i + 1] for i in range(8)
    ]
    bias_up = lax.dynamic_index_in_dim(packed_all[:, :, shard, :unit], core, 1, keepdims=False)
    bias_up = bias_up.astype(F32).reshape(1, hidden)
    proj_cols = proj_all.reshape(2, width, width)
    proj_own = lax.dynamic_index_in_dim(proj_cols, core, 0, keepdims=False)
    proj_other = swap(lax.dynamic_index_in_dim(proj_cols, 1 - core, 0, keepdims=False))
    weight_proj = by_core(core, proj_own, proj_other, 1)
    qkv_bias = jnp.concatenate(
        [
            lax.dynamic_slice_in_dim(bias_query, core * width, width, 1),
            jnp.zeros((1, width), F32),
            lax.dynamic_slice_in_dim(bias_value, core * width, width, 1),
        ],
        1,
    )

    own_tokens = tokens.reshape(own_rows, features)
    other_tokens = swap(own_tokens)
    marks = jnp.stack([valid_slots, swap(valid_slots)])
    own_cotangent = cotangent.reshape(own_rows, features)
    penalty = jnp.where(marks > 0, 0.0, -1000000000.0).astype(F32)[..., None]
    norm_one, projected = project(own_tokens, other_tokens, gain_one, shift_one, weight_qkv, qkv_bias)
    projected = projected.reshape(2, micro, rows, 3 * width)
    attended, logs = attend(projected, penalty)
    attended_flat = attended.reshape(every, width)
    mixed = swap(product(attended_flat[own_rows:], weight_proj).astype(BF))
    middle, norm_own = second_norm(
        attended_flat, weight_proj, own_tokens, mixed, bias_proj, gain_two, shift_two
    )
    activation, grad_pre, norm_two, grad_out, passed, passed_other, up_sums, weight_down = feed(
        norm_own, swap(norm_own), own_cotangent, swap(own_cotangent),
        (marks > 0).astype(F32).reshape(every, 1), feed_weights, bias_up, unit,
    )
    grad_bias_up = up_sums[0]
    passed_other = swap(passed_other)

    grad_down = outer(activation, grad_out)
    passed_other, grad_down = lax.optimization_barrier((passed_other, grad_down))
    grad_middle, grad_low, second_sums = second_back(passed, passed_other, middle, grad_out, gain_two)
    grad_low = jnp.concatenate([grad_low, swap(grad_low)], 0)
    grad_attended = product_right_t(grad_low, weight_proj).astype(BF).reshape(2, micro, rows, width)
    grad_proj = product_left_t(attended_flat, grad_low).astype(BF)
    grad_attended, grad_proj = lax.optimization_barrier((grad_attended, grad_proj))
    grad_proj_own = lax.dynamic_slice_in_dim(grad_proj, core * width, width, 1)
    grad_proj_other = swap(lax.dynamic_slice_in_dim(grad_proj, (1 - core) * width, width, 1))
    grad_proj = by_core(core, grad_proj_own, grad_proj_other, 0)
    grad_projected, grad_bias, down_weight_grad, grad_up = attend_back(
        projected, penalty, logs, attended, grad_attended, grad_down.reshape(chips, 2, unit // 2, features),
        norm_two, grad_pre,
    )
    grad_projected = grad_projected.reshape(every, 3 * width)

    grad_bias = jnp.sum(grad_bias, axis=0).transpose(1, 0, 2).reshape(2, width)
    grad_bias = by_core(core, grad_bias, jnp.zeros_like(grad_bias), 1)
    sums = [grad_bias, second_sums[2:3], second_sums[:2], second_sums[3:4]]
    up_units = grad_bias_up.astype(BF).reshape(chips, 1, unit)
    up_units = by_core(core, up_units, jnp.zeros_like(up_units), 1).reshape(chips, 2, 1, unit)
    grad_up = grad_up.reshape(chips, 2, shard, hidden)
    grad_proj = grad_proj.reshape(chips, 2, shard, width)
    if devices == 32:
        bias_rows = jnp.pad(up_units, ((0, 0), (0, 0), (0, 15), (0, 0)))
        sums = jnp.concatenate([jnp.zeros((2, features), F32)] + sums, 0)
        up_weight_grad, qkv_weight_grad, proj_weight_grad, packed_sum, tokens_grad, block_output = tail(
            grad_up, grad_proj, sums, bias_rows, gain_one, bias_down, grad_projected, weight_qkv, norm_one, own_tokens,
            grad_middle, weight_down, activation, middle,
        )
    else:
        lifted = swap(product(activation[own_rows:], weight_down).astype(BF)).astype(F32)
        block_output = (middle + product(activation[:own_rows], weight_down) + lifted + bias_down).astype(BF)
        passed = swap(product_right_t(grad_projected[own_rows:], weight_qkv).astype(BF))
        grad_qkv = outer(norm_one, grad_projected)
        tokens_grad, first_sums = first_back(
            grad_projected, weight_qkv, passed, own_tokens, grad_middle, gain_one
        )
        sums = jnp.concatenate([first_sums[:2]] + sums, 0)
        sums = sums.astype(BF).T.reshape(chips, 2, shard, 8)
        sums = jnp.pad(sums, ((0, 0), (0, 0), (0, 16), (0, lanes - 8)))
        sums = lax.dynamic_update_slice(sums, up_units, (0, 0, shard, 0))
        up_weight_grad, qkv_weight_grad, proj_weight_grad, packed_sum = scatter_chips(
            [grad_up, grad_qkv.reshape(chips, 2, shard, 3 * width), grad_proj, sums], (chips, 3, 1, "sum")
        )
    (
        up_weight_grad, qkv_weight_grad, proj_weight_grad, down_weight_grad, tokens_grad, block_output,
        vector_sum, up_bias_grad,
    ) = finish(
        up_weight_grad, qkv_weight_grad, proj_weight_grad, down_weight_grad, tokens_grad, block_output,
        packed_sum, shard, unit,
    )
    tokens_grad = tokens_grad.reshape(micro, rows, features)
    block_output = block_output.reshape(micro, rows, features)
    up_bias_grad = up_bias_grad[0]
    return (
        block_output, tokens_grad, vector_sum[0], vector_sum[1], qkv_weight_grad, vector_sum[2], vector_sum[3],
        proj_weight_grad, vector_sum[4], vector_sum[5], vector_sum[6], up_weight_grad, up_bias_grad,
        down_weight_grad, vector_sum[7],
    )


def solution(mesh):
    row = P(None, AX, None)
    vec = P(AX)
    mat = P(AX, None)
    return jax.shard_map(
        per_device,
        mesh=mesh,
        in_specs=(row, P(None, AX), row, vec, vec, mat, vec, vec, mat, vec, vec, vec, mat, vec, mat, vec),
        out_specs=(row, row, vec, vec, mat, vec, vec, mat, vec, vec, vec, mat, vec, mat, vec),
        check_vma=False,
    )
```
